32 devices in a mesh: dp: 8 (over z, y), tensor: 4 (over x, core).
Axes of the slice: x: 2, y: 2, z: 4, core: 2. Of those that a mesh axis runs over, the one named last changes fastest.
Arguments:
- tokens: bfloat16 [2048, 2048], P('dp'), may hold values from -6 to 6
- qkv_weight: bfloat16 [2048, 3, 2048], P('dp', None, 'tensor'), may hold values from -0.13258252 to 0.13258252
- out_weight: bfloat16 [2048, 2048], P('dp', 'tensor'), may hold values from -0.125 to 0.125
- gu_weight: bfloat16 [2048, 2, 8192], P('dp', None, 'tensor'), may hold values from -0.125 to 0.125
- down_weight: bfloat16 [2048, 8192], P('dp', 'tensor'), may hold values from -0.0625 to 0.0625
- attn_gain: bfloat16 [2048], P('dp'), may hold values from 0.25 to 1.75
- ffn_gain: bfloat16 [2048], P('dp'), may hold values from 0.25 to 1.75
- q_gain: bfloat16 [2048], P(('tensor', 'dp')), may hold values from 0.5 to 5
- k_gain: bfloat16 [2048], P(('tensor', 'dp')), may hold values from 0.5 to 5
- out_grad: float32 [2048, 2048], P('dp'), may hold values from -6 to 6
Outputs:
- block_out: float32 [2048, 2048], P('dp')
- grad_tokens: float32 [2048, 2048], P('dp')
- grad_qkv_weight: float32 [2048, 3, 2048], P('dp', None, 'tensor')
- grad_out_weight: float32 [2048, 2048], P('dp', 'tensor')
- grad_gu_weight: float32 [2048, 2, 8192], P('dp', None, 'tensor')
- grad_down_weight: float32 [2048, 8192], P('dp', 'tensor')
- grad_attn_gain: float32 [2048], P('dp')
- grad_ffn_gain: float32 [2048], P('dp')
- grad_q_gain: float32 [2048], P(('tensor', 'dp'))
- grad_k_gain: float32 [2048], P(('tensor', 'dp'))
The draws below stay inside these ranges and needn't reach their ends.
All inputs are finite; a program needn't handle non-finite values.
Results may differ from the reference program's by a relative error of at most 0.015.
The reference program's roundings to bfloat16 on the way count: a program that leaves them out, or rounds other values in their place, can miss the bound.
Values may be sent and summed in bfloat16 or wider, within the bound.
A program may use at most 256 MiB of HBM per device.

```python
import math
import jax
import jax.numpy as jnp
from jax import lax

D = 2048
HEADS = 16
HD = 128
FF = 8192
SEQ_LEN = 256
HQ = 2048
TOKENS = 2048


def draw_qkv_weight(key, part):
    drawn = jax.random.normal(jax.random.fold_in(key, 11), (D, 3, HQ), jnp.float32)
    drawn = jnp.clip(drawn, -6.0, 6.0) * D ** (-0.5)
    return drawn.astype(jnp.bfloat16)


def gain_law(key, salt):
    position = jnp.arange(HQ).astype(jnp.float32) / HQ
    rough = jax.random.uniform(jax.random.fold_in(key, salt), (HQ,), jnp.float32, 0.8, 1.2)
    spread = 0.7 * jnp.exp(position * jnp.log(5.0)) * rough
    return spread.astype(jnp.bfloat16)


def draw_q_gain(key, part):
    return gain_law(key, 21)


def draw_k_gain(key, part):
    return gain_law(key, 41)


def with_spikes(entries, own_key, source, target, blocks, factor):
    def block_of(dim):
        return (jnp.arange(entries.shape[dim]) // (entries.shape[dim] // blocks)).reshape((-1,) + (1,) * (entries.ndim - 1 - dim))

    near = jax.random.permutation(own_key, blocks)[block_of(target)]
    far = (block_of(target) + blocks // 2) % blocks
    return jnp.where((block_of(source) == near) | (block_of(source) == far), factor * entries, entries)


def level_of(key, extent, cuts, low, largest):
    def one(dim, shards_of):
        steps = jax.random.uniform(jax.random.fold_in(jax.random.fold_in(key, 6), dim), (shards_of,), jnp.float32, low / len(cuts), largest / len(cuts))
        return jnp.repeat(jnp.exp(steps), extent[dim] // shards_of).reshape((-1,) + (1,) * (len(extent) - dim - 1))

    level = one(*cuts[0])
    for cut in cuts[1:]:
        level = level * one(*cut)
    return level


def bell_draw(rng, dims, scale, most, split=(), held_as=jnp.bfloat16):
    values = scale * jax.random.normal(rng, dims, jnp.float32)
    if split:
        values = values * level_of(rng, dims, split, -0.22, 0.18)
    return jnp.clip(values, -most, most).astype(held_as)


def noise_with(own_key, dims, deviation, limit, shards, heavy, kind=jnp.bfloat16):
    entries = deviation * jax.random.normal(own_key, dims, jnp.float32)
    if shards:
        entries = entries * level_of(own_key, dims, shards, -0.22, 0.18)
    return jnp.clip(with_spikes(entries, jax.random.fold_in(own_key, 3), *heavy), -limit, limit).astype(kind)


def setup_inputs(seed: int = 0) -> dict:
    arg_keys = jax.random.split(jax.random.key(seed), 11)
    return {
        "tokens": bell_draw(arg_keys[0], (TOKENS, D), 1.0, 6.0, ((0, 8),)),
        "qkv_weight": draw_qkv_weight(jax.random.fold_in(arg_keys[10], 71), 0),
        "out_weight": bell_draw(arg_keys[2], (D, HQ), HQ ** -0.5, 0.125, ((0, 8), (1, 4))),
        "gu_weight": bell_draw(arg_keys[3], (D, 2, FF), D ** -0.5, 0.125, ((0, 8), (2, 4))),
        "down_weight": bell_draw(arg_keys[4], (D, FF), FF ** -0.5, 0.0625, ((0, 8), (1, 4))),
        "attn_gain": jnp.clip(1.0 + 0.15 * jax.random.normal(arg_keys[5], (D,), jnp.float32), 0.25, 1.75).astype(jnp.bfloat16),
        "ffn_gain": jnp.clip(1.0 + 0.15 * jax.random.normal(arg_keys[6], (D,), jnp.float32), 0.25, 1.75).astype(jnp.bfloat16),
        "q_gain": draw_q_gain(jax.random.fold_in(arg_keys[10], 71), 0),
        "k_gain": draw_k_gain(jax.random.fold_in(arg_keys[10], 71), 0),
        "out_grad": noise_with(arg_keys[9], (TOKENS, D), 1.0, 6.0, ((0, 8),), (0, 1, 8, 2.0), jnp.float32),
    }


epsilon = 1e-06
rope_base = 500000.0

def rope_tables(length, width):
    half_width = width // 2
    inv_freq = rope_base ** (-(jnp.arange(half_width, dtype=jnp.float32) * 2.0) / width)
    angles = jnp.arange(length, dtype=jnp.float32)[:, None] * inv_freq[None, :]
    cos_table = jnp.concatenate([jnp.cos(angles), jnp.cos(angles)], axis=1)
    sine_table = jnp.concatenate([jnp.sin(angles), jnp.sin(angles)], axis=1)
    return (cos_table[None, :, None, :], sine_table[None, :, None, :])

def rotate(operand):
    half_width = operand.shape[-1] // 2
    return jnp.concatenate([-operand[..., half_width:], operand[..., :half_width]], axis=-1)

def rotate_back(operand):
    half_width = operand.shape[-1] // 2
    return jnp.concatenate([operand[..., half_width:], -operand[..., :half_width]], axis=-1)

def norm_back(upstream, source, inverse, gain):
    scaled = upstream * gain
    return inverse * scaled - source * inverse ** 3 * lax.optimization_barrier(jnp.mean(scaled * source, axis=1, keepdims=True))

def block_pass(params, tok_block, grad_block):
    w_qkv, w_out, w_gu, w_down, g_attn, g_ffn, g_query, g_key = params
    tok_rows = tok_block.shape[0]
    local_seqs = tok_rows // SEQ_LEN
    head_shape = (local_seqs, SEQ_LEN, HEADS, HD)
    score_scale = HD ** (-0.5)
    f32 = jnp.float32
    bf16 = jnp.bfloat16
    qkv_proj = jnp.dot(tok_block, w_qkv.reshape(D, 3 * HQ), preferred_element_type=f32)
    queries = qkv_proj[:, :HQ]
    key_rows = qkv_proj[:, HQ:2 * HQ]
    value_rows = qkv_proj[:, 2 * HQ:].astype(bf16)
    q_inv = lax.rsqrt(lax.optimization_barrier(jnp.mean(queries * queries, axis=1, keepdims=True)) + epsilon)
    k_inv = lax.rsqrt(lax.optimization_barrier(jnp.mean(key_rows * key_rows, axis=1, keepdims=True)) + epsilon)
    q_normed = queries * q_inv * g_query
    k_normed = key_rows * k_inv * g_key
    cos_table, sine_table = rope_tables(SEQ_LEN, HD)
    q_heads = q_normed.reshape(head_shape)
    k_heads = k_normed.reshape(head_shape)
    q_rot = (q_heads * cos_table + rotate(q_heads) * sine_table).astype(bf16)
    k_rot = (k_heads * cos_table + rotate(k_heads) * sine_table).astype(bf16)
    v_heads = value_rows.reshape(head_shape)
    causal = (jnp.arange(SEQ_LEN)[:, None] >= jnp.arange(SEQ_LEN)[None, :])[None, None]

    def score_of(q_side, k_side):
        raw = jnp.einsum('sqhd,skhd->shqk', q_side.astype(f32), k_side.astype(f32)) * score_scale
        return jnp.where(causal, raw, -1e+30)
    scores = score_of(q_rot, k_rot)
    row_max = lax.optimization_barrier(jnp.max(scores, axis=-1, keepdims=True))
    shifted = jnp.exp(scores - row_max)
    row_total = lax.optimization_barrier(jnp.sum(shifted, axis=-1, keepdims=True))
    log_total = row_max + jnp.log(row_total)
    prob_rows = (shifted / row_total).astype(bf16)
    attended = jnp.einsum('shqk,skhd->sqhd', prob_rows.astype(f32), v_heads.astype(f32)).astype(bf16).reshape(tok_rows, HQ)
    attn_proj = jnp.dot(attended, w_out.T, preferred_element_type=f32)
    attn_inv = lax.rsqrt(lax.optimization_barrier(jnp.mean(attn_proj * attn_proj, axis=1, keepdims=True)) + epsilon)
    residual = tok_block.astype(f32) + attn_proj * attn_inv * g_attn
    residual_b = residual.astype(bf16)
    gate_up = jnp.dot(residual_b, w_gu.reshape(D, 2 * FF), preferred_element_type=f32)
    gate_proj = gate_up[:, :FF]
    up_proj = gate_up[:, FF:]
    gate_sigmoid = jax.nn.sigmoid(gate_proj)
    active = gate_proj * gate_sigmoid
    hidden = (active * up_proj).astype(bf16)
    mlp_proj = jnp.dot(hidden, w_down.T, preferred_element_type=f32)
    mlp_inv = lax.rsqrt(lax.optimization_barrier(jnp.mean(mlp_proj * mlp_proj, axis=1, keepdims=True)) + epsilon)
    block_out = residual + mlp_proj * mlp_inv * g_ffn
    grad_ffn_gain = lax.optimization_barrier(jnp.sum(grad_block * mlp_proj * mlp_inv, axis=0))
    grad_mlp = norm_back(grad_block, mlp_proj, mlp_inv, g_ffn).astype(bf16)
    grad_hidden = jnp.dot(grad_mlp, w_down, preferred_element_type=f32)
    grad_down = jnp.dot(grad_mlp.T, hidden, preferred_element_type=f32)
    grad_gate = grad_hidden * up_proj * (gate_sigmoid * (1.0 + gate_proj * (1.0 - gate_sigmoid)))
    grad_up = grad_hidden * active
    grad_gu = jnp.concatenate([grad_gate, grad_up], axis=1).astype(bf16)
    grad_gu_w = jnp.dot(residual_b.T, grad_gu, preferred_element_type=f32).reshape(D, 2, FF)
    grad_residual = grad_block + jnp.dot(grad_gu, w_gu.reshape(D, 2 * FF).T, preferred_element_type=f32)
    grad_attn_gain = lax.optimization_barrier(jnp.sum(grad_residual * attn_proj * attn_inv, axis=0))
    grad_proj = norm_back(grad_residual, attn_proj, attn_inv, g_attn).astype(bf16)
    grad_attended = jnp.dot(grad_proj, w_out, preferred_element_type=f32).astype(bf16)
    grad_out_w = jnp.dot(grad_proj.T, attended, preferred_element_type=f32)
    grad_heads = grad_attended.reshape(head_shape)
    prob_again = jnp.exp(score_of(q_rot, k_rot) - log_total)
    prob_again_b = prob_again.astype(bf16)
    grad_v = jnp.einsum('shqk,sqhd->skhd', prob_again_b.astype(f32), grad_heads.astype(f32))
    grad_p = jnp.einsum('sqhd,skhd->shqk', grad_heads.astype(f32), v_heads.astype(f32))
    delta = lax.optimization_barrier(jnp.sum(prob_again * grad_p, axis=-1, keepdims=True))
    grad_scores = (prob_again * (grad_p - delta) * score_scale).astype(bf16)
    grad_q_rot = jnp.einsum('shqk,skhd->sqhd', grad_scores.astype(f32), k_rot.astype(f32))
    grad_k_rot = jnp.einsum('shqk,sqhd->skhd', grad_scores.astype(f32), q_rot.astype(f32))
    grad_q_normed = (grad_q_rot * cos_table + rotate_back(grad_q_rot * sine_table)).reshape(tok_rows, HQ)
    grad_k_normed = (grad_k_rot * cos_table + rotate_back(grad_k_rot * sine_table)).reshape(tok_rows, HQ)
    grad_q_gain = lax.optimization_barrier(jnp.sum(grad_q_normed * queries * q_inv, axis=0))
    grad_k_gain = lax.optimization_barrier(jnp.sum(grad_k_normed * key_rows * k_inv, axis=0))
    grad_q = norm_back(grad_q_normed, queries, q_inv, g_query)
    grad_k = norm_back(grad_k_normed, key_rows, k_inv, g_key)
    grad_qkv = jnp.concatenate([grad_q, grad_k, grad_v.reshape(tok_rows, HQ)], axis=1).astype(bf16)
    grad_qkv_w = jnp.dot(tok_block.T, grad_qkv, preferred_element_type=f32).reshape(D, 3, HQ)
    grad_tok = grad_residual + jnp.dot(grad_qkv, w_qkv.reshape(D, 3 * HQ).T, preferred_element_type=f32)
    return (block_out, grad_tok, grad_qkv_w, grad_out_w, grad_gu_w, grad_down, grad_attn_gain, grad_ffn_gain, grad_q_gain, grad_k_gain)

def reference(tokens, qkv_weight, out_weight, gu_weight, down_weight, attn_gain, ffn_gain, q_gain, k_gain, out_grad):
    f32 = jnp.float32
    block_rows = math.gcd(TOKENS, 4096)
    block_count = TOKENS // block_rows
    params = (qkv_weight, out_weight, gu_weight, down_weight, attn_gain.astype(f32), ffn_gain.astype(f32), q_gain.astype(f32), k_gain.astype(f32))
    starting = (jnp.zeros((D, 3, HQ), f32), jnp.zeros((D, HQ), f32), jnp.zeros((D, 2, FF), f32), jnp.zeros((D, FF), f32), jnp.zeros((D,), f32), jnp.zeros((D,), f32), jnp.zeros((HQ,), f32), jnp.zeros((HQ,), f32))

    def one_block(carry, inputs):
        results = block_pass(params, inputs[0], inputs[1])
        summed = tuple((acc + new_term for acc, new_term in zip(carry, results[2:])))
        return (summed, (results[0], results[1]))
    sums, (outputs, grads) = lax.scan(one_block, starting, (tokens.reshape(block_count, block_rows, D), out_grad.reshape(block_count, block_rows, D)))
    return (outputs.reshape(TOKENS, D), grads.reshape(TOKENS, D), sums[0], sums[1], sums[2], sums[3], sums[4], sums[5], sums[6], sums[7])
```

```python
import functools

import jax
import jax.numpy as jnp
from jax import lax
from jax.experimental import pallas as pl
from jax.experimental.pallas import tpu as pltpu
from jax.sharding import Mesh, PartitionSpec as P

HEADS = 16
HD = 128
SEQ_LEN = 256
HQ = 2048

epsilon = 1e-06
rope_base = 500000.0

f32 = jnp.float32
bf16 = jnp.bfloat16
MESH = pl.DeviceIdType.MESH
EXACT = lax.Precision.HIGHEST
VMEM_LIMIT = 60 * 1024 * 1024
TILE = 64


def flip(index, bit):
    return index + bit - 2 * bit * ((index // bit) % 2)


def across(index, k):
    bit = 1
    while bit <= k:
        if k & bit:
            index = flip(index, bit)
        bit *= 2
    return index


def swap(operand, axis, k=1):
    n = lax.axis_size(axis)
    return lax.ppermute(operand, axis, [(i, i ^ k) for i in range(n)])


def pick(operand, index, axis):
    return lax.dynamic_index_in_dim(operand, index, axis, keepdims=False)


def span(index, size):
    return pl.ds(pl.multiple_of(index * size, size), size)


def lead(na):
    return list(range(1, na)) + [0]


class Links:
    def __init__(self, send_sem, recv_sem):
        self.send_sem, self.recv_sem, self.count, self.copies = send_sem, recv_sem, 0, []

    def send(self, source, target, device):
        copy = pltpu.make_async_remote_copy(
            src_ref=source,
            dst_ref=target,
            send_sem=self.send_sem.at[self.count],
            recv_sem=self.recv_sem.at[self.count],
            device_id=device,
            device_id_type=MESH,
        )
        copy.start()
        self.count += 1
        self.copies.append(copy)
        return copy

    def finish(self):
        for copy in self.copies:
            copy.wait_send()


def greet(peers):
    barrier = pltpu.get_barrier_semaphore()
    for peer in peers:
        pl.semaphore_signal(barrier, inc=1, device_id=peer, device_id_type=MESH)
    pl.semaphore_wait(barrier, len(peers))


def tiles(rows, body):
    def step(i, carry):
        body(pl.ds(pl.multiple_of(i * TILE, TILE), TILE))
        return carry

    lax.fori_loop(0, rows // TILE, step, 0)


def fold(block):
    total = block[:, :128]
    for i in range(1, block.shape[1] // 128):
        total = total + block[:, i * 128 : (i + 1) * 128]
    return total


def wide(column, width):
    return jnp.concatenate([column] * (width // 128), axis=1)


def row_mask(row):
    return (lax.broadcasted_iota(jnp.int32, (8, 128), 0) == row).astype(f32)


def to_row(block, row):
    return lax.dot_general(
        row_mask(row), block, (((1,), (1,)), ((), ())), precision=EXACT, preferred_element_type=f32
    )


def to_column(stats, row):
    return lax.dot_general(
        stats, row_mask(row), (((0,), (0,)), ((), ())), precision=EXACT, preferred_element_type=f32
    )


def spread_copies(links, out, na, a, p, q, forward):
    quarter = out.shape[-1] // 4
    half = 2 * quarter
    mine = span(2 * q + p, quarter)
    pair = span(q, half)
    blocks = range(na) if forward else range(1)
    first = {
        k: links.send(out.at[0, :, mine], out.at[k, :, mine], {"a": across(a, k)}) for k in blocks if k
    }
    second, third = {}, {}
    for k in blocks:
        if k:
            first[k].wait_recv()
        second[k] = links.send(out.at[k, :, mine], out.at[k, :, mine], {"p": 1 - p})
    for k in blocks:
        second[k].wait_recv()
        third[k] = links.send(out.at[k, :, pair], out.at[k, :, pair], {"q": 1 - q})
    for k in blocks:
        third[k].wait_recv()


def reduce_kernel(na, mode, *refs):
    n_in = {"attn": 3, "mlp": 4, "back": 5, "tok": 2}[mode]
    n_out = {"attn": 4, "mlp": 3, "back": 3, "tok": 1}[mode]
    ins, outs, scratch = refs[:n_in], refs[n_in : n_in + n_out], refs[n_in + n_out :]
    from_q, half_sum, from_p, to_a, from_a, total, parts, cols, stat, send_sem, recv_sem = scratch
    part_ref, out = ins[0], outs[0]
    a, p, q = lax.axis_index("a"), lax.axis_index("p"), lax.axis_index("q")
    rows, width = part_ref.shape[1], part_ref.shape[2]
    quarter, half = width // 4, width // 2
    greet([{"q": 1 - q}, {"p": 1 - p}] + [{"a": across(a, k)} for k in range(1, na)])
    links = Links(send_sem, recv_sem)

    give, keep = span(1 - q, half), span(q, half)
    step_q = {
        k: links.send(part_ref.at[k, :, give], from_q.at[k], {"q": 1 - q}) for k in lead(na)
    }
    step_p, step_a = {}, {}
    for k in lead(na):
        step_q[k].wait_recv()

        def add_half(at, k=k):
            own = part_ref[k, at, keep].astype(f32)
            half_sum[k, at] = (own + from_q[k, at].astype(f32)).astype(bf16)

        tiles(rows, add_half)
        step_p[k] = links.send(half_sum.at[k, :, span(1 - p, quarter)], from_p.at[k], {"p": 1 - p})
    for k in lead(na):
        step_p[k].wait_recv()
        if k:

            def add_quarter(at, k=k):
                own = half_sum[k, at, span(p, quarter)].astype(f32)
                to_a[k - 1, at] = (own + from_p[k, at].astype(f32)).astype(bf16)

            tiles(rows, add_quarter)
            step_a[k] = links.send(to_a.at[k - 1], from_a.at[k - 1], {"a": across(a, k)})
    for k in range(1, na):
        step_a[k].wait_recv()

    def add_all(at):
        own = half_sum[0, at, span(p, quarter)].astype(f32) + from_p[0, at].astype(f32)
        for k in range(1, na):
            own = own + from_a[k - 1, at].astype(f32)
        return own

    mine = span(2 * q + p, quarter)

    def exchange(count):
        stats = to_row(parts[0], 0)
        if count == 2:
            stats = stats + to_row(parts[1], 1)
        stat[0] = stats
        links.send(stat.at[0], stat.at[1], {"p": 1 - p}).wait_recv()
        stat[2] = stat[0] + stat[1]
        links.send(stat.at[2], stat.at[3], {"q": 1 - q}).wait_recv()
        stats = (stat[2] + stat[3]) / width
        for i in range(count):
            cols[i] = to_column(stats, i)

    if mode == "attn":
        _, tok_ref, gain_ref = ins
        _, proj_ref, inv_ref, res_ref = outs

        def first(at):
            own = add_all(at)
            proj_ref[at] = own
            parts[0, at] = fold(own * own)

        tiles(rows, first)
        exchange(1)

        def second(at):
            own = proj_ref[at]
            inv = lax.rsqrt(cols[0, at] + epsilon)
            inv_ref[at] = inv
            residual = tok_ref[at].astype(f32) + own * wide(inv, quarter) * gain_ref[0:1]
            res_ref[at] = residual
            out[0, at, mine] = residual.astype(bf16)

        tiles(rows, second)
    elif mode == "mlp":
        _, res_ref, grad_ref, gain_ref = ins
        _, block_ref, sum_ref = outs

        def first(at):
            own = add_all(at)
            total[at] = own
            parts[0, at] = fold(own * own)
            parts[1, at] = fold(grad_ref[at] * gain_ref[0:1] * own)

        tiles(rows, first)
        exchange(2)
        sum_ref[...] = jnp.zeros_like(sum_ref)

        def second(at):
            own = total[at]
            inv = wide(lax.rsqrt(cols[0, at] + epsilon), quarter)
            upstream = grad_ref[at]
            scaled = upstream * gain_ref[0:1]
            normed = own * inv
            block_ref[0, at, mine] = (res_ref[at] + normed * gain_ref[0:1]).astype(bf16)
            gains = upstream * normed
            sum_ref[...] += jnp.sum(gains.reshape(TILE // 8, 8, quarter), axis=0)
            grad = inv * scaled - own * inv * inv * inv * wide(cols[1, at], quarter)
            out[0, at, mine] = grad.astype(bf16)

        tiles(rows, second)
    elif mode == "back":
        _, grad_ref, proj_ref, inv_ref, gain_ref = ins
        _, res_ref, sum_ref = outs

        def first(at):
            grad = grad_ref[at] + add_all(at)
            res_ref[at] = grad
            parts[0, at] = fold(grad * gain_ref[0:1] * proj_ref[at])

        tiles(rows, first)
        exchange(1)
        sum_ref[...] = jnp.zeros_like(sum_ref)

        def second(at):
            own = proj_ref[at]
            inv = wide(inv_ref[at], quarter)
            upstream = res_ref[at]
            gains = upstream * own * inv
            sum_ref[...] += jnp.sum(gains.reshape(TILE // 8, 8, quarter), axis=0)
            grad = inv * (upstream * gain_ref[0:1])
            grad = grad - own * inv * inv * inv * wide(cols[0, at], quarter)
            out[0, at, mine] = grad.astype(bf16)

        tiles(rows, second)
    else:
        _, grad_ref = ins

        def first(at):
            out[0, at, mine] = (grad_ref[at] + add_all(at)).astype(bf16)

        tiles(rows, first)

    if mode == "mlp":
        spread_copies(links, out, na, a, p, q, True)
        spread_copies(links, block_ref, na, a, p, q, False)
    else:
        spread_copies(links, out, na, a, p, q, mode != "tok")
    links.finish()


def reduce_call(mode, part, *operands):
    na, rows, width = part.shape
    quarter = width // 4
    shape = jax.ShapeDtypeStruct
    full = shape((na, rows, width), bf16)
    one = shape((1, rows, width), bf16)
    share = shape((rows, quarter), f32)
    sums = shape((8, quarter), f32)
    outs = {
        "attn": (full, share, shape((rows, 128), f32), share),
        "mlp": (full, one, sums),
        "back": (full, share, sums),
        "tok": (one,),
    }[mode]
    copies = 3 * na + 1 + {"attn": 3 * na + 1, "mlp": 3 * na + 3, "back": 3 * na + 1, "tok": 2}[mode]
    return pl.pallas_call(
        functools.partial(reduce_kernel, na, mode),
        out_shape=outs,
        in_specs=[pl.BlockSpec(memory_space=pltpu.VMEM)] * (1 + len(operands)),
        out_specs=tuple([pl.BlockSpec(memory_space=pltpu.VMEM)] * len(outs)),
        scratch_shapes=[
            pltpu.VMEM((na, rows, width // 2), bf16),
            pltpu.VMEM((na, rows, width // 2), bf16),
            pltpu.VMEM((na, rows, quarter), bf16),
            pltpu.VMEM((na - 1, rows, quarter), bf16),
            pltpu.VMEM((na - 1, rows, quarter), bf16),
            pltpu.VMEM((rows, quarter), f32),
            pltpu.VMEM((2, rows, 128), f32),
            pltpu.VMEM((2, rows, 128), f32),
            pltpu.VMEM((4, 8, rows), f32),
            pltpu.SemaphoreType.DMA((copies,)),
            pltpu.SemaphoreType.DMA((copies,)),
        ],
        compiler_params=pltpu.CompilerParams(
            collective_id={"attn": 1, "mlp": 2, "back": 3, "tok": 4}[mode],
            has_side_effects=True,
            vmem_limit_bytes=VMEM_LIMIT,
        ),
        cost_estimate=pl.CostEstimate(flops=10**8, bytes_accessed=10**8, transcendentals=0),
        name="reduce_" + mode,
    )(part, *operands)


def start_kernel(na, nb, tok_ref, qkv_ref, wout_ref, x_ref, w_ref, local_sem, send_sem, recv_sem):
    a, b, p, q = (lax.axis_index(axis) for axis in ("a", "b", "p", "q"))
    rows = wout_ref.shape[0]
    quarter = tok_ref.shape[1]
    greet(
        [{"q": 1 - q}, {"p": 1 - p}]
        + [{"a": across(a, k)} for k in range(1, na)]
        + [{"b": across(b, j)} for j in range(1, nb)]
    )
    links = Links(send_sem, recv_sem)
    mine = span(2 * q + p, quarter)
    pair = span(q, 2 * quarter)
    place = span(a * nb + b, rows)
    locals_ = [pltpu.make_async_copy(tok_ref, x_ref.at[0, :, mine], local_sem.at[0])]
    arrive = {}
    for k in range(na):
        block = span(across(a, k), HD)
        sources = [qkv_ref.at[c, :, block] for c in range(3)] + [wout_ref.at[:, block]]
        for c, source in enumerate(sources):
            target = w_ref.at[place, c * HD : (c + 1) * HD]
            if k:
                arrive[k, c] = links.send(source, target, {"a": across(a, k)})
            else:
                locals_.append(pltpu.make_async_copy(source, target, local_sem.at[1 + c]))
    first = {
        k: links.send(tok_ref, x_ref.at[k, :, mine], {"a": across(a, k)}) for k in range(1, na)
    }
    for copy in locals_:
        copy.start()
    for copy in locals_:
        copy.wait()
    ends, second, third = [], {}, {}
    for k in range(na):
        if k:
            for c in range(4):
                arrive[k, c].wait_recv()
        at = w_ref.at[span(across(a, k) * nb + b, rows), :]
        for j in range(1, nb):
            ends.append(links.send(at, at, {"b": across(b, j)}))
        if k:
            first[k].wait_recv()
        second[k] = links.send(x_ref.at[k, :, mine], x_ref.at[k, :, mine], {"p": 1 - p})
    for k in range(na):
        second[k].wait_recv()
        third[k] = links.send(x_ref.at[k, :, pair], x_ref.at[k, :, pair], {"q": 1 - q})
    for copy in list(third.values()) + ends:
        copy.wait_recv()
    links.finish()


def start_call(na, nb, tok_mine, qkv, w_out):
    rows, quarter = tok_mine.shape
    width = 4 * quarter
    copies = (na - 1) * 5 + na * (nb - 1) + 2 * na
    return pl.pallas_call(
        functools.partial(start_kernel, na, nb),
        out_shape=(
            jax.ShapeDtypeStruct((na, rows, width), bf16),
            jax.ShapeDtypeStruct((width, 4 * HD), bf16),
        ),
        in_specs=[pl.BlockSpec(memory_space=pltpu.VMEM)] * 3,
        out_specs=(pl.BlockSpec(memory_space=pltpu.VMEM), pl.BlockSpec(memory_space=pltpu.VMEM)),
        scratch_shapes=[
            pltpu.SemaphoreType.DMA((5,)),
            pltpu.SemaphoreType.DMA((copies,)),
            pltpu.SemaphoreType.DMA((copies,)),
        ],
        compiler_params=pltpu.CompilerParams(
            collective_id=5, has_side_effects=True, vmem_limit_bytes=VMEM_LIMIT
        ),
        name="start",
    )(tok_mine, qkv, w_out)


def stats_kernel(na, stats_ref, out_ref, held, from_a, send_sem, recv_sem):
    a, p, q = lax.axis_index("a"), lax.axis_index("p"), lax.axis_index("q")
    greet([{"q": 1 - q}, {"p": 1 - p}] + [{"a": across(a, k)} for k in range(1, na)])
    links = Links(send_sem, recv_sem)
    links.send(stats_ref, held.at[0], {"p": 1 - p}).wait_recv()
    held[1] = stats_ref[...] + held[0]
    links.send(held.at[1], held.at[2], {"q": 1 - q}).wait_recv()
    held[3] = held[1] + held[2]
    copies = [links.send(held.at[3], from_a.at[k - 1], {"a": across(a, k)}) for k in range(1, na)]
    for copy in copies:
        copy.wait_recv()
    for k in range(na):
        for i in range(2):
            at = 2 * k + i
            total = held[3, at : at + 1]
            for j in range(1, na):
                other = 2 * (k ^ j) + i
                total = total + from_a[j - 1, other : other + 1]
            out_ref[at : at + 1] = total
    links.finish()


def stats_call(na, stats, ident):
    return pl.pallas_call(
        functools.partial(stats_kernel, na),
        out_shape=jax.ShapeDtypeStruct(stats.shape, f32),
        in_specs=[pl.BlockSpec(memory_space=pltpu.VMEM)],
        out_specs=pl.BlockSpec(memory_space=pltpu.VMEM),
        scratch_shapes=[
            pltpu.VMEM((4,) + stats.shape, f32),
            pltpu.VMEM((na - 1,) + stats.shape, f32),
            pltpu.SemaphoreType.DMA((na + 1,)),
            pltpu.SemaphoreType.DMA((na + 1,)),
        ],
        compiler_params=pltpu.CompilerParams(collective_id=ident, has_side_effects=True),
        name="stats" + str(ident),
    )(stats)


def local_call(kernel, name, na, operands, outs, scratch=(), flops=10**9):
    def spec(shape, kind):
        if kind == "row":
            return pl.BlockSpec((1,) + tuple(shape[1:]), lambda k: (k,) + (0,) * (len(shape) - 1))
        if kind == "all":
            return pl.BlockSpec(tuple(shape), lambda k: (0,) * len(shape))
        return pl.BlockSpec(memory_space=pl.ANY)

    return pl.pallas_call(
        kernel,
        grid=(na,),
        out_shape=tuple(jax.ShapeDtypeStruct(shape, dtype) for shape, dtype, _ in outs),
        in_specs=[spec(array.shape, kind) for array, kind in operands],
        out_specs=tuple(spec(shape, kind) for shape, _, kind in outs),
        scratch_shapes=list(scratch),
        compiler_params=pltpu.CompilerParams(
            dimension_semantics=("arbitrary",), vmem_limit_bytes=VMEM_LIMIT
        ),
        cost_estimate=pl.CostEstimate(flops=flops, bytes_accessed=2 * 10**7, transcendentals=0),
        name=name,
    )(*[array for array, _ in operands])


def dot(left, right):
    return jnp.dot(left, right, preferred_element_type=f32)


def dot_t(left, right):
    return lax.dot_general(left, right, (((1,), (1,)), ((), ())), preferred_element_type=f32)


def t_dot(left, right):
    return lax.dot_general(left, right, (((0,), (0,)), ((), ())), preferred_element_type=f32)


def add_stats(stats_ref, first, second):
    k = pl.program_id(0)

    @pl.when(k == 0)
    def _():
        stats_ref[...] = jnp.zeros_like(stats_ref)

    stats_ref[...] += to_row(first, 2 * k) + to_row(second, 2 * k + 1)


def qkv_kernel(x_ref, w_ref, qkv_ref, stats_ref):
    out = dot(x_ref[0], w_ref[:, : 3 * HD])
    qkv_ref[0] = out
    queries, key_rows = out[:, :HD], out[:, HD : 2 * HD]
    add_stats(stats_ref, queries * queries, key_rows * key_rows)


def rotate(operand):
    half = HD // 2
    return jnp.concatenate([-operand[:, half:], operand[:, :half]], axis=1)


def rotate_back(operand):
    half = HD // 2
    return jnp.concatenate([operand[:, half:], -operand[:, :half]], axis=1)


def attention(qkv_ref, stats_ref, gain_ref, cos_ref, sin_ref):
    k = pl.program_id(0)
    stats = stats_ref[...] / HQ
    q_inv = lax.rsqrt(to_column(stats, 2 * k) + epsilon)
    k_inv = lax.rsqrt(to_column(stats, 2 * k + 1) + epsilon)
    queries, key_rows = qkv_ref[0, :, :HD], qkv_ref[0, :, HD : 2 * HD]
    values = qkv_ref[0, :, 2 * HD :].astype(bf16)
    cos_table, sine_table = cos_ref[...], sin_ref[...]
    q_normed = queries * q_inv * gain_ref[0:1]
    k_normed = key_rows * k_inv * gain_ref[1:2]
    q_rot = (q_normed * cos_table + rotate(q_normed) * sine_table).astype(bf16)
    k_rot = (k_normed * cos_table + rotate(k_normed) * sine_table).astype(bf16)
    scores = dot_t(q_rot, k_rot) * HD ** (-0.5)
    ahead = lax.broadcasted_iota(jnp.int32, scores.shape, 1) > lax.broadcasted_iota(
        jnp.int32, scores.shape, 0
    )
    scores = jnp.where(ahead, -1e30, scores)
    shifted = jnp.exp(scores - jnp.max(scores, axis=1, keepdims=True))
    probs = shifted / jnp.sum(shifted, axis=1, keepdims=True)
    return queries, key_rows, values, q_inv, k_inv, q_rot, k_rot, probs


def attend_kernel(qkv_ref, stats_ref, gain_ref, cos_ref, sin_ref, w_ref, att_ref, part_ref):
    values, probs = (attention(qkv_ref, stats_ref, gain_ref, cos_ref, sin_ref)[i] for i in (2, 7))
    attended = dot(probs.astype(bf16), values).astype(bf16)
    att_ref[0] = attended
    part_ref[0] = dot_t(attended, w_ref[:, 3 * HD :]).astype(bf16)


def attend_back_kernel(
    proj_ref, qkv_ref, stats_ref, gain_ref, cos_ref, sin_ref, w_ref, grad_ref, inner_ref, sums_ref
):
    k = pl.program_id(0)
    queries, key_rows, values, q_inv, k_inv, q_rot, k_rot, probs = attention(
        qkv_ref, stats_ref, gain_ref, cos_ref, sin_ref
    )
    cos_table, sine_table = cos_ref[...], sin_ref[...]
    grad_att = dot(proj_ref[0], w_ref[:, 3 * HD :]).astype(bf16)
    grad_v = t_dot(probs.astype(bf16), grad_att)
    grad_p = dot_t(grad_att, values)
    delta = jnp.sum(probs * grad_p, axis=1, keepdims=True)
    grad_scores = (probs * (grad_p - delta) * HD ** (-0.5)).astype(bf16)
    grad_q = dot(grad_scores, k_rot)
    grad_k = t_dot(grad_scores, q_rot)
    grad_q = grad_q * cos_table + rotate_back(grad_q * sine_table)
    grad_k = grad_k * cos_table + rotate_back(grad_k * sine_table)

    @pl.when(k == 0)
    def _():
        sums_ref[...] = jnp.zeros_like(sums_ref)

    sums_ref[0:1] += jnp.sum(grad_q * queries * q_inv, axis=0, keepdims=True)
    sums_ref[1:2] += jnp.sum(grad_k * key_rows * k_inv, axis=0, keepdims=True)
    scaled_q = grad_q * gain_ref[0:1]
    scaled_k = grad_k * gain_ref[1:2]
    grad_ref[0, :, :HD] = scaled_q
    grad_ref[0, :, HD : 2 * HD] = scaled_k
    grad_ref[0, :, 2 * HD :] = grad_v
    add_stats(inner_ref, scaled_q * queries, scaled_k * key_rows)


def qkv_back_kernel(scaled_ref, qkv_ref, stats_ref, inner_ref, w_ref, grad_ref, part_ref):
    k = pl.program_id(0)
    for i in range(2):
        at = slice(i * HD, (i + 1) * HD)
        inv = lax.rsqrt(to_column(stats_ref[...] / HQ, 2 * k + i) + epsilon)
        mean = to_column(inner_ref[...] / HQ, 2 * k + i)
        grad = inv * scaled_ref[0, :, at] - qkv_ref[0, :, at] * inv * inv * inv * mean
        grad_ref[0, :, at] = grad.astype(bf16)
    grad_ref[0, :, 2 * HD :] = scaled_ref[0, :, 2 * HD :].astype(bf16)
    part_ref[0] = dot_t(grad_ref[0], w_ref[:, : 3 * HD]).astype(bf16)


def load_weights(na, nb, pieces, w_ref, sem):
    a, b = lax.axis_index("a"), lax.axis_index("b")

    @pl.when(pl.program_id(0) == 0)
    def _():
        rows, units = pieces[0].shape[1:]
        copies = []
        for k in range(na):
            for j in range(nb):
                place = span(across(a, k) * nb + across(b, j), rows)
                for c in range(3):
                    copies.append(
                        pltpu.make_async_copy(
                            pieces[k * nb + j].at[c],
                            w_ref.at[place, c * units : (c + 1) * units],
                            sem.at[len(copies)],
                        )
                    )
        for copy in copies:
            copy.start()
        for copy in copies:
            copy.wait()


def mlp_kernel(na, nb, *refs):
    pieces, (x_ref, gu_ref, hidden_ref, part_ref, w_ref, sem) = refs[: na * nb], refs[na * nb :]
    load_weights(na, nb, pieces, w_ref, sem)
    units = hidden_ref.shape[2]
    gate_up = dot(x_ref[0], w_ref[:, : 2 * units])
    gu_ref[0] = gate_up
    gate, up = gate_up[:, :units], gate_up[:, units:]
    hidden = (gate * jax.nn.sigmoid(gate) * up).astype(bf16)
    hidden_ref[0] = hidden
    part_ref[0] = dot_t(hidden, w_ref[:, 2 * units :]).astype(bf16)


def mlp_back_kernel(na, nb, *refs):
    pieces, (grad_ref, gu_ref, out_ref, part_ref, w_ref, sem) = refs[: na * nb], refs[na * nb :]
    load_weights(na, nb, pieces, w_ref, sem)
    units = gu_ref.shape[2] // 2
    grad_hidden = dot(grad_ref[0], w_ref[:, 2 * units :])
    gate, up = gu_ref[0, :, :units], gu_ref[0, :, units:]
    sigmoid = jax.nn.sigmoid(gate)
    active = gate * sigmoid
    out_ref[0, :, :units] = (
        grad_hidden * up * (sigmoid * (1.0 + gate * (1.0 - sigmoid)))
    ).astype(bf16)
    out_ref[0, :, units:] = (grad_hidden * active).astype(bf16)
    part_ref[0] = dot_t(out_ref[0], w_ref[:, : 2 * units]).astype(bf16)


def widen_kernel(na, count, *refs):
    pieces, out = refs[:na], refs[na]
    a = lax.axis_index("a")
    columns = out.shape[2] // na
    for k in range(na):
        for c in range(count):
            out[c, :, span(across(a, k), columns)] = pieces[k][
                :, c * columns : (c + 1) * columns
            ].astype(f32)


def widen(pieces, count, name):
    na = len(pieces)
    rows, width = pieces[0].shape
    return pl.pallas_call(
        functools.partial(widen_kernel, na, count),
        out_shape=jax.ShapeDtypeStruct((count, rows, na * width // count), f32),
        in_specs=[pl.BlockSpec(memory_space=pltpu.VMEM)] * na,
        out_specs=pl.BlockSpec(memory_space=pltpu.VMEM),
        compiler_params=pltpu.CompilerParams(vmem_limit_bytes=VMEM_LIMIT),
        name=name,
    )(*pieces)


def rope_tables(length, width):
    half_width = width // 2
    inv_freq = rope_base ** (-(jnp.arange(half_width, dtype=f32) * 2.0) / width)
    angles = jnp.arange(length, dtype=f32)[:, None] * inv_freq[None, :]
    cos_table = jnp.concatenate([jnp.cos(angles), jnp.cos(angles)], axis=1)
    sine_table = jnp.concatenate([jnp.sin(angles), jnp.sin(angles)], axis=1)
    return cos_table, sine_table


def on_device(
    tokens,
    qkv_weight,
    out_weight,
    gu_weight,
    down_weight,
    attn_gain,
    ffn_gain,
    q_gain,
    k_gain,
    out_grad,
):
    na, nb = lax.axis_size("a"), lax.axis_size("b")
    a, b = lax.axis_index("a"), lax.axis_index("b")
    share = lax.axis_index("q") * 2 + lax.axis_index("p")
    rows, width = tokens.shape
    quarter = width // 4
    w_rows = out_weight.shape[0]
    units = down_weight.shape[1] // na

    def quarter_of(operand):
        return lax.dynamic_slice_in_dim(operand, share * quarter, quarter, 1)

    def whole_gain(gain):
        own = jnp.zeros((HQ,), f32)
        return lax.dynamic_update_slice_in_dim(own, gain.astype(f32), (a * nb + b) * gain.shape[0], 0)

    tok_mine, grad_mine = quarter_of(tokens), quarter_of(out_grad)
    x_all, w_attn = start_call(
        na, nb, tok_mine, qkv_weight.transpose(1, 0, 2), out_weight
    )

    shards = jnp.concatenate([gu_weight.transpose(1, 0, 2), down_weight[None]], axis=0)
    shards = shards.reshape(3, w_rows, na, units)
    pieces = []
    for k in range(na):
        piece = pick(shards, a ^ k, 2)
        if k:
            piece = swap(piece, "a", k)
        pieces += [piece] + [swap(piece, "b", j) for j in range(1, nb)]

    gains = lax.psum(jnp.stack([whole_gain(attn_gain), whole_gain(ffn_gain)]), ("a", "b"))
    gains = lax.dynamic_slice_in_dim(gains, share * quarter, quarter, 1)
    gain_attn = jnp.broadcast_to(gains[0:1], (8, quarter))
    gain_ffn = jnp.broadcast_to(gains[1:2], (8, quarter))
    n_h = q_gain.shape[0]
    head_gain = jnp.zeros((nb, 2, n_h), f32)
    own = jnp.stack([q_gain, k_gain]).astype(f32)
    head_gain = lax.psum(lax.dynamic_update_index_in_dim(head_gain, own, b, 0), "b")
    head_gain = head_gain.transpose(1, 0, 2).reshape(2, HD)
    head_gain = jnp.concatenate([head_gain, jnp.zeros((6, HD), f32)])
    cos_table, sine_table = rope_tables(SEQ_LEN, HD)

    qkv, stats = local_call(
        qkv_kernel,
        "qkv",
        na,
        [(x_all, "row"), (w_attn, "all")],
        [((na, rows, 3 * HD), f32, "row"), ((8, rows), f32, "all")],
    )
    stats = stats_call(na, stats, 6)
    tables = [(stats, "all"), (head_gain, "all"), (cos_table, "all"), (sine_table, "all")]
    full = (na, rows, width)
    attended, part = local_call(
        attend_kernel,
        "attend",
        na,
        [(qkv, "row")] + tables + [(w_attn, "all")],
        [((na, rows, HD), bf16, "row"), (full, bf16, "row")],
    )
    res_all, proj_mine, inv_mine, res_mine = reduce_call("attn", part, tok_mine, gain_attn)

    mlp_scratch = [
        pltpu.VMEM((width, 3 * units), bf16),
        pltpu.SemaphoreType.DMA((3 * na * nb,)),
    ]
    far = [(piece, "far") for piece in pieces]
    gate_up, hidden, part = local_call(
        functools.partial(mlp_kernel, na, nb),
        "mlp",
        na,
        far + [(res_all, "row")],
        [((na, rows, 2 * units), f32, "row"), ((na, rows, units), bf16, "row"), (full, bf16, "row")],
        mlp_scratch,
    )
    grad_mlp, block_rows, ffn_sums = reduce_call("mlp", part, res_mine, grad_mine, gain_ffn)
    grad_gu, part = local_call(
        functools.partial(mlp_back_kernel, na, nb),
        "mlp_back",
        na,
        far + [(grad_mlp, "row"), (gate_up, "row")],
        [((na, rows, 2 * units), bf16, "row"), (full, bf16, "row")],
        mlp_scratch,
    )

    def weight_grad(left, right):
        out = jnp.einsum("krd,kru->du", left, right, preferred_element_type=f32)
        return out.astype(bf16).reshape(na, nb, w_rows, right.shape[2])

    def reduce_b(grad):
        total = pick(grad, b, 1).astype(f32)
        for j in range(1, nb):
            total = total + swap(pick(grad, b ^ j, 1), "b", j).astype(f32)
        return total.astype(bf16)

    def to_owner(grad):
        return [pick(grad, a, 0)] + [swap(pick(grad, a ^ k, 0), "a", k) for k in range(1, na)]

    down_sum = to_owner(reduce_b(weight_grad(grad_mlp, hidden)))
    gu_sum = to_owner(reduce_b(weight_grad(res_all, grad_gu)))
    grad_proj, grad_res, attn_sums = reduce_call(
        "back", part, grad_mine, proj_mine, inv_mine, gain_attn
    )
    scaled, inner, head_sums = local_call(
        attend_back_kernel,
        "attend_back",
        na,
        [(grad_proj, "row"), (qkv, "row")] + tables + [(w_attn, "all")],
        [((na, rows, 3 * HD), f32, "row"), ((8, rows), f32, "all"), ((8, HD), f32, "all")],
    )
    out_sum = to_owner(reduce_b(weight_grad(grad_proj, attended)))
    inner = stats_call(na, inner, 7)
    grad_qkv, part = local_call(
        qkv_back_kernel,
        "qkv_back",
        na,
        [(scaled, "row"), (qkv, "row"), (stats, "all"), (inner, "all"), (w_attn, "all")],
        [((na, rows, 3 * HD), bf16, "row"), (full, bf16, "row")],
    )
    qkv_sum = to_owner(reduce_b(weight_grad(x_all, grad_qkv)))
    (grad_rows,) = reduce_call("tok", part, grad_res)

    sums = jnp.stack([jnp.sum(attn_sums, axis=0), jnp.sum(ffn_sums, axis=0)])
    place = jnp.zeros((2, width), f32)
    width_sums = lax.dynamic_update_slice_in_dim(place, sums, share * quarter, 1)
    width_sums = lax.psum(width_sums, ("a", "b", "p", "q"))
    n_d = attn_gain.shape[0]
    width_sums = lax.dynamic_slice_in_dim(width_sums, (a * nb + b) * n_d, n_d, 1)
    head_sums = lax.psum(head_sums[:2], "b")
    head_sums = lax.dynamic_slice_in_dim(head_sums, b * n_h, n_h, 1)
    return (
        block_rows[0].astype(f32),
        grad_rows[0].astype(f32),
        widen(qkv_sum, 3, "widen_qkv").transpose(1, 0, 2),
        widen(out_sum, 1, "widen_out")[0],
        widen(gu_sum, 2, "widen_gu").transpose(1, 0, 2),
        widen(down_sum, 1, "widen_down")[0],
        width_sums[0],
        width_sums[1],
        head_sums[0],
        head_sums[1],
    )


def solution(mesh):
    dp, tp = mesh.shape["dp"], mesh.shape["tensor"]
    na = HEADS // tp
    fine = Mesh(mesh.devices.reshape(na, dp // na, tp // 2, 2), ("a", "b", "p", "q"))
    dp_axes, tp_axes = ("a", "b"), ("p", "q")
    both = tp_axes + dp_axes
    return jax.shard_map(
        on_device,
        mesh=fine,
        in_specs=(
            P(dp_axes, None),
            P(dp_axes, None, tp_axes),
            P(dp_axes, tp_axes),
            P(dp_axes, None, tp_axes),
            P(dp_axes, tp_axes),
            P(dp_axes),
            P(dp_axes),
            P(both),
            P(both),
            P(dp_axes, None),
        ),
        out_specs=(
            P(dp_axes, None),
            P(dp_axes, None),
            P(dp_axes, None, tp_axes),
            P(dp_axes, tp_axes),
            P(dp_axes, None, tp_axes),
            P(dp_axes, tp_axes),
            P(dp_axes),
            P(dp_axes),
            P(both),
            P(both),
        ),
        check_vma=False,
    )
```

```python
import functools

import jax
import jax.numpy as jnp
from jax import lax
from jax.experimental import pallas as pl
from jax.experimental.pallas import tpu as pltpu
from jax.sharding import Mesh, PartitionSpec as P


HEADS = 16
HD = 128
SEQ_LEN = 256
HQ = 2048

epsilon = 1e-06
rope_base = 500000.0

f32 = jnp.float32
bf16 = jnp.bfloat16
MESH = pl.DeviceIdType.MESH
EXACT = lax.Precision.HIGHEST
VMEM_LIMIT = 60 * 1024 * 1024
TILE = 64
HALVES = 2


def flip(index, bit):
    return index + bit - 2 * bit * ((index // bit) % 2)


def across(index, k):
    bit = 1
    while bit <= k:
        if k & bit:
            index = flip(index, bit)
        bit *= 2
    return index


def swap(operand, axis, k=1):
    n = lax.axis_size(axis)
    return lax.ppermute(operand, axis, [(i, i ^ k) for i in range(n)])


def pick(operand, index, axis):
    return lax.dynamic_index_in_dim(operand, index, axis, keepdims=False)


def span(index, size):
    return pl.ds(pl.multiple_of(index * size, size), size)


class Links:
    def __init__(self, send_sem, recv_sem):
        self.send_sem, self.recv_sem, self.count, self.copies = send_sem, recv_sem, 0, []

    def send(self, source, target, device):
        copy = pltpu.make_async_remote_copy(
            src_ref=source,
            dst_ref=target,
            send_sem=self.send_sem.at[self.count],
            recv_sem=self.recv_sem.at[self.count],
            device_id=device,
            device_id_type=MESH,
        )
        copy.start()
        self.count += 1
        self.copies.append(copy)
        return copy

    def finish(self):
        for copy in self.copies:
            copy.wait_send()


def greet(peers):
    barrier = pltpu.get_barrier_semaphore()
    for peer in peers:
        pl.semaphore_signal(barrier, inc=1, device_id=peer, device_id_type=MESH)
    pl.semaphore_wait(barrier, len(peers))


def fold(block):
    total = block[:, :128]
    for i in range(1, block.shape[1] // 128):
        total = total + block[:, i * 128 : (i + 1) * 128]
    return total


def wide(column, width):
    return jnp.concatenate([column] * (width // 128), axis=1)


def row_mask(row):
    return (lax.broadcasted_iota(jnp.int32, (8, 128), 0) == row).astype(f32)


def to_row(block, row):
    return lax.dot_general(
        row_mask(row), block, (((1,), (1,)), ((), ())), precision=EXACT, preferred_element_type=f32
    )


def to_column(stats, row):
    return lax.dot_general(
        stats, row_mask(row), (((0,), (0,)), ((), ())), precision=EXACT, preferred_element_type=f32
    )


def reduce_kernel(na, nb, mode, *refs):
    n_in = {"attn": 3, "mlp": 4, "back": 5, "tok": 5}[mode]
    n_out = {"attn": 4, "mlp": 3, "back": 3, "tok": 2}[mode]
    ins, outs, scratch = refs[:n_in], refs[n_in : n_in + n_out], refs[n_in + n_out :]
    from_q, half_sum, from_p, to_a, from_a, total, parts, cols, stat, *scratch = scratch
    send_sem, recv_sem = scratch[-2:]
    part_ref, out = ins[0], outs[0]
    a, b = lax.axis_index("a"), lax.axis_index("b")
    p, q = lax.axis_index("p"), lax.axis_index("q")
    rows, width = part_ref.shape[1], part_ref.shape[2]
    quarter, half = width // 4, width // 2
    count = rows // HALVES
    mine, pair = span(2 * q + p, quarter), span(q, half)
    peers = [{"q": 1 - q}, {"p": 1 - p}] + [{"a": across(a, k)} for k in range(1, na)]
    if mode == "tok":
        own_sums, a_sums, b_sums = scratch[:3]
        sums_ref = outs[1]
        own_sums[...] = jnp.zeros_like(own_sums)
        own_sums[0:1, mine] = jnp.sum(ins[2][...], axis=0, keepdims=True)
        own_sums[1:2, mine] = jnp.sum(ins[3][...], axis=0, keepdims=True)
        peers += [{"b": across(b, j)} for j in range(1, nb)]
    greet(peers)
    links = Links(send_sem, recv_sem)
    halves = [slice(h * count, (h + 1) * count) for h in range(HALVES)]
    lead = list(range(2, na)) + [1, 0]
    give, keep = span(1 - q, half), span(q, half)

    def each(h, body):
        def step(i, carry):
            body(pl.ds(pl.multiple_of(h * count + i * TILE, TILE), TILE))
            return carry

        lax.fori_loop(0, count // TILE, step, 0)

    if mode == "tok":
        sums_p = links.send(own_sums.at[:, mine], own_sums.at[:, mine], {"p": 1 - p})

    step_q, step_p, step_a = {}, {}, {}
    for h, at_h in enumerate(halves):
        for k in lead:
            step_q[h, k] = links.send(
                part_ref.at[k, at_h, give], from_q.at[k, at_h], {"q": 1 - q}
            )
    for h, at_h in enumerate(halves):
        for k in lead:
            step_q[h, k].wait_recv()

            def add_half(at, k=k):
                own = part_ref[k, at, keep].astype(f32)
                half_sum[k, at] = (own + from_q[k, at].astype(f32)).astype(bf16)

            each(h, add_half)
            step_p[h, k] = links.send(
                half_sum.at[k, at_h, span(1 - p, quarter)], from_p.at[k, at_h], {"p": 1 - p}
            )
    if mode == "tok":
        sums_p.wait_recv()
        sums_q = links.send(own_sums.at[:, pair], own_sums.at[:, pair], {"q": 1 - q})

    def send_a(h):
        at_h = halves[h]
        for k in lead[:-1]:
            step_p[h, k].wait_recv()

            def add_quarter(at, k=k):
                own = half_sum[k, at, span(p, quarter)].astype(f32)
                to_a[k - 1, at] = (own + from_p[k, at].astype(f32)).astype(bf16)

            each(h, add_quarter)
            step_a[h, k] = links.send(
                to_a.at[k - 1, at_h], from_a.at[k - 1, at_h], {"a": across(a, k)}
            )

    for h in range(HALVES):
        send_a(h)
    if mode == "tok":
        sums_q.wait_recv()
        sums_a = [
            links.send(own_sums.at[:, span(across(a, k), quarter)], a_sums.at[k - 1], {"a": across(a, k)})
            for k in range(1, na)
        ]

    def add_all(at):
        own = half_sum[0, at, span(p, quarter)].astype(f32) + from_p[0, at].astype(f32)
        for k in range(1, na):
            own = own + from_a[k - 1, at].astype(f32)
        return own

    def exchange(h, number):
        at_h = halves[h]
        stats = to_row(parts[0, at_h], 0)
        if number == 2:
            stats = stats + to_row(parts[1, at_h], 1)
        stat[h, 0] = stats
        links.send(stat.at[h, 0], stat.at[h, 1], {"p": 1 - p}).wait_recv()
        stat[h, 2] = stat[h, 0] + stat[h, 1]
        links.send(stat.at[h, 2], stat.at[h, 3], {"q": 1 - q}).wait_recv()
        stats = (stat[h, 2] + stat[h, 3]) / width
        for i in range(number):
            cols[i, at_h] = to_column(stats, i)

    if mode == "attn":
        _, tok_ref, gain_ref = ins
        _, proj_ref, inv_ref, res_ref = outs
        number = 1

        def first(at):
            own = add_all(at)
            proj_ref[at] = own
            parts[0, at] = fold(own * own)

        def second(at):
            own = proj_ref[at]
            inv = lax.rsqrt(cols[0, at] + epsilon)
            inv_ref[at] = inv
            residual = tok_ref[at].astype(f32) + own * wide(inv, quarter) * gain_ref[0:1]
            res_ref[at] = residual
            out[0, at, mine] = residual.astype(bf16)

    elif mode == "mlp":
        _, res_ref, grad_ref, gain_ref = ins
        _, block_ref, sum_ref = outs
        number = 2

        def first(at):
            own = add_all(at)
            total[at] = own
            parts[0, at] = fold(own * own)
            parts[1, at] = fold(grad_ref[at] * gain_ref[1:2] * own)

        sum_ref[...] = jnp.zeros_like(sum_ref)

        def second(at):
            own = total[at]
            inv = wide(lax.rsqrt(cols[0, at] + epsilon), quarter)
            upstream = grad_ref[at]
            scaled = upstream * gain_ref[1:2]
            normed = own * inv
            block_ref[0, at, mine] = (res_ref[at] + normed * gain_ref[1:2]).astype(bf16)
            gains = upstream * normed
            sum_ref[...] += jnp.sum(gains.reshape(TILE // 8, 8, quarter), axis=0)
            grad = inv * scaled - own * inv * inv * inv * wide(cols[1, at], quarter)
            out[0, at, mine] = grad.astype(bf16)

    elif mode == "back":
        _, grad_ref, proj_ref, inv_ref, gain_ref = ins
        _, res_ref, sum_ref = outs
        number = 1

        def first(at):
            grad = grad_ref[at] + add_all(at)
            res_ref[at] = grad
            parts[0, at] = fold(grad * gain_ref[0:1] * proj_ref[at])

        sum_ref[...] = jnp.zeros_like(sum_ref)

        def second(at):
            own = proj_ref[at]
            inv = wide(inv_ref[at], quarter)
            upstream = res_ref[at]
            gains = upstream * own * inv
            sum_ref[...] += jnp.sum(gains.reshape(TILE // 8, 8, quarter), axis=0)
            grad = inv * (upstream * gain_ref[0:1])
            grad = grad - own * inv * inv * inv * wide(cols[0, at], quarter)
            out[0, at, mine] = grad.astype(bf16)

    else:
        grad_ref = ins[1]
        number = 0

        def first(at):
            out[0, at, mine] = (grad_ref[at] + add_all(at)).astype(bf16)

    blocks = range(1) if mode == "tok" else range(na)
    spread_a, spread_p, spread_q = {}, {}, {}
    for h, at_h in enumerate(halves):
        step_p[h, 0].wait_recv()
        for k in range(1, na):
            step_a[h, k].wait_recv()
        each(h, first)
        if number:
            exchange(h, number)
            each(h, second)
        here = out.at[0, at_h, mine]
        for k in blocks:
            if k:
                spread_a[h, k] = links.send(here, out.at[k, at_h, mine], {"a": across(a, k)})
        spread_p[h, 0] = links.send(here, here, {"p": 1 - p})
    if mode == "tok":
        for copy in sums_a:
            copy.wait_recv()
        held = own_sums[:, span(a, quarter)]
        for k in range(1, na):
            held = held + a_sums[k - 1]
        b_sums[0, :, :quarter] = held
        b_sums[0, :, quarter:] = ins[4][...]
        sums_b = [
            links.send(b_sums.at[0], b_sums.at[j], {"b": across(b, j)}) for j in range(1, nb)
        ]
    for h, at_h in enumerate(halves):
        for k in blocks:
            if k:
                spread_a[h, k].wait_recv()
                here = out.at[k, at_h, mine]
                spread_p[h, k] = links.send(here, here, {"p": 1 - p})
    if mode == "mlp":
        here = block_ref.at[0, :, mine]
        block_p = links.send(here, here, {"p": 1 - p})
    for h, at_h in enumerate(halves):
        for k in blocks:
            spread_p[h, k].wait_recv()
            here = out.at[k, at_h, pair]
            spread_q[h, k] = links.send(here, here, {"q": 1 - q})
    if mode == "mlp":
        block_p.wait_recv()
        here = block_ref.at[0, :, pair]
        links.send(here, here, {"q": 1 - q}).wait_recv()
    if mode == "tok":
        for copy in sums_b:
            copy.wait_recv()
        held = b_sums[0]
        for j in range(1, nb):
            held = held + b_sums[j]
        sums_ref[...] = held
    for copy in spread_q.values():
        copy.wait_recv()
    links.finish()


def reduce_call(mode, nb, part, *operands):
    na, rows, width = part.shape
    quarter = width // 4
    shape = jax.ShapeDtypeStruct
    full = shape((na, rows, width), bf16)
    one = shape((1, rows, width), bf16)
    share = shape((rows, quarter), f32)
    sums = shape((8, quarter), f32)
    outs = {
        "attn": (full, share, shape((rows, 128), f32), share),
        "mlp": (full, one, sums),
        "back": (full, share, sums),
        "tok": (one, shape((8, quarter + HD), f32)),
    }[mode]
    copies = HALVES * (3 * na - 1)
    if mode == "tok":
        copies += HALVES * 2 + 1 + na + nb
        extra = [
            pltpu.VMEM((8, width), f32),
            pltpu.VMEM((na - 1, 8, quarter), f32),
            pltpu.VMEM((nb, 8, quarter + HD), f32),
        ]
    else:
        copies += HALVES * (2 + 3 * na - 1) + (2 if mode == "mlp" else 0)
        extra = []
    vmem = pl.BlockSpec(memory_space=pltpu.VMEM)
    return pl.pallas_call(
        functools.partial(reduce_kernel, na, nb, mode),
        out_shape=outs,
        in_specs=[vmem] * (1 + len(operands)),
        out_specs=(vmem,) * len(outs),
        scratch_shapes=[
            pltpu.VMEM((na, rows, width // 2), bf16),
            pltpu.VMEM((na, rows, width // 2), bf16),
            pltpu.VMEM((na, rows, quarter), bf16),
            pltpu.VMEM((na - 1, rows, quarter), bf16),
            pltpu.VMEM((na - 1, rows, quarter), bf16),
            pltpu.VMEM((rows, quarter), f32),
            pltpu.VMEM((2, rows, 128), f32),
            pltpu.VMEM((2, rows, 128), f32),
            pltpu.VMEM((HALVES, 4, 8, rows // HALVES), f32),
        ]
        + extra
        + [pltpu.SemaphoreType.DMA((copies,)), pltpu.SemaphoreType.DMA((copies,))],
        compiler_params=pltpu.CompilerParams(
            collective_id={"attn": 1, "mlp": 2, "back": 3, "tok": 4}[mode],
            has_side_effects=True,
            vmem_limit_bytes=VMEM_LIMIT,
        ),
        cost_estimate=pl.CostEstimate(flops=10**8, bytes_accessed=10**8, transcendentals=0),
    )(part, *operands)


def start_kernel(na, nb, *refs):
    tok_ref, qkv_ref, wout_ref, gu_ref, down_ref = refs[:5]
    gain_refs, (x_ref, w_ref, gains_ref) = refs[5:9], refs[9:12]
    piece_refs, (own_gains, local_sem, send_sem, recv_sem) = refs[12 : 12 + na], refs[12 + na :]
    a, b, p, q = (lax.axis_index(axis) for axis in ("a", "b", "p", "q"))
    rows = wout_ref.shape[0]
    quarter = tok_ref.shape[1]
    own_gains[...] = jnp.zeros_like(own_gains)
    for i, ref in enumerate(gain_refs):
        own_gains[i : i + 1, : ref.shape[1]] = ref[...].astype(f32)
    gains_ref[a, b] = own_gains[...]
    greet(
        [{"q": 1 - q}, {"p": 1 - p}]
        + [{"a": across(a, k)} for k in range(1, na)]
        + [{"b": across(b, j)} for j in range(1, nb)]
    )
    links = Links(send_sem, recv_sem)
    gains_a = [
        links.send(own_gains, gains_ref.at[a, b], {"a": across(a, k)}) for k in range(1, na)
    ]
    mine, pair = span(2 * q + p, quarter), span(q, 2 * quarter)
    place = span(a * nb + b, rows)
    locals_ = [pltpu.make_async_copy(tok_ref, x_ref.at[0, :, mine], local_sem.at[0])]
    arrive, first = {}, {}
    for k in list(range(1, na)) + [0]:
        block = span(across(a, k), HD)
        sources = [qkv_ref.at[c, :, block] for c in range(3)] + [wout_ref.at[:, block]]
        for c, source in enumerate(sources):
            target = w_ref.at[place, c * HD : (c + 1) * HD]
            if k:
                arrive[k, c] = links.send(source, target, {"a": across(a, k)})
            else:
                locals_.append(pltpu.make_async_copy(source, target, local_sem.at[1 + c]))
        if k:
            first[k] = links.send(tok_ref, x_ref.at[k, :, mine], {"a": across(a, k)})
    for copy in locals_:
        copy.start()
    for copy in locals_:
        copy.wait()
    ends, second = [], {}

    def forward(k):
        at = w_ref.at[span(across(a, k) * nb + b, rows), :]
        for j in range(1, nb):
            ends.append(links.send(at, at, {"b": across(b, j)}))
        at = x_ref.at[k, :, mine]
        second[k] = links.send(at, at, {"p": 1 - p})

    forward(0)
    units = down_ref.shape[1] // na
    for k in range(na):
        block = span(across(a, k), units)

        def cut(i, carry, k=k, block=block):
            at = pl.ds(pl.multiple_of(i * TILE, TILE), TILE)
            piece_refs[k][0, at] = gu_ref[at, 0, block]
            piece_refs[k][1, at] = gu_ref[at, 1, block]
            piece_refs[k][2, at] = down_ref[at, block]
            return carry

        lax.fori_loop(0, rows // TILE, cut, 0)
    for copy in gains_a:
        copy.wait_recv()
    at = gains_ref.at[:, b]
    for j in range(1, nb):
        ends.append(links.send(at, at, {"b": across(b, j)}))
    for k in range(1, na):
        for c in range(4):
            arrive[k, c].wait_recv()
        first[k].wait_recv()
        forward(k)
    for k in range(na):
        second[k].wait_recv()
        at = x_ref.at[k, :, pair]
        ends.append(links.send(at, at, {"q": 1 - q}))
    for copy in ends:
        copy.wait_recv()
    links.finish()


def start_call(na, nb, tok_mine, qkv, w_out, gu, down, gains):
    rows, quarter = tok_mine.shape
    width = 4 * quarter
    w_rows, units = down.shape[0], down.shape[1] // na
    lanes = max(128, gains[0].shape[1])
    copies = (na - 1) * 6 + na * (nb - 1) + (nb - 1) + 2 * na
    vmem = pl.BlockSpec(memory_space=pltpu.VMEM)
    outs = [
        jax.ShapeDtypeStruct((na, rows, width), bf16),
        jax.ShapeDtypeStruct((width, 4 * HD), bf16),
        jax.ShapeDtypeStruct((na, nb, 8, lanes), f32),
    ] + [jax.ShapeDtypeStruct((3, w_rows, units), bf16)] * na
    x_all, w_attn, gains_all, *pieces = pl.pallas_call(
        functools.partial(start_kernel, na, nb),
        out_shape=tuple(outs),
        in_specs=[vmem] * 9,
        out_specs=(vmem,) * len(outs),
        scratch_shapes=[
            pltpu.VMEM((8, lanes), f32),
            pltpu.SemaphoreType.DMA((5,)),
            pltpu.SemaphoreType.DMA((copies,)),
            pltpu.SemaphoreType.DMA((copies,)),
        ],
        compiler_params=pltpu.CompilerParams(
            collective_id=5, has_side_effects=True, vmem_limit_bytes=VMEM_LIMIT
        ),
        name="start",
    )(tok_mine, qkv, w_out, gu, down, *gains)
    return x_all, w_attn, gains_all, pieces


def stats_kernel(na, stats_ref, out_ref, held, from_a, send_sem, recv_sem):
    a, p, q = lax.axis_index("a"), lax.axis_index("p"), lax.axis_index("q")
    greet([{"q": 1 - q}, {"p": 1 - p}] + [{"a": across(a, k)} for k in range(1, na)])
    links = Links(send_sem, recv_sem)
    links.send(stats_ref, held.at[0], {"p": 1 - p}).wait_recv()
    held[1] = stats_ref[...] + held[0]
    links.send(held.at[1], held.at[2], {"q": 1 - q}).wait_recv()
    held[3] = held[1] + held[2]
    copies = [links.send(held.at[3], from_a.at[k - 1], {"a": across(a, k)}) for k in range(1, na)]
    for copy in copies:
        copy.wait_recv()
    for k in range(na):
        for i in range(2):
            at = 2 * k + i
            total = held[3, at : at + 1]
            for j in range(1, na):
                other = 2 * (k ^ j) + i
                total = total + from_a[j - 1, other : other + 1]
            out_ref[at : at + 1] = total
    links.finish()


def stats_call(na, stats, ident):
    return pl.pallas_call(
        functools.partial(stats_kernel, na),
        out_shape=jax.ShapeDtypeStruct(stats.shape, f32),
        in_specs=[pl.BlockSpec(memory_space=pltpu.VMEM)],
        out_specs=pl.BlockSpec(memory_space=pltpu.VMEM),
        scratch_shapes=[
            pltpu.VMEM((4,) + stats.shape, f32),
            pltpu.VMEM((na - 1,) + stats.shape, f32),
            pltpu.SemaphoreType.DMA((na + 1,)),
            pltpu.SemaphoreType.DMA((na + 1,)),
        ],
        compiler_params=pltpu.CompilerParams(collective_id=ident, has_side_effects=True),
    )(stats)


def local_call(kernel, na, operands, outs, scratch=(), flops=10**9):
    def spec(shape, kind):
        if kind == "row":
            return pl.BlockSpec((1,) + tuple(shape[1:]), lambda k: (k,) + (0,) * (len(shape) - 1))
        if kind == "all":
            return pl.BlockSpec(tuple(shape), lambda k: (0,) * len(shape))
        return pl.BlockSpec(memory_space=pl.ANY)

    return pl.pallas_call(
        kernel,
        grid=(na,),
        out_shape=tuple(jax.ShapeDtypeStruct(shape, dtype) for shape, dtype, _ in outs),
        in_specs=[spec(array.shape, kind) for array, kind in operands],
        out_specs=tuple(spec(shape, kind) for shape, _, kind in outs),
        scratch_shapes=list(scratch),
        compiler_params=pltpu.CompilerParams(
            dimension_semantics=("arbitrary",), vmem_limit_bytes=VMEM_LIMIT
        ),
        cost_estimate=pl.CostEstimate(flops=flops, bytes_accessed=2 * 10**7, transcendentals=0),
    )(*[array for array, _ in operands])


def dot(left, right):
    return jnp.dot(left, right, preferred_element_type=f32)


def dot_t(left, right):
    return lax.dot_general(left, right, (((1,), (1,)), ((), ())), preferred_element_type=f32)


def t_dot(left, right):
    return lax.dot_general(left, right, (((0,), (0,)), ((), ())), preferred_element_type=f32)


def add_stats(stats_ref, first, second):
    k = pl.program_id(0)

    @pl.when(k == 0)
    def _():
        stats_ref[...] = jnp.zeros_like(stats_ref)

    stats_ref[...] += to_row(first, 2 * k) + to_row(second, 2 * k + 1)


def qkv_kernel(x_ref, w_ref, qkv_ref, stats_ref):
    out = dot(x_ref[0], w_ref[:, : 3 * HD])
    qkv_ref[0] = out
    queries, key_rows = out[:, :HD], out[:, HD : 2 * HD]
    add_stats(stats_ref, queries * queries, key_rows * key_rows)


def rotate(operand):
    half = HD // 2
    return jnp.concatenate([-operand[:, half:], operand[:, :half]], axis=1)


def rotate_back(operand):
    half = HD // 2
    return jnp.concatenate([operand[:, half:], -operand[:, :half]], axis=1)


def attention(qkv_ref, stats_ref, gain_ref, cos_ref, sin_ref):
    k = pl.program_id(0)
    stats = stats_ref[...] / HQ
    q_inv = lax.rsqrt(to_column(stats, 2 * k) + epsilon)
    k_inv = lax.rsqrt(to_column(stats, 2 * k + 1) + epsilon)
    queries, key_rows = qkv_ref[0, :, :HD], qkv_ref[0, :, HD : 2 * HD]
    values = qkv_ref[0, :, 2 * HD :].astype(bf16)
    cos_table, sine_table = cos_ref[...], sin_ref[...]
    q_normed = queries * q_inv * gain_ref[0:1]
    k_normed = key_rows * k_inv * gain_ref[1:2]
    q_rot = (q_normed * cos_table + rotate(q_normed) * sine_table).astype(bf16)
    k_rot = (k_normed * cos_table + rotate(k_normed) * sine_table).astype(bf16)
    scores = dot_t(q_rot, k_rot) * HD ** (-0.5)
    ahead = lax.broadcasted_iota(jnp.int32, scores.shape, 1) > lax.broadcasted_iota(
        jnp.int32, scores.shape, 0
    )
    scores = jnp.where(ahead, -1e30, scores)
    shifted = jnp.exp(scores - jnp.max(scores, axis=1, keepdims=True))
    probs = shifted / jnp.sum(shifted, axis=1, keepdims=True)
    return queries, key_rows, values, q_inv, k_inv, q_rot, k_rot, probs


def attend_kernel(qkv_ref, stats_ref, gain_ref, cos_ref, sin_ref, w_ref, att_ref, part_ref):
    values, probs = (attention(qkv_ref, stats_ref, gain_ref, cos_ref, sin_ref)[i] for i in (2, 7))
    attended = dot(probs.astype(bf16), values).astype(bf16)
    att_ref[0] = attended
    part_ref[0] = dot_t(attended, w_ref[:, 3 * HD :]).astype(bf16)


def attend_back_kernel(
    proj_ref, qkv_ref, stats_ref, gain_ref, cos_ref, sin_ref, w_ref, grad_ref, inner_ref, sums_ref
):
    k = pl.program_id(0)
    queries, key_rows, values, q_inv, k_inv, q_rot, k_rot, probs = attention(
        qkv_ref, stats_ref, gain_ref, cos_ref, sin_ref
    )
    cos_table, sine_table = cos_ref[...], sin_ref[...]
    grad_att = dot(proj_ref[0], w_ref[:, 3 * HD :]).astype(bf16)
    grad_v = t_dot(probs.astype(bf16), grad_att)
    grad_p = dot_t(grad_att, values)
    delta = jnp.sum(probs * grad_p, axis=1, keepdims=True)
    grad_scores = (probs * (grad_p - delta) * HD ** (-0.5)).astype(bf16)
    grad_q = dot(grad_scores, k_rot)
    grad_k = t_dot(grad_scores, q_rot)
    grad_q = grad_q * cos_table + rotate_back(grad_q * sine_table)
    grad_k = grad_k * cos_table + rotate_back(grad_k * sine_table)

    @pl.when(k == 0)
    def _():
        sums_ref[...] = jnp.zeros_like(sums_ref)

    sums_ref[0:1] += jnp.sum(grad_q * queries * q_inv, axis=0, keepdims=True)
    sums_ref[1:2] += jnp.sum(grad_k * key_rows * k_inv, axis=0, keepdims=True)
    scaled_q = grad_q * gain_ref[0:1]
    scaled_k = grad_k * gain_ref[1:2]
    grad_ref[0, :, :HD] = scaled_q
    grad_ref[0, :, HD : 2 * HD] = scaled_k
    grad_ref[0, :, 2 * HD :] = grad_v
    add_stats(inner_ref, scaled_q * queries, scaled_k * key_rows)


def qkv_back_kernel(scaled_ref, qkv_ref, stats_ref, inner_ref, w_ref, grad_ref, part_ref):
    k = pl.program_id(0)
    for i in range(2):
        at = slice(i * HD, (i + 1) * HD)
        inv = lax.rsqrt(to_column(stats_ref[...] / HQ, 2 * k + i) + epsilon)
        mean = to_column(inner_ref[...] / HQ, 2 * k + i)
        grad = inv * scaled_ref[0, :, at] - qkv_ref[0, :, at] * inv * inv * inv * mean
        grad_ref[0, :, at] = grad.astype(bf16)
    grad_ref[0, :, 2 * HD :] = scaled_ref[0, :, 2 * HD :].astype(bf16)
    part_ref[0] = dot_t(grad_ref[0], w_ref[:, : 3 * HD]).astype(bf16)


def load_weights(na, nb, pieces, w_ref, sem):
    a, b = lax.axis_index("a"), lax.axis_index("b")

    @pl.when(pl.program_id(0) == 0)
    def _():
        rows, units = pieces[0].shape[1:]
        copies = []
        for k in range(na):
            for j in range(nb):
                place = span(across(a, k) * nb + across(b, j), rows)
                for c in range(3):
                    copies.append(
                        pltpu.make_async_copy(
                            pieces[k * nb + j].at[c],
                            w_ref.at[place, c * units : (c + 1) * units],
                            sem.at[len(copies)],
                        )
                    )
        for copy in copies:
            copy.start()
        for copy in copies:
            copy.wait()


def mlp_kernel(na, nb, *refs):
    pieces, (x_ref, gu_ref, hidden_ref, part_ref, w_ref, sem) = refs[: na * nb], refs[na * nb :]
    load_weights(na, nb, pieces, w_ref, sem)
    units = hidden_ref.shape[2]
    gate_up = dot(x_ref[0], w_ref[:, : 2 * units])
    gu_ref[0] = gate_up
    gate, up = gate_up[:, :units], gate_up[:, units:]
    hidden = (gate * jax.nn.sigmoid(gate) * up).astype(bf16)
    hidden_ref[0] = hidden
    part_ref[0] = dot_t(hidden, w_ref[:, 2 * units :]).astype(bf16)


def mlp_back_kernel(na, nb, *refs):
    pieces, (grad_ref, gu_ref, out_ref, part_ref, w_ref, sem) = refs[: na * nb], refs[na * nb :]
    load_weights(na, nb, pieces, w_ref, sem)
    units = gu_ref.shape[2] // 2
    grad_hidden = dot(grad_ref[0], w_ref[:, 2 * units :])
    gate, up = gu_ref[0, :, :units], gu_ref[0, :, units:]
    sigmoid = jax.nn.sigmoid(gate)
    active = gate * sigmoid
    out_ref[0, :, :units] = (
        grad_hidden * up * (sigmoid * (1.0 + gate * (1.0 - sigmoid)))
    ).astype(bf16)
    out_ref[0, :, units:] = (grad_hidden * active).astype(bf16)
    part_ref[0] = dot_t(out_ref[0], w_ref[:, : 2 * units]).astype(bf16)


def widen_kernel(na, count, *refs):
    pieces, out = refs[:na], refs[na]
    a = lax.axis_index("a")
    columns = out.shape[2] // na
    for k in range(na):
        for c in range(count):
            out[c, :, span(across(a, k), columns)] = pieces[k][
                :, c * columns : (c + 1) * columns
            ].astype(f32)


def widen(pieces, count):
    na = len(pieces)
    rows, width = pieces[0].shape
    return pl.pallas_call(
        functools.partial(widen_kernel, na, count),
        out_shape=jax.ShapeDtypeStruct((count, rows, na * width // count), f32),
        in_specs=[pl.BlockSpec(memory_space=pltpu.VMEM)] * na,
        out_specs=pl.BlockSpec(memory_space=pltpu.VMEM),
        compiler_params=pltpu.CompilerParams(vmem_limit_bytes=VMEM_LIMIT),
    )(*pieces)


def rope_tables(length, width):
    half_width = width // 2
    inv_freq = rope_base ** (-(jnp.arange(half_width, dtype=f32) * 2.0) / width)
    angles = jnp.arange(length, dtype=f32)[:, None] * inv_freq[None, :]
    cos_table = jnp.concatenate([jnp.cos(angles), jnp.cos(angles)], axis=1)
    sine_table = jnp.concatenate([jnp.sin(angles), jnp.sin(angles)], axis=1)
    return cos_table, sine_table


def block(
    tokens,
    qkv_weight,
    out_weight,
    gu_weight,
    down_weight,
    attn_gain,
    ffn_gain,
    q_gain,
    k_gain,
    out_grad,
):
    na, nb = lax.axis_size("a"), lax.axis_size("b")
    a, b = lax.axis_index("a"), lax.axis_index("b")
    share = lax.axis_index("q") * 2 + lax.axis_index("p")
    rows, width = tokens.shape
    quarter = width // 4
    w_rows = out_weight.shape[0]
    units = down_weight.shape[1] // na

    def quarter_of(operand):
        return lax.dynamic_slice_in_dim(operand, share * quarter, quarter, 1)

    tok_mine, grad_mine = quarter_of(tokens), quarter_of(out_grad)
    x_all, w_attn, gains, cuts = start_call(
        na,
        nb,
        tok_mine,
        qkv_weight.transpose(1, 0, 2),
        out_weight,
        gu_weight,
        down_weight,
        [gain[None] for gain in (attn_gain, ffn_gain, q_gain, k_gain)],
    )
    n_d, n_h = attn_gain.shape[0], q_gain.shape[0]
    width_gain = pick(gains, share, 0)[:, :2, :n_d].transpose(1, 0, 2).reshape(2, quarter)
    head_gain = pick(gains, a, 0)[:, 2:4, :n_h].transpose(1, 0, 2).reshape(2, HD)
    cos_table, sine_table = rope_tables(SEQ_LEN, HD)

    arrived = [cuts[k] if k == 0 else swap(cuts[k], "a", k) for k in range(na)]

    qkv, stats = local_call(
        qkv_kernel,
        na,
        [(x_all, "row"), (w_attn, "all")],
        [((na, rows, 3 * HD), f32, "row"), ((8, rows), f32, "all")],
    )
    stats = stats_call(na, stats, 6)
    tables = [(stats, "all"), (head_gain, "all"), (cos_table, "all"), (sine_table, "all")]
    full = (na, rows, width)
    attended, part = local_call(
        attend_kernel,
        na,
        [(qkv, "row")] + tables + [(w_attn, "all")],
        [((na, rows, HD), bf16, "row"), (full, bf16, "row")],
    )
    part, arrived = lax.optimization_barrier((part, arrived))
    pieces = []
    for piece in arrived:
        pieces += [piece] + [swap(piece, "b", j) for j in range(1, nb)]
    res_all, proj_mine, inv_mine, res_mine = reduce_call("attn", nb, part, tok_mine, width_gain)

    mlp_scratch = [
        pltpu.VMEM((width, 3 * units), bf16),
        pltpu.SemaphoreType.DMA((3 * na * nb,)),
    ]
    far = [(piece, "far") for piece in pieces]
    gate_up, hidden, part = local_call(
        functools.partial(mlp_kernel, na, nb),
        na,
        far + [(res_all, "row")],
        [((na, rows, 2 * units), f32, "row"), ((na, rows, units), bf16, "row"), (full, bf16, "row")],
        mlp_scratch,
    )
    grad_mlp, block_rows, ffn_sums = reduce_call("mlp", nb, part, res_mine, grad_mine, width_gain)
    grad_gu, part = local_call(
        functools.partial(mlp_back_kernel, na, nb),
        na,
        far + [(grad_mlp, "row"), (gate_up, "row")],
        [((na, rows, 2 * units), bf16, "row"), (full, bf16, "row")],
        mlp_scratch,
    )

    def weight_grad(left, right):
        out = jnp.einsum("krd,kru->du", left, right, preferred_element_type=f32)
        return out.astype(bf16).reshape(na, nb, w_rows, right.shape[2])

    def reduce_b(grad):
        total = pick(grad, b, 1).astype(f32)
        for j in range(1, nb):
            total = total + swap(pick(grad, b ^ j, 1), "b", j).astype(f32)
        return total.astype(bf16)

    def to_owner(grad):
        parts = [pick(grad, a ^ k, 0) for k in range(na)]
        return parts[:1] + [swap(parts[k], "a", k) for k in range(1, na)]

    down_sum = reduce_b(weight_grad(grad_mlp, hidden))
    gu_sum = reduce_b(weight_grad(res_all, grad_gu))
    grad_proj, grad_res, attn_sums = reduce_call(
        "back", nb, part, grad_mine, proj_mine, inv_mine, width_gain
    )
    grad_proj, down_sum, gu_sum = lax.optimization_barrier((grad_proj, down_sum, gu_sum))
    down_sum = to_owner(down_sum)
    scaled, inner, head_sums = local_call(
        attend_back_kernel,
        na,
        [(grad_proj, "row"), (qkv, "row")] + tables + [(w_attn, "all")],
        [((na, rows, 3 * HD), f32, "row"), ((8, rows), f32, "all"), ((8, HD), f32, "all")],
    )
    out_sum = reduce_b(weight_grad(grad_proj, attended))
    inner = stats_call(na, inner, 7)
    inner, gu_sum = lax.optimization_barrier((inner, gu_sum))
    gu_sum = to_owner(gu_sum)
    grad_qkv, part = local_call(
        qkv_back_kernel,
        na,
        [(scaled, "row"), (qkv, "row"), (stats, "all"), (inner, "all"), (w_attn, "all")],
        [((na, rows, 3 * HD), bf16, "row"), (full, bf16, "row")],
    )
    qkv_sum = to_owner(reduce_b(weight_grad(x_all, grad_qkv)))
    out_sum = to_owner(out_sum)
    grad_rows, sums = reduce_call("tok", nb, part, grad_res, attn_sums, ffn_sums, head_sums)
    width_sums = lax.dynamic_slice_in_dim(sums[:2, :quarter], b * n_d, n_d, 1)
    head_sums = lax.dynamic_slice_in_dim(sums[:2, quarter:], b * n_h, n_h, 1)
    return (
        block_rows[0].astype(f32),
        grad_rows[0].astype(f32),
        widen(qkv_sum, 3).transpose(1, 0, 2),
        widen(out_sum, 1)[0],
        widen(gu_sum, 2).transpose(1, 0, 2),
        widen(down_sum, 1)[0],
        width_sums[0],
        width_sums[1],
        head_sums[0],
        head_sums[1],
    )


def solution(mesh):
    dp, tp = mesh.shape["dp"], mesh.shape["tensor"]
    na = HEADS // tp
    fine = Mesh(mesh.devices.reshape(na, dp // na, tp // 2, 2), ("a", "b", "p", "q"))
    dp_axes, tp_axes = ("a", "b"), ("p", "q")
    both = tp_axes + dp_axes
    return jax.shard_map(
        block,
        mesh=fine,
        in_specs=(
            P(dp_axes, None),
            P(dp_axes, None, tp_axes),
            P(dp_axes, tp_axes),
            P(dp_axes, None, tp_axes),
            P(dp_axes, tp_axes),
            P(dp_axes),
            P(dp_axes),
            P(both),
            P(both),
            P(dp_axes, None),
        ),
        out_specs=(
            P(dp_axes, None),
            P(dp_axes, None),
            P(dp_axes, None, tp_axes),
            P(dp_axes, tp_axes),
            P(dp_axes, None, tp_axes),
            P(dp_axes, tp_axes),
            P(dp_axes),
            P(dp_axes),
            P(both),
            P(both),
        ),
        check_vma=False,
    )
```

```python
import functools

import jax
import jax.numpy as jnp
from jax import lax
from jax.experimental import pallas as pl
from jax.experimental.pallas import tpu as pltpu
from jax.sharding import Mesh, PartitionSpec as P


HEADS = 16
HD = 128
SEQ_LEN = 256
HQ = 2048

epsilon = 1e-06
rope_base = 500000.0

f32 = jnp.float32
bf16 = jnp.bfloat16
MESH = pl.DeviceIdType.MESH
EXACT = lax.Precision.HIGHEST
VMEM_LIMIT = 60 * 1024 * 1024
TILE = 64
HALVES = 2


def flip(index, bit):
    return index + bit - 2 * bit * ((index // bit) % 2)


def across(index, k):
    bit = 1
    while bit <= k:
        if k & bit:
            index = flip(index, bit)
        bit *= 2
    return index


def swap(operand, axis, k=1):
    n = lax.axis_size(axis)
    return lax.ppermute(operand, axis, [(i, i ^ k) for i in range(n)])


def pick(operand, index, axis):
    return lax.dynamic_index_in_dim(operand, index, axis, keepdims=False)


def span(index, size):
    return pl.ds(pl.multiple_of(index * size, size), size)


class Links:
    def __init__(self, send_sem, recv_sem):
        self.send_sem, self.recv_sem, self.count, self.copies = send_sem, recv_sem, 0, []

    def send(self, source, target, device):
        copy = pltpu.make_async_remote_copy(
            src_ref=source,
            dst_ref=target,
            send_sem=self.send_sem.at[self.count],
            recv_sem=self.recv_sem.at[self.count],
            device_id=device,
            device_id_type=MESH,
        )
        copy.start()
        self.count += 1
        self.copies.append(copy)
        return copy

    def finish(self):
        for copy in self.copies:
            copy.wait_send()


def greet(peers):
    barrier = pltpu.get_barrier_semaphore()
    for peer in peers:
        pl.semaphore_signal(barrier, inc=1, device_id=peer, device_id_type=MESH)
    pl.semaphore_wait(barrier, len(peers))


def fold(block):
    total = block[:, :128]
    for i in range(1, block.shape[1] // 128):
        total = total + block[:, i * 128 : (i + 1) * 128]
    return total


def wide(column, width):
    return jnp.concatenate([column] * (width // 128), axis=1)


def row_mask(row):
    return (lax.broadcasted_iota(jnp.int32, (8, 128), 0) == row).astype(f32)


def to_row(block, row):
    return lax.dot_general(
        row_mask(row), block, (((1,), (1,)), ((), ())), precision=EXACT, preferred_element_type=f32
    )


def to_column(stats, row):
    return lax.dot_general(
        stats, row_mask(row), (((0,), (0,)), ((), ())), precision=EXACT, preferred_element_type=f32
    )


def dot(left, right):
    return jnp.dot(left, right, preferred_element_type=f32)


def dot_t(left, right):
    return lax.dot_general(left, right, (((1,), (1,)), ((), ())), preferred_element_type=f32)


def t_dot(left, right):
    return lax.dot_general(left, right, (((0,), (0,)), ((), ())), preferred_element_type=f32)


def rotate(operand):
    half = HD // 2
    return jnp.concatenate([-operand[:, half:], operand[:, :half]], axis=1)


def rotate_back(operand):
    half = HD // 2
    return jnp.concatenate([operand[:, half:], -operand[:, :half]], axis=1)


def attention(k, qkv, stats, gain_ref, cos_ref, sin_ref):
    stats = stats / HQ
    q_inv = lax.rsqrt(to_column(stats, 2 * k) + epsilon)
    k_inv = lax.rsqrt(to_column(stats, 2 * k + 1) + epsilon)
    queries, key_rows = qkv[:, :HD], qkv[:, HD : 2 * HD]
    values = qkv[:, 2 * HD :].astype(bf16)
    cos_table, sine_table = cos_ref[...], sin_ref[...]
    q_normed = queries * q_inv * gain_ref[0:1]
    k_normed = key_rows * k_inv * gain_ref[1:2]
    q_rot = (q_normed * cos_table + rotate(q_normed) * sine_table).astype(bf16)
    k_rot = (k_normed * cos_table + rotate(k_normed) * sine_table).astype(bf16)
    scores = dot_t(q_rot, k_rot) * HD ** (-0.5)
    ahead = lax.broadcasted_iota(jnp.int32, scores.shape, 1) > lax.broadcasted_iota(
        jnp.int32, scores.shape, 0
    )
    scores = jnp.where(ahead, -1e30, scores)
    shifted = jnp.exp(scores - jnp.max(scores, axis=1, keepdims=True))
    probs = shifted / jnp.sum(shifted, axis=1, keepdims=True)
    return queries, key_rows, values, q_inv, k_inv, q_rot, k_rot, probs


def reduce_kernel(na, nb, mode, *refs):
    n_in = {"mlp": 4, "back": 5, "tok": 5}[mode]
    n_out = {"mlp": 3, "back": 3, "tok": 2}[mode]
    links = Links(*refs[-2:])
    reduce(na, nb, mode, links, refs[:n_in], refs[n_in : n_in + n_out], refs[n_in + n_out : -2])
    links.finish()


def reduce(na, nb, mode, links, ins, outs, scratch, hooks=None):
    from_q, half_sum, from_p, to_a, from_a, total, parts, cols, stat, *scratch = scratch
    part_ref, out = ins[0], outs[0]
    a, b = lax.axis_index("a"), lax.axis_index("b")
    p, q = lax.axis_index("p"), lax.axis_index("q")
    rows, width = part_ref.shape[1], part_ref.shape[2]
    quarter, half = width // 4, width // 2
    count = rows // HALVES
    mine, pair = span(2 * q + p, quarter), span(q, half)
    peers = [{"q": 1 - q}, {"p": 1 - p}] + [{"a": across(a, k)} for k in range(1, na)]
    if mode == "tok":
        own_sums, a_sums, b_sums = scratch[:3]
        sums_ref = outs[1]
        own_sums[...] = jnp.zeros_like(own_sums)
        own_sums[0:1, mine] = jnp.sum(ins[2][...], axis=0, keepdims=True)
        own_sums[1:2, mine] = jnp.sum(ins[3][...], axis=0, keepdims=True)
        peers += [{"b": across(b, j)} for j in range(1, nb)]
    if hooks is None:
        greet(peers)
    hooks = hooks or {}
    halves = [slice(h * count, (h + 1) * count) for h in range(HALVES)]
    lead = list(range(2, na)) + [1, 0]
    give, keep = span(1 - q, half), span(q, half)

    def each(h, body):
        def step(i, carry):
            body(pl.ds(pl.multiple_of(h * count + i * TILE, TILE), TILE))
            return carry

        lax.fori_loop(0, count // TILE, step, 0)

    if mode == "tok":
        sums_p = links.send(own_sums.at[:, mine], own_sums.at[:, mine], {"p": 1 - p})

    step_q, step_p, step_a = {}, {}, {}
    for h, at_h in enumerate(halves):
        for k in lead:
            step_q[h, k] = links.send(
                part_ref.at[k, at_h, give], from_q.at[k, at_h], {"q": 1 - q}
            )
    for h, at_h in enumerate(halves):
        for k in lead:
            step_q[h, k].wait_recv()

            def add_half(at, k=k):
                own = part_ref[k, at, keep].astype(f32)
                half_sum[k, at] = (own + from_q[k, at].astype(f32)).astype(bf16)

            each(h, add_half)
            step_p[h, k] = links.send(
                half_sum.at[k, at_h, span(1 - p, quarter)], from_p.at[k, at_h], {"p": 1 - p}
            )
    if mode == "tok":
        sums_p.wait_recv()
        sums_q = links.send(own_sums.at[:, pair], own_sums.at[:, pair], {"q": 1 - q})

    def send_a(h):
        at_h = halves[h]
        for k in lead[:-1]:
            step_p[h, k].wait_recv()

            def add_quarter(at, k=k):
                own = half_sum[k, at, span(p, quarter)].astype(f32)
                to_a[k - 1, at] = (own + from_p[k, at].astype(f32)).astype(bf16)

            each(h, add_quarter)
            step_a[h, k] = links.send(
                to_a.at[k - 1, at_h], from_a.at[k - 1, at_h], {"a": across(a, k)}
            )

    for h in range(HALVES):
        send_a(h)
    hooks.get("scattered", lambda: None)()
    if mode == "tok":
        sums_q.wait_recv()
        sums_a = [
            links.send(own_sums.at[:, span(across(a, k), quarter)], a_sums.at[k - 1], {"a": across(a, k)})
            for k in range(1, na)
        ]

    def add_all(at):
        own = half_sum[0, at, span(p, quarter)].astype(f32) + from_p[0, at].astype(f32)
        for k in range(1, na):
            own = own + from_a[k - 1, at].astype(f32)
        return own

    def exchange(h, number):
        at_h = halves[h]
        stats = to_row(parts[0, at_h], 0)
        if number == 2:
            stats = stats + to_row(parts[1, at_h], 1)
        stat[h, 0] = stats
        links.send(stat.at[h, 0], stat.at[h, 1], {"p": 1 - p}).wait_recv()
        stat[h, 2] = stat[h, 0] + stat[h, 1]
        links.send(stat.at[h, 2], stat.at[h, 3], {"q": 1 - q}).wait_recv()
        stats = (stat[h, 2] + stat[h, 3]) / width
        for i in range(number):
            cols[i, at_h] = to_column(stats, i)

    if mode == "attn":
        _, tok_ref, gain_ref = ins
        _, proj_ref, inv_ref, res_ref = outs
        number = 1

        def first(at):
            own = add_all(at)
            proj_ref[at] = own
            parts[0, at] = fold(own * own)

        def second(at):
            own = proj_ref[at]
            inv = lax.rsqrt(cols[0, at] + epsilon)
            inv_ref[at] = inv
            residual = tok_ref[at].astype(f32) + own * wide(inv, quarter) * gain_ref[0:1]
            res_ref[at] = residual
            out[0, at, mine] = residual.astype(bf16)

    elif mode == "mlp":
        _, res_ref, grad_ref, gain_ref = ins
        _, block_ref, sum_ref = outs
        number = 2

        def first(at):
            own = add_all(at)
            total[at] = own
            parts[0, at] = fold(own * own)
            parts[1, at] = fold(grad_ref[at] * gain_ref[1:2] * own)

        sum_ref[...] = jnp.zeros_like(sum_ref)

        def second(at):
            own = total[at]
            inv = wide(lax.rsqrt(cols[0, at] + epsilon), quarter)
            upstream = grad_ref[at]
            scaled = upstream * gain_ref[1:2]
            normed = own * inv
            block_ref[0, at, mine] = (res_ref[at] + normed * gain_ref[1:2]).astype(bf16)
            gains = upstream * normed
            sum_ref[...] += jnp.sum(gains.reshape(TILE // 8, 8, quarter), axis=0)
            grad = inv * scaled - own * inv * inv * inv * wide(cols[1, at], quarter)
            out[0, at, mine] = grad.astype(bf16)

    elif mode == "back":
        _, grad_ref, proj_ref, inv_ref, gain_ref = ins
        _, res_ref, sum_ref = outs
        number = 1

        def first(at):
            grad = grad_ref[at] + add_all(at)
            res_ref[at] = grad
            parts[0, at] = fold(grad * gain_ref[0:1] * proj_ref[at])

        sum_ref[...] = jnp.zeros_like(sum_ref)

        def second(at):
            own = proj_ref[at]
            inv = wide(inv_ref[at], quarter)
            upstream = res_ref[at]
            gains = upstream * own * inv
            sum_ref[...] += jnp.sum(gains.reshape(TILE // 8, 8, quarter), axis=0)
            grad = inv * (upstream * gain_ref[0:1])
            grad = grad - own * inv * inv * inv * wide(cols[0, at], quarter)
            out[0, at, mine] = grad.astype(bf16)

    else:
        grad_ref = ins[1]
        number = 0

        def first(at):
            out[0, at, mine] = (grad_ref[at] + add_all(at)).astype(bf16)

    blocks = range(1) if mode == "tok" else range(na)
    spread_a, spread_p, spread_q = {}, {}, {}
    for h, at_h in enumerate(halves):
        step_p[h, 0].wait_recv()
        for k in range(1, na):
            step_a[h, k].wait_recv()
        each(h, first)
        if number:
            exchange(h, number)
            each(h, second)
        here = out.at[0, at_h, mine]
        for k in blocks:
            if k:
                spread_a[h, k] = links.send(here, out.at[k, at_h, mine], {"a": across(a, k)})
        spread_p[h, 0] = links.send(here, here, {"p": 1 - p})
    if mode == "tok":
        for copy in sums_a:
            copy.wait_recv()
        held = own_sums[:, span(a, quarter)]
        for k in range(1, na):
            held = held + a_sums[k - 1]
        b_sums[0, :, :quarter] = held
        b_sums[0, :, quarter:] = ins[4][...]
        sums_b = [
            links.send(b_sums.at[0], b_sums.at[j], {"b": across(b, j)}) for j in range(1, nb)
        ]
    hooks.get("spread", lambda: None)()
    for h, at_h in enumerate(halves):
        for k in blocks:
            if k:
                spread_a[h, k].wait_recv()
                here = out.at[k, at_h, mine]
                spread_p[h, k] = links.send(here, here, {"p": 1 - p})
    if mode == "mlp":
        here = block_ref.at[0, :, mine]
        block_p = links.send(here, here, {"p": 1 - p})
    for h, at_h in enumerate(halves):
        for k in blocks:
            spread_p[h, k].wait_recv()
            here = out.at[k, at_h, pair]
            spread_q[h, k] = links.send(here, here, {"q": 1 - q})
    if mode == "mlp":
        block_p.wait_recv()
        here = block_ref.at[0, :, pair]
        links.send(here, here, {"q": 1 - q}).wait_recv()
    if mode == "tok":
        for copy in sums_b:
            copy.wait_recv()
        held = b_sums[0]
        for j in range(1, nb):
            held = held + b_sums[j]
        sums_ref[...] = held
    for copy in spread_q.values():
        copy.wait_recv()


def reduce_scratch(na, rows, width):
    quarter = width // 4
    return [
        pltpu.VMEM((na, rows, width // 2), bf16),
        pltpu.VMEM((na, rows, width // 2), bf16),
        pltpu.VMEM((na, rows, quarter), bf16),
        pltpu.VMEM((na - 1, rows, quarter), bf16),
        pltpu.VMEM((na - 1, rows, quarter), bf16),
        pltpu.VMEM((rows, quarter), f32),
        pltpu.VMEM((2, rows, 128), f32),
        pltpu.VMEM((2, rows, 128), f32),
        pltpu.VMEM((HALVES, 4, 8, rows // HALVES), f32),
    ]


def reduce_call(mode, nb, part, *operands):
    na, rows, width = part.shape
    quarter = width // 4
    shape = jax.ShapeDtypeStruct
    full = shape((na, rows, width), bf16)
    one = shape((1, rows, width), bf16)
    share = shape((rows, quarter), f32)
    sums = shape((8, quarter), f32)
    outs = {
        "mlp": (full, one, sums),
        "back": (full, share, sums),
        "tok": (one, shape((8, quarter + HD), f32)),
    }[mode]
    copies = HALVES * (3 * na - 1)
    if mode == "tok":
        copies += HALVES * 2 + 1 + na + nb
        extra = [
            pltpu.VMEM((8, width), f32),
            pltpu.VMEM((na - 1, 8, quarter), f32),
            pltpu.VMEM((nb, 8, quarter + HD), f32),
        ]
    else:
        copies += HALVES * (2 + 3 * na - 1) + (2 if mode == "mlp" else 0)
        extra = []
    vmem = pl.BlockSpec(memory_space=pltpu.VMEM)
    return pl.pallas_call(
        functools.partial(reduce_kernel, na, nb, mode),
        out_shape=outs,
        in_specs=[vmem] * (1 + len(operands)),
        out_specs=(vmem,) * len(outs),
        scratch_shapes=reduce_scratch(na, rows, width)
        + extra
        + [pltpu.SemaphoreType.DMA((copies,)), pltpu.SemaphoreType.DMA((copies,))],
        compiler_params=pltpu.CompilerParams(
            collective_id={"mlp": 2, "back": 3, "tok": 4}[mode],
            has_side_effects=True,
            vmem_limit_bytes=VMEM_LIMIT,
        ),
        cost_estimate=pl.CostEstimate(flops=10**8, bytes_accessed=10**8, transcendentals=0),
    )(part, *operands)


def enter_kernel(na, nb, *refs):
    tok_ref, qkv_w_ref, wout_ref, gu_ref, down_ref, cos_ref, sin_ref = refs[:7]
    gain_refs = refs[7:11]
    x_ref, w_ref, mlp_w_ref, width_gain_ref, head_gain_ref, qkv_ref, stats_ref, att_ref = refs[11:19]
    out, proj_ref, inv_ref, res_ref = refs[19:23]
    own_gains, gains_ref, piece_ref, part_ref, held, stats_a = refs[23:29]
    scratch, (local_sem, send_sem, recv_sem) = refs[29:-3], refs[-3:]
    a, b, p, q = (lax.axis_index(axis) for axis in ("a", "b", "p", "q"))
    rows = wout_ref.shape[0]
    quarter = tok_ref.shape[1]
    units = down_ref.shape[1] // na
    own_gains[...] = jnp.zeros_like(own_gains)
    for i, ref in enumerate(gain_refs):
        own_gains[i : i + 1, : ref.shape[1]] = ref[...].astype(f32)
    gains_ref[a, b] = own_gains[...]
    greet(
        [{"q": 1 - q}, {"p": 1 - p}]
        + [{"a": across(a, k)} for k in range(1, na)]
        + [{"b": across(b, j)} for j in range(1, nb)]
    )
    links = Links(send_sem, recv_sem)
    mine, pair = span(2 * q + p, quarter), span(q, 2 * quarter)
    place = span(a * nb + b, rows)

    gains_a = [
        links.send(own_gains, gains_ref.at[a, b], {"a": across(a, k)}) for k in range(1, na)
    ]
    locals_ = [pltpu.make_async_copy(tok_ref, x_ref.at[0, :, mine], local_sem.at[0])]
    arrive, first = {}, {}
    for k in list(range(1, na)) + [0]:
        block = span(across(a, k), HD)
        sources = [qkv_w_ref.at[c, :, block] for c in range(3)] + [wout_ref.at[:, block]]
        for c, source in enumerate(sources):
            target = w_ref.at[place, c * HD : (c + 1) * HD]
            if k:
                arrive[k, c] = links.send(source, target, {"a": across(a, k)})
            else:
                locals_.append(pltpu.make_async_copy(source, target, local_sem.at[1 + c]))
        if k:
            first[k] = links.send(tok_ref, x_ref.at[k, :, mine], {"a": across(a, k)})
    for copy in locals_:
        copy.start()
    for copy in locals_:
        copy.wait()
    ends, second = [], {}

    def forward(k):
        at = w_ref.at[span(across(a, k) * nb + b, rows), :]
        for j in range(1, nb):
            ends.append(links.send(at, at, {"b": across(b, j)}))
        at = x_ref.at[k, :, mine]
        second[k] = links.send(at, at, {"p": 1 - p})

    forward(0)

    for k in range(na):
        block = span(across(a, k), units)

        def cut(i, carry, k=k, block=block):
            at = pl.ds(pl.multiple_of(i * TILE, TILE), TILE)
            cuts = (gu_ref[at, 0, block], gu_ref[at, 1, block], down_ref[at, block])
            for c in range(3):
                if k:
                    piece_ref[k - 1, c, at] = cuts[c]
                else:
                    to = pl.ds(pl.multiple_of((a * nb + b) * rows + i * TILE, TILE), TILE)
                    mlp_w_ref[to, c * units : (c + 1) * units] = cuts[c]
            return carry

        lax.fori_loop(0, rows // TILE, cut, 0)
    mlp_copies, mlp_ends = {}, []

    def queue(c):
        for k in list(range(2, na)) + [1]:
            target = mlp_w_ref.at[place, c * units : (c + 1) * units]
            mlp_copies[k, c] = links.send(piece_ref.at[k - 1, c], target, {"a": across(a, k)})

    def relay(c, k):
        if k:
            mlp_copies[k, c].wait_recv()
        at = mlp_w_ref.at[span(across(a, k) * nb + b, rows), c * units : (c + 1) * units]
        for j in range(1, nb):
            mlp_ends.append(links.send(at, at, {"b": across(b, j)}))

    queue(0)
    for copy in gains_a:
        copy.wait_recv()
    at = gains_ref.at[:, b]
    for j in range(1, nb):
        ends.append(links.send(at, at, {"b": across(b, j)}))
    for k in range(1, na):
        for c in range(4):
            arrive[k, c].wait_recv()
        first[k].wait_recv()
        forward(k)
    for c in range(3):
        relay(c, 0)
    for k in range(na):
        second[k].wait_recv()
        at = x_ref.at[k, :, pair]
        ends.append(links.send(at, at, {"q": 1 - q}))
    for copy in ends:
        copy.wait_recv()

    n_d, n_h = gain_refs[0].shape[1], gain_refs[2].shape[1]
    width_gain_ref[...] = jnp.zeros_like(width_gain_ref)
    head_gain_ref[...] = jnp.zeros_like(head_gain_ref)
    for i in range(2):
        width_gain_ref[i : i + 1] = jnp.concatenate(
            [gains_ref[2 * q + p, j, i : i + 1, :n_d] for j in range(nb)], axis=1
        )
        head_gain_ref[i : i + 1] = jnp.concatenate(
            [gains_ref[a, j, i + 2 : i + 3, :n_h] for j in range(nb)], axis=1
        )

    held[0] = jnp.zeros_like(held[0])

    def project(k, carry):
        proj = dot(x_ref[k], w_ref[:, : 3 * HD])
        qkv_ref[k] = proj
        queries, key_rows = proj[:, :HD], proj[:, HD : 2 * HD]
        held[0] += to_row(queries * queries, 2 * k) + to_row(key_rows * key_rows, 2 * k + 1)
        return carry

    lax.fori_loop(0, na, project, 0)
    add_over_heads(links, na, a, p, q, held, stats_a, stats_ref, lambda: queue(1))
    for k in range(1, na):
        relay(0, k)

    def attend(k, carry):
        values, probs = (
            attention(k, qkv_ref[k], stats_ref[...], head_gain_ref, cos_ref, sin_ref)[i] for i in (2, 7)
        )
        attended = dot(probs.astype(bf16), values).astype(bf16)
        att_ref[k] = attended
        part_ref[k] = dot_t(attended, w_ref[:, 3 * HD :]).astype(bf16)
        return carry

    lax.fori_loop(0, na, attend, 0)

    def scattered():
        for k in range(1, na):
            relay(1, k)

    reduce(
        na,
        nb,
        "attn",
        links,
        (part_ref, tok_ref, width_gain_ref),
        (out, proj_ref, inv_ref, res_ref),
        scratch,
        {"scattered": scattered, "spread": lambda: queue(2)},
    )
    for k in range(1, na):
        relay(2, k)
    for copy in mlp_ends:
        copy.wait_recv()
    links.finish()


def enter_call(na, nb, tok_mine, qkv, w_out, gu, down, cos_table, sine_table, gains):
    rows, quarter = tok_mine.shape
    width = 4 * quarter
    w_rows, units = down.shape[0], down.shape[1] // na
    lanes = max(128, gains[0].shape[1])
    vmem = pl.BlockSpec(memory_space=pltpu.VMEM)
    shape = jax.ShapeDtypeStruct
    full = shape((na, rows, width), bf16)
    outs = [
        full,
        shape((width, 4 * HD), bf16),
        shape((width, 3 * units), bf16),
        shape((8, quarter), f32),
        shape((8, HD), f32),
        shape((na, rows, 3 * HD), f32),
        shape((8, rows), f32),
        shape((na, rows, HD), bf16),
        full,
        shape((rows, quarter), f32),
        shape((rows, 128), f32),
        shape((rows, quarter), f32),
    ]
    copies = 90 + 16 * nb
    return pl.pallas_call(
        functools.partial(enter_kernel, na, nb),
        out_shape=tuple(outs),
        in_specs=[vmem] * 11,
        out_specs=(vmem,) * len(outs),
        scratch_shapes=[
            pltpu.VMEM((8, lanes), f32),
            pltpu.VMEM((na, nb, 8, lanes), f32),
            pltpu.VMEM((na - 1, 3, w_rows, units), bf16),
            pltpu.VMEM((na, rows, width), bf16),
            pltpu.VMEM((5, 8, rows), f32),
            pltpu.VMEM((na - 1, 8, rows), f32),
        ]
        + reduce_scratch(na, rows, width)
        + [
            pltpu.SemaphoreType.DMA((5,)),
            pltpu.SemaphoreType.DMA((copies,)),
            pltpu.SemaphoreType.DMA((copies,)),
        ],
        compiler_params=pltpu.CompilerParams(
            collective_id=5, has_side_effects=True, vmem_limit_bytes=VMEM_LIMIT
        ),
        name="enter",
    )(tok_mine, qkv, w_out, gu, down, cos_table, sine_table, *gains)


def add_over_heads(links, na, a, p, q, held, from_a, out_ref, sent=None):
    links.send(held.at[0], held.at[1], {"p": 1 - p}).wait_recv()
    held[2] = held[0] + held[1]
    links.send(held.at[2], held.at[3], {"q": 1 - q}).wait_recv()
    held[4] = held[2] + held[3]
    copies = [links.send(held.at[4], from_a.at[k - 1], {"a": across(a, k)}) for k in range(1, na)]
    if sent is not None:
        sent()
    for copy in copies:
        copy.wait_recv()
    for k in range(na):
        for i in range(2):
            at = 2 * k + i
            total = held[4, at : at + 1]
            for j in range(1, na):
                other = 2 * (k ^ j) + i
                total = total + from_a[j - 1, other : other + 1]
            out_ref[at : at + 1] = total


def stats_kernel(na, stats_ref, out_ref, held, from_a, send_sem, recv_sem):
    a, p, q = lax.axis_index("a"), lax.axis_index("p"), lax.axis_index("q")
    greet([{"q": 1 - q}, {"p": 1 - p}] + [{"a": across(a, k)} for k in range(1, na)])
    links = Links(send_sem, recv_sem)
    held[0] = stats_ref[...]
    add_over_heads(links, na, a, p, q, held, from_a, out_ref)
    links.finish()


def stats_call(na, stats, ident):
    return pl.pallas_call(
        functools.partial(stats_kernel, na),
        out_shape=jax.ShapeDtypeStruct(stats.shape, f32),
        in_specs=[pl.BlockSpec(memory_space=pltpu.VMEM)],
        out_specs=pl.BlockSpec(memory_space=pltpu.VMEM),
        scratch_shapes=[
            pltpu.VMEM((5,) + stats.shape, f32),
            pltpu.VMEM((na - 1,) + stats.shape, f32),
            pltpu.SemaphoreType.DMA((na + 1,)),
            pltpu.SemaphoreType.DMA((na + 1,)),
        ],
        compiler_params=pltpu.CompilerParams(collective_id=ident, has_side_effects=True),
    )(stats)


def local_call(kernel, na, operands, outs, scratch=(), flops=10**9):
    def spec(shape, kind):
        if kind == "row":
            return pl.BlockSpec((1,) + tuple(shape[1:]), lambda k: (k,) + (0,) * (len(shape) - 1))
        if kind == "all":
            return pl.BlockSpec(tuple(shape), lambda k: (0,) * len(shape))
        return pl.BlockSpec(memory_space=pl.ANY)

    return pl.pallas_call(
        kernel,
        grid=(na,),
        out_shape=tuple(jax.ShapeDtypeStruct(shape, dtype) for shape, dtype, _ in outs),
        in_specs=[spec(array.shape, kind) for array, kind in operands],
        out_specs=tuple(spec(shape, kind) for shape, _, kind in outs),
        scratch_shapes=list(scratch),
        compiler_params=pltpu.CompilerParams(
            dimension_semantics=("arbitrary",), vmem_limit_bytes=VMEM_LIMIT
        ),
        cost_estimate=pl.CostEstimate(flops=flops, bytes_accessed=2 * 10**7, transcendentals=0),
    )(*[array for array, _ in operands])


def add_stats(stats_ref, first, second):
    k = pl.program_id(0)

    @pl.when(k == 0)
    def _():
        stats_ref[...] = jnp.zeros_like(stats_ref)

    stats_ref[...] += to_row(first, 2 * k) + to_row(second, 2 * k + 1)


def attend_back_kernel(
    proj_ref, qkv_ref, stats_ref, gain_ref, cos_ref, sin_ref, w_ref, grad_ref, inner_ref, sums_ref
):
    k = pl.program_id(0)
    queries, key_rows, values, q_inv, k_inv, q_rot, k_rot, probs = attention(
        k, qkv_ref[0], stats_ref[...], gain_ref, cos_ref, sin_ref
    )
    cos_table, sine_table = cos_ref[...], sin_ref[...]
    grad_att = dot(proj_ref[0], w_ref[:, 3 * HD :]).astype(bf16)
    grad_v = t_dot(probs.astype(bf16), grad_att)
    grad_p = dot_t(grad_att, values)
    delta = jnp.sum(probs * grad_p, axis=1, keepdims=True)
    grad_scores = (probs * (grad_p - delta) * HD ** (-0.5)).astype(bf16)
    grad_q = dot(grad_scores, k_rot)
    grad_k = t_dot(grad_scores, q_rot)
    grad_q = grad_q * cos_table + rotate_back(grad_q * sine_table)
    grad_k = grad_k * cos_table + rotate_back(grad_k * sine_table)

    @pl.when(k == 0)
    def _():
        sums_ref[...] = jnp.zeros_like(sums_ref)

    sums_ref[0:1] += jnp.sum(grad_q * queries * q_inv, axis=0, keepdims=True)
    sums_ref[1:2] += jnp.sum(grad_k * key_rows * k_inv, axis=0, keepdims=True)
    scaled_q = grad_q * gain_ref[0:1]
    scaled_k = grad_k * gain_ref[1:2]
    grad_ref[0, :, :HD] = scaled_q
    grad_ref[0, :, HD : 2 * HD] = scaled_k
    grad_ref[0, :, 2 * HD :] = grad_v
    add_stats(inner_ref, scaled_q * queries, scaled_k * key_rows)


def qkv_back_kernel(scaled_ref, qkv_ref, stats_ref, inner_ref, w_ref, grad_ref, part_ref):
    k = pl.program_id(0)
    for i in range(2):
        at = slice(i * HD, (i + 1) * HD)
        inv = lax.rsqrt(to_column(stats_ref[...] / HQ, 2 * k + i) + epsilon)
        mean = to_column(inner_ref[...] / HQ, 2 * k + i)
        grad = inv * scaled_ref[0, :, at] - qkv_ref[0, :, at] * inv * inv * inv * mean
        grad_ref[0, :, at] = grad.astype(bf16)
    grad_ref[0, :, 2 * HD :] = scaled_ref[0, :, 2 * HD :].astype(bf16)
    part_ref[0] = dot_t(grad_ref[0], w_ref[:, : 3 * HD]).astype(bf16)


def mlp_kernel(x_ref, w_ref, gu_ref, hidden_ref, part_ref):
    units = hidden_ref.shape[2]
    gate_up = dot(x_ref[0], w_ref[:, : 2 * units])
    gu_ref[0] = gate_up
    gate, up = gate_up[:, :units], gate_up[:, units:]
    hidden = (gate * jax.nn.sigmoid(gate) * up).astype(bf16)
    hidden_ref[0] = hidden
    part_ref[0] = dot_t(hidden, w_ref[:, 2 * units :]).astype(bf16)


def mlp_back_kernel(grad_ref, gu_ref, w_ref, out_ref, part_ref):
    units = gu_ref.shape[2] // 2
    grad_hidden = dot(grad_ref[0], w_ref[:, 2 * units :])
    gate, up = gu_ref[0, :, :units], gu_ref[0, :, units:]
    sigmoid = jax.nn.sigmoid(gate)
    active = gate * sigmoid
    out_ref[0, :, :units] = (
        grad_hidden * up * (sigmoid * (1.0 + gate * (1.0 - sigmoid)))
    ).astype(bf16)
    out_ref[0, :, units:] = (grad_hidden * active).astype(bf16)
    part_ref[0] = dot_t(out_ref[0], w_ref[:, : 2 * units]).astype(bf16)


def widen_kernel(na, count, *refs):
    pieces, out = refs[:na], refs[na]
    a = lax.axis_index("a")
    columns = out.shape[2] // na
    for k in range(na):
        for c in range(count):
            out[c, :, span(across(a, k), columns)] = pieces[k][
                :, c * columns : (c + 1) * columns
            ].astype(f32)


def widen(pieces, count):
    na = len(pieces)
    rows, width = pieces[0].shape
    return pl.pallas_call(
        functools.partial(widen_kernel, na, count),
        out_shape=jax.ShapeDtypeStruct((count, rows, na * width // count), f32),
        in_specs=[pl.BlockSpec(memory_space=pltpu.VMEM)] * na,
        out_specs=pl.BlockSpec(memory_space=pltpu.VMEM),
        compiler_params=pltpu.CompilerParams(vmem_limit_bytes=VMEM_LIMIT),
    )(*pieces)


def rope_tables(length, width):
    half_width = width // 2
    inv_freq = rope_base ** (-(jnp.arange(half_width, dtype=f32) * 2.0) / width)
    angles = jnp.arange(length, dtype=f32)[:, None] * inv_freq[None, :]
    cos_table = jnp.concatenate([jnp.cos(angles), jnp.cos(angles)], axis=1)
    sine_table = jnp.concatenate([jnp.sin(angles), jnp.sin(angles)], axis=1)
    return cos_table, sine_table


def block(
    tokens,
    qkv_weight,
    out_weight,
    gu_weight,
    down_weight,
    attn_gain,
    ffn_gain,
    q_gain,
    k_gain,
    out_grad,
):
    na, nb = lax.axis_size("a"), lax.axis_size("b")
    a, b = lax.axis_index("a"), lax.axis_index("b")
    share = lax.axis_index("q") * 2 + lax.axis_index("p")
    rows, width = tokens.shape
    quarter = width // 4
    w_rows = out_weight.shape[0]
    units = down_weight.shape[1] // na

    def quarter_of(operand):
        return lax.dynamic_slice_in_dim(operand, share * quarter, quarter, 1)

    tok_mine, grad_mine = quarter_of(tokens), quarter_of(out_grad)
    cos_table, sine_table = rope_tables(SEQ_LEN, HD)
    (
        x_all,
        w_attn,
        w_mlp,
        width_gain,
        head_gain,
        qkv,
        stats,
        attended,
        res_all,
        proj_mine,
        inv_mine,
        res_mine,
    ) = enter_call(
        na,
        nb,
        tok_mine,
        qkv_weight.transpose(1, 0, 2),
        out_weight,
        gu_weight,
        down_weight,
        cos_table,
        sine_table,
        [gain[None] for gain in (attn_gain, ffn_gain, q_gain, k_gain)],
    )
    n_d, n_h = attn_gain.shape[0], q_gain.shape[0]
    tables = [(stats, "all"), (head_gain, "all"), (cos_table, "all"), (sine_table, "all")]
    full = (na, rows, width)
    gate_up, hidden, part = local_call(
        mlp_kernel,
        na,
        [(res_all, "row"), (w_mlp, "all")],
        [((na, rows, 2 * units), f32, "row"), ((na, rows, units), bf16, "row"), (full, bf16, "row")],
    )
    grad_mlp, block_rows, ffn_sums = reduce_call("mlp", nb, part, res_mine, grad_mine, width_gain)
    grad_gu, part = local_call(
        mlp_back_kernel,
        na,
        [(grad_mlp, "row"), (gate_up, "row"), (w_mlp, "all")],
        [((na, rows, 2 * units), bf16, "row"), (full, bf16, "row")],
    )

    def weight_grad(left, right):
        out = jnp.einsum("krd,kru->du", left, right, preferred_element_type=f32)
        return out.astype(bf16).reshape(na, nb, w_rows, right.shape[2])

    def reduce_b(grad):
        total = pick(grad, b, 1).astype(f32)
        for j in range(1, nb):
            total = total + swap(pick(grad, b ^ j, 1), "b", j).astype(f32)
        return total.astype(bf16)

    def to_owner(grad):
        parts = [pick(grad, a ^ k, 0) for k in range(na)]
        return parts[:1] + [swap(parts[k], "a", k) for k in range(1, na)]

    down_sum = reduce_b(weight_grad(grad_mlp, hidden))
    gu_sum = reduce_b(weight_grad(res_all, grad_gu))
    grad_proj, grad_res, attn_sums = reduce_call(
        "back", nb, part, grad_mine, proj_mine, inv_mine, width_gain
    )
    grad_proj, down_sum, gu_sum = lax.optimization_barrier((grad_proj, down_sum, gu_sum))
    down_sum = to_owner(down_sum)
    scaled, inner, head_sums = local_call(
        attend_back_kernel,
        na,
        [(grad_proj, "row"), (qkv, "row")] + tables + [(w_attn, "all")],
        [((na, rows, 3 * HD), f32, "row"), ((8, rows), f32, "all"), ((8, HD), f32, "all")],
    )
    out_sum = reduce_b(weight_grad(grad_proj, attended))
    inner = stats_call(na, inner, 7)
    inner, gu_sum = lax.optimization_barrier((inner, gu_sum))
    gu_sum = to_owner(gu_sum)
    grad_qkv, part = local_call(
        qkv_back_kernel,
        na,
        [(scaled, "row"), (qkv, "row"), (stats, "all"), (inner, "all"), (w_attn, "all")],
        [((na, rows, 3 * HD), bf16, "row"), (full, bf16, "row")],
    )
    qkv_sum = to_owner(reduce_b(weight_grad(x_all, grad_qkv)))
    out_sum = to_owner(out_sum)
    grad_rows, sums = reduce_call("tok", nb, part, grad_res, attn_sums, ffn_sums, head_sums)
    width_sums = lax.dynamic_slice_in_dim(sums[:2, :quarter], b * n_d, n_d, 1)
    head_sums = lax.dynamic_slice_in_dim(sums[:2, quarter:], b * n_h, n_h, 1)
    return (
        block_rows[0].astype(f32),
        grad_rows[0].astype(f32),
        widen(qkv_sum, 3).transpose(1, 0, 2),
        widen(out_sum, 1)[0],
        widen(gu_sum, 2).transpose(1, 0, 2),
        widen(down_sum, 1)[0],
        width_sums[0],
        width_sums[1],
        head_sums[0],
        head_sums[1],
    )


def solution(mesh):
    dp, tp = mesh.shape["dp"], mesh.shape["tensor"]
    na = HEADS // tp
    fine = Mesh(mesh.devices.reshape(na, dp // na, tp // 2, 2), ("a", "b", "p", "q"))
    dp_axes, tp_axes = ("a", "b"), ("p", "q")
    both = tp_axes + dp_axes
    return jax.shard_map(
        block,
        mesh=fine,
        in_specs=(
            P(dp_axes, None),
            P(dp_axes, None, tp_axes),
            P(dp_axes, tp_axes),
            P(dp_axes, None, tp_axes),
            P(dp_axes, tp_axes),
            P(dp_axes),
            P(dp_axes),
            P(both),
            P(both),
            P(dp_axes, None),
        ),
        out_specs=(
            P(dp_axes, None),
            P(dp_axes, None),
            P(dp_axes, None, tp_axes),
            P(dp_axes, tp_axes),
            P(dp_axes, None, tp_axes),
            P(dp_axes, tp_axes),
            P(dp_axes),
            P(dp_axes),
            P(both),
            P(both),
        ),
        check_vma=False,
    )
```

```python
import functools

import jax
import jax.numpy as jnp
from jax import lax
from jax.experimental import pallas as pl
from jax.experimental.pallas import tpu as pltpu
from jax.sharding import Mesh, PartitionSpec as P


HEADS = 16
HD = 128
SEQ_LEN = 256
HQ = 2048

epsilon = 1e-06
rope_base = 500000.0

f32 = jnp.float32
bf16 = jnp.bfloat16
MESH = pl.DeviceIdType.MESH
EXACT = lax.Precision.HIGHEST
VMEM_LIMIT = 60 * 1024 * 1024
TILE = 64
HALVES = 2


def flip(index, bit):
    return index + bit - 2 * bit * ((index // bit) % 2)


def across(index, k):
    bit = 1
    while bit <= k:
        if k & bit:
            index = flip(index, bit)
        bit *= 2
    return index


def swap(operand, axis, k=1):
    n = lax.axis_size(axis)
    return lax.ppermute(operand, axis, [(i, i ^ k) for i in range(n)])


def pick(operand, index, axis):
    return lax.dynamic_index_in_dim(operand, index, axis, keepdims=False)


def span(index, size):
    return pl.ds(pl.multiple_of(index * size, size), size)


class Links:
    def __init__(self, send_sem, recv_sem):
        self.send_sem, self.recv_sem, self.count, self.copies = send_sem, recv_sem, 0, []

    def send(self, source, target, device):
        copy = pltpu.make_async_remote_copy(
            src_ref=source,
            dst_ref=target,
            send_sem=self.send_sem.at[self.count],
            recv_sem=self.recv_sem.at[self.count],
            device_id=device,
            device_id_type=MESH,
        )
        copy.start()
        self.count += 1
        self.copies.append(copy)
        return copy

    def finish(self):
        for copy in self.copies:
            copy.wait_send()


def greet(peers):
    barrier = pltpu.get_barrier_semaphore()
    for peer in peers:
        pl.semaphore_signal(barrier, inc=1, device_id=peer, device_id_type=MESH)
    pl.semaphore_wait(barrier, len(peers))


def fold(block):
    total = block[:, :128]
    for i in range(1, block.shape[1] // 128):
        total = total + block[:, i * 128 : (i + 1) * 128]
    return total


def wide(column, width):
    return jnp.concatenate([column] * (width // 128), axis=1)


def row_mask(row):
    return (lax.broadcasted_iota(jnp.int32, (8, 128), 0) == row).astype(f32)


def to_row(block, row):
    return lax.dot_general(
        row_mask(row), block, (((1,), (1,)), ((), ())), precision=EXACT, preferred_element_type=f32
    )


def to_column(stats, row):
    return lax.dot_general(
        stats, row_mask(row), (((0,), (0,)), ((), ())), precision=EXACT, preferred_element_type=f32
    )


def dot(left, right):
    return jnp.dot(left, right, preferred_element_type=f32)


def dot_t(left, right):
    return lax.dot_general(left, right, (((1,), (1,)), ((), ())), preferred_element_type=f32)


def t_dot(left, right):
    return lax.dot_general(left, right, (((0,), (0,)), ((), ())), preferred_element_type=f32)


def rotate(operand):
    half = HD // 2
    return jnp.concatenate([-operand[:, half:], operand[:, :half]], axis=1)


def rotate_back(operand):
    half = HD // 2
    return jnp.concatenate([operand[:, half:], -operand[:, :half]], axis=1)


def attention(k, qkv, stats, gain_ref, cos_ref, sin_ref):
    stats = stats / HQ
    q_inv = lax.rsqrt(to_column(stats, 2 * k) + epsilon)
    k_inv = lax.rsqrt(to_column(stats, 2 * k + 1) + epsilon)
    queries, key_rows = qkv[:, :HD], qkv[:, HD : 2 * HD]
    values = qkv[:, 2 * HD :].astype(bf16)
    cos_table, sine_table = cos_ref[...], sin_ref[...]
    q_normed = queries * q_inv * gain_ref[0:1]
    k_normed = key_rows * k_inv * gain_ref[1:2]
    q_rot = (q_normed * cos_table + rotate(q_normed) * sine_table).astype(bf16)
    k_rot = (k_normed * cos_table + rotate(k_normed) * sine_table).astype(bf16)
    scores = dot_t(q_rot, k_rot) * HD ** (-0.5)
    ahead = lax.broadcasted_iota(jnp.int32, scores.shape, 1) > lax.broadcasted_iota(
        jnp.int32, scores.shape, 0
    )
    scores = jnp.where(ahead, -1e30, scores)
    shifted = jnp.exp(scores - jnp.max(scores, axis=1, keepdims=True))
    probs = shifted / jnp.sum(shifted, axis=1, keepdims=True)
    return queries, key_rows, values, q_inv, k_inv, q_rot, k_rot, probs


class Reduce:
    def __init__(self, na, links, part, out, scratch):
        self.na, self.links, self.part, self.out = na, links, part, out
        self.from_q, self.half_sum, self.from_p, self.to_a, self.from_a = scratch[:5]
        self.total, self.parts, self.cols, self.stat = scratch[5:9]
        self.a, self.p, self.q = (lax.axis_index(axis) for axis in ("a", "p", "q"))
        self.rows, self.width = out.shape[1:]
        self.quarter, self.half = self.width // 4, self.width // 2
        self.count = self.rows // HALVES
        self.mine, self.pair = span(2 * self.q + self.p, self.quarter), span(self.q, self.half)
        self.lead = list(range(2, na)) + [1, 0]
        self.step_q, self.step_p, self.step_a = {}, {}, {}
        self.spread_a, self.spread_p, self.spread_q, self.stats = {}, {}, {}, {}

    def at(self, h):
        return slice(h * self.count, (h + 1) * self.count)

    def each(self, h, body):
        def step(i, carry):
            body(pl.ds(pl.multiple_of(h * self.count + i * TILE, TILE), TILE))
            return carry

        lax.fori_loop(0, self.count // TILE, step, 0)

    def send_q(self, h, k):
        at, q = self.at(h), self.q
        source = self.part.at[k, at, span(1 - q, self.half)]
        self.step_q[h, k] = self.links.send(source, self.from_q.at[k, at], {"q": 1 - q})

    def send_p(self, h, k):
        self.step_q[h, k].wait_recv()

        def add(at):
            own = self.part[k, at, span(self.q, self.half)].astype(f32)
            self.half_sum[k, at] = (own + self.from_q[k, at].astype(f32)).astype(bf16)

        self.each(h, add)
        at, p = self.at(h), self.p
        source = self.half_sum.at[k, at, span(1 - p, self.quarter)]
        self.step_p[h, k] = self.links.send(source, self.from_p.at[k, at], {"p": 1 - p})

    def send_a(self, h, k):
        if not k:
            return
        self.step_p[h, k].wait_recv()

        def add(at):
            own = self.half_sum[k, at, span(self.p, self.quarter)].astype(f32)
            self.to_a[k - 1, at] = (own + self.from_p[k, at].astype(f32)).astype(bf16)

        self.each(h, add)
        at = self.at(h)
        self.step_a[h, k] = self.links.send(
            self.to_a.at[k - 1, at], self.from_a.at[k - 1, at], {"a": across(self.a, k)}
        )

    def add_all(self, at):
        own = self.half_sum[0, at, span(self.p, self.quarter)].astype(f32)
        own = own + self.from_p[0, at].astype(f32)
        for k in range(1, self.na):
            own = own + self.from_a[k - 1, at].astype(f32)
        return own

    def scattered(self, h, first, number):
        self.step_p[h, 0].wait_recv()
        for k in range(1, self.na):
            self.step_a[h, k].wait_recv()
        self.each(h, first)
        if number:
            at = self.at(h)
            stats = to_row(self.parts[0, at], 0)
            if number == 2:
                stats = stats + to_row(self.parts[1, at], 1)
            stat = self.stat
            stat[h, 0] = stats
            self.stats[h] = self.links.send(stat.at[h, 0], stat.at[h, 1], {"p": 1 - self.p})

    def stats_q(self, h):
        stat = self.stat
        self.stats[h].wait_recv()
        stat[h, 2] = stat[h, 0] + stat[h, 1]
        self.stats[h] = self.links.send(stat.at[h, 2], stat.at[h, 3], {"q": 1 - self.q})

    def stats_done(self, h, number):
        stat = self.stat
        self.stats[h].wait_recv()
        stats = (stat[h, 2] + stat[h, 3]) / self.width
        for i in range(number):
            self.cols[i, self.at(h)] = to_column(stats, i)

    def spread(self, h, blocks):
        here = self.out.at[0, self.at(h), self.mine]
        for k in blocks:
            if k:
                target = self.out.at[k, self.at(h), self.mine]
                self.spread_a[h, k] = self.links.send(here, target, {"a": across(self.a, k)})
        self.spread_p[h, 0] = self.links.send(here, here, {"p": 1 - self.p})

    def relay_p(self, h, k):
        if not k:
            return
        self.spread_a[h, k].wait_recv()
        here = self.out.at[k, self.at(h), self.mine]
        self.spread_p[h, k] = self.links.send(here, here, {"p": 1 - self.p})

    def relay_q(self, h, k):
        self.spread_p[h, k].wait_recv()
        here = self.out.at[k, self.at(h), self.pair]
        self.spread_q[h, k] = self.links.send(here, here, {"q": 1 - self.q})

    def arrived(self, h, k):
        self.spread_q[h, k].wait_recv()


def reduce_peers(na):
    a, p, q = lax.axis_index("a"), lax.axis_index("p"), lax.axis_index("q")
    return [{"q": 1 - q}, {"p": 1 - p}] + [{"a": across(a, k)} for k in range(1, na)]


def attn_math(r, tok_ref, gain_ref, proj_ref, inv_ref, res_ref):
    def first(at):
        own = r.add_all(at)
        proj_ref[at] = own
        r.parts[0, at] = fold(own * own)

    def second(at):
        own = proj_ref[at]
        inv = lax.rsqrt(r.cols[0, at] + epsilon)
        inv_ref[at] = inv
        residual = tok_ref[at].astype(f32) + own * wide(inv, r.quarter) * gain_ref[0:1]
        res_ref[at] = residual
        r.out[0, at, r.mine] = residual.astype(bf16)

    return first, second


def mlp_math(r, res_ref, grad_ref, gain_ref, block_ref, sum_ref):
    def first(at):
        own = r.add_all(at)
        r.total[at] = own
        r.parts[0, at] = fold(own * own)
        r.parts[1, at] = fold(grad_ref[at] * gain_ref[1:2] * own)

    def second(at):
        own = r.total[at]
        inv = wide(lax.rsqrt(r.cols[0, at] + epsilon), r.quarter)
        upstream = grad_ref[at]
        scaled = upstream * gain_ref[1:2]
        normed = own * inv
        block_ref[0, at, r.mine] = (res_ref[at] + normed * gain_ref[1:2]).astype(bf16)
        gains = upstream * normed
        sum_ref[...] += jnp.sum(gains.reshape(TILE // 8, 8, r.quarter), axis=0)
        grad = inv * scaled - own * inv * inv * inv * wide(r.cols[1, at], r.quarter)
        r.out[0, at, r.mine] = grad.astype(bf16)

    return first, second


def back_math(r, grad_ref, proj_ref, inv_ref, gain_ref, res_ref, sum_ref):
    def first(at):
        grad = grad_ref[at] + r.add_all(at)
        res_ref[at] = grad
        r.parts[0, at] = fold(grad * gain_ref[0:1] * proj_ref[at])

    def second(at):
        own = proj_ref[at]
        inv = wide(inv_ref[at], r.quarter)
        upstream = res_ref[at]
        gains = upstream * own * inv
        sum_ref[...] += jnp.sum(gains.reshape(TILE // 8, 8, r.quarter), axis=0)
        grad = inv * (upstream * gain_ref[0:1])
        grad = grad - own * inv * inv * inv * wide(r.cols[0, at], r.quarter)
        r.out[0, at, r.mine] = grad.astype(bf16)

    return first, second


def middle_kernel(na, *refs):
    x_ref, w_ref, res_ref, grad_ref, proj_ref, inv_ref, gain_ref = refs[:7]
    out, block_ref, hidden_ref, grad_gu_ref, back_out = refs[7:12]
    ffn_sum_ref, grad_res_ref, attn_sum_ref = refs[12:15]
    gu_ref, part_ref, back_part_ref = refs[15:18]
    scratch, (send_sem, recv_sem) = refs[18:-2], refs[-2:]
    units = hidden_ref.shape[2]
    width = x_ref.shape[2]
    greet(reduce_peers(na))
    links = Links(send_sem, recv_sem)
    r = Reduce(na, links, part_ref, out, scratch[:9])
    s = Reduce(na, links, back_part_ref, back_out, scratch[9:])
    ffn_sum_ref[...] = jnp.zeros_like(ffn_sum_ref)
    attn_sum_ref[...] = jnp.zeros_like(attn_sum_ref)
    wide_tile = 512

    def forward(k):
        def gated(n, carry):
            at, up_at = span(n, 256), pl.ds(pl.multiple_of(units + n * 256, 256), 256)
            gate = dot(x_ref[k], w_ref[:, at])
            up = dot(x_ref[k], w_ref[:, up_at])
            gu_ref[k, :, at] = gate
            gu_ref[k, :, up_at] = up
            hidden_ref[k, :, at] = (gate * jax.nn.sigmoid(gate) * up).astype(bf16)
            return carry

        lax.fori_loop(0, units // 256, gated, 0)

        def down(n, carry):
            at = span(n, wide_tile)
            part_ref[k, :, at] = dot_t(hidden_ref[k], w_ref[at, 2 * units :]).astype(bf16)
            return carry

        lax.fori_loop(0, width // wide_tile, down, 0)

    def backward(h, k):
        rows = r.at(h)

        def gated(n, carry):
            at, up_at = span(n, 256), pl.ds(pl.multiple_of(units + n * 256, 256), 256)
            down_at = pl.ds(pl.multiple_of(2 * units + n * 256, 256), 256)
            grad_hidden = dot(out[k, rows], w_ref[:, down_at])
            gate, up = gu_ref[k, rows, at], gu_ref[k, rows, up_at]
            sigmoid = jax.nn.sigmoid(gate)
            active = gate * sigmoid
            grad_gu_ref[k, rows, at] = (
                grad_hidden * up * (sigmoid * (1.0 + gate * (1.0 - sigmoid)))
            ).astype(bf16)
            grad_gu_ref[k, rows, up_at] = (grad_hidden * active).astype(bf16)
            return carry

        lax.fori_loop(0, units // 256, gated, 0)

        def back(n, carry):
            at = span(n, wide_tile)
            back_part_ref[k, rows, at] = dot_t(
                grad_gu_ref[k, rows], w_ref[at, : 2 * units]
            ).astype(bf16)
            return carry

        lax.fori_loop(0, width // wide_tile, back, 0)

    lead = r.lead
    for i, k in enumerate(lead):
        forward(k)
        for h in range(HALVES):
            r.send_q(h, k)
        if i:
            r.send_p(0, lead[i - 1])
    r.send_p(0, lead[-1])
    for k in lead:
        r.send_a(0, k)
        r.send_p(1, k)
    first, second = mlp_math(r, res_ref, grad_ref, gain_ref, block_ref, ffn_sum_ref)
    for k in lead[:-2]:
        r.send_a(1, k)
    r.scattered(0, first, 2)
    r.send_a(1, lead[-2])
    r.stats_q(0)
    r.stats_done(0, 2)
    r.each(0, second)
    r.spread(0, lead)
    r.scattered(1, first, 2)
    r.relay_q(0, 0)
    r.stats_q(1)
    r.arrived(0, 0)
    r.stats_done(1, 2)
    r.each(1, second)
    r.spread(1, lead)
    here = block_ref.at[0, :, r.mine]
    block_p = links.send(here, here, {"p": 1 - r.p})
    backward(0, 0)
    s.send_q(0, 0)
    r.relay_q(1, 0)
    s.send_p(0, 0)
    block_p.wait_recv()
    here = block_ref.at[0, :, r.pair]
    block_q = links.send(here, here, {"q": 1 - r.q})
    r.arrived(1, 0)
    backward(1, 0)
    s.send_q(1, 0)
    order = [(h, k) for h in range(HALVES) for k in lead[:-1]]
    s.send_p(1, 0)
    steps = len(order)
    back_first, back_second = back_math(
        s, grad_ref, proj_ref, inv_ref, gain_ref, grad_res_ref, attn_sum_ref
    )
    for i in range(steps + 4):
        if 0 <= i - 4 < steps:
            s.send_a(*order[i - 4])
        if 0 <= i - 3 < steps:
            s.send_p(*order[i - 3])
        if 0 <= i - 2 < steps:
            r.arrived(*order[i - 2])
            backward(*order[i - 2])
            s.send_q(*order[i - 2])
        if 0 <= i - 1 < steps:
            r.relay_q(*order[i - 1])
        if i < steps:
            r.relay_p(*order[i])
    s.scattered(0, back_first, 1)
    s.stats_q(0)
    s.stats_done(0, 1)
    s.each(0, back_second)
    s.spread(0, lead)
    s.scattered(1, back_first, 1)
    s.relay_q(0, 0)
    s.stats_q(1)
    s.stats_done(1, 1)
    s.each(1, back_second)
    s.spread(1, lead)
    for h, k in order:
        s.relay_p(h, k)
    s.relay_q(1, 0)
    for h, k in order:
        s.relay_q(h, k)
    for h in range(HALVES):
        for k in range(na):
            s.arrived(h, k)
    block_q.wait_recv()
    links.finish()


def middle_call(x_all, w_mlp, res_mine, grad_mine, proj_mine, inv_mine, width_gain):
    na, rows, width = x_all.shape
    quarter, units = width // 4, w_mlp.shape[1] // 3
    vmem = pl.BlockSpec(memory_space=pltpu.VMEM)
    shape = jax.ShapeDtypeStruct
    full = shape((na, rows, width), bf16)
    outs = (
        full,
        shape((1, rows, width), bf16),
        shape((na, rows, units), bf16),
        shape((na, rows, 2 * units), bf16),
        full,
        shape((8, quarter), f32),
        shape((rows, quarter), f32),
        shape((8, quarter), f32),
    )
    copies = 2 * HALVES * (6 * na + 1) + 2
    return pl.pallas_call(
        functools.partial(middle_kernel, na),
        out_shape=outs,
        in_specs=[vmem] * 7,
        out_specs=(vmem,) * len(outs),
        scratch_shapes=[
            pltpu.VMEM((na, rows, 2 * units), f32),
            pltpu.VMEM((na, rows, width), bf16),
            pltpu.VMEM((na, rows, width), bf16),
        ]
        + reduce_scratch(na, rows, width)
        + reduce_scratch(na, rows, width)
        + [pltpu.SemaphoreType.DMA((copies,)), pltpu.SemaphoreType.DMA((copies,))],
        compiler_params=pltpu.CompilerParams(
            collective_id=2, has_side_effects=True, vmem_limit_bytes=VMEM_LIMIT
        ),
        name="middle",
    )(x_all, w_mlp, res_mine, grad_mine, proj_mine, inv_mine, width_gain)


def last_kernel(na, nb, part_ref, grad_ref, attn_sum_ref, ffn_sum_ref, head_sum_ref, out, sums_ref, *refs):
    own_sums, a_sums, b_sums = refs[:3]
    scratch, (send_sem, recv_sem) = refs[3:-2], refs[-2:]
    links = Links(send_sem, recv_sem)
    r = Reduce(na, links, part_ref, out, scratch)
    a, b, p, q, mine, pair, quarter = (
        r.a, lax.axis_index("b"), r.p, r.q, r.mine, r.pair, r.quarter,
    )
    own_sums[...] = jnp.zeros_like(own_sums)
    own_sums[0:1, mine] = jnp.sum(attn_sum_ref[...], axis=0, keepdims=True)
    own_sums[1:2, mine] = jnp.sum(ffn_sum_ref[...], axis=0, keepdims=True)
    greet(reduce_peers(na) + [{"b": across(b, j)} for j in range(1, nb)])
    here = own_sums.at[:, mine]
    sums_p = links.send(here, here, {"p": 1 - p})
    for h in range(HALVES):
        for k in r.lead:
            r.send_q(h, k)
    for h in range(HALVES):
        for k in r.lead:
            r.send_p(h, k)
    sums_p.wait_recv()
    here = own_sums.at[:, pair]
    sums_q = links.send(here, here, {"q": 1 - q})
    for h in range(HALVES):
        for k in r.lead:
            r.send_a(h, k)
    sums_q.wait_recv()
    sums_a = [
        links.send(own_sums.at[:, span(across(a, k), quarter)], a_sums.at[k - 1], {"a": across(a, k)})
        for k in range(1, na)
    ]

    def first(at):
        out[0, at, mine] = (grad_ref[at] + r.add_all(at)).astype(bf16)

    for h in range(HALVES):
        r.scattered(h, first, 0)
        r.spread(h, [0])
    for copy in sums_a:
        copy.wait_recv()
    held = own_sums[:, span(a, quarter)]
    for k in range(1, na):
        held = held + a_sums[k - 1]
    b_sums[0, :, :quarter] = held
    b_sums[0, :, quarter:] = head_sum_ref[...]
    sums_b = [links.send(b_sums.at[0], b_sums.at[j], {"b": across(b, j)}) for j in range(1, nb)]
    for h in range(HALVES):
        r.relay_q(h, 0)
    for copy in sums_b:
        copy.wait_recv()
    held = b_sums[0]
    for j in range(1, nb):
        held = held + b_sums[j]
    sums_ref[...] = held
    for h in range(HALVES):
        r.arrived(h, 0)
    links.finish()


def last_call(nb, part, grad_res, attn_sums, ffn_sums, head_sums):
    na, rows, width = part.shape
    quarter = width // 4
    vmem = pl.BlockSpec(memory_space=pltpu.VMEM)
    shape = jax.ShapeDtypeStruct
    copies = HALVES * (3 * na + 1) + 1 + na + nb
    return pl.pallas_call(
        functools.partial(last_kernel, na, nb),
        out_shape=(shape((1, rows, width), bf16), shape((8, quarter + HD), f32)),
        in_specs=[vmem] * 5,
        out_specs=(vmem, vmem),
        scratch_shapes=[
            pltpu.VMEM((8, width), f32),
            pltpu.VMEM((na - 1, 8, quarter), f32),
            pltpu.VMEM((nb, 8, quarter + HD), f32),
        ]
        + reduce_scratch(na, rows, width)
        + [pltpu.SemaphoreType.DMA((copies,)), pltpu.SemaphoreType.DMA((copies,))],
        compiler_params=pltpu.CompilerParams(
            collective_id=4, has_side_effects=True, vmem_limit_bytes=VMEM_LIMIT
        ),
        cost_estimate=pl.CostEstimate(flops=10**8, bytes_accessed=10**8, transcendentals=0),
        name="last",
    )(part, grad_res, attn_sums, ffn_sums, head_sums)


def reduce_scratch(na, rows, width):
    quarter = width // 4
    return [
        pltpu.VMEM((na, rows, width // 2), bf16),
        pltpu.VMEM((na, rows, width // 2), bf16),
        pltpu.VMEM((na, rows, quarter), bf16),
        pltpu.VMEM((na - 1, rows, quarter), bf16),
        pltpu.VMEM((na - 1, rows, quarter), bf16),
        pltpu.VMEM((rows, quarter), f32),
        pltpu.VMEM((2, rows, 128), f32),
        pltpu.VMEM((2, rows, 128), f32),
        pltpu.VMEM((HALVES, 4, 8, rows // HALVES), f32),
    ]


def enter_kernel(na, nb, *refs):
    tok_ref, qkv_w_ref, wout_ref, gu_ref, down_ref, cos_ref, sin_ref = refs[:7]
    gain_refs = refs[7:11]
    x_ref, w_ref, mlp_w_ref, width_gain_ref, head_gain_ref, qkv_ref, stats_ref, att_ref = refs[11:19]
    out, proj_ref, inv_ref, res_ref = refs[19:23]
    own_gains, gains_ref, piece_ref, part_ref, held, stats_a = refs[23:29]
    scratch, (local_sem, send_sem, recv_sem) = refs[29:-3], refs[-3:]
    a, b, p, q = (lax.axis_index(axis) for axis in ("a", "b", "p", "q"))
    rows = wout_ref.shape[0]
    quarter = tok_ref.shape[1]
    units = down_ref.shape[1] // na
    own_gains[...] = jnp.zeros_like(own_gains)
    for i, ref in enumerate(gain_refs):
        own_gains[i : i + 1, : ref.shape[1]] = ref[...].astype(f32)
    gains_ref[a, b] = own_gains[...]
    greet(
        [{"q": 1 - q}, {"p": 1 - p}]
        + [{"a": across(a, k)} for k in range(1, na)]
        + [{"b": across(b, j)} for j in range(1, nb)]
    )
    links = Links(send_sem, recv_sem)
    mine, pair = span(2 * q + p, quarter), span(q, 2 * quarter)
    place = span(a * nb + b, rows)

    gains_a = [
        links.send(own_gains, gains_ref.at[a, b], {"a": across(a, k)}) for k in range(1, na)
    ]
    locals_ = [pltpu.make_async_copy(tok_ref, x_ref.at[0, :, mine], local_sem.at[0])]
    arrive, first = {}, {}
    for k in list(range(1, na)) + [0]:
        block = span(across(a, k), HD)
        sources = [qkv_w_ref.at[c, :, block] for c in range(3)] + [wout_ref.at[:, block]]
        for c, source in enumerate(sources):
            target = w_ref.at[place, c * HD : (c + 1) * HD]
            if k:
                arrive[k, c] = links.send(source, target, {"a": across(a, k)})
            else:
                locals_.append(pltpu.make_async_copy(source, target, local_sem.at[1 + c]))
        if k:
            first[k] = links.send(tok_ref, x_ref.at[k, :, mine], {"a": across(a, k)})
    for copy in locals_:
        copy.start()
    for copy in locals_:
        copy.wait()
    ends, second = [], {}

    def forward(k):
        at = w_ref.at[span(across(a, k) * nb + b, rows), :]
        for j in range(1, nb):
            ends.append(links.send(at, at, {"b": across(b, j)}))
        at = x_ref.at[k, :, mine]
        second[k] = links.send(at, at, {"p": 1 - p})

    forward(0)

    for k in range(na):
        block = span(across(a, k), units)

        def cut(i, carry, k=k, block=block):
            at = pl.ds(pl.multiple_of(i * TILE, TILE), TILE)
            cuts = (gu_ref[at, 0, block], gu_ref[at, 1, block], down_ref[at, block])
            for c in range(3):
                if k:
                    piece_ref[k - 1, c, at] = cuts[c]
                else:
                    to = pl.ds(pl.multiple_of((a * nb + b) * rows + i * TILE, TILE), TILE)
                    mlp_w_ref[to, c * units : (c + 1) * units] = cuts[c]
            return carry

        lax.fori_loop(0, rows // TILE, cut, 0)
    mlp_copies, mlp_ends = {}, []

    def queue(c):
        for k in list(range(2, na)) + [1]:
            target = mlp_w_ref.at[place, c * units : (c + 1) * units]
            mlp_copies[k, c] = links.send(piece_ref.at[k - 1, c], target, {"a": across(a, k)})

    def relay(c, k):
        if k:
            mlp_copies[k, c].wait_recv()
        at = mlp_w_ref.at[span(across(a, k) * nb + b, rows), c * units : (c + 1) * units]
        for j in range(1, nb):
            mlp_ends.append(links.send(at, at, {"b": across(b, j)}))

    queue(0)
    for copy in gains_a:
        copy.wait_recv()
    at = gains_ref.at[:, b]
    for j in range(1, nb):
        ends.append(links.send(at, at, {"b": across(b, j)}))
    for k in range(1, na):
        for c in range(4):
            arrive[k, c].wait_recv()
        first[k].wait_recv()
        forward(k)
    for c in range(3):
        relay(c, 0)
    for k in range(na):
        second[k].wait_recv()
        at = x_ref.at[k, :, pair]
        ends.append(links.send(at, at, {"q": 1 - q}))
    for copy in ends:
        copy.wait_recv()

    n_d, n_h = gain_refs[0].shape[1], gain_refs[2].shape[1]
    width_gain_ref[...] = jnp.zeros_like(width_gain_ref)
    head_gain_ref[...] = jnp.zeros_like(head_gain_ref)
    for i in range(2):
        width_gain_ref[i : i + 1] = jnp.concatenate(
            [gains_ref[2 * q + p, j, i : i + 1, :n_d] for j in range(nb)], axis=1
        )
        head_gain_ref[i : i + 1] = jnp.concatenate(
            [gains_ref[a, j, i + 2 : i + 3, :n_h] for j in range(nb)], axis=1
        )

    held[0] = jnp.zeros_like(held[0])

    def project(k, carry):
        proj = dot(x_ref[k], w_ref[:, : 3 * HD])
        qkv_ref[k] = proj
        queries, key_rows = proj[:, :HD], proj[:, HD : 2 * HD]
        held[0] += to_row(queries * queries, 2 * k) + to_row(key_rows * key_rows, 2 * k + 1)
        return carry

    lax.fori_loop(0, na, project, 0)
    add_over_heads(links, na, a, p, q, held, stats_a, stats_ref, lambda: queue(1))
    for k in range(1, na):
        relay(0, k)

    def attend(k, carry):
        values, probs = (
            attention(k, qkv_ref[k], stats_ref[...], head_gain_ref, cos_ref, sin_ref)[i] for i in (2, 7)
        )
        attended = dot(probs.astype(bf16), values).astype(bf16)
        att_ref[k] = attended
        part_ref[k] = dot_t(attended, w_ref[:, 3 * HD :]).astype(bf16)
        return carry

    lax.fori_loop(0, na, attend, 0)

    r = Reduce(na, links, part_ref, out, scratch)
    for h in range(HALVES):
        for k in r.lead:
            r.send_q(h, k)
    for h in range(HALVES):
        for k in r.lead:
            r.send_p(h, k)
    for h in range(HALVES):
        for k in r.lead:
            r.send_a(h, k)
    for k in range(1, na):
        relay(1, k)
    attn_first, attn_second = attn_math(r, tok_ref, width_gain_ref, proj_ref, inv_ref, res_ref)
    for h in range(HALVES):
        r.scattered(h, attn_first, 1)
        r.stats_q(h)
        r.stats_done(h, 1)
        r.each(h, attn_second)
        r.spread(h, range(na))
    queue(2)
    for h in range(HALVES):
        for k in range(na):
            r.relay_p(h, k)
    for h in range(HALVES):
        for k in range(na):
            r.relay_q(h, k)
    for h in range(HALVES):
        for k in range(na):
            r.arrived(h, k)
    for k in range(1, na):
        relay(2, k)
    for copy in mlp_ends:
        copy.wait_recv()
    links.finish()


def enter_call(na, nb, tok_mine, qkv, w_out, gu, down, cos_table, sine_table, gains):
    rows, quarter = tok_mine.shape
    width = 4 * quarter
    w_rows, units = down.shape[0], down.shape[1] // na
    lanes = max(128, gains[0].shape[1])
    vmem = pl.BlockSpec(memory_space=pltpu.VMEM)
    shape = jax.ShapeDtypeStruct
    full = shape((na, rows, width), bf16)
    outs = [
        full,
        shape((width, 4 * HD), bf16),
        shape((width, 3 * units), bf16),
        shape((8, quarter), f32),
        shape((8, HD), f32),
        shape((na, rows, 3 * HD), f32),
        shape((8, rows), f32),
        shape((na, rows, HD), bf16),
        full,
        shape((rows, quarter), f32),
        shape((rows, 128), f32),
        shape((rows, quarter), f32),
    ]
    copies = 90 + 16 * nb
    return pl.pallas_call(
        functools.partial(enter_kernel, na, nb),
        out_shape=tuple(outs),
        in_specs=[vmem] * 11,
        out_specs=(vmem,) * len(outs),
        scratch_shapes=[
            pltpu.VMEM((8, lanes), f32),
            pltpu.VMEM((na, nb, 8, lanes), f32),
            pltpu.VMEM((na - 1, 3, w_rows, units), bf16),
            pltpu.VMEM((na, rows, width), bf16),
            pltpu.VMEM((5, 8, rows), f32),
            pltpu.VMEM((na - 1, 8, rows), f32),
        ]
        + reduce_scratch(na, rows, width)
        + [
            pltpu.SemaphoreType.DMA((5,)),
            pltpu.SemaphoreType.DMA((copies,)),
            pltpu.SemaphoreType.DMA((copies,)),
        ],
        compiler_params=pltpu.CompilerParams(
            collective_id=5, has_side_effects=True, vmem_limit_bytes=VMEM_LIMIT
        ),
        name="enter",
    )(tok_mine, qkv, w_out, gu, down, cos_table, sine_table, *gains)


def add_over_heads(links, na, a, p, q, held, from_a, out_ref, sent=None):
    links.send(held.at[0], held.at[1], {"p": 1 - p}).wait_recv()
    held[2] = held[0] + held[1]
    links.send(held.at[2], held.at[3], {"q": 1 - q}).wait_recv()
    held[4] = held[2] + held[3]
    copies = [links.send(held.at[4], from_a.at[k - 1], {"a": across(a, k)}) for k in range(1, na)]
    if sent is not None:
        sent()
    for copy in copies:
        copy.wait_recv()
    for k in range(na):
        for i in range(2):
            at = 2 * k + i
            total = held[4, at : at + 1]
            for j in range(1, na):
                other = 2 * (k ^ j) + i
                total = total + from_a[j - 1, other : other + 1]
            out_ref[at : at + 1] = total


def stats_kernel(na, stats_ref, out_ref, held, from_a, send_sem, recv_sem):
    a, p, q = lax.axis_index("a"), lax.axis_index("p"), lax.axis_index("q")
    greet([{"q": 1 - q}, {"p": 1 - p}] + [{"a": across(a, k)} for k in range(1, na)])
    links = Links(send_sem, recv_sem)
    held[0] = stats_ref[...]
    add_over_heads(links, na, a, p, q, held, from_a, out_ref)
    links.finish()


def stats_call(na, stats, ident):
    return pl.pallas_call(
        functools.partial(stats_kernel, na),
        out_shape=jax.ShapeDtypeStruct(stats.shape, f32),
        in_specs=[pl.BlockSpec(memory_space=pltpu.VMEM)],
        out_specs=pl.BlockSpec(memory_space=pltpu.VMEM),
        scratch_shapes=[
            pltpu.VMEM((5,) + stats.shape, f32),
            pltpu.VMEM((na - 1,) + stats.shape, f32),
            pltpu.SemaphoreType.DMA((na + 1,)),
            pltpu.SemaphoreType.DMA((na + 1,)),
        ],
        compiler_params=pltpu.CompilerParams(collective_id=ident, has_side_effects=True),
    )(stats)


def local_call(kernel, na, operands, outs, scratch=(), flops=10**9):
    def spec(shape, kind):
        if kind == "row":
            return pl.BlockSpec((1,) + tuple(shape[1:]), lambda k: (k,) + (0,) * (len(shape) - 1))
        if kind == "all":
            return pl.BlockSpec(tuple(shape), lambda k: (0,) * len(shape))
        return pl.BlockSpec(memory_space=pl.ANY)

    return pl.pallas_call(
        kernel,
        grid=(na,),
        out_shape=tuple(jax.ShapeDtypeStruct(shape, dtype) for shape, dtype, _ in outs),
        in_specs=[spec(array.shape, kind) for array, kind in operands],
        out_specs=tuple(spec(shape, kind) for shape, _, kind in outs),
        scratch_shapes=list(scratch),
        compiler_params=pltpu.CompilerParams(
            dimension_semantics=("arbitrary",), vmem_limit_bytes=VMEM_LIMIT
        ),
        cost_estimate=pl.CostEstimate(flops=flops, bytes_accessed=2 * 10**7, transcendentals=0),
    )(*[array for array, _ in operands])


def add_stats(stats_ref, first, second):
    k = pl.program_id(0)

    @pl.when(k == 0)
    def _():
        stats_ref[...] = jnp.zeros_like(stats_ref)

    stats_ref[...] += to_row(first, 2 * k) + to_row(second, 2 * k + 1)


def attend_back_kernel(
    proj_ref, qkv_ref, stats_ref, gain_ref, cos_ref, sin_ref, w_ref, grad_ref, inner_ref, sums_ref
):
    k = pl.program_id(0)
    queries, key_rows, values, q_inv, k_inv, q_rot, k_rot, probs = attention(
        k, qkv_ref[0], stats_ref[...], gain_ref, cos_ref, sin_ref
    )
    cos_table, sine_table = cos_ref[...], sin_ref[...]
    grad_att = dot(proj_ref[0], w_ref[:, 3 * HD :]).astype(bf16)
    grad_v = t_dot(probs.astype(bf16), grad_att)
    grad_p = dot_t(grad_att, values)
    delta = jnp.sum(probs * grad_p, axis=1, keepdims=True)
    grad_scores = (probs * (grad_p - delta) * HD ** (-0.5)).astype(bf16)
    grad_q = dot(grad_scores, k_rot)
    grad_k = t_dot(grad_scores, q_rot)
    grad_q = grad_q * cos_table + rotate_back(grad_q * sine_table)
    grad_k = grad_k * cos_table + rotate_back(grad_k * sine_table)

    @pl.when(k == 0)
    def _():
        sums_ref[...] = jnp.zeros_like(sums_ref)

    sums_ref[0:1] += jnp.sum(grad_q * queries * q_inv, axis=0, keepdims=True)
    sums_ref[1:2] += jnp.sum(grad_k * key_rows * k_inv, axis=0, keepdims=True)
    scaled_q = grad_q * gain_ref[0:1]
    scaled_k = grad_k * gain_ref[1:2]
    grad_ref[0, :, :HD] = scaled_q
    grad_ref[0, :, HD : 2 * HD] = scaled_k
    grad_ref[0, :, 2 * HD :] = grad_v
    add_stats(inner_ref, scaled_q * queries, scaled_k * key_rows)


def qkv_back_kernel(scaled_ref, qkv_ref, stats_ref, inner_ref, w_ref, grad_ref, part_ref):
    k = pl.program_id(0)
    for i in range(2):
        at = slice(i * HD, (i + 1) * HD)
        inv = lax.rsqrt(to_column(stats_ref[...] / HQ, 2 * k + i) + epsilon)
        mean = to_column(inner_ref[...] / HQ, 2 * k + i)
        grad = inv * scaled_ref[0, :, at] - qkv_ref[0, :, at] * inv * inv * inv * mean
        grad_ref[0, :, at] = grad.astype(bf16)
    grad_ref[0, :, 2 * HD :] = scaled_ref[0, :, 2 * HD :].astype(bf16)
    part_ref[0] = dot_t(grad_ref[0], w_ref[:, : 3 * HD]).astype(bf16)


def widen_kernel(na, count, *refs):
    pieces, out = refs[:na], refs[na]
    a = lax.axis_index("a")
    columns = out.shape[2] // na
    for k in range(na):
        for c in range(count):
            out[c, :, span(across(a, k), columns)] = pieces[k][
                :, c * columns : (c + 1) * columns
            ].astype(f32)


def widen(pieces, count):
    na = len(pieces)
    rows, width = pieces[0].shape
    return pl.pallas_call(
        functools.partial(widen_kernel, na, count),
        out_shape=jax.ShapeDtypeStruct((count, rows, na * width // count), f32),
        in_specs=[pl.BlockSpec(memory_space=pltpu.VMEM)] * na,
        out_specs=pl.BlockSpec(memory_space=pltpu.VMEM),
        compiler_params=pltpu.CompilerParams(vmem_limit_bytes=VMEM_LIMIT),
    )(*pieces)


def rope_tables(length, width):
    half_width = width // 2
    inv_freq = rope_base ** (-(jnp.arange(half_width, dtype=f32) * 2.0) / width)
    angles = jnp.arange(length, dtype=f32)[:, None] * inv_freq[None, :]
    cos_table = jnp.concatenate([jnp.cos(angles), jnp.cos(angles)], axis=1)
    sine_table = jnp.concatenate([jnp.sin(angles), jnp.sin(angles)], axis=1)
    return cos_table, sine_table


def block(
    tokens,
    qkv_weight,
    out_weight,
    gu_weight,
    down_weight,
    attn_gain,
    ffn_gain,
    q_gain,
    k_gain,
    out_grad,
):
    na, nb = lax.axis_size("a"), lax.axis_size("b")
    a, b = lax.axis_index("a"), lax.axis_index("b")
    share = lax.axis_index("q") * 2 + lax.axis_index("p")
    rows, width = tokens.shape
    quarter = width // 4
    w_rows = out_weight.shape[0]

    def quarter_of(operand):
        return lax.dynamic_slice_in_dim(operand, share * quarter, quarter, 1)

    tok_mine, grad_mine = quarter_of(tokens), quarter_of(out_grad)
    cos_table, sine_table = rope_tables(SEQ_LEN, HD)
    (
        x_all,
        w_attn,
        w_mlp,
        width_gain,
        head_gain,
        qkv,
        stats,
        attended,
        res_all,
        proj_mine,
        inv_mine,
        res_mine,
    ) = enter_call(
        na,
        nb,
        tok_mine,
        qkv_weight.transpose(1, 0, 2),
        out_weight,
        gu_weight,
        down_weight,
        cos_table,
        sine_table,
        [gain[None] for gain in (attn_gain, ffn_gain, q_gain, k_gain)],
    )
    n_d, n_h = attn_gain.shape[0], q_gain.shape[0]
    tables = [(stats, "all"), (head_gain, "all"), (cos_table, "all"), (sine_table, "all")]
    full = (na, rows, width)
    grad_mlp, block_rows, hidden, grad_gu, grad_proj, ffn_sums, grad_res, attn_sums = middle_call(
        res_all, w_mlp, res_mine, grad_mine, proj_mine, inv_mine, width_gain
    )

    def weight_grad(left, right):
        out = jnp.einsum("krd,kru->du", left, right, preferred_element_type=f32)
        return out.astype(bf16).reshape(na, nb, w_rows, right.shape[2])

    def reduce_b(grad):
        total = pick(grad, b, 1).astype(f32)
        for j in range(1, nb):
            total = total + swap(pick(grad, b ^ j, 1), "b", j).astype(f32)
        return total.astype(bf16)

    def to_owner(grad):
        parts = [pick(grad, a ^ k, 0) for k in range(na)]
        return parts[:1] + [swap(parts[k], "a", k) for k in range(1, na)]

    down_sum = reduce_b(weight_grad(grad_mlp, hidden))
    gu_sum = reduce_b(weight_grad(res_all, grad_gu))
    scaled, inner, head_sums = local_call(
        attend_back_kernel,
        na,
        [(grad_proj, "row"), (qkv, "row")] + tables + [(w_attn, "all")],
        [((na, rows, 3 * HD), f32, "row"), ((8, rows), f32, "all"), ((8, HD), f32, "all")],
    )
    out_sum = reduce_b(weight_grad(grad_proj, attended))
    inner = stats_call(na, inner, 7)
    inner, down_sum = lax.optimization_barrier((inner, down_sum))
    down_sum = to_owner(down_sum)
    grad_qkv, part = local_call(
        qkv_back_kernel,
        na,
        [(scaled, "row"), (qkv, "row"), (stats, "all"), (inner, "all"), (w_attn, "all")],
        [((na, rows, 3 * HD), bf16, "row"), (full, bf16, "row")],
    )
    part, gu_sum = lax.optimization_barrier((part, gu_sum))
    gu_sum = to_owner(gu_sum)
    qkv_sum = to_owner(reduce_b(weight_grad(x_all, grad_qkv)))
    out_sum = to_owner(out_sum)
    grad_rows, sums = last_call(nb, part, grad_res, attn_sums, ffn_sums, head_sums)
    width_sums = lax.dynamic_slice_in_dim(sums[:2, :quarter], b * n_d, n_d, 1)
    head_sums = lax.dynamic_slice_in_dim(sums[:2, quarter:], b * n_h, n_h, 1)
    return (
        block_rows[0].astype(f32),
        grad_rows[0].astype(f32),
        widen(qkv_sum, 3).transpose(1, 0, 2),
        widen(out_sum, 1)[0],
        widen(gu_sum, 2).transpose(1, 0, 2),
        widen(down_sum, 1)[0],
        width_sums[0],
        width_sums[1],
        head_sums[0],
        head_sums[1],
    )


def solution(mesh):
    dp, tp = mesh.shape["dp"], mesh.shape["tensor"]
    na = HEADS // tp
    fine = Mesh(mesh.devices.reshape(na, dp // na, tp // 2, 2), ("a", "b", "p", "q"))
    dp_axes, tp_axes = ("a", "b"), ("p", "q")
    both = tp_axes + dp_axes
    return jax.shard_map(
        block,
        mesh=fine,
        in_specs=(
            P(dp_axes, None),
            P(dp_axes, None, tp_axes),
            P(dp_axes, tp_axes),
            P(dp_axes, None, tp_axes),
            P(dp_axes, tp_axes),
            P(dp_axes),
            P(dp_axes),
            P(both),
            P(both),
            P(dp_axes, None),
        ),
        out_specs=(
            P(dp_axes, None),
            P(dp_axes, None),
            P(dp_axes, None, tp_axes),
            P(dp_axes, tp_axes),
            P(dp_axes, None, tp_axes),
            P(dp_axes, tp_axes),
            P(dp_axes),
            P(dp_axes),
            P(both),
            P(both),
        ),
        check_vma=False,
    )
```

```python
import functools

import jax
import jax.numpy as jnp
from jax import lax
from jax.experimental import pallas as pl
from jax.experimental.pallas import tpu as pltpu
from jax.sharding import Mesh, PartitionSpec as P

HEADS = 16
HD = 128
SEQ_LEN = 256
HQ = 2048

epsilon = 1e-06
rope_base = 500000.0

f32 = jnp.float32
bf16 = jnp.bfloat16
MESH = pl.DeviceIdType.MESH
EXACT = lax.Precision.HIGHEST
VMEM_LIMIT = 60 * 1024 * 1024
TILE = 64
HALVES = 2


def flip(index, bit):
    return index + bit - 2 * bit * ((index // bit) % 2)


def across(index, k):
    bit = 1
    while bit <= k:
        if k & bit:
            index = flip(index, bit)
        bit *= 2
    return index


def swap(operand, axis, k=1):
    n = lax.axis_size(axis)
    return lax.ppermute(operand, axis, [(i, i ^ k) for i in range(n)])


def pick(operand, index, axis):
    return lax.dynamic_index_in_dim(operand, index, axis, keepdims=False)


def span(index, size):
    return pl.ds(pl.multiple_of(index * size, size), size)


class Links:
    def __init__(self, send_sem, recv_sem):
        self.send_sem, self.recv_sem, self.count, self.copies = send_sem, recv_sem, 0, []

    def send(self, source, target, device):
        copy = pltpu.make_async_remote_copy(
            src_ref=source,
            dst_ref=target,
            send_sem=self.send_sem.at[self.count],
            recv_sem=self.recv_sem.at[self.count],
            device_id=device,
            device_id_type=MESH,
        )
        copy.start()
        self.count += 1
        self.copies.append(copy)
        return copy

    def sent(self, copies):
        done = [id(copy) for copy in copies]
        for copy in self.copies:
            if id(copy) in done:
                copy.wait_send()
        self.copies = [copy for copy in self.copies if id(copy) not in done]

    def finish(self):
        for copy in self.copies:
            copy.wait_send()


def greet(peers):
    barrier = pltpu.get_barrier_semaphore()
    for peer in peers:
        pl.semaphore_signal(barrier, inc=1, device_id=peer, device_id_type=MESH)
    pl.semaphore_wait(barrier, len(peers))


def fold(block):
    total = block[:, :128]
    for i in range(1, block.shape[1] // 128):
        total = total + block[:, i * 128 : (i + 1) * 128]
    return total


def wide(column, width):
    return jnp.concatenate([column] * (width // 128), axis=1)


def row_mask(row):
    return (lax.broadcasted_iota(jnp.int32, (8, 128), 0) == row).astype(f32)


def to_row(block, row):
    return lax.dot_general(
        row_mask(row), block, (((1,), (1,)), ((), ())), precision=EXACT, preferred_element_type=f32
    )


def to_column(stats, row):
    return lax.dot_general(
        stats, row_mask(row), (((0,), (0,)), ((), ())), precision=EXACT, preferred_element_type=f32
    )


def dot(left, right):
    return jnp.dot(left, right, preferred_element_type=f32)


def dot_t(left, right):
    return lax.dot_general(left, right, (((1,), (1,)), ((), ())), preferred_element_type=f32)


def t_dot(left, right):
    return lax.dot_general(left, right, (((0,), (0,)), ((), ())), preferred_element_type=f32)


def rotate(operand):
    half = HD // 2
    return jnp.concatenate([-operand[:, half:], operand[:, :half]], axis=1)


def rotate_back(operand):
    half = HD // 2
    return jnp.concatenate([operand[:, half:], -operand[:, :half]], axis=1)


def attention(k, qkv, stats, gain_ref, cos_ref, sin_ref):
    stats = stats / HQ
    q_inv = lax.rsqrt(to_column(stats, 2 * k) + epsilon)
    k_inv = lax.rsqrt(to_column(stats, 2 * k + 1) + epsilon)
    queries, key_rows = qkv[:, :HD], qkv[:, HD : 2 * HD]
    values = qkv[:, 2 * HD :].astype(bf16)
    cos_table, sine_table = cos_ref[...], sin_ref[...]
    q_normed = queries * q_inv * gain_ref[0:1]
    k_normed = key_rows * k_inv * gain_ref[1:2]
    q_rot = (q_normed * cos_table + rotate(q_normed) * sine_table).astype(bf16)
    k_rot = (k_normed * cos_table + rotate(k_normed) * sine_table).astype(bf16)
    scores = dot_t(q_rot, k_rot) * HD ** (-0.5)
    ahead = lax.broadcasted_iota(jnp.int32, scores.shape, 1) > lax.broadcasted_iota(
        jnp.int32, scores.shape, 0
    )
    scores = jnp.where(ahead, -1e30, scores)
    shifted = jnp.exp(scores - jnp.max(scores, axis=1, keepdims=True))
    probs = shifted / jnp.sum(shifted, axis=1, keepdims=True)
    return queries, key_rows, values, q_inv, k_inv, q_rot, k_rot, probs


def weight_grad(left, right, out, block):
    na, nb = left.shape[0], out.shape[1]
    rows = out.shape[2]
    total = None
    for k in range(na):
        term = t_dot(left[k, :, block * nb * rows : (block + 1) * nb * rows], right[k])
        total = term if total is None else total + term
    for j in range(nb):
        out[block, j] = total[j * rows : (j + 1) * rows].astype(bf16)


def exchange_b(links, grad, held, columns):
    b = lax.axis_index("b")
    return [
        links.send(
            grad.at[:, across(b, j), :, columns], held.at[j - 1, :, :, columns], {"b": across(b, j)}
        )
        for j in range(1, held.shape[0] + 1)
    ]


def sum_b(copies, grad, held, out, columns):
    b = lax.axis_index("b")
    for copy in copies:
        copy.wait_recv()

    def add(block, carry):
        total = grad[block, b, :, columns].astype(f32)
        for j in range(held.shape[0]):
            total = total + held[j, block, :, columns].astype(f32)
        out[block, :, columns] = total.astype(bf16)
        return carry

    lax.fori_loop(0, grad.shape[0], add, 0)


class Reduce:
    def __init__(self, na, links, part, out, scratch):
        self.na, self.links, self.part, self.out = na, links, part, out
        self.from_q, self.half_sum, self.from_p, self.to_a, self.from_a = scratch[:5]
        self.total, self.parts, self.cols, self.stat = scratch[5:9]
        self.a, self.p, self.q = (lax.axis_index(axis) for axis in ("a", "p", "q"))
        self.rows, self.width = out.shape[1:]
        self.quarter, self.half = self.width // 4, self.width // 2
        self.count = self.rows // HALVES
        self.mine, self.pair = span(2 * self.q + self.p, self.quarter), span(self.q, self.half)
        self.lead = list(range(2, na)) + [1, 0]
        self.step_q, self.step_p, self.step_a = {}, {}, {}
        self.spread_a, self.spread_p, self.spread_q, self.stats = {}, {}, {}, {}

    def at(self, h):
        return slice(h * self.count, (h + 1) * self.count)

    def each(self, h, body):
        def step(i, carry):
            body(pl.ds(pl.multiple_of(h * self.count + i * TILE, TILE), TILE))
            return carry

        lax.fori_loop(0, self.count // TILE, step, 0)

    def send_q(self, h, k):
        at, q = self.at(h), self.q
        source = self.part.at[k, at, span(1 - q, self.half)]
        self.step_q[h, k] = self.links.send(source, self.from_q.at[k, at], {"q": 1 - q})

    def send_p(self, h, k):
        self.step_q[h, k].wait_recv()

        def add(at):
            own = self.part[k, at, span(self.q, self.half)].astype(f32)
            self.half_sum[k, at] = (own + self.from_q[k, at].astype(f32)).astype(bf16)

        self.each(h, add)
        at, p = self.at(h), self.p
        source = self.half_sum.at[k, at, span(1 - p, self.quarter)]
        self.step_p[h, k] = self.links.send(source, self.from_p.at[k, at], {"p": 1 - p})

    def send_a(self, h, k):
        if not k:
            return
        self.step_p[h, k].wait_recv()

        def add(at):
            own = self.half_sum[k, at, span(self.p, self.quarter)].astype(f32)
            self.to_a[k - 1, at] = (own + self.from_p[k, at].astype(f32)).astype(bf16)

        self.each(h, add)
        at = self.at(h)
        self.step_a[h, k] = self.links.send(
            self.to_a.at[k - 1, at], self.from_a.at[k - 1, at], {"a": across(self.a, k)}
        )

    def add_all(self, at):
        own = self.half_sum[0, at, span(self.p, self.quarter)].astype(f32)
        own = own + self.from_p[0, at].astype(f32)
        for k in range(1, self.na):
            own = own + self.from_a[k - 1, at].astype(f32)
        return own

    def scattered(self, h, first, number):
        self.step_p[h, 0].wait_recv()
        for k in range(1, self.na):
            self.step_a[h, k].wait_recv()
        self.each(h, first)
        if number:
            at = self.at(h)
            stats = to_row(self.parts[0, at], 0)
            if number == 2:
                stats = stats + to_row(self.parts[1, at], 1)
            stat = self.stat
            stat[h, 0] = stats
            self.stats[h] = self.links.send(stat.at[h, 0], stat.at[h, 1], {"p": 1 - self.p})

    def stats_q(self, h):
        stat = self.stat
        self.stats[h].wait_recv()
        stat[h, 2] = stat[h, 0] + stat[h, 1]
        self.stats[h] = self.links.send(stat.at[h, 2], stat.at[h, 3], {"q": 1 - self.q})

    def stats_done(self, h, number):
        stat = self.stat
        self.stats[h].wait_recv()
        stats = (stat[h, 2] + stat[h, 3]) / self.width
        for i in range(number):
            self.cols[i, self.at(h)] = to_column(stats, i)

    def spread(self, h, blocks):
        here = self.out.at[0, self.at(h), self.mine]
        for k in blocks:
            if k:
                target = self.out.at[k, self.at(h), self.mine]
                self.spread_a[h, k] = self.links.send(here, target, {"a": across(self.a, k)})
        self.spread_p[h, 0] = self.links.send(here, here, {"p": 1 - self.p})

    def relay_p(self, h, k):
        if not k:
            return
        self.spread_a[h, k].wait_recv()
        here = self.out.at[k, self.at(h), self.mine]
        self.spread_p[h, k] = self.links.send(here, here, {"p": 1 - self.p})

    def relay_q(self, h, k):
        self.spread_p[h, k].wait_recv()
        here = self.out.at[k, self.at(h), self.pair]
        self.spread_q[h, k] = self.links.send(here, here, {"q": 1 - self.q})

    def arrived(self, h, k):
        self.spread_q[h, k].wait_recv()


def reduce_peers(na):
    a, p, q = lax.axis_index("a"), lax.axis_index("p"), lax.axis_index("q")
    return [{"q": 1 - q}, {"p": 1 - p}] + [{"a": across(a, k)} for k in range(1, na)]


def attn_math(r, tok_ref, gain_ref, proj_ref, inv_ref, res_ref):
    def first(at):
        own = r.add_all(at)
        proj_ref[at] = own
        r.parts[0, at] = fold(own * own)

    def second(at):
        own = proj_ref[at]
        inv = lax.rsqrt(r.cols[0, at] + epsilon)
        inv_ref[at] = inv
        residual = tok_ref[at].astype(f32) + own * wide(inv, r.quarter) * gain_ref[0:1]
        res_ref[at] = residual
        r.out[0, at, r.mine] = residual.astype(bf16)

    return first, second


def mlp_math(r, res_ref, grad_ref, gain_ref, block_ref, sum_ref):
    def first(at):
        own = r.add_all(at)
        r.total[at] = own
        r.parts[0, at] = fold(own * own)
        r.parts[1, at] = fold(grad_ref[at] * gain_ref[1:2] * own)

    def second(at):
        own = r.total[at]
        inv = wide(lax.rsqrt(r.cols[0, at] + epsilon), r.quarter)
        upstream = grad_ref[at]
        scaled = upstream * gain_ref[1:2]
        normed = own * inv
        block_ref[0, at, r.mine] = (res_ref[at] + normed * gain_ref[1:2]).astype(bf16)
        gains = upstream * normed
        sum_ref[...] += jnp.sum(gains.reshape(TILE // 8, 8, r.quarter), axis=0)
        grad = inv * scaled - own * inv * inv * inv * wide(r.cols[1, at], r.quarter)
        r.out[0, at, r.mine] = grad.astype(bf16)

    return first, second


def back_math(r, grad_ref, proj_ref, inv_ref, gain_ref, res_ref, sum_ref):
    def first(at):
        grad = grad_ref[at] + r.add_all(at)
        res_ref[at] = grad
        r.parts[0, at] = fold(grad * gain_ref[0:1] * proj_ref[at])

    def second(at):
        own = proj_ref[at]
        inv = wide(inv_ref[at], r.quarter)
        upstream = res_ref[at]
        gains = upstream * own * inv
        sum_ref[...] += jnp.sum(gains.reshape(TILE // 8, 8, r.quarter), axis=0)
        grad = inv * (upstream * gain_ref[0:1])
        grad = grad - own * inv * inv * inv * wide(r.cols[0, at], r.quarter)
        r.out[0, at, r.mine] = grad.astype(bf16)

    return first, second


def middle_kernel(na, nb, *refs):
    x_ref, w_ref, res_ref, grad_ref, proj_ref, inv_ref, gain_ref = refs[:7]
    block_ref, back_out, ffn_sum_ref, grad_res_ref, attn_sum_ref, down_sum_ref, gu_grad_ref = refs[7:14]
    out, hidden_ref, grad_gu_ref, gu_ref, part_ref, down_grad, down_held = refs[14:21]
    scratch, (send_sem, recv_sem) = refs[21:-2], refs[-2:]
    units = hidden_ref.shape[2]
    width = x_ref.shape[2]
    b = lax.axis_index("b")
    greet(reduce_peers(na) + [{"b": across(b, j)} for j in range(1, nb)])
    links = Links(send_sem, recv_sem)
    r = Reduce(na, links, part_ref, out, scratch[:9])
    s = Reduce(na, links, part_ref, back_out, scratch[9:])
    ffn_sum_ref[...] = jnp.zeros_like(ffn_sum_ref)
    attn_sum_ref[...] = jnp.zeros_like(attn_sum_ref)
    wide_tile = 512

    def forward(k):
        def gated(n, carry):
            at, up_at = span(n, 256), pl.ds(pl.multiple_of(units + n * 256, 256), 256)
            gate = dot(x_ref[k], w_ref[:, at])
            up = dot(x_ref[k], w_ref[:, up_at])
            gu_ref[k, :, at] = gate
            gu_ref[k, :, up_at] = up
            hidden_ref[k, :, at] = (gate * jax.nn.sigmoid(gate) * up).astype(bf16)
            return carry

        lax.fori_loop(0, units // 256, gated, 0)

        def down(n, carry):
            at = span(n, wide_tile)
            part_ref[k, :, at] = dot_t(hidden_ref[k], w_ref[at, 2 * units :]).astype(bf16)
            return carry

        lax.fori_loop(0, width // wide_tile, down, 0)

    def backward(h, k):
        rows = r.at(h)

        def gated(n, carry):
            at, up_at = span(n, 256), pl.ds(pl.multiple_of(units + n * 256, 256), 256)
            down_at = pl.ds(pl.multiple_of(2 * units + n * 256, 256), 256)
            grad_hidden = dot(out[k, rows], w_ref[:, down_at])
            gate, up = gu_ref[k, rows, at], gu_ref[k, rows, up_at]
            sigmoid = jax.nn.sigmoid(gate)
            active = gate * sigmoid
            grad_gu_ref[k, rows, at] = (
                grad_hidden * up * (sigmoid * (1.0 + gate * (1.0 - sigmoid)))
            ).astype(bf16)
            grad_gu_ref[k, rows, up_at] = (grad_hidden * active).astype(bf16)
            return carry

        lax.fori_loop(0, units // 256, gated, 0)

        def back(n, carry):
            at = span(n, wide_tile)
            part_ref[k, rows, at] = dot_t(
                grad_gu_ref[k, rows], w_ref[at, : 2 * units]
            ).astype(bf16)
            return carry

        lax.fori_loop(0, width // wide_tile, back, 0)

    lead = r.lead
    for i, k in enumerate(lead):
        forward(k)
        for h in range(HALVES):
            r.send_q(h, k)
        if i:
            r.send_p(0, lead[i - 1])
    r.send_p(0, lead[-1])
    r.send_p(1, lead[0])
    r.send_a(0, lead[0])
    r.send_p(1, lead[1])
    for k in lead[1:]:
        r.send_a(0, k)
    first, second = mlp_math(r, res_ref, grad_ref, gain_ref, block_ref, ffn_sum_ref)
    r.scattered(0, first, 2)
    for k in lead[2:]:
        r.send_p(1, k)
    for k in lead[:-2]:
        r.send_a(1, k)
    r.stats_q(0)
    r.stats_done(0, 2)
    r.each(0, second)
    r.spread(0, lead)
    r.send_a(1, lead[-2])
    r.scattered(1, first, 2)
    r.relay_q(0, 0)
    r.stats_q(1)
    r.arrived(0, 0)
    r.stats_done(1, 2)
    r.each(1, second)
    r.spread(1, lead)
    here = block_ref.at[0, :, r.mine]
    block_p = links.send(here, here, {"p": 1 - r.p})
    links.sent(r.step_q.values())
    backward(0, 0)
    s.send_q(0, 0)
    r.relay_q(1, 0)
    s.send_p(0, 0)
    block_p.wait_recv()
    here = block_ref.at[0, :, r.pair]
    block_q = links.send(here, here, {"q": 1 - r.q})
    r.arrived(1, 0)
    backward(1, 0)
    s.send_q(1, 0)
    order = [(h, k) for h in range(HALVES) for k in lead[:-1]]
    s.send_p(1, 0)
    steps = len(order)
    back_first, back_second = back_math(
        s, grad_ref, proj_ref, inv_ref, gain_ref, grad_res_ref, attn_sum_ref
    )
    for i in range(steps + 3):
        if 0 <= i - 3 < steps:
            s.send_a(*order[i - 3])
        if i == steps + 1:
            s.scattered(0, back_first, 1)
        if 0 <= i - 2 < steps:
            s.send_p(*order[i - 2])
        if 0 <= i - 1 < steps:
            r.relay_q(*order[i - 1])
            r.arrived(*order[i - 1])
            backward(*order[i - 1])
            s.send_q(*order[i - 1])
        if i < steps:
            r.relay_p(*order[i])
    s.stats_q(0)
    for block in range(na):
        weight_grad(out, hidden_ref, down_grad, block)
    columns = slice(0, units)
    down_copies = exchange_b(links, down_grad, down_held, columns)
    s.stats_done(0, 1)
    s.each(0, back_second)
    s.spread(0, lead)
    s.scattered(1, back_first, 1)
    weight_grad(x_ref, grad_gu_ref, gu_grad_ref, 0)
    s.relay_q(0, 0)
    s.stats_q(1)
    weight_grad(x_ref, grad_gu_ref, gu_grad_ref, 1)
    s.stats_done(1, 1)
    s.each(1, back_second)
    s.spread(1, lead)
    weight_grad(x_ref, grad_gu_ref, gu_grad_ref, 2)
    late = [(0, 0)] + order
    for i, (h, k) in enumerate(order):
        s.relay_p(h, k)
        if i == 1:
            weight_grad(x_ref, grad_gu_ref, gu_grad_ref, 3)
        if i:
            s.relay_q(*late[i])
    s.relay_q(1, 0)
    s.relay_q(*order[-1])
    sum_b(down_copies, down_grad, down_held, down_sum_ref, columns)
    for h in range(HALVES):
        for k in range(na):
            s.arrived(h, k)
    block_q.wait_recv()
    links.finish()


def middle_call(nb, x_all, w_mlp, res_mine, grad_mine, proj_mine, inv_mine, width_gain):
    na, rows, width = x_all.shape
    quarter, units = width // 4, w_mlp.shape[1] // 3
    w_rows = width // (na * nb)
    vmem = pl.BlockSpec(memory_space=pltpu.VMEM)
    shape = jax.ShapeDtypeStruct
    outs = (
        shape((1, rows, width), bf16),
        shape((na, rows, width), bf16),
        shape((8, quarter), f32),
        shape((rows, quarter), f32),
        shape((8, quarter), f32),
        shape((na, w_rows, units), bf16),
        shape((na, nb, w_rows, 2 * units), bf16),
    )
    copies = 2 * HALVES * (6 * na + 1) + 2 + nb
    return pl.pallas_call(
        functools.partial(middle_kernel, na, nb),
        out_shape=outs,
        in_specs=[vmem] * 7,
        out_specs=(vmem,) * len(outs),
        scratch_shapes=[
            pltpu.VMEM((na, rows, width), bf16),
            pltpu.VMEM((na, rows, units), bf16),
            pltpu.VMEM((na, rows, 2 * units), bf16),
            pltpu.VMEM((na, rows, 2 * units), f32),
            pltpu.VMEM((na, rows, width), bf16),
            pltpu.VMEM((na, nb, w_rows, units), bf16),
            pltpu.VMEM((nb - 1, na, w_rows, units), bf16),
        ]
        + reduce_scratch(na, rows, width)
        + reduce_scratch(na, rows, width)
        + [pltpu.SemaphoreType.DMA((copies,)), pltpu.SemaphoreType.DMA((copies,))],
        compiler_params=pltpu.CompilerParams(
            collective_id=2, has_side_effects=True, vmem_limit_bytes=VMEM_LIMIT
        ),
        name="middle",
    )(x_all, w_mlp, res_mine, grad_mine, proj_mine, inv_mine, width_gain)


def last_kernel(na, nb, *refs):
    proj_ref, x_ref, qkv_ref, stats_ref, gain_ref, cos_ref, sin_ref, w_ref, att_ref = refs[:9]
    grad_ref, attn_sum_ref, ffn_sum_ref, down_sum_ref, gu_grad_ref = refs[9:14]
    out, sums_ref, down_out, gu_out, qkv_out, wout_out = refs[14:20]
    scaled_ref, grad_qkv_ref, part_ref, head_sums, held, stats_a, inner_ref = refs[20:27]
    own_sums, a_sums, b_sums, gu_held, gu_sum, attn_grad, attn_held, attn_sum = refs[27:35]
    down_in, gu_in, attn_in = refs[35:38]
    scratch, (send_sem, recv_sem) = refs[38:-2], refs[-2:]
    links = Links(send_sem, recv_sem)
    r = Reduce(na, links, part_ref, out, scratch)
    a, b, p, q, mine, pair, quarter = (
        r.a, lax.axis_index("b"), r.p, r.q, r.mine, r.pair, r.quarter,
    )
    units = down_sum_ref.shape[2]
    own_sums[...] = jnp.zeros_like(own_sums)
    own_sums[0:1, mine] = jnp.sum(attn_sum_ref[...], axis=0, keepdims=True)
    own_sums[1:2, mine] = jnp.sum(ffn_sum_ref[...], axis=0, keepdims=True)
    greet(reduce_peers(na) + [{"b": across(b, j)} for j in range(1, nb)])
    far = list(range(2, na)) + [1]

    def to_owners(source, target, columns):
        return [
            (k, links.send(
                source.at[across(a, k), :, columns], target.at[k - 1, :, columns], {"a": across(a, k)}
            ))
            for k in far
        ]

    whole = slice(0, units)
    halves = [slice(0, units), slice(units, 2 * units)]
    down_copies = to_owners(down_sum_ref, down_in, whole)
    gu_b = [exchange_b(links, gu_grad_ref, gu_held, columns) for columns in halves]
    here = own_sums.at[:, mine]
    sums_p = links.send(here, here, {"p": 1 - p})

    held[0] = jnp.zeros_like(held[0])
    head_sums[...] = jnp.zeros_like(head_sums)

    def attend_back(k, carry):
        queries, key_rows, values, q_inv, k_inv, q_rot, k_rot, probs = attention(
            k, qkv_ref[k], stats_ref[...], gain_ref, cos_ref, sin_ref
        )
        cos_table, sine_table = cos_ref[...], sin_ref[...]
        grad_att = dot(proj_ref[k], w_ref[:, 3 * HD :]).astype(bf16)
        grad_v = t_dot(probs.astype(bf16), grad_att)
        grad_p = dot_t(grad_att, values)
        delta = jnp.sum(probs * grad_p, axis=1, keepdims=True)
        grad_scores = (probs * (grad_p - delta) * HD ** (-0.5)).astype(bf16)
        grad_q = dot(grad_scores, k_rot)
        grad_k = t_dot(grad_scores, q_rot)
        grad_q = grad_q * cos_table + rotate_back(grad_q * sine_table)
        grad_k = grad_k * cos_table + rotate_back(grad_k * sine_table)
        head_sums[0:1] += jnp.sum(grad_q * queries * q_inv, axis=0, keepdims=True)
        head_sums[1:2] += jnp.sum(grad_k * key_rows * k_inv, axis=0, keepdims=True)
        scaled_q = grad_q * gain_ref[0:1]
        scaled_k = grad_k * gain_ref[1:2]
        scaled_ref[k, :, :HD] = scaled_q
        scaled_ref[k, :, HD:] = scaled_k
        grad_qkv_ref[k, :, 2 * HD :] = grad_v.astype(bf16)
        held[0] += to_row(scaled_q * queries, 2 * k) + to_row(scaled_k * key_rows, 2 * k + 1)
        return carry

    lax.fori_loop(0, na, attend_back, 0)
    sums_p.wait_recv()
    here = own_sums.at[:, pair]
    sums_q = links.send(here, here, {"q": 1 - q})
    gu_copies = []

    def sent():
        for block in range(na):
            total = None
            for k in range(na):
                term = t_dot(proj_ref[k, :, block * quarter : (block + 1) * quarter], att_ref[k])
                total = term if total is None else total + term
            rows = attn_grad.shape[2]
            for j in range(nb):
                attn_grad[block, j, :, 3 * HD :] = total[j * rows : (j + 1) * rows].astype(bf16)
        sum_b(gu_b[0], gu_grad_ref, gu_held, gu_sum, halves[0])
        gu_copies.append(to_owners(gu_sum, gu_in, halves[0]))

    add_over_heads(links, na, a, p, q, held, stats_a, inner_ref, sent)

    def qkv_back(k, carry):
        for i in range(2):
            at = slice(i * HD, (i + 1) * HD)
            inv = lax.rsqrt(to_column(stats_ref[...] / HQ, 2 * k + i) + epsilon)
            mean = to_column(inner_ref[...] / HQ, 2 * k + i)
            grad = inv * scaled_ref[k, :, at] - qkv_ref[k, :, at] * inv * inv * inv * mean
            grad_qkv_ref[k, :, at] = grad.astype(bf16)
        part_ref[k] = dot_t(grad_qkv_ref[k], w_ref[:, : 3 * HD]).astype(bf16)
        return carry

    for k in r.lead:
        qkv_back(k, 0)
        for h in range(HALVES):
            r.send_q(h, k)
    for h in range(HALVES):
        for k in r.lead:
            r.send_p(h, k)
    for block in range(na):
        total = None
        for k in range(na):
            term = t_dot(x_ref[k, :, block * quarter : (block + 1) * quarter], grad_qkv_ref[k])
            total = term if total is None else total + term
        rows = attn_grad.shape[2]
        for j in range(nb):
            attn_grad[block, j, :, : 3 * HD] = total[j * rows : (j + 1) * rows].astype(bf16)
    attn_columns = slice(0, 4 * HD)
    attn_b = exchange_b(links, attn_grad, attn_held, attn_columns)
    for h in range(HALVES):
        for k in r.lead:
            r.send_a(h, k)
    sums_q.wait_recv()
    sums_a = [
        links.send(own_sums.at[:, span(across(a, k), quarter)], a_sums.at[k - 1], {"a": across(a, k)})
        for k in range(1, na)
    ]
    sum_b(gu_b[1], gu_grad_ref, gu_held, gu_sum, halves[1])
    gu_copies.append(to_owners(gu_sum, gu_in, halves[1]))

    def first(at):
        out[0, at, mine] = (grad_ref[at] + r.add_all(at)).astype(bf16)

    for h in range(HALVES):
        r.scattered(h, first, 0)
        r.spread(h, [0])
    for copy in sums_a:
        copy.wait_recv()
    total = own_sums[:, span(a, quarter)]
    for k in range(1, na):
        total = total + a_sums[k - 1]
    b_sums[0, :, :quarter] = total
    b_sums[0, :, quarter:] = head_sums[...]
    sums_b = [links.send(b_sums.at[0], b_sums.at[j], {"b": across(b, j)}) for j in range(1, nb)]
    for h in range(HALVES):
        r.relay_q(h, 0)
    sum_b(attn_b, attn_grad, attn_held, attn_sum, attn_columns)
    attn_copies = to_owners(attn_sum, attn_in, attn_columns)

    def store(target, index, size, value):
        target[:, span(index, size)] = value.astype(f32)

    store(down_out, a, units, down_sum_ref[a])
    for c in range(2):
        store(gu_out.at[c], a, units, gu_sum[a, :, halves[c]])
    for c in range(3):
        store(qkv_out.at[c], a, HD, attn_sum[a, :, c * HD : (c + 1) * HD])
    store(wout_out, a, HD, attn_sum[a, :, 3 * HD :])
    for k, copy in down_copies:
        copy.wait_recv()
        store(down_out, across(a, k), units, down_in[k - 1])
    for copy in sums_b:
        copy.wait_recv()
    total = b_sums[0]
    for j in range(1, nb):
        total = total + b_sums[j]
    sums_ref[...] = total
    for c in range(2):
        for k, copy in gu_copies[c]:
            copy.wait_recv()
            store(gu_out.at[c], across(a, k), units, gu_in[k - 1, :, halves[c]])
    for k, copy in attn_copies:
        copy.wait_recv()
        for c in range(3):
            store(qkv_out.at[c], across(a, k), HD, attn_in[k - 1, :, c * HD : (c + 1) * HD])
        store(wout_out, across(a, k), HD, attn_in[k - 1, :, 3 * HD :])
    for h in range(HALVES):
        r.arrived(h, 0)
    links.finish()


def last_call(nb, *operands):
    na, rows, width = operands[0].shape
    w_rows, units = operands[12].shape[1:]
    quarter = width // 4
    vmem = pl.BlockSpec(memory_space=pltpu.VMEM)
    shape = jax.ShapeDtypeStruct
    outs = (
        shape((1, rows, width), bf16),
        shape((8, quarter + HD), f32),
        shape((w_rows, na * units), f32),
        shape((2, w_rows, na * units), f32),
        shape((3, w_rows, na * HD), f32),
        shape((w_rows, na * HD), f32),
    )
    copies = HALVES * (3 * na + 1) + 2 + 6 * na + 4 * nb
    return pl.pallas_call(
        functools.partial(last_kernel, na, nb),
        out_shape=outs,
        in_specs=[vmem] * 14,
        out_specs=(vmem,) * len(outs),
        scratch_shapes=[
            pltpu.VMEM((na, rows, 2 * HD), f32),
            pltpu.VMEM((na, rows, 3 * HD), bf16),
            pltpu.VMEM((na, rows, width), bf16),
            pltpu.VMEM((8, HD), f32),
            pltpu.VMEM((5, 8, rows), f32),
            pltpu.VMEM((na - 1, 8, rows), f32),
            pltpu.VMEM((8, rows), f32),
            pltpu.VMEM((8, width), f32),
            pltpu.VMEM((na - 1, 8, quarter), f32),
            pltpu.VMEM((nb, 8, quarter + HD), f32),
            pltpu.VMEM((nb - 1, na, w_rows, 2 * units), bf16),
            pltpu.VMEM((na, w_rows, 2 * units), bf16),
            pltpu.VMEM((na, nb, w_rows, 4 * HD), bf16),
            pltpu.VMEM((nb - 1, na, w_rows, 4 * HD), bf16),
            pltpu.VMEM((na, w_rows, 4 * HD), bf16),
            pltpu.VMEM((na - 1, w_rows, units), bf16),
            pltpu.VMEM((na - 1, w_rows, 2 * units), bf16),
            pltpu.VMEM((na - 1, w_rows, 4 * HD), bf16),
        ]
        + reduce_scratch(na, rows, width)
        + [pltpu.SemaphoreType.DMA((copies,)), pltpu.SemaphoreType.DMA((copies,))],
        compiler_params=pltpu.CompilerParams(
            collective_id=4, has_side_effects=True, vmem_limit_bytes=VMEM_LIMIT
        ),
        name="last",
    )(*operands)


def reduce_scratch(na, rows, width):
    quarter = width // 4
    return [
        pltpu.VMEM((na, rows, width // 2), bf16),
        pltpu.VMEM((na, rows, width // 2), bf16),
        pltpu.VMEM((na, rows, quarter), bf16),
        pltpu.VMEM((na - 1, rows, quarter), bf16),
        pltpu.VMEM((na - 1, rows, quarter), bf16),
        pltpu.VMEM((rows, quarter), f32),
        pltpu.VMEM((2, rows, 128), f32),
        pltpu.VMEM((2, rows, 128), f32),
        pltpu.VMEM((HALVES, 4, 8, rows // HALVES), f32),
    ]


def enter_kernel(na, nb, *refs):
    tok_ref, qkv_w_ref, wout_ref, gu_ref, down_ref, cos_ref, sin_ref = refs[:7]
    gain_refs = refs[7:11]
    x_ref, w_ref, mlp_w_ref, width_gain_ref, head_gain_ref, qkv_ref, stats_ref, att_ref = refs[11:19]
    out, proj_ref, inv_ref, res_ref = refs[19:23]
    own_gains, gains_ref, piece_ref, part_ref, held, stats_a = refs[23:29]
    scratch, (local_sem, send_sem, recv_sem) = refs[29:-3], refs[-3:]
    a, b, p, q = (lax.axis_index(axis) for axis in ("a", "b", "p", "q"))
    rows = wout_ref.shape[0]
    quarter = tok_ref.shape[1]
    units = down_ref.shape[1] // na
    own_gains[...] = jnp.zeros_like(own_gains)
    for i, ref in enumerate(gain_refs):
        own_gains[i : i + 1, : ref.shape[1]] = ref[...].astype(f32)
    gains_ref[a, b] = own_gains[...]
    greet(
        [{"q": 1 - q}, {"p": 1 - p}]
        + [{"a": across(a, k)} for k in range(1, na)]
        + [{"b": across(b, j)} for j in range(1, nb)]
    )
    links = Links(send_sem, recv_sem)
    mine, pair = span(2 * q + p, quarter), span(q, 2 * quarter)
    place = span(a * nb + b, rows)

    gains_a = [
        links.send(own_gains, gains_ref.at[a, b], {"a": across(a, k)}) for k in range(1, na)
    ]
    locals_ = [pltpu.make_async_copy(tok_ref, x_ref.at[0, :, mine], local_sem.at[0])]
    arrive, first = {}, {}
    for k in list(range(1, na)) + [0]:
        block = span(across(a, k), HD)
        sources = [qkv_w_ref.at[c, :, block] for c in range(3)] + [wout_ref.at[:, block]]
        for c, source in enumerate(sources):
            target = w_ref.at[place, c * HD : (c + 1) * HD]
            if k:
                arrive[k, c] = links.send(source, target, {"a": across(a, k)})
            else:
                locals_.append(pltpu.make_async_copy(source, target, local_sem.at[1 + c]))
        if k:
            first[k] = links.send(tok_ref, x_ref.at[k, :, mine], {"a": across(a, k)})
    for copy in locals_:
        copy.start()
    for copy in locals_:
        copy.wait()
    ends, second = [], {}

    def forward(k):
        at = w_ref.at[span(across(a, k) * nb + b, rows), :]
        for j in range(1, nb):
            ends.append(links.send(at, at, {"b": across(b, j)}))
        at = x_ref.at[k, :, mine]
        second[k] = links.send(at, at, {"p": 1 - p})

    forward(0)

    for k in range(na):
        block = span(across(a, k), units)

        def cut(i, carry, k=k, block=block):
            at = pl.ds(pl.multiple_of(i * TILE, TILE), TILE)
            cuts = (gu_ref[at, 0, block], gu_ref[at, 1, block], down_ref[at, block])
            for c in range(3):
                if k:
                    piece_ref[k - 1, c, at] = cuts[c]
                else:
                    to = pl.ds(pl.multiple_of((a * nb + b) * rows + i * TILE, TILE), TILE)
                    mlp_w_ref[to, c * units : (c + 1) * units] = cuts[c]
            return carry

        lax.fori_loop(0, rows // TILE, cut, 0)
    mlp_copies, mlp_ends = {}, []

    def queue(c):
        for k in list(range(2, na)) + [1]:
            target = mlp_w_ref.at[place, c * units : (c + 1) * units]
            mlp_copies[k, c] = links.send(piece_ref.at[k - 1, c], target, {"a": across(a, k)})

    def relay(c, k):
        if k:
            mlp_copies[k, c].wait_recv()
        at = mlp_w_ref.at[span(across(a, k) * nb + b, rows), c * units : (c + 1) * units]
        for j in range(1, nb):
            mlp_ends.append(links.send(at, at, {"b": across(b, j)}))

    queue(0)
    for copy in gains_a:
        copy.wait_recv()
    at = gains_ref.at[:, b]
    for j in range(1, nb):
        ends.append(links.send(at, at, {"b": across(b, j)}))
    for k in range(1, na):
        for c in range(4):
            arrive[k, c].wait_recv()
        first[k].wait_recv()
        forward(k)
    for c in range(3):
        relay(c, 0)
    for k in range(na):
        second[k].wait_recv()
        at = x_ref.at[k, :, pair]
        ends.append(links.send(at, at, {"q": 1 - q}))
    for copy in ends:
        copy.wait_recv()

    n_d, n_h = gain_refs[0].shape[1], gain_refs[2].shape[1]
    width_gain_ref[...] = jnp.zeros_like(width_gain_ref)
    head_gain_ref[...] = jnp.zeros_like(head_gain_ref)
    for i in range(2):
        width_gain_ref[i : i + 1] = jnp.concatenate(
            [gains_ref[2 * q + p, j, i : i + 1, :n_d] for j in range(nb)], axis=1
        )
        head_gain_ref[i : i + 1] = jnp.concatenate(
            [gains_ref[a, j, i + 2 : i + 3, :n_h] for j in range(nb)], axis=1
        )

    held[0] = jnp.zeros_like(held[0])

    def project(k, carry):
        proj = dot(x_ref[k], w_ref[:, : 3 * HD])
        qkv_ref[k] = proj
        queries, key_rows = proj[:, :HD], proj[:, HD : 2 * HD]
        held[0] += to_row(queries * queries, 2 * k) + to_row(key_rows * key_rows, 2 * k + 1)
        return carry

    lax.fori_loop(0, na, project, 0)
    add_over_heads(links, na, a, p, q, held, stats_a, stats_ref, lambda: queue(1))
    for k in range(1, na):
        relay(0, k)

    def attend(k, carry):
        values, probs = (
            attention(k, qkv_ref[k], stats_ref[...], head_gain_ref, cos_ref, sin_ref)[i] for i in (2, 7)
        )
        attended = dot(probs.astype(bf16), values).astype(bf16)
        att_ref[k] = attended
        part_ref[k] = dot_t(attended, w_ref[:, 3 * HD :]).astype(bf16)
        return carry

    lax.fori_loop(0, na, attend, 0)

    r = Reduce(na, links, part_ref, out, scratch)
    for h in range(HALVES):
        for k in r.lead:
            r.send_q(h, k)
    for h in range(HALVES):
        for k in r.lead:
            r.send_p(h, k)
    for h in range(HALVES):
        for k in r.lead:
            r.send_a(h, k)
    for k in range(1, na):
        relay(1, k)
    attn_first, attn_second = attn_math(r, tok_ref, width_gain_ref, proj_ref, inv_ref, res_ref)
    for h in range(HALVES):
        r.scattered(h, attn_first, 1)
        r.stats_q(h)
        r.stats_done(h, 1)
        r.each(h, attn_second)
        r.spread(h, range(na))
    queue(2)
    for h in range(HALVES):
        for k in range(na):
            r.relay_p(h, k)
    for h in range(HALVES):
        for k in range(na):
            r.relay_q(h, k)
    for h in range(HALVES):
        for k in range(na):
            r.arrived(h, k)
    for k in range(1, na):
        relay(2, k)
    for copy in mlp_ends:
        copy.wait_recv()
    links.finish()


def enter_call(na, nb, tok_mine, qkv, w_out, gu, down, cos_table, sine_table, gains):
    rows, quarter = tok_mine.shape
    width = 4 * quarter
    w_rows, units = down.shape[0], down.shape[1] // na
    lanes = max(128, gains[0].shape[1])
    vmem = pl.BlockSpec(memory_space=pltpu.VMEM)
    shape = jax.ShapeDtypeStruct
    full = shape((na, rows, width), bf16)
    outs = [
        full,
        shape((width, 4 * HD), bf16),
        shape((width, 3 * units), bf16),
        shape((8, quarter), f32),
        shape((8, HD), f32),
        shape((na, rows, 3 * HD), f32),
        shape((8, rows), f32),
        shape((na, rows, HD), bf16),
        full,
        shape((rows, quarter), f32),
        shape((rows, 128), f32),
        shape((rows, quarter), f32),
    ]
    copies = 90 + 16 * nb
    return pl.pallas_call(
        functools.partial(enter_kernel, na, nb),
        out_shape=tuple(outs),
        in_specs=[vmem] * 11,
        out_specs=(vmem,) * len(outs),
        scratch_shapes=[
            pltpu.VMEM((8, lanes), f32),
            pltpu.VMEM((na, nb, 8, lanes), f32),
            pltpu.VMEM((na - 1, 3, w_rows, units), bf16),
            pltpu.VMEM((na, rows, width), bf16),
            pltpu.VMEM((5, 8, rows), f32),
            pltpu.VMEM((na - 1, 8, rows), f32),
        ]
        + reduce_scratch(na, rows, width)
        + [
            pltpu.SemaphoreType.DMA((5,)),
            pltpu.SemaphoreType.DMA((copies,)),
            pltpu.SemaphoreType.DMA((copies,)),
        ],
        compiler_params=pltpu.CompilerParams(
            collective_id=5, has_side_effects=True, vmem_limit_bytes=VMEM_LIMIT
        ),
        name="enter",
    )(tok_mine, qkv, w_out, gu, down, cos_table, sine_table, *gains)


def add_over_heads(links, na, a, p, q, held, from_a, out_ref, sent=None):
    links.send(held.at[0], held.at[1], {"p": 1 - p}).wait_recv()
    held[2] = held[0] + held[1]
    links.send(held.at[2], held.at[3], {"q": 1 - q}).wait_recv()
    held[4] = held[2] + held[3]
    copies = [links.send(held.at[4], from_a.at[k - 1], {"a": across(a, k)}) for k in range(1, na)]
    if sent is not None:
        sent()
    for copy in copies:
        copy.wait_recv()
    for k in range(na):
        for i in range(2):
            at = 2 * k + i
            total = held[4, at : at + 1]
            for j in range(1, na):
                other = 2 * (k ^ j) + i
                total = total + from_a[j - 1, other : other + 1]
            out_ref[at : at + 1] = total


def rope_tables(length, width):
    half_width = width // 2
    inv_freq = rope_base ** (-(jnp.arange(half_width, dtype=f32) * 2.0) / width)
    angles = jnp.arange(length, dtype=f32)[:, None] * inv_freq[None, :]
    cos_table = jnp.concatenate([jnp.cos(angles), jnp.cos(angles)], axis=1)
    sine_table = jnp.concatenate([jnp.sin(angles), jnp.sin(angles)], axis=1)
    return cos_table, sine_table


def on_device(
    tokens,
    qkv_weight,
    out_weight,
    gu_weight,
    down_weight,
    attn_gain,
    ffn_gain,
    q_gain,
    k_gain,
    out_grad,
):
    na, nb = lax.axis_size("a"), lax.axis_size("b")
    a, b = lax.axis_index("a"), lax.axis_index("b")
    share = lax.axis_index("q") * 2 + lax.axis_index("p")
    rows, width = tokens.shape
    quarter = width // 4
    w_rows = out_weight.shape[0]
    units = down_weight.shape[1] // na

    def quarter_of(operand):
        return lax.dynamic_slice_in_dim(operand, share * quarter, quarter, 1)

    tok_mine, grad_mine = quarter_of(tokens), quarter_of(out_grad)
    cos_table, sine_table = rope_tables(SEQ_LEN, HD)
    (
        x_all,
        w_attn,
        w_mlp,
        width_gain,
        head_gain,
        qkv,
        stats,
        attended,
        res_all,
        proj_mine,
        inv_mine,
        res_mine,
    ) = enter_call(
        na,
        nb,
        tok_mine,
        qkv_weight.transpose(1, 0, 2),
        out_weight,
        gu_weight,
        down_weight,
        cos_table,
        sine_table,
        [gain[None] for gain in (attn_gain, ffn_gain, q_gain, k_gain)],
    )
    n_d, n_h = attn_gain.shape[0], q_gain.shape[0]
    block_rows, grad_proj, ffn_sums, grad_res, attn_sums, down_sum, gu_grad = middle_call(
        nb, res_all, w_mlp, res_mine, grad_mine, proj_mine, inv_mine, width_gain
    )
    grad_rows, sums, down_grad, gu_grad, qkv_grad, out_grad_w = last_call(
        nb,
        grad_proj,
        x_all,
        qkv,
        stats,
        head_gain,
        cos_table,
        sine_table,
        w_attn,
        attended,
        grad_res,
        attn_sums,
        ffn_sums,
        down_sum,
        gu_grad,
    )
    width_sums = lax.dynamic_slice_in_dim(sums[:2, :quarter], b * n_d, n_d, 1)
    head_sums = lax.dynamic_slice_in_dim(sums[:2, quarter:], b * n_h, n_h, 1)
    return (
        block_rows[0].astype(f32),
        grad_rows[0].astype(f32),
        qkv_grad.transpose(1, 0, 2),
        out_grad_w,
        gu_grad.transpose(1, 0, 2),
        down_grad,
        width_sums[0],
        width_sums[1],
        head_sums[0],
        head_sums[1],
    )


def solution(mesh):
    dp, tp = mesh.shape["dp"], mesh.shape["tensor"]
    na = HEADS // tp
    fine = Mesh(mesh.devices.reshape(na, dp // na, tp // 2, 2), ("a", "b", "p", "q"))
    dp_axes, tp_axes = ("a", "b"), ("p", "q")
    both = tp_axes + dp_axes
    return jax.shard_map(
        on_device,
        mesh=fine,
        in_specs=(
            P(dp_axes, None),
            P(dp_axes, None, tp_axes),
            P(dp_axes, tp_axes),
            P(dp_axes, None, tp_axes),
            P(dp_axes, tp_axes),
            P(dp_axes),
            P(dp_axes),
            P(both),
            P(both),
            P(dp_axes, None),
        ),
        out_specs=(
            P(dp_axes, None),
            P(dp_axes, None),
            P(dp_axes, None, tp_axes),
            P(dp_axes, tp_axes),
            P(dp_axes, None, tp_axes),
            P(dp_axes, tp_axes),
            P(dp_axes),
            P(dp_axes),
            P(both),
            P(both),
        ),
        check_vma=False,
    )
```

```python
import functools

import jax
import jax.numpy as jnp
from jax import lax
from jax.experimental import pallas as pl
from jax.experimental.pallas import tpu as pltpu
from jax.sharding import Mesh, PartitionSpec as P

HEADS = 16
HD = 128
SEQ_LEN = 256
HQ = 2048

epsilon = 1e-06
rope_base = 500000.0

f32 = jnp.float32
bf16 = jnp.bfloat16
MESH = pl.DeviceIdType.MESH
EXACT = lax.Precision.HIGHEST
VMEM_LIMIT = 60 * 1024 * 1024
TILE = 64
HALVES = 2


def flip(index, bit):
    return index + bit - 2 * bit * ((index // bit) % 2)


def across(index, k):
    bit = 1
    while bit <= k:
        if k & bit:
            index = flip(index, bit)
        bit *= 2
    return index


def swap(operand, axis, k=1):
    n = lax.axis_size(axis)
    return lax.ppermute(operand, axis, [(i, i ^ k) for i in range(n)])


def pick(operand, index, axis):
    return lax.dynamic_index_in_dim(operand, index, axis, keepdims=False)


def span(index, size):
    return pl.ds(pl.multiple_of(index * size, size), size)


class Links:
    def __init__(self, send_sem, recv_sem):
        self.send_sem, self.recv_sem, self.count, self.copies = send_sem, recv_sem, 0, []

    def send(self, source, target, device):
        copy = pltpu.make_async_remote_copy(
            src_ref=source,
            dst_ref=target,
            send_sem=self.send_sem.at[self.count],
            recv_sem=self.recv_sem.at[self.count],
            device_id=device,
            device_id_type=MESH,
        )
        copy.start()
        self.count += 1
        self.copies.append(copy)
        return copy

    def sent(self, copies):
        done = [id(copy) for copy in copies]
        for copy in self.copies:
            if id(copy) in done:
                copy.wait_send()
        self.copies = [copy for copy in self.copies if id(copy) not in done]

    def finish(self):
        for copy in self.copies:
            copy.wait_send()


def greet(peers):
    barrier = pltpu.get_barrier_semaphore()
    for peer in peers:
        pl.semaphore_signal(barrier, inc=1, device_id=peer, device_id_type=MESH)
    pl.semaphore_wait(barrier, len(peers))


def fold(block):
    total = block[:, :128]
    for i in range(1, block.shape[1] // 128):
        total = total + block[:, i * 128 : (i + 1) * 128]
    return total


def wide(column, width):
    return jnp.concatenate([column] * (width // 128), axis=1)


def row_mask(row):
    return (lax.broadcasted_iota(jnp.int32, (8, 128), 0) == row).astype(f32)


def to_row(block, row):
    return lax.dot_general(
        row_mask(row), block, (((1,), (1,)), ((), ())), precision=EXACT, preferred_element_type=f32
    )


def to_column(stats, row):
    return lax.dot_general(
        stats, row_mask(row), (((0,), (0,)), ((), ())), precision=EXACT, preferred_element_type=f32
    )


def dot(left, right):
    return jnp.dot(left, right, preferred_element_type=f32)


def dot_t(left, right):
    return lax.dot_general(left, right, (((1,), (1,)), ((), ())), preferred_element_type=f32)


def t_dot(left, right):
    return lax.dot_general(left, right, (((0,), (0,)), ((), ())), preferred_element_type=f32)


def rotate(operand):
    half = HD // 2
    return jnp.concatenate([-operand[:, half:], operand[:, :half]], axis=1)


def rotate_back(operand):
    half = HD // 2
    return jnp.concatenate([operand[:, half:], -operand[:, :half]], axis=1)


def attention(k, qkv, stats, gain_ref, cos_ref, sin_ref):
    stats = stats / HQ
    q_inv = lax.rsqrt(to_column(stats, 2 * k) + epsilon)
    k_inv = lax.rsqrt(to_column(stats, 2 * k + 1) + epsilon)
    queries, key_rows = qkv[:, :HD], qkv[:, HD : 2 * HD]
    values = qkv[:, 2 * HD :].astype(bf16)
    cos_table, sine_table = cos_ref[...], sin_ref[...]
    q_normed = queries * q_inv * gain_ref[0:1]
    k_normed = key_rows * k_inv * gain_ref[1:2]
    q_rot = (q_normed * cos_table + rotate(q_normed) * sine_table).astype(bf16)
    k_rot = (k_normed * cos_table + rotate(k_normed) * sine_table).astype(bf16)
    scores = dot_t(q_rot, k_rot) * HD ** (-0.5)
    ahead = lax.broadcasted_iota(jnp.int32, scores.shape, 1) > lax.broadcasted_iota(
        jnp.int32, scores.shape, 0
    )
    scores = jnp.where(ahead, -1e30, scores)
    shifted = jnp.exp(scores - jnp.max(scores, axis=1, keepdims=True))
    probs = shifted / jnp.sum(shifted, axis=1, keepdims=True)
    return queries, key_rows, values, q_inv, k_inv, q_rot, k_rot, probs


def weight_grad(left, right, out, block):
    na, nb = left.shape[0], out.shape[1]
    rows = out.shape[2]
    total = None
    for k in range(na):
        term = t_dot(left[k, :, block * nb * rows : (block + 1) * nb * rows], right[k])
        total = term if total is None else total + term
    for j in range(nb):
        out[block, j] = total[j * rows : (j + 1) * rows].astype(bf16)


def exchange_b(links, grad, held, columns):
    b = lax.axis_index("b")
    return [
        links.send(
            grad.at[:, across(b, j), :, columns], held.at[j - 1, :, :, columns], {"b": across(b, j)}
        )
        for j in range(1, held.shape[0] + 1)
    ]


def sum_b(copies, grad, held, out, columns):
    b = lax.axis_index("b")
    for copy in copies:
        copy.wait_recv()

    def add(block, carry):
        total = grad[block, b, :, columns].astype(f32)
        for j in range(held.shape[0]):
            total = total + held[j, block, :, columns].astype(f32)
        out[block, :, columns] = total.astype(bf16)
        return carry

    lax.fori_loop(0, grad.shape[0], add, 0)


class Reduce:
    def __init__(self, na, links, part, out, scratch):
        self.na, self.links, self.part, self.out = na, links, part, out
        self.from_q, self.half_sum, self.from_p, self.to_a, self.from_a = scratch[:5]
        self.total, self.parts, self.cols, self.stat = scratch[5:9]
        self.a, self.p, self.q = (lax.axis_index(axis) for axis in ("a", "p", "q"))
        self.rows, self.width = out.shape[1:]
        self.quarter, self.half = self.width // 4, self.width // 2
        self.count = self.rows // HALVES
        self.mine, self.pair = span(2 * self.q + self.p, self.quarter), span(self.q, self.half)
        self.lead = list(range(2, na)) + [1, 0]
        self.step_q, self.step_p, self.step_a = {}, {}, {}
        self.spread_a, self.spread_p, self.spread_q, self.stats = {}, {}, {}, {}

    def at(self, h):
        return slice(h * self.count, (h + 1) * self.count)

    def each(self, h, body):
        def step(i, carry):
            body(pl.ds(pl.multiple_of(h * self.count + i * TILE, TILE), TILE))
            return carry

        lax.fori_loop(0, self.count // TILE, step, 0)

    def send_q(self, h, k):
        at, q = self.at(h), self.q
        source = self.part.at[k, at, span(1 - q, self.half)]
        self.step_q[h, k] = self.links.send(source, self.from_q.at[k, at], {"q": 1 - q})

    def send_p(self, h, k):
        self.step_q[h, k].wait_recv()

        def add(at):
            own = self.part[k, at, span(self.q, self.half)].astype(f32)
            self.half_sum[k, at] = (own + self.from_q[k, at].astype(f32)).astype(bf16)

        self.each(h, add)
        at, p = self.at(h), self.p
        source = self.half_sum.at[k, at, span(1 - p, self.quarter)]
        self.step_p[h, k] = self.links.send(source, self.from_p.at[k, at], {"p": 1 - p})

    def send_a(self, h, k):
        if not k:
            return
        self.step_p[h, k].wait_recv()

        def add(at):
            own = self.half_sum[k, at, span(self.p, self.quarter)].astype(f32)
            self.to_a[k - 1, at] = (own + self.from_p[k, at].astype(f32)).astype(bf16)

        self.each(h, add)
        at = self.at(h)
        self.step_a[h, k] = self.links.send(
            self.to_a.at[k - 1, at], self.from_a.at[k - 1, at], {"a": across(self.a, k)}
        )

    def add_all(self, at):
        own = self.half_sum[0, at, span(self.p, self.quarter)].astype(f32)
        own = own + self.from_p[0, at].astype(f32)
        for k in range(1, self.na):
            own = own + self.from_a[k - 1, at].astype(f32)
        return own

    def scattered(self, h, first, number):
        self.step_p[h, 0].wait_recv()
        for k in range(1, self.na):
            self.step_a[h, k].wait_recv()
        self.each(h, first)
        if number:
            at = self.at(h)
            stats = to_row(self.parts[0, at], 0)
            if number == 2:
                stats = stats + to_row(self.parts[1, at], 1)
            stat = self.stat
            stat[h, 0] = stats
            self.stats[h] = self.links.send(stat.at[h, 0], stat.at[h, 1], {"p": 1 - self.p})

    def stats_q(self, h):
        stat = self.stat
        self.stats[h].wait_recv()
        stat[h, 2] = stat[h, 0] + stat[h, 1]
        self.stats[h] = self.links.send(stat.at[h, 2], stat.at[h, 3], {"q": 1 - self.q})

    def stats_done(self, h, number):
        stat = self.stat
        self.stats[h].wait_recv()
        stats = (stat[h, 2] + stat[h, 3]) / self.width
        for i in range(number):
            self.cols[i, self.at(h)] = to_column(stats, i)

    def spread(self, h, blocks):
        here = self.out.at[0, self.at(h), self.mine]
        for k in blocks:
            if k:
                target = self.out.at[k, self.at(h), self.mine]
                self.spread_a[h, k] = self.links.send(here, target, {"a": across(self.a, k)})
        self.spread_p[h, 0] = self.links.send(here, here, {"p": 1 - self.p})

    def relay_p(self, h, k):
        if not k:
            return
        self.spread_a[h, k].wait_recv()
        here = self.out.at[k, self.at(h), self.mine]
        self.spread_p[h, k] = self.links.send(here, here, {"p": 1 - self.p})

    def relay_q(self, h, k):
        self.spread_p[h, k].wait_recv()
        here = self.out.at[k, self.at(h), self.pair]
        self.spread_q[h, k] = self.links.send(here, here, {"q": 1 - self.q})

    def arrived(self, h, k):
        self.spread_q[h, k].wait_recv()

    def steps(self, first, second, number):
        def normed(h):
            self.stats_done(h, number)
            self.each(h, second)

        def spread_own(h):
            here = self.out.at[0, self.at(h), self.mine]
            self.spread_p[h, 0] = self.links.send(here, here, {"p": 1 - self.p})

        def spread_far(h, k):
            here = self.out.at[0, self.at(h), self.mine]
            target = self.out.at[k, self.at(h), self.mine]
            self.spread_a[h, k] = self.links.send(here, target, {"a": across(self.a, k)})

        return {
            "P": self.send_p,
            "A": self.send_a,
            "SC": lambda h: self.scattered(h, first, number),
            "SQ": self.stats_q,
            "SD": normed,
            "X": spread_own,
            "Z": spread_far,
            "RP": self.relay_p,
            "RQ": self.relay_q,
        }


def reduce_peers(na):
    a, p, q = lax.axis_index("a"), lax.axis_index("p"), lax.axis_index("q")
    return [{"q": 1 - q}, {"p": 1 - p}] + [{"a": across(a, k)} for k in range(1, na)]


def attn_math(r, tok_ref, gain_ref, proj_ref, inv_ref, res_ref):
    def first(at):
        own = r.add_all(at)
        proj_ref[at] = own
        r.parts[0, at] = fold(own * own)

    def second(at):
        own = proj_ref[at]
        inv = lax.rsqrt(r.cols[0, at] + epsilon)
        inv_ref[at] = inv
        residual = tok_ref[at].astype(f32) + own * wide(inv, r.quarter) * gain_ref[0:1]
        res_ref[at] = residual
        r.out[0, at, r.mine] = residual.astype(bf16)

    return first, second


def mlp_math(r, res_ref, grad_ref, gain_ref, block_ref, sum_ref):
    def first(at):
        own = r.add_all(at)
        r.total[at] = own
        r.parts[0, at] = fold(own * own)
        r.parts[1, at] = fold(grad_ref[at] * gain_ref[1:2] * own)

    def second(at):
        own = r.total[at]
        inv = wide(lax.rsqrt(r.cols[0, at] + epsilon), r.quarter)
        upstream = grad_ref[at]
        scaled = upstream * gain_ref[1:2]
        normed = own * inv
        block_ref[0, at, r.mine] = (res_ref[at] + normed * gain_ref[1:2]).astype(bf16)
        gains = upstream * normed
        sum_ref[...] += jnp.sum(gains.reshape(TILE // 8, 8, r.quarter), axis=0)
        grad = inv * scaled - own * inv * inv * inv * wide(r.cols[1, at], r.quarter)
        r.out[0, at, r.mine] = grad.astype(bf16)

    return first, second


def back_math(r, grad_ref, proj_ref, inv_ref, gain_ref, res_ref, sum_ref):
    def first(at):
        grad = grad_ref[at] + r.add_all(at)
        res_ref[at] = grad
        r.parts[0, at] = fold(grad * gain_ref[0:1] * proj_ref[at])

    def second(at):
        own = proj_ref[at]
        inv = wide(inv_ref[at], r.quarter)
        upstream = res_ref[at]
        gains = upstream * own * inv
        sum_ref[...] += jnp.sum(gains.reshape(TILE // 8, 8, r.quarter), axis=0)
        grad = inv * (upstream * gain_ref[0:1])
        grad = grad - own * inv * inv * inv * wide(r.cols[0, at], r.quarter)
        r.out[0, at, r.mine] = grad.astype(bf16)

    return first, second


MIDDLE = (
    ("F", 1), ("F", 2), ("rP", 0, 1), ("F", 3), ("rP", 0, 2), ("rA", 0, 1), ("rP", 0, 3), ("rP", 1, 1),
    ("rP", 1, 3), ("rA", 0, 2), ("F", 0), ("rA", 0, 3), ("rA", 1, 1), ("rA", 1, 3), ("rP", 0, 0),
    ("rP", 1, 2), ("rSC", 0), ("rP", 1, 0), ("rSQ", 0), ("rA", 1, 2), ("rSD", 0), ("rZ", 0, 1),
    ("rZ", 0, 2), ("rX", 0), ("rRP", 0, 1), ("rSC", 1), ("rRP", 0, 2), ("rRQ", 0, 1), ("rSQ", 1),
    ("rZ", 0, 3), ("rRQ", 0, 0), ("rRQ", 0, 2), ("rSD", 1), ("rZ", 1, 2), ("B", 0, 2), ("rRP", 0, 3),
    ("sP", 0, 2), ("B", 0, 1), ("sP", 0, 1), ("rZ", 1, 3), ("rRQ", 0, 3), ("rZ", 1, 1), ("B", 0, 0),
    ("rRP", 1, 2), ("B", 0, 3), ("rRP", 1, 3), ("sA", 0, 2), ("rRQ", 1, 2), ("sP", 0, 3), ("B", 1, 2),
    ("rRP", 1, 1), ("rRQ", 1, 3), ("rX", 1), ("sA", 0, 3), ("sP", 1, 2), ("B", 1, 3), ("rRQ", 1, 1),
    ("sA", 0, 1), ("sP", 0, 0), ("rRQ", 1, 0), ("B", 1, 1), ("sA", 1, 2), ("sP", 1, 3), ("B", 1, 0),
    ("sP", 1, 1), ("sSC", 0), ("sA", 1, 3), ("sP", 1, 0), ("sA", 1, 1), ("BP",), ("sSQ", 0), ("sSD", 0),
    ("sZ", 0, 2), ("sX", 0), ("D",), ("sSC", 1), ("sZ", 0, 1), ("sRP", 0, 2), ("sZ", 0, 3), ("G", 3),
    ("sSQ", 1), ("sSD", 1), ("sZ", 1, 2), ("sX", 1), ("sZ", 1, 1), ("G", 1), ("sRP", 0, 3), ("sZ", 1, 3),
    ("G", 0), ("sRP", 0, 1), ("sRP", 1, 2), ("sRQ", 1, 0), ("BQ",), ("sRP", 1, 1), ("sRP", 1, 3),
    ("sRQ", 0, 1), ("sRQ", 1, 2), ("sRQ", 0, 2), ("G", 2), ("sRQ", 0, 3), ("DS",), ("sRQ", 1, 1),
    ("sRQ", 0, 0), ("sRQ", 1, 3),
)


def middle_kernel(na, nb, *refs):
    x_ref, w_ref, res_ref, grad_ref, proj_ref, inv_ref, gain_ref = refs[:7]
    block_ref, back_out, ffn_sum_ref, grad_res_ref, attn_sum_ref, down_sum_ref, gu_grad_ref = refs[7:14]
    out, hidden_ref, grad_gu_ref, gu_ref, part_ref, down_grad, down_held = refs[14:21]
    scratch, (send_sem, recv_sem) = refs[21:-2], refs[-2:]
    units = hidden_ref.shape[2]
    width = x_ref.shape[2]
    b = lax.axis_index("b")
    greet(reduce_peers(na) + [{"b": across(b, j)} for j in range(1, nb)])
    links = Links(send_sem, recv_sem)
    r = Reduce(na, links, part_ref, out, scratch[:9])
    s = Reduce(na, links, part_ref, back_out, scratch[9:])
    ffn_sum_ref[...] = jnp.zeros_like(ffn_sum_ref)
    attn_sum_ref[...] = jnp.zeros_like(attn_sum_ref)
    wide_tile = 512

    def forward(k):
        def gated(n, carry):
            at, up_at = span(n, 256), pl.ds(pl.multiple_of(units + n * 256, 256), 256)
            gate = dot(x_ref[k], w_ref[:, at])
            up = dot(x_ref[k], w_ref[:, up_at])
            gu_ref[k, :, at] = gate
            gu_ref[k, :, up_at] = up
            hidden_ref[k, :, at] = (gate * jax.nn.sigmoid(gate) * up).astype(bf16)
            return carry

        lax.fori_loop(0, units // 256, gated, 0)

        def down(n, carry):
            at = span(n, wide_tile)
            part_ref[k, :, at] = dot_t(hidden_ref[k], w_ref[at, 2 * units :]).astype(bf16)
            return carry

        lax.fori_loop(0, width // wide_tile, down, 0)

    def backward(h, k):
        rows = r.at(h)

        def gated(n, carry):
            at, up_at = span(n, 256), pl.ds(pl.multiple_of(units + n * 256, 256), 256)
            down_at = pl.ds(pl.multiple_of(2 * units + n * 256, 256), 256)
            grad_hidden = dot(out[k, rows], w_ref[:, down_at])
            gate, up = gu_ref[k, rows, at], gu_ref[k, rows, up_at]
            sigmoid = jax.nn.sigmoid(gate)
            active = gate * sigmoid
            grad_gu_ref[k, rows, at] = (
                grad_hidden * up * (sigmoid * (1.0 + gate * (1.0 - sigmoid)))
            ).astype(bf16)
            grad_gu_ref[k, rows, up_at] = (grad_hidden * active).astype(bf16)
            return carry

        lax.fori_loop(0, units // 256, gated, 0)

        def back(n, carry):
            at = span(n, wide_tile)
            part_ref[k, rows, at] = dot_t(
                grad_gu_ref[k, rows], w_ref[at, : 2 * units]
            ).astype(bf16)
            return carry

        lax.fori_loop(0, width // wide_tile, back, 0)

    first, second = mlp_math(r, res_ref, grad_ref, gain_ref, block_ref, ffn_sum_ref)
    back_first, back_second = back_math(
        s, grad_ref, proj_ref, inv_ref, gain_ref, grad_res_ref, attn_sum_ref
    )
    copies, reused = {}, []
    columns = slice(0, units)

    def forward_step(k):
        forward(k)
        for h in range(HALVES):
            r.send_q(h, k)

    def backward_step(h, k):
        if not reused:
            links.sent(r.step_q.values())
            reused.append(True)
        r.arrived(h, k)
        backward(h, k)
        s.send_q(h, k)

    def block_p():
        here = block_ref.at[0, :, r.mine]
        copies["p"] = links.send(here, here, {"p": 1 - r.p})

    def block_q():
        copies["p"].wait_recv()
        here = block_ref.at[0, :, r.pair]
        copies["q"] = links.send(here, here, {"q": 1 - r.q})

    def down_grads():
        for block in range(na):
            weight_grad(out, hidden_ref, down_grad, block)
        copies["b"] = exchange_b(links, down_grad, down_held, columns)

    table = {
        "F": forward_step,
        "B": backward_step,
        "BP": block_p,
        "BQ": block_q,
        "D": down_grads,
        "DS": lambda: sum_b(copies["b"], down_grad, down_held, down_sum_ref, columns),
        "G": lambda block: weight_grad(x_ref, grad_gu_ref, gu_grad_ref, block),
    }
    table.update({"r" + key: step for key, step in r.steps(first, second, 2).items()})
    table.update({"s" + key: step for key, step in s.steps(back_first, back_second, 1).items()})
    for key, *where in MIDDLE:
        table[key](*where)
    for h in range(HALVES):
        for k in range(na):
            s.arrived(h, k)
    copies["q"].wait_recv()
    links.finish()


def middle_call(nb, x_all, w_mlp, res_mine, grad_mine, proj_mine, inv_mine, width_gain):
    na, rows, width = x_all.shape
    quarter, units = width // 4, w_mlp.shape[1] // 3
    w_rows = width // (na * nb)
    vmem = pl.BlockSpec(memory_space=pltpu.VMEM)
    shape = jax.ShapeDtypeStruct
    outs = (
        shape((1, rows, width), bf16),
        shape((na, rows, width), bf16),
        shape((8, quarter), f32),
        shape((rows, quarter), f32),
        shape((8, quarter), f32),
        shape((na, w_rows, units), bf16),
        shape((na, nb, w_rows, 2 * units), bf16),
    )
    copies = 2 * HALVES * (6 * na + 1) + 2 + nb
    return pl.pallas_call(
        functools.partial(middle_kernel, na, nb),
        out_shape=outs,
        in_specs=[vmem] * 7,
        out_specs=(vmem,) * len(outs),
        scratch_shapes=[
            pltpu.VMEM((na, rows, width), bf16),
            pltpu.VMEM((na, rows, units), bf16),
            pltpu.VMEM((na, rows, 2 * units), bf16),
            pltpu.VMEM((na, rows, 2 * units), f32),
            pltpu.VMEM((na, rows, width), bf16),
            pltpu.VMEM((na, nb, w_rows, units), bf16),
            pltpu.VMEM((nb - 1, na, w_rows, units), bf16),
        ]
        + reduce_scratch(na, rows, width)
        + reduce_scratch(na, rows, width)
        + [pltpu.SemaphoreType.DMA((copies,)), pltpu.SemaphoreType.DMA((copies,))],
        compiler_params=pltpu.CompilerParams(
            collective_id=2, has_side_effects=True, vmem_limit_bytes=VMEM_LIMIT
        ),
        name="middle",
    )(x_all, w_mlp, res_mine, grad_mine, proj_mine, inv_mine, width_gain)


def last_kernel(na, nb, *refs):
    proj_ref, x_ref, qkv_ref, stats_ref, gain_ref, cos_ref, sin_ref, w_ref, att_ref = refs[:9]
    grad_ref, attn_sum_ref, ffn_sum_ref, down_sum_ref, gu_grad_ref = refs[9:14]
    out, sums_ref, down_out, gu_out, qkv_out, wout_out = refs[14:20]
    scaled_ref, grad_qkv_ref, part_ref, head_sums, held, stats_a, inner_ref = refs[20:27]
    own_sums, a_sums, b_sums, gu_held, gu_sum, attn_grad, attn_held, attn_sum = refs[27:35]
    down_in, gu_in, attn_in = refs[35:38]
    scratch, (send_sem, recv_sem) = refs[38:-2], refs[-2:]
    links = Links(send_sem, recv_sem)
    r = Reduce(na, links, part_ref, out, scratch)
    a, b, p, q, mine, pair, quarter = (
        r.a, lax.axis_index("b"), r.p, r.q, r.mine, r.pair, r.quarter,
    )
    units = down_sum_ref.shape[2]
    own_sums[...] = jnp.zeros_like(own_sums)
    own_sums[0:1, mine] = jnp.sum(attn_sum_ref[...], axis=0, keepdims=True)
    own_sums[1:2, mine] = jnp.sum(ffn_sum_ref[...], axis=0, keepdims=True)
    greet(reduce_peers(na) + [{"b": across(b, j)} for j in range(1, nb)])
    far = list(range(2, na)) + [1]

    def to_owners(source, target, columns):
        return [
            (k, links.send(
                source.at[across(a, k), :, columns], target.at[k - 1, :, columns], {"a": across(a, k)}
            ))
            for k in far
        ]

    whole = slice(0, units)
    halves = [slice(0, units), slice(units, 2 * units)]
    down_copies = to_owners(down_sum_ref, down_in, whole)
    gu_b = [exchange_b(links, gu_grad_ref, gu_held, columns) for columns in halves]
    here = own_sums.at[:, mine]
    sums_p = links.send(here, here, {"p": 1 - p})

    held[0] = jnp.zeros_like(held[0])
    head_sums[...] = jnp.zeros_like(head_sums)

    def attend_back(k, carry):
        queries, key_rows, values, q_inv, k_inv, q_rot, k_rot, probs = attention(
            k, qkv_ref[k], stats_ref[...], gain_ref, cos_ref, sin_ref
        )
        cos_table, sine_table = cos_ref[...], sin_ref[...]
        grad_att = dot(proj_ref[k], w_ref[:, 3 * HD :]).astype(bf16)
        grad_v = t_dot(probs.astype(bf16), grad_att)
        grad_p = dot_t(grad_att, values)
        delta = jnp.sum(probs * grad_p, axis=1, keepdims=True)
        grad_scores = (probs * (grad_p - delta) * HD ** (-0.5)).astype(bf16)
        grad_q = dot(grad_scores, k_rot)
        grad_k = t_dot(grad_scores, q_rot)
        grad_q = grad_q * cos_table + rotate_back(grad_q * sine_table)
        grad_k = grad_k * cos_table + rotate_back(grad_k * sine_table)
        head_sums[0:1] += jnp.sum(grad_q * queries * q_inv, axis=0, keepdims=True)
        head_sums[1:2] += jnp.sum(grad_k * key_rows * k_inv, axis=0, keepdims=True)
        scaled_q = grad_q * gain_ref[0:1]
        scaled_k = grad_k * gain_ref[1:2]
        scaled_ref[k, :, :HD] = scaled_q
        scaled_ref[k, :, HD:] = scaled_k
        grad_qkv_ref[k, :, 2 * HD :] = grad_v.astype(bf16)
        held[0] += to_row(scaled_q * queries, 2 * k) + to_row(scaled_k * key_rows, 2 * k + 1)
        return carry

    lax.fori_loop(0, na, attend_back, 0)
    sums_p.wait_recv()
    here = own_sums.at[:, pair]
    sums_q = links.send(here, here, {"q": 1 - q})
    gu_copies = []

    def sent():
        for block in range(na):
            total = None
            for k in range(na):
                term = t_dot(proj_ref[k, :, block * quarter : (block + 1) * quarter], att_ref[k])
                total = term if total is None else total + term
            rows = attn_grad.shape[2]
            for j in range(nb):
                attn_grad[block, j, :, 3 * HD :] = total[j * rows : (j + 1) * rows].astype(bf16)
        sum_b(gu_b[0], gu_grad_ref, gu_held, gu_sum, halves[0])
        gu_copies.append(to_owners(gu_sum, gu_in, halves[0]))

    add_over_heads(links, na, a, p, q, held, stats_a, inner_ref, sent)

    def qkv_back(k, carry):
        for i in range(2):
            at = slice(i * HD, (i + 1) * HD)
            inv = lax.rsqrt(to_column(stats_ref[...] / HQ, 2 * k + i) + epsilon)
            mean = to_column(inner_ref[...] / HQ, 2 * k + i)
            grad = inv * scaled_ref[k, :, at] - qkv_ref[k, :, at] * inv * inv * inv * mean
            grad_qkv_ref[k, :, at] = grad.astype(bf16)
        part_ref[k] = dot_t(grad_qkv_ref[k], w_ref[:, : 3 * HD]).astype(bf16)
        return carry

    for k in r.lead:
        qkv_back(k, 0)
        for h in range(HALVES):
            r.send_q(h, k)
    for h in range(HALVES):
        for k in r.lead:
            r.send_p(h, k)
    for block in range(na):
        total = None
        for k in range(na):
            term = t_dot(x_ref[k, :, block * quarter : (block + 1) * quarter], grad_qkv_ref[k])
            total = term if total is None else total + term
        rows = attn_grad.shape[2]
        for j in range(nb):
            attn_grad[block, j, :, : 3 * HD] = total[j * rows : (j + 1) * rows].astype(bf16)
    attn_columns = slice(0, 4 * HD)
    attn_b = exchange_b(links, attn_grad, attn_held, attn_columns)
    for h in range(HALVES):
        for k in r.lead:
            r.send_a(h, k)
    sums_q.wait_recv()
    sums_a = [
        links.send(own_sums.at[:, span(across(a, k), quarter)], a_sums.at[k - 1], {"a": across(a, k)})
        for k in range(1, na)
    ]
    sum_b(gu_b[1], gu_grad_ref, gu_held, gu_sum, halves[1])
    gu_copies.append(to_owners(gu_sum, gu_in, halves[1]))

    def first(at):
        out[0, at, mine] = (grad_ref[at] + r.add_all(at)).astype(bf16)

    for h in range(HALVES):
        r.scattered(h, first, 0)
        r.spread(h, [0])
    for copy in sums_a:
        copy.wait_recv()
    total = own_sums[:, span(a, quarter)]
    for k in range(1, na):
        total = total + a_sums[k - 1]
    b_sums[0, :, :quarter] = total
    b_sums[0, :, quarter:] = head_sums[...]
    sums_b = [links.send(b_sums.at[0], b_sums.at[j], {"b": across(b, j)}) for j in range(1, nb)]
    for h in range(HALVES):
        r.relay_q(h, 0)
    sum_b(attn_b, attn_grad, attn_held, attn_sum, attn_columns)
    attn_copies = to_owners(attn_sum, attn_in, attn_columns)

    def store(target, index, size, value):
        target[:, span(index, size)] = value.astype(f32)

    store(down_out, a, units, down_sum_ref[a])
    for c in range(2):
        store(gu_out.at[c], a, units, gu_sum[a, :, halves[c]])
    for c in range(3):
        store(qkv_out.at[c], a, HD, attn_sum[a, :, c * HD : (c + 1) * HD])
    store(wout_out, a, HD, attn_sum[a, :, 3 * HD :])
    for k, copy in down_copies:
        copy.wait_recv()
        store(down_out, across(a, k), units, down_in[k - 1])
    for copy in sums_b:
        copy.wait_recv()
    total = b_sums[0]
    for j in range(1, nb):
        total = total + b_sums[j]
    sums_ref[...] = total
    for c in range(2):
        for k, copy in gu_copies[c]:
            copy.wait_recv()
            store(gu_out.at[c], across(a, k), units, gu_in[k - 1, :, halves[c]])
    for k, copy in attn_copies:
        copy.wait_recv()
        for c in range(3):
            store(qkv_out.at[c], across(a, k), HD, attn_in[k - 1, :, c * HD : (c + 1) * HD])
        store(wout_out, across(a, k), HD, attn_in[k - 1, :, 3 * HD :])
    for h in range(HALVES):
        r.arrived(h, 0)
    links.finish()


def last_call(nb, *operands):
    na, rows, width = operands[0].shape
    w_rows, units = operands[12].shape[1:]
    quarter = width // 4
    vmem = pl.BlockSpec(memory_space=pltpu.VMEM)
    shape = jax.ShapeDtypeStruct
    outs = (
        shape((1, rows, width), bf16),
        shape((8, quarter + HD), f32),
        shape((w_rows, na * units), f32),
        shape((2, w_rows, na * units), f32),
        shape((3, w_rows, na * HD), f32),
        shape((w_rows, na * HD), f32),
    )
    copies = HALVES * (3 * na + 1) + 2 + 6 * na + 4 * nb
    return pl.pallas_call(
        functools.partial(last_kernel, na, nb),
        out_shape=outs,
        in_specs=[vmem] * 14,
        out_specs=(vmem,) * len(outs),
        scratch_shapes=[
            pltpu.VMEM((na, rows, 2 * HD), f32),
            pltpu.VMEM((na, rows, 3 * HD), bf16),
            pltpu.VMEM((na, rows, width), bf16),
            pltpu.VMEM((8, HD), f32),
            pltpu.VMEM((5, 8, rows), f32),
            pltpu.VMEM((na - 1, 8, rows), f32),
            pltpu.VMEM((8, rows), f32),
            pltpu.VMEM((8, width), f32),
            pltpu.VMEM((na - 1, 8, quarter), f32),
            pltpu.VMEM((nb, 8, quarter + HD), f32),
            pltpu.VMEM((nb - 1, na, w_rows, 2 * units), bf16),
            pltpu.VMEM((na, w_rows, 2 * units), bf16),
            pltpu.VMEM((na, nb, w_rows, 4 * HD), bf16),
            pltpu.VMEM((nb - 1, na, w_rows, 4 * HD), bf16),
            pltpu.VMEM((na, w_rows, 4 * HD), bf16),
            pltpu.VMEM((na - 1, w_rows, units), bf16),
            pltpu.VMEM((na - 1, w_rows, 2 * units), bf16),
            pltpu.VMEM((na - 1, w_rows, 4 * HD), bf16),
        ]
        + reduce_scratch(na, rows, width)
        + [pltpu.SemaphoreType.DMA((copies,)), pltpu.SemaphoreType.DMA((copies,))],
        compiler_params=pltpu.CompilerParams(
            collective_id=4, has_side_effects=True, vmem_limit_bytes=VMEM_LIMIT
        ),
        name="last",
    )(*operands)


def reduce_scratch(na, rows, width):
    quarter = width // 4
    return [
        pltpu.VMEM((na, rows, width // 2), bf16),
        pltpu.VMEM((na, rows, width // 2), bf16),
        pltpu.VMEM((na, rows, quarter), bf16),
        pltpu.VMEM((na - 1, rows, quarter), bf16),
        pltpu.VMEM((na - 1, rows, quarter), bf16),
        pltpu.VMEM((rows, quarter), f32),
        pltpu.VMEM((2, rows, 128), f32),
        pltpu.VMEM((2, rows, 128), f32),
        pltpu.VMEM((HALVES, 4, 8, rows // HALVES), f32),
    ]


def enter_kernel(na, nb, *refs):
    tok_ref, qkv_w_ref, wout_ref, gu_ref, down_ref, cos_ref, sin_ref = refs[:7]
    gain_refs = refs[7:11]
    x_ref, w_ref, mlp_w_ref, width_gain_ref, head_gain_ref, qkv_ref, stats_ref, att_ref = refs[11:19]
    out, proj_ref, inv_ref, res_ref = refs[19:23]
    own_gains, gains_ref, piece_ref, part_ref, held, stats_a = refs[23:29]
    scratch, (local_sem, send_sem, recv_sem) = refs[29:-3], refs[-3:]
    a, b, p, q = (lax.axis_index(axis) for axis in ("a", "b", "p", "q"))
    rows = wout_ref.shape[0]
    quarter = tok_ref.shape[1]
    units = down_ref.shape[1] // na
    own_gains[...] = jnp.zeros_like(own_gains)
    for i, ref in enumerate(gain_refs):
        own_gains[i : i + 1, : ref.shape[1]] = ref[...].astype(f32)
    gains_ref[a, b] = own_gains[...]
    greet(
        [{"q": 1 - q}, {"p": 1 - p}]
        + [{"a": across(a, k)} for k in range(1, na)]
        + [{"b": across(b, j)} for j in range(1, nb)]
    )
    links = Links(send_sem, recv_sem)
    mine, pair = span(2 * q + p, quarter), span(q, 2 * quarter)
    place = span(a * nb + b, rows)

    gains_a = [
        links.send(own_gains, gains_ref.at[a, b], {"a": across(a, k)}) for k in range(1, na)
    ]
    locals_ = [pltpu.make_async_copy(tok_ref, x_ref.at[0, :, mine], local_sem.at[0])]
    arrive, first = {}, {}
    for k in list(range(1, na)) + [0]:
        block = span(across(a, k), HD)
        sources = [qkv_w_ref.at[c, :, block] for c in range(3)] + [wout_ref.at[:, block]]
        for c, source in enumerate(sources):
            target = w_ref.at[place, c * HD : (c + 1) * HD]
            if k:
                arrive[k, c] = links.send(source, target, {"a": across(a, k)})
            else:
                locals_.append(pltpu.make_async_copy(source, target, local_sem.at[1 + c]))
        if k:
            first[k] = links.send(tok_ref, x_ref.at[k, :, mine], {"a": across(a, k)})
    for copy in locals_:
        copy.start()
    for copy in locals_:
        copy.wait()
    ends, second = [], {}

    def forward(k):
        at = w_ref.at[span(across(a, k) * nb + b, rows), :]
        for j in range(1, nb):
            ends.append(links.send(at, at, {"b": across(b, j)}))
        at = x_ref.at[k, :, mine]
        second[k] = links.send(at, at, {"p": 1 - p})

    forward(0)

    for k in range(na):
        block = span(across(a, k), units)

        def cut(i, carry, k=k, block=block):
            at = pl.ds(pl.multiple_of(i * TILE, TILE), TILE)
            cuts = (gu_ref[at, 0, block], gu_ref[at, 1, block], down_ref[at, block])
            for c in range(3):
                if k:
                    piece_ref[k - 1, c, at] = cuts[c]
                else:
                    to = pl.ds(pl.multiple_of((a * nb + b) * rows + i * TILE, TILE), TILE)
                    mlp_w_ref[to, c * units : (c + 1) * units] = cuts[c]
            return carry

        lax.fori_loop(0, rows // TILE, cut, 0)
    mlp_copies, mlp_ends = {}, []

    def queue(c):
        for k in list(range(2, na)) + [1]:
            target = mlp_w_ref.at[place, c * units : (c + 1) * units]
            mlp_copies[k, c] = links.send(piece_ref.at[k - 1, c], target, {"a": across(a, k)})

    def relay(c, k):
        if k:
            mlp_copies[k, c].wait_recv()
        at = mlp_w_ref.at[span(across(a, k) * nb + b, rows), c * units : (c + 1) * units]
        for j in range(1, nb):
            mlp_ends.append(links.send(at, at, {"b": across(b, j)}))

    queue(0)
    for copy in gains_a:
        copy.wait_recv()
    at = gains_ref.at[:, b]
    for j in range(1, nb):
        ends.append(links.send(at, at, {"b": across(b, j)}))
    for k in range(1, na):
        for c in range(4):
            arrive[k, c].wait_recv()
        first[k].wait_recv()
        forward(k)
    for c in range(3):
        relay(c, 0)
    for k in range(na):
        second[k].wait_recv()
        at = x_ref.at[k, :, pair]
        ends.append(links.send(at, at, {"q": 1 - q}))
    for copy in ends:
        copy.wait_recv()

    n_d, n_h = gain_refs[0].shape[1], gain_refs[2].shape[1]
    width_gain_ref[...] = jnp.zeros_like(width_gain_ref)
    head_gain_ref[...] = jnp.zeros_like(head_gain_ref)
    for i in range(2):
        width_gain_ref[i : i + 1] = jnp.concatenate(
            [gains_ref[2 * q + p, j, i : i + 1, :n_d] for j in range(nb)], axis=1
        )
        head_gain_ref[i : i + 1] = jnp.concatenate(
            [gains_ref[a, j, i + 2 : i + 3, :n_h] for j in range(nb)], axis=1
        )

    held[0] = jnp.zeros_like(held[0])

    def project(k, carry):
        proj = dot(x_ref[k], w_ref[:, : 3 * HD])
        qkv_ref[k] = proj
        queries, key_rows = proj[:, :HD], proj[:, HD : 2 * HD]
        held[0] += to_row(queries * queries, 2 * k) + to_row(key_rows * key_rows, 2 * k + 1)
        return carry

    lax.fori_loop(0, na, project, 0)
    add_over_heads(links, na, a, p, q, held, stats_a, stats_ref, lambda: queue(1))
    for k in range(1, na):
        relay(0, k)

    def attend(k, carry):
        values, probs = (
            attention(k, qkv_ref[k], stats_ref[...], head_gain_ref, cos_ref, sin_ref)[i] for i in (2, 7)
        )
        attended = dot(probs.astype(bf16), values).astype(bf16)
        att_ref[k] = attended
        part_ref[k] = dot_t(attended, w_ref[:, 3 * HD :]).astype(bf16)
        return carry

    lax.fori_loop(0, na, attend, 0)

    r = Reduce(na, links, part_ref, out, scratch)
    for h in range(HALVES):
        for k in r.lead:
            r.send_q(h, k)
    for h in range(HALVES):
        for k in r.lead:
            r.send_p(h, k)
    for h in range(HALVES):
        for k in r.lead:
            r.send_a(h, k)
    for k in range(1, na):
        relay(1, k)
    attn_first, attn_second = attn_math(r, tok_ref, width_gain_ref, proj_ref, inv_ref, res_ref)
    for h in range(HALVES):
        r.scattered(h, attn_first, 1)
        r.stats_q(h)
        r.stats_done(h, 1)
        r.each(h, attn_second)
        r.spread(h, range(na))
    queue(2)
    for h in range(HALVES):
        for k in range(na):
            r.relay_p(h, k)
    for h in range(HALVES):
        for k in range(na):
            r.relay_q(h, k)
    for h in range(HALVES):
        for k in range(na):
            r.arrived(h, k)
    for k in range(1, na):
        relay(2, k)
    for copy in mlp_ends:
        copy.wait_recv()
    links.finish()


def enter_call(na, nb, tok_mine, qkv, w_out, gu, down, cos_table, sine_table, gains):
    rows, quarter = tok_mine.shape
    width = 4 * quarter
    w_rows, units = down.shape[0], down.shape[1] // na
    lanes = max(128, gains[0].shape[1])
    vmem = pl.BlockSpec(memory_space=pltpu.VMEM)
    shape = jax.ShapeDtypeStruct
    full = shape((na, rows, width), bf16)
    outs = [
        full,
        shape((width, 4 * HD), bf16),
        shape((width, 3 * units), bf16),
        shape((8, quarter), f32),
        shape((8, HD), f32),
        shape((na, rows, 3 * HD), f32),
        shape((8, rows), f32),
        shape((na, rows, HD), bf16),
        full,
        shape((rows, quarter), f32),
        shape((rows, 128), f32),
        shape((rows, quarter), f32),
    ]
    copies = 90 + 16 * nb
    return pl.pallas_call(
        functools.partial(enter_kernel, na, nb),
        out_shape=tuple(outs),
        in_specs=[vmem] * 11,
        out_specs=(vmem,) * len(outs),
        scratch_shapes=[
            pltpu.VMEM((8, lanes), f32),
            pltpu.VMEM((na, nb, 8, lanes), f32),
            pltpu.VMEM((na - 1, 3, w_rows, units), bf16),
            pltpu.VMEM((na, rows, width), bf16),
            pltpu.VMEM((5, 8, rows), f32),
            pltpu.VMEM((na - 1, 8, rows), f32),
        ]
        + reduce_scratch(na, rows, width)
        + [
            pltpu.SemaphoreType.DMA((5,)),
            pltpu.SemaphoreType.DMA((copies,)),
            pltpu.SemaphoreType.DMA((copies,)),
        ],
        compiler_params=pltpu.CompilerParams(
            collective_id=5, has_side_effects=True, vmem_limit_bytes=VMEM_LIMIT
        ),
        name="enter",
    )(tok_mine, qkv, w_out, gu, down, cos_table, sine_table, *gains)


def add_over_heads(links, na, a, p, q, held, from_a, out_ref, sent=None):
    links.send(held.at[0], held.at[1], {"p": 1 - p}).wait_recv()
    held[2] = held[0] + held[1]
    links.send(held.at[2], held.at[3], {"q": 1 - q}).wait_recv()
    held[4] = held[2] + held[3]
    copies = [links.send(held.at[4], from_a.at[k - 1], {"a": across(a, k)}) for k in range(1, na)]
    if sent is not None:
        sent()
    for copy in copies:
        copy.wait_recv()
    for k in range(na):
        for i in range(2):
            at = 2 * k + i
            total = held[4, at : at + 1]
            for j in range(1, na):
                other = 2 * (k ^ j) + i
                total = total + from_a[j - 1, other : other + 1]
            out_ref[at : at + 1] = total


def rope_tables(length, width):
    half_width = width // 2
    inv_freq = rope_base ** (-(jnp.arange(half_width, dtype=f32) * 2.0) / width)
    angles = jnp.arange(length, dtype=f32)[:, None] * inv_freq[None, :]
    cos_table = jnp.concatenate([jnp.cos(angles), jnp.cos(angles)], axis=1)
    sine_table = jnp.concatenate([jnp.sin(angles), jnp.sin(angles)], axis=1)
    return cos_table, sine_table


def on_device(
    tokens,
    qkv_weight,
    out_weight,
    gu_weight,
    down_weight,
    attn_gain,
    ffn_gain,
    q_gain,
    k_gain,
    out_grad,
):
    na, nb = lax.axis_size("a"), lax.axis_size("b")
    a, b = lax.axis_index("a"), lax.axis_index("b")
    share = lax.axis_index("q") * 2 + lax.axis_index("p")
    rows, width = tokens.shape
    quarter = width // 4
    w_rows = out_weight.shape[0]
    units = down_weight.shape[1] // na

    def quarter_of(operand):
        return lax.dynamic_slice_in_dim(operand, share * quarter, quarter, 1)

    tok_mine, grad_mine = quarter_of(tokens), quarter_of(out_grad)
    cos_table, sine_table = rope_tables(SEQ_LEN, HD)
    (
        x_all,
        w_attn,
        w_mlp,
        width_gain,
        head_gain,
        qkv,
        stats,
        attended,
        res_all,
        proj_mine,
        inv_mine,
        res_mine,
    ) = enter_call(
        na,
        nb,
        tok_mine,
        qkv_weight.transpose(1, 0, 2),
        out_weight,
        gu_weight,
        down_weight,
        cos_table,
        sine_table,
        [gain[None] for gain in (attn_gain, ffn_gain, q_gain, k_gain)],
    )
    n_d, n_h = attn_gain.shape[0], q_gain.shape[0]
    block_rows, grad_proj, ffn_sums, grad_res, attn_sums, down_sum, gu_grad = middle_call(
        nb, res_all, w_mlp, res_mine, grad_mine, proj_mine, inv_mine, width_gain
    )
    grad_rows, sums, down_grad, gu_grad, qkv_grad, out_grad_w = last_call(
        nb,
        grad_proj,
        x_all,
        qkv,
        stats,
        head_gain,
        cos_table,
        sine_table,
        w_attn,
        attended,
        grad_res,
        attn_sums,
        ffn_sums,
        down_sum,
        gu_grad,
    )
    width_sums = lax.dynamic_slice_in_dim(sums[:2, :quarter], b * n_d, n_d, 1)
    head_sums = lax.dynamic_slice_in_dim(sums[:2, quarter:], b * n_h, n_h, 1)
    return (
        block_rows[0].astype(f32),
        grad_rows[0].astype(f32),
        qkv_grad.transpose(1, 0, 2),
        out_grad_w,
        gu_grad.transpose(1, 0, 2),
        down_grad,
        width_sums[0],
        width_sums[1],
        head_sums[0],
        head_sums[1],
    )


def solution(mesh):
    dp, tp = mesh.shape["dp"], mesh.shape["tensor"]
    na = HEADS // tp
    fine = Mesh(mesh.devices.reshape(na, dp // na, tp // 2, 2), ("a", "b", "p", "q"))
    dp_axes, tp_axes = ("a", "b"), ("p", "q")
    both = tp_axes + dp_axes
    return jax.shard_map(
        on_device,
        mesh=fine,
        in_specs=(
            P(dp_axes, None),
            P(dp_axes, None, tp_axes),
            P(dp_axes, tp_axes),
            P(dp_axes, None, tp_axes),
            P(dp_axes, tp_axes),
            P(dp_axes),
            P(dp_axes),
            P(both),
            P(both),
            P(dp_axes, None),
        ),
        out_specs=(
            P(dp_axes, None),
            P(dp_axes, None),
            P(dp_axes, None, tp_axes),
            P(dp_axes, tp_axes),
            P(dp_axes, None, tp_axes),
            P(dp_axes, tp_axes),
            P(dp_axes),
            P(dp_axes),
            P(both),
            P(both),
        ),
        check_vma=False,
    )
```

```python
import functools

import jax
import jax.numpy as jnp
from jax import lax
from jax.experimental import pallas as pl
from jax.experimental.pallas import tpu as pltpu
from jax.sharding import Mesh, PartitionSpec as P

HEADS = 16
HD = 128
SEQ_LEN = 256
HQ = 2048

epsilon = 1e-06
rope_base = 500000.0

f32 = jnp.float32
bf16 = jnp.bfloat16
MESH = pl.DeviceIdType.MESH
EXACT = lax.Precision.HIGHEST
VMEM_LIMIT = 60 * 1024 * 1024
TILE = 64
HALVES = 2


def flip(index, bit):
    return index + bit - 2 * bit * ((index // bit) % 2)


def across(index, k):
    bit = 1
    while bit <= k:
        if k & bit:
            index = flip(index, bit)
        bit *= 2
    return index


def exclusive_or(left, right, count):
    total, bit = 0, 1
    while bit < count:
        total = total + bit * ((left // bit + right // bit) % 2)
        bit *= 2
    return total


def pick(operand, index, axis):
    return lax.dynamic_index_in_dim(operand, index, axis, keepdims=False)


def span(index, size):
    return pl.ds(pl.multiple_of(index * size, size), size)


class Links:
    def __init__(self, send_sem, recv_sem):
        self.send_sem, self.recv_sem, self.count = send_sem, recv_sem, 0
        self.copies, self.lines = [], []

    def send(self, source, target, device):
        copy = self.copy(self.count, source, target, device)
        copy.start()
        self.count += 1
        self.copies.append(copy)
        return copy

    def reserve(self, number):
        self.count += number
        return self.count - number

    def copy(self, index, source, target, device):
        return pltpu.make_async_remote_copy(
            src_ref=source,
            dst_ref=target,
            send_sem=self.send_sem.at[index],
            recv_sem=self.recv_sem.at[index],
            device_id=device,
            device_id_type=MESH,
        )

    def sent(self, copies):
        done = [id(copy) for copy in copies]
        for copy in self.copies:
            if id(copy) in done:
                copy.wait_send()
        self.copies = [copy for copy in self.copies if id(copy) not in done]

    def finish(self):
        for copy in self.copies:
            copy.wait_send()
        for line in self.lines:
            line.finish()


def greet(peers):
    barrier = pltpu.get_barrier_semaphore()
    for peer in peers:
        pl.semaphore_signal(barrier, inc=1, device_id=peer, device_id_type=MESH)
    pl.semaphore_wait(barrier, len(peers))


def fold(block):
    total = block[:, :128]
    for i in range(1, block.shape[1] // 128):
        total = total + block[:, i * 128 : (i + 1) * 128]
    return total


def wide(column, width):
    return jnp.concatenate([column] * (width // 128), axis=1)


def row_mask(row):
    return (lax.broadcasted_iota(jnp.int32, (8, 128), 0) == row).astype(f32)


def to_row(block, row):
    return lax.dot_general(
        row_mask(row), block, (((1,), (1,)), ((), ())), precision=EXACT, preferred_element_type=f32
    )


def to_column(stats, row):
    return lax.dot_general(
        stats, row_mask(row), (((0,), (0,)), ((), ())), precision=EXACT, preferred_element_type=f32
    )


def dot(left, right):
    return jnp.dot(left, right, preferred_element_type=f32)


def dot_t(left, right):
    return lax.dot_general(left, right, (((1,), (1,)), ((), ())), preferred_element_type=f32)


def t_dot(left, right):
    return lax.dot_general(left, right, (((0,), (0,)), ((), ())), preferred_element_type=f32)


def rotate(operand):
    half = HD // 2
    return jnp.concatenate([-operand[:, half:], operand[:, :half]], axis=1)


def rotate_back(operand):
    half = HD // 2
    return jnp.concatenate([operand[:, half:], -operand[:, :half]], axis=1)


def attention(k, qkv, stats, gain_ref, cos_ref, sin_ref):
    stats = stats / HQ
    q_inv = lax.rsqrt(to_column(stats, 2 * k) + epsilon)
    k_inv = lax.rsqrt(to_column(stats, 2 * k + 1) + epsilon)
    queries, key_rows = qkv[:, :HD], qkv[:, HD : 2 * HD]
    values = qkv[:, 2 * HD :].astype(bf16)
    cos_table, sine_table = cos_ref[...], sin_ref[...]
    q_normed = queries * q_inv * gain_ref[0:1]
    k_normed = key_rows * k_inv * gain_ref[1:2]
    q_rot = (q_normed * cos_table + rotate(q_normed) * sine_table).astype(bf16)
    k_rot = (k_normed * cos_table + rotate(k_normed) * sine_table).astype(bf16)
    scores = dot_t(q_rot, k_rot) * HD ** (-0.5)
    ahead = lax.broadcasted_iota(jnp.int32, scores.shape, 1) > lax.broadcasted_iota(
        jnp.int32, scores.shape, 0
    )
    scores = jnp.where(ahead, -1e30, scores)
    shifted = jnp.exp(scores - jnp.max(scores, axis=1, keepdims=True))
    probs = shifted / jnp.sum(shifted, axis=1, keepdims=True)
    return queries, key_rows, values, q_inv, k_inv, q_rot, k_rot, probs


def weight_grad(left, right, out, block, columns=None):
    na, nb, rows = left.shape[0], out.shape[1], out.shape[2]
    columns = columns or slice(0, right.shape[2])
    size = max(rows, 256)

    def chunk(i, carry):
        at = span(block * (nb * rows // size) + i, size)
        total = t_dot(left[0, :, at], right[0])
        for k in range(1, na):
            total = total + t_dot(left[k, :, at], right[k])
        for j in range(size // rows):
            part = total[j * rows : (j + 1) * rows].astype(bf16)
            out[block, i * (size // rows) + j, :, columns] = part
        return carry

    lax.fori_loop(0, nb * rows // size, chunk, 0)


def exchange_b(links, grad, held, columns):
    b = lax.axis_index("b")
    return [
        links.send(
            grad.at[:, across(b, j), :, columns], held.at[j - 1, :, :, columns], {"b": across(b, j)}
        )
        for j in range(1, held.shape[0] + 1)
    ]


def sum_b(copies, grad, held, out, columns):
    b = lax.axis_index("b")
    for copy in copies:
        copy.wait_recv()

    def add(block, carry):
        total = grad[block, b, :, columns].astype(f32)
        for j in range(held.shape[0]):
            total = total + held[j, block, :, columns].astype(f32)
        out[block, :, columns] = total.astype(bf16)
        return carry

    lax.fori_loop(0, grad.shape[0], add, 0)


class Line:
    def __init__(self, links, na, block, own):
        self.links, self.na, self.block, self.own = links, na, block, own
        self.a, self.p = lax.axis_index("a"), lax.axis_index("p")
        self.hop_base = {1: links.reserve(na - 1), -1: links.reserve(na - 1)}
        self.pass_base = links.reserve(na)
        links.lines.append(self)

    def hop(self, way, t):
        a, na = self.a, self.na
        first = a - way * (t - 1)
        source = self.own if t == 1 else self.block(exclusive_or(first, a, na))
        target = self.block(exclusive_or(first, a + way, na))
        return self.links.copy(self.hop_base[way] + t - 1, source, target, {"a": (a + way) % na})

    def sends(self, way, t):
        first, last = self.a - way * (t - 1), self.a + way
        return (first >= 0) & (first < self.na) & (last >= 0) & (last < self.na)

    def to_pair(self, k, source=None):
        at = self.block(k)
        return self.links.copy(self.pass_base + k, at if source is None else source, at, {"p": 1 - self.p})

    def start(self):
        for way in (1, -1):

            @pl.when(self.sends(way, 1))
            def _(way=way):
                self.hop(way, 1).start()

    def pass_on(self, way, t):
        came = self.a - way * t

        @pl.when((came >= 0) & (came < self.na))
        def _():
            self.hop(way, t).wait_recv()
            self.to_pair(exclusive_or(came, self.a, self.na)).start()

        if t < self.na - 1:

            @pl.when(self.sends(way, t + 1))
            def _():
                self.hop(way, t + 1).start()

    def finish(self):
        for way in (1, -1):
            for t in range(1, self.na):

                @pl.when(self.sends(way, t))
                def _(way=way, t=t):
                    self.hop(way, t).wait_send()

        for k in range(self.na):
            self.to_pair(k).wait_send()


class Reduce:
    def __init__(self, na, links, part, out, scratch):
        self.na, self.links, self.part, self.out = na, links, part, out
        self.from_q, self.half_sum, self.from_p, self.to_a, self.from_a = scratch[:5]
        self.total, self.parts, self.cols, self.stat = scratch[5:9]
        self.a, self.p, self.q = (lax.axis_index(axis) for axis in ("a", "p", "q"))
        self.rows, self.width = out.shape[1:]
        self.quarter, self.half = self.width // 4, self.width // 2
        self.count = self.rows // HALVES
        self.mine, self.pair = span(2 * self.q + self.p, self.quarter), span(self.q, self.half)
        self.lead = list(range(2, na)) + [1, 0]
        self.step_q, self.step_p, self.step_a = {}, {}, {}
        self.spread_a, self.spread_p, self.spread_q, self.stats = {}, {}, {}, {}

    def at(self, h):
        return slice(h * self.count, (h + 1) * self.count)

    def each(self, h, body):
        def step(i, carry):
            body(pl.ds(pl.multiple_of(h * self.count + i * TILE, TILE), TILE))
            return carry

        lax.fori_loop(0, self.count // TILE, step, 0)

    def send_q(self, h, k):
        at, q = self.at(h), self.q
        source = self.part.at[k, at, span(1 - q, self.half)]
        self.step_q[h, k] = self.links.send(source, self.from_q.at[k, at], {"q": 1 - q})

    def send_p(self, h, k):
        self.step_q[h, k].wait_recv()

        def add(at):
            own = self.part[k, at, span(self.q, self.half)].astype(f32)
            self.half_sum[k, at] = (own + self.from_q[k, at].astype(f32)).astype(bf16)

        self.each(h, add)
        at, p = self.at(h), self.p
        source = self.half_sum.at[k, at, span(1 - p, self.quarter)]
        self.step_p[h, k] = self.links.send(source, self.from_p.at[k, at], {"p": 1 - p})

    def send_a(self, h, k):
        if not k:
            return
        self.step_p[h, k].wait_recv()

        def add(at):
            own = self.half_sum[k, at, span(self.p, self.quarter)].astype(f32)
            self.to_a[k - 1, at] = (own + self.from_p[k, at].astype(f32)).astype(bf16)

        self.each(h, add)
        at = self.at(h)
        self.step_a[h, k] = self.links.send(
            self.to_a.at[k - 1, at], self.from_a.at[k - 1, at], {"a": across(self.a, k)}
        )

    def add_all(self, at):
        own = self.half_sum[0, at, span(self.p, self.quarter)].astype(f32)
        own = own + self.from_p[0, at].astype(f32)
        for k in range(1, self.na):
            own = own + self.from_a[k - 1, at].astype(f32)
        return own

    def scattered(self, h, first, number):
        self.step_p[h, 0].wait_recv()
        for k in range(1, self.na):
            self.step_a[h, k].wait_recv()
        self.each(h, first)
        if number:
            at = self.at(h)
            stats = to_row(self.parts[0, at], 0)
            if number == 2:
                stats = stats + to_row(self.parts[1, at], 1)
            stat = self.stat
            stat[h, 0] = stats
            self.stats[h] = self.links.send(stat.at[h, 0], stat.at[h, 1], {"p": 1 - self.p})

    def stats_q(self, h):
        stat = self.stat
        self.stats[h].wait_recv()
        stat[h, 2] = stat[h, 0] + stat[h, 1]
        self.stats[h] = self.links.send(stat.at[h, 2], stat.at[h, 3], {"q": 1 - self.q})

    def stats_done(self, h, number):
        stat = self.stat
        self.stats[h].wait_recv()
        stats = (stat[h, 2] + stat[h, 3]) / self.width
        for i in range(number):
            self.cols[i, self.at(h)] = to_column(stats, i)

    def spread(self, h, blocks):
        here = self.out.at[0, self.at(h), self.mine]
        for k in blocks:
            if k:
                target = self.out.at[k, self.at(h), self.mine]
                self.spread_a[h, k] = self.links.send(here, target, {"a": across(self.a, k)})
        self.spread_p[h, 0] = self.links.send(here, here, {"p": 1 - self.p})

    def relay_p(self, h, k):
        if not k:
            return
        self.spread_a[h, k].wait_recv()
        here = self.out.at[k, self.at(h), self.mine]
        self.spread_p[h, k] = self.links.send(here, here, {"p": 1 - self.p})

    def relay_q(self, h, k):
        self.spread_p[h, k].wait_recv()
        here = self.out.at[k, self.at(h), self.pair]
        self.spread_q[h, k] = self.links.send(here, here, {"q": 1 - self.q})

    def arrived(self, h, k):
        self.spread_q[h, k].wait_recv()

    def steps(self, first, second, number, chain=False):
        def normed(h):
            self.stats_done(h, number)
            self.each(h, second)

        def spread_own(h):
            here = self.out.at[0, self.at(h), self.mine]
            self.spread_p[h, 0] = self.links.send(here, here, {"p": 1 - self.p})

        def spread_far(h, k):
            here = self.out.at[0, self.at(h), self.mine]
            target = self.out.at[k, self.at(h), self.mine]
            self.spread_a[h, k] = self.links.send(here, target, {"a": across(self.a, k)})

        table = {
            "P": self.send_p,
            "A": self.send_a,
            "SC": lambda h: self.scattered(h, first, number),
            "SQ": self.stats_q,
            "SD": normed,
            "X": spread_own,
            "Z": spread_far,
            "RP": self.relay_p,
            "RQ": self.relay_q,
        }
        if chain:
            lines = [
                Line(
                    self.links,
                    self.na,
                    lambda k, h=h: self.out.at[k, self.at(h), self.mine],
                    self.out.at[0, self.at(h), self.mine],
                )
                for h in range(HALVES)
            ]

            def pair_arrived(h, k):
                self.spread_p[h, k] = lines[h].to_pair(k)
                self.relay_q(h, k)

            table.update(
                X=lambda h: lines[h].to_pair(0).start(),
                Z=lambda h: lines[h].start(),
                FL=lambda h, t: lines[h].pass_on(1, t),
                FR=lambda h, t: lines[h].pass_on(-1, t),
                RQ=pair_arrived,
            )
        return table


class OverHeads:
    def __init__(self, links, na, a, p, q, held, from_a, out_ref):
        self.links, self.na, self.a, self.p, self.q = links, na, a, p, q
        self.held, self.from_a, self.out_ref = held, from_a, out_ref

    def to_pair(self):
        self.copy = self.links.send(self.held.at[0], self.held.at[1], {"p": 1 - self.p})

    def to_core(self):
        held = self.held
        self.copy.wait_recv()
        held[2] = held[0] + held[1]
        self.copy = self.links.send(held.at[2], held.at[3], {"q": 1 - self.q})

    def to_all(self):
        held = self.held
        self.copy.wait_recv()
        held[4] = held[2] + held[3]
        self.copies = [
            self.links.send(held.at[4], self.from_a.at[k - 1], {"a": across(self.a, k)})
            for k in range(1, self.na)
        ]

    def done(self):
        for copy in self.copies:
            copy.wait_recv()
        for k in range(self.na):
            for i in range(2):
                at = 2 * k + i
                total = self.held[4, at : at + 1]
                for j in range(1, self.na):
                    other = 2 * (k ^ j) + i
                    total = total + self.from_a[j - 1, other : other + 1]
                self.out_ref[at : at + 1] = total


def reduce_peers(na):
    a, p, q = lax.axis_index("a"), lax.axis_index("p"), lax.axis_index("q")
    return [{"q": 1 - q}, {"p": 1 - p}] + [{"a": across(a, k)} for k in range(1, na)]


def attn_math(r, tok_ref, gain_ref, proj_ref, inv_ref, res_ref):
    def first(at):
        own = r.add_all(at)
        proj_ref[at] = own
        r.parts[0, at] = fold(own * own)

    def second(at):
        own = proj_ref[at]
        inv = lax.rsqrt(r.cols[0, at] + epsilon)
        inv_ref[at] = inv
        residual = tok_ref[at].astype(f32) + own * wide(inv, r.quarter) * gain_ref[0:1]
        res_ref[at] = residual
        r.out[0, at, r.mine] = residual.astype(bf16)

    return first, second


def mlp_math(r, res_ref, grad_ref, gain_ref, block_ref, sum_ref):
    def first(at):
        own = r.add_all(at)
        r.total[at] = own
        r.parts[0, at] = fold(own * own)
        r.parts[1, at] = fold(grad_ref[at] * gain_ref[1:2] * own)

    def second(at):
        own = r.total[at]
        inv = wide(lax.rsqrt(r.cols[0, at] + epsilon), r.quarter)
        upstream = grad_ref[at]
        scaled = upstream * gain_ref[1:2]
        normed = own * inv
        block_ref[0, at, r.mine] = (res_ref[at] + normed * gain_ref[1:2]).astype(bf16)
        gains = upstream * normed
        sum_ref[...] += jnp.sum(gains.reshape(TILE // 8, 8, r.quarter), axis=0)
        grad = inv * scaled - own * inv * inv * inv * wide(r.cols[1, at], r.quarter)
        r.out[0, at, r.mine] = grad.astype(bf16)

    return first, second


def back_math(r, grad_ref, proj_ref, inv_ref, gain_ref, res_ref, sum_ref):
    def first(at):
        grad = grad_ref[at] + r.add_all(at)
        res_ref[at] = grad
        r.parts[0, at] = fold(grad * gain_ref[0:1] * proj_ref[at])

    def second(at):
        own = proj_ref[at]
        inv = wide(inv_ref[at], r.quarter)
        upstream = res_ref[at]
        gains = upstream * own * inv
        sum_ref[...] += jnp.sum(gains.reshape(TILE // 8, 8, r.quarter), axis=0)
        grad = inv * (upstream * gain_ref[0:1])
        grad = grad - own * inv * inv * inv * wide(r.cols[0, at], r.quarter)
        r.out[0, at, r.mine] = grad.astype(bf16)

    return first, second


MIDDLE = (
    ("F", 2), ("rP", 0, 2), ("F", 3), ("rP", 0, 3), ("rA", 0, 2), ("rP", 1, 3), ("rP", 1, 2), ("F", 1),
    ("rA", 0, 3), ("F", 0), ("rP", 0, 1), ("rA", 1, 3), ("rP", 1, 1), ("rP", 0, 0), ("rA", 1, 2),
    ("rP", 1, 0), ("rA", 0, 1), ("rA", 1, 1), ("rSC", 0), ("rSQ", 0), ("rSC", 1), ("rSD", 0), ("rZ", 0, 3),
    ("rX", 0), ("rSQ", 1), ("rSD", 1), ("rZ", 0, 1), ("BP",), ("rZ", 1, 3), ("rZ", 0, 2), ("rZ", 1, 1),
    ("rRP", 0, 3), ("rX", 1), ("rRP", 0, 1), ("rZ", 1, 2), ("rRQ", 0, 3), ("B", 0, 3), ("rRP", 0, 2),
    ("rRP", 1, 3), ("sP", 0, 3), ("rRQ", 0, 1), ("rRP", 1, 2), ("rRQ", 0, 2), ("rRQ", 1, 3), ("rRP", 1, 1),
    ("B", 0, 2), ("B", 0, 1), ("rRQ", 0, 0), ("sP", 0, 2), ("B", 1, 3), ("sP", 0, 1), ("rRQ", 1, 2),
    ("sA", 0, 3), ("B", 0, 0), ("sP", 1, 3), ("rRQ", 1, 1), ("sA", 0, 2), ("rRQ", 1, 0), ("B", 1, 2),
    ("sP", 0, 0), ("sA", 0, 1), ("B", 1, 1), ("sP", 1, 2), ("B", 1, 0), ("sA", 1, 3), ("sP", 1, 1),
    ("sSC", 0), ("sA", 1, 2), ("BQ",), ("sP", 1, 0), ("sSQ", 0), ("sA", 1, 1), ("sSD", 0), ("sZ", 0, 2),
    ("D",), ("sX", 0), ("sZ", 0, 1), ("sSC", 1), ("sSQ", 1), ("sZ", 0, 3), ("sRP", 0, 2), ("sSD", 1),
    ("sZ", 1, 1), ("sRP", 0, 1), ("sX", 1), ("sRQ", 0, 0), ("G", 2), ("sZ", 1, 3), ("G", 3), ("G", 1),
    ("sRP", 0, 3), ("G", 0), ("sZ", 1, 2), ("sRP", 1, 3), ("sRQ", 0, 1), ("sRQ", 1, 0), ("sRP", 1, 1),
    ("sRP", 1, 2), ("sRQ", 0, 2), ("sRQ", 0, 3), ("sRQ", 1, 3), ("sRQ", 1, 1), ("DS",), ("sRQ", 1, 2),
)


def middle_kernel(na, nb, *refs):
    x_ref, w_ref, res_ref, grad_ref, proj_ref, inv_ref, gain_ref = refs[:7]
    block_ref, back_out, ffn_sum_ref, grad_res_ref, attn_sum_ref, down_sum_ref, gu_grad_ref = refs[7:14]
    out, hidden_ref, grad_gu_ref, gu_ref, part_ref, down_grad, down_held = refs[14:21]
    scratch, (send_sem, recv_sem) = refs[21:-2], refs[-2:]
    units = hidden_ref.shape[2]
    width = x_ref.shape[2]
    b = lax.axis_index("b")
    greet(reduce_peers(na) + [{"b": across(b, j)} for j in range(1, nb)])
    links = Links(send_sem, recv_sem)
    r = Reduce(na, links, part_ref, out, scratch[:9])
    s = Reduce(na, links, part_ref, back_out, scratch[9:])
    ffn_sum_ref[...] = jnp.zeros_like(ffn_sum_ref)
    attn_sum_ref[...] = jnp.zeros_like(attn_sum_ref)
    wide_tile = 512

    def forward(k):
        def gated(n, carry):
            at, up_at = span(n, 256), pl.ds(pl.multiple_of(units + n * 256, 256), 256)
            gate = dot(x_ref[k], w_ref[:, at])
            up = dot(x_ref[k], w_ref[:, up_at])
            gu_ref[k, :, at] = gate
            gu_ref[k, :, up_at] = up
            hidden_ref[k, :, at] = (gate * jax.nn.sigmoid(gate) * up).astype(bf16)
            return carry

        lax.fori_loop(0, units // 256, gated, 0)

        def down(n, carry):
            at = span(n, wide_tile)
            part_ref[k, :, at] = dot_t(hidden_ref[k], w_ref[at, 2 * units :]).astype(bf16)
            return carry

        lax.fori_loop(0, width // wide_tile, down, 0)

    def backward(h, k):
        rows = r.at(h)

        def gated(n, carry):
            at, up_at = span(n, 256), pl.ds(pl.multiple_of(units + n * 256, 256), 256)
            down_at = pl.ds(pl.multiple_of(2 * units + n * 256, 256), 256)
            grad_hidden = dot(out[k, rows], w_ref[:, down_at])
            gate, up = gu_ref[k, rows, at], gu_ref[k, rows, up_at]
            sigmoid = jax.nn.sigmoid(gate)
            active = gate * sigmoid
            grad_gu_ref[k, rows, at] = (
                grad_hidden * up * (sigmoid * (1.0 + gate * (1.0 - sigmoid)))
            ).astype(bf16)
            grad_gu_ref[k, rows, up_at] = (grad_hidden * active).astype(bf16)
            return carry

        lax.fori_loop(0, units // 256, gated, 0)

        def back(n, carry):
            at = span(n, wide_tile)
            part_ref[k, rows, at] = dot_t(
                grad_gu_ref[k, rows], w_ref[at, : 2 * units]
            ).astype(bf16)
            return carry

        lax.fori_loop(0, width // wide_tile, back, 0)

    first, second = mlp_math(r, res_ref, grad_ref, gain_ref, block_ref, ffn_sum_ref)
    back_first, back_second = back_math(
        s, grad_ref, proj_ref, inv_ref, gain_ref, grad_res_ref, attn_sum_ref
    )
    copies, reused = {}, []
    columns = slice(0, units)

    def forward_step(k):
        forward(k)
        for h in range(HALVES):
            r.send_q(h, k)

    def backward_step(h, k):
        if not reused:
            links.sent(r.step_q.values())
            reused.append(True)
        r.arrived(h, k)
        backward(h, k)
        s.send_q(h, k)

    def block_p():
        here = block_ref.at[0, :, r.mine]
        copies["p"] = links.send(here, here, {"p": 1 - r.p})

    def block_q():
        copies["p"].wait_recv()
        here = block_ref.at[0, :, r.pair]
        copies["q"] = links.send(here, here, {"q": 1 - r.q})

    def down_grads():
        for block in range(na):
            weight_grad(out, hidden_ref, down_grad, block)
        copies["b"] = exchange_b(links, down_grad, down_held, columns)

    table = {
        "F": forward_step,
        "B": backward_step,
        "BP": block_p,
        "BQ": block_q,
        "D": down_grads,
        "DS": lambda: sum_b(copies["b"], down_grad, down_held, down_sum_ref, columns),
        "G": lambda block: weight_grad(x_ref, grad_gu_ref, gu_grad_ref, block),
    }
    table.update({"r" + key: step for key, step in r.steps(first, second, 2).items()})
    table.update({"s" + key: step for key, step in s.steps(back_first, back_second, 1).items()})
    for key, *where in MIDDLE:
        table[key](*where)
    for h in range(HALVES):
        for k in range(na):
            s.arrived(h, k)
    copies["q"].wait_recv()
    links.finish()


def middle_call(nb, x_all, w_mlp, res_mine, grad_mine, proj_mine, inv_mine, width_gain):
    na, rows, width = x_all.shape
    quarter, units = width // 4, w_mlp.shape[1] // 3
    w_rows = width // (na * nb)
    vmem = pl.BlockSpec(memory_space=pltpu.VMEM)
    shape = jax.ShapeDtypeStruct
    outs = (
        shape((1, rows, width), bf16),
        shape((na, rows, width), bf16),
        shape((8, quarter), f32),
        shape((rows, quarter), f32),
        shape((8, quarter), f32),
        shape((na, w_rows, units), bf16),
        shape((na, nb, w_rows, 2 * units), bf16),
    )
    copies = 2 * HALVES * (6 * na + 1) + 2 + nb
    return pl.pallas_call(
        functools.partial(middle_kernel, na, nb),
        out_shape=outs,
        in_specs=[vmem] * 7,
        out_specs=(vmem,) * len(outs),
        scratch_shapes=[
            pltpu.VMEM((na, rows, width), bf16),
            pltpu.VMEM((na, rows, units), bf16),
            pltpu.VMEM((na, rows, 2 * units), bf16),
            pltpu.VMEM((na, rows, 2 * units), f32),
            pltpu.VMEM((na, rows, width), bf16),
            pltpu.VMEM((na, nb, w_rows, units), bf16),
            pltpu.VMEM((nb - 1, na, w_rows, units), bf16),
        ]
        + reduce_scratch(na, rows, width)
        + reduce_scratch(na, rows, width)
        + [pltpu.SemaphoreType.DMA((copies,)), pltpu.SemaphoreType.DMA((copies,))],
        compiler_params=pltpu.CompilerParams(
            collective_id=2, has_side_effects=True, vmem_limit_bytes=VMEM_LIMIT
        ),
        name="middle",
    )(x_all, w_mlp, res_mine, grad_mine, proj_mine, inv_mine, width_gain)


def last_kernel(na, nb, *refs):
    proj_ref, x_ref, qkv_ref, stats_ref, gain_ref, cos_ref, sin_ref, w_ref, att_ref = refs[:9]
    grad_ref, attn_sum_ref, ffn_sum_ref, down_sum_ref, gu_grad_ref = refs[9:14]
    out, sums_ref, down_out, gu_out, qkv_out, wout_out = refs[14:20]
    scaled_ref, grad_qkv_ref, part_ref, head_sums, held, stats_a, inner_ref = refs[20:27]
    own_sums, a_sums, b_sums, gu_held, gu_sum, attn_grad, attn_held, attn_sum = refs[27:35]
    down_in, gu_in, attn_in = refs[35:38]
    scratch, (send_sem, recv_sem) = refs[38:-2], refs[-2:]
    links = Links(send_sem, recv_sem)
    r = Reduce(na, links, part_ref, out, scratch)
    a, b, p, q, mine, pair, quarter = (
        r.a, lax.axis_index("b"), r.p, r.q, r.mine, r.pair, r.quarter,
    )
    units = down_sum_ref.shape[2]
    own_sums[...] = jnp.zeros_like(own_sums)
    own_sums[0:1, mine] = jnp.sum(attn_sum_ref[...], axis=0, keepdims=True)
    own_sums[1:2, mine] = jnp.sum(ffn_sum_ref[...], axis=0, keepdims=True)
    greet(reduce_peers(na) + [{"b": across(b, j)} for j in range(1, nb)])
    far = list(range(2, na)) + [1]

    def to_owners(source, target, columns):
        return [
            (k, links.send(
                source.at[across(a, k), :, columns], target.at[k - 1, :, columns], {"a": across(a, k)}
            ))
            for k in far
        ]

    whole = slice(0, units)
    halves = [slice(0, units), slice(units, 2 * units)]
    down_copies = to_owners(down_sum_ref, down_in, whole)
    gu_b = [exchange_b(links, gu_grad_ref, gu_held, columns) for columns in halves]
    here = own_sums.at[:, mine]
    sums_p = links.send(here, here, {"p": 1 - p})

    held[0] = jnp.zeros_like(held[0])
    head_sums[...] = jnp.zeros_like(head_sums)

    def attend_back(k, carry):
        queries, key_rows, values, q_inv, k_inv, q_rot, k_rot, probs = attention(
            k, qkv_ref[k], stats_ref[...], gain_ref, cos_ref, sin_ref
        )
        cos_table, sine_table = cos_ref[...], sin_ref[...]
        grad_att = dot(proj_ref[k], w_ref[:, 3 * HD :]).astype(bf16)
        grad_v = t_dot(probs.astype(bf16), grad_att)
        grad_p = dot_t(grad_att, values)
        delta = jnp.sum(probs * grad_p, axis=1, keepdims=True)
        grad_scores = (probs * (grad_p - delta) * HD ** (-0.5)).astype(bf16)
        grad_q = dot(grad_scores, k_rot)
        grad_k = t_dot(grad_scores, q_rot)
        grad_q = grad_q * cos_table + rotate_back(grad_q * sine_table)
        grad_k = grad_k * cos_table + rotate_back(grad_k * sine_table)
        head_sums[0:1] += jnp.sum(grad_q * queries * q_inv, axis=0, keepdims=True)
        head_sums[1:2] += jnp.sum(grad_k * key_rows * k_inv, axis=0, keepdims=True)
        scaled_q = grad_q * gain_ref[0:1]
        scaled_k = grad_k * gain_ref[1:2]
        scaled_ref[k, :, :HD] = scaled_q
        scaled_ref[k, :, HD:] = scaled_k
        grad_qkv_ref[k, :, 2 * HD :] = grad_v.astype(bf16)
        held[0] += to_row(scaled_q * queries, 2 * k) + to_row(scaled_k * key_rows, 2 * k + 1)
        return carry

    lax.fori_loop(0, na, attend_back, 0)
    sums_p.wait_recv()
    here = own_sums.at[:, pair]
    sums_q = links.send(here, here, {"q": 1 - q})
    gu_copies = []

    def sent():
        for block in range(na):
            weight_grad(proj_ref, att_ref, attn_grad, block, slice(3 * HD, 4 * HD))
        sum_b(gu_b[0], gu_grad_ref, gu_held, gu_sum, halves[0])
        gu_copies.append(to_owners(gu_sum, gu_in, halves[0]))

    over_heads = OverHeads(links, na, a, p, q, held, stats_a, inner_ref)
    over_heads.to_pair()
    over_heads.to_core()
    over_heads.to_all()
    sent()
    over_heads.done()

    def qkv_back(k, carry):
        for i in range(2):
            at = slice(i * HD, (i + 1) * HD)
            inv = lax.rsqrt(to_column(stats_ref[...] / HQ, 2 * k + i) + epsilon)
            mean = to_column(inner_ref[...] / HQ, 2 * k + i)
            grad = inv * scaled_ref[k, :, at] - qkv_ref[k, :, at] * inv * inv * inv * mean
            grad_qkv_ref[k, :, at] = grad.astype(bf16)
        part_ref[k] = dot_t(grad_qkv_ref[k], w_ref[:, : 3 * HD]).astype(bf16)
        return carry

    for k in r.lead:
        qkv_back(k, 0)
        for h in range(HALVES):
            r.send_q(h, k)
    for h in range(HALVES):
        for k in r.lead:
            r.send_p(h, k)
    for block in range(na):
        weight_grad(x_ref, grad_qkv_ref, attn_grad, block, slice(0, 3 * HD))
    attn_columns = slice(0, 4 * HD)
    attn_b = exchange_b(links, attn_grad, attn_held, attn_columns)
    for h in range(HALVES):
        for k in r.lead:
            r.send_a(h, k)
    sums_q.wait_recv()
    sums_a = [
        links.send(own_sums.at[:, span(across(a, k), quarter)], a_sums.at[k - 1], {"a": across(a, k)})
        for k in range(1, na)
    ]
    sum_b(gu_b[1], gu_grad_ref, gu_held, gu_sum, halves[1])
    gu_copies.append(to_owners(gu_sum, gu_in, halves[1]))

    def first(at):
        out[0, at, mine] = (grad_ref[at] + r.add_all(at)).astype(bf16)

    for h in range(HALVES):
        r.scattered(h, first, 0)
        r.spread(h, [0])
    for copy in sums_a:
        copy.wait_recv()
    total = own_sums[:, span(a, quarter)]
    for k in range(1, na):
        total = total + a_sums[k - 1]
    b_sums[0, :, :quarter] = total
    b_sums[0, :, quarter:] = head_sums[...]
    sums_b = [links.send(b_sums.at[0], b_sums.at[j], {"b": across(b, j)}) for j in range(1, nb)]
    for h in range(HALVES):
        r.relay_q(h, 0)
    sum_b(attn_b, attn_grad, attn_held, attn_sum, attn_columns)
    attn_copies = to_owners(attn_sum, attn_in, attn_columns)

    def store(target, index, size, value):
        target[:, span(index, size)] = value.astype(f32)

    store(down_out, a, units, down_sum_ref[a])
    for c in range(2):
        store(gu_out.at[c], a, units, gu_sum[a, :, halves[c]])
    for c in range(3):
        store(qkv_out.at[c], a, HD, attn_sum[a, :, c * HD : (c + 1) * HD])
    store(wout_out, a, HD, attn_sum[a, :, 3 * HD :])
    for k, copy in down_copies:
        copy.wait_recv()
        store(down_out, across(a, k), units, down_in[k - 1])
    for copy in sums_b:
        copy.wait_recv()
    total = b_sums[0]
    for j in range(1, nb):
        total = total + b_sums[j]
    sums_ref[...] = total
    for c in range(2):
        for k, copy in gu_copies[c]:
            copy.wait_recv()
            store(gu_out.at[c], across(a, k), units, gu_in[k - 1, :, halves[c]])
    for k, copy in attn_copies:
        copy.wait_recv()
        for c in range(3):
            store(qkv_out.at[c], across(a, k), HD, attn_in[k - 1, :, c * HD : (c + 1) * HD])
        store(wout_out, across(a, k), HD, attn_in[k - 1, :, 3 * HD :])
    for h in range(HALVES):
        r.arrived(h, 0)
    links.finish()


def last_call(nb, *operands):
    na, rows, width = operands[0].shape
    w_rows, units = operands[12].shape[1:]
    quarter = width // 4
    vmem = pl.BlockSpec(memory_space=pltpu.VMEM)
    shape = jax.ShapeDtypeStruct
    outs = (
        shape((1, rows, width), bf16),
        shape((8, quarter + HD), f32),
        shape((w_rows, na * units), f32),
        shape((2, w_rows, na * units), f32),
        shape((3, w_rows, na * HD), f32),
        shape((w_rows, na * HD), f32),
    )
    copies = HALVES * (3 * na + 1) + 2 + 6 * na + 4 * nb
    return pl.pallas_call(
        functools.partial(last_kernel, na, nb),
        out_shape=outs,
        in_specs=[vmem] * 14,
        out_specs=(vmem,) * len(outs),
        scratch_shapes=[
            pltpu.VMEM((na, rows, 2 * HD), f32),
            pltpu.VMEM((na, rows, 3 * HD), bf16),
            pltpu.VMEM((na, rows, width), bf16),
            pltpu.VMEM((8, HD), f32),
            pltpu.VMEM((5, 8, rows), f32),
            pltpu.VMEM((na - 1, 8, rows), f32),
            pltpu.VMEM((8, rows), f32),
            pltpu.VMEM((8, width), f32),
            pltpu.VMEM((na - 1, 8, quarter), f32),
            pltpu.VMEM((nb, 8, quarter + HD), f32),
            pltpu.VMEM((nb - 1, na, w_rows, 2 * units), bf16),
            pltpu.VMEM((na, w_rows, 2 * units), bf16),
            pltpu.VMEM((na, nb, w_rows, 4 * HD), bf16),
            pltpu.VMEM((nb - 1, na, w_rows, 4 * HD), bf16),
            pltpu.VMEM((na, w_rows, 4 * HD), bf16),
            pltpu.VMEM((na - 1, w_rows, units), bf16),
            pltpu.VMEM((na - 1, w_rows, 2 * units), bf16),
            pltpu.VMEM((na - 1, w_rows, 4 * HD), bf16),
        ]
        + reduce_scratch(na, rows, width)
        + [pltpu.SemaphoreType.DMA((copies,)), pltpu.SemaphoreType.DMA((copies,))],
        compiler_params=pltpu.CompilerParams(
            collective_id=4, has_side_effects=True, vmem_limit_bytes=VMEM_LIMIT
        ),
        name="last",
    )(*operands)


def reduce_scratch(na, rows, width):
    quarter = width // 4
    return [
        pltpu.VMEM((na, rows, width // 2), bf16),
        pltpu.VMEM((na, rows, width // 2), bf16),
        pltpu.VMEM((na, rows, quarter), bf16),
        pltpu.VMEM((na - 1, rows, quarter), bf16),
        pltpu.VMEM((na - 1, rows, quarter), bf16),
        pltpu.VMEM((rows, quarter), f32),
        pltpu.VMEM((2, rows, 128), f32),
        pltpu.VMEM((2, rows, 128), f32),
        pltpu.VMEM((HALVES, 4, 8, rows // HALVES), f32),
    ]


ENTER = (
    ("Z", 0), ("W", 3), ("FW", 0), ("FR", 0, 1), ("FL", 0, 1), ("W", 1), ("CUT", 2), ("FW", 1), ("W", 2),
    ("FR", 0, 2), ("FR", 0, 3), ("CUT", 3), ("M", 0, 3), ("FL", 0, 2), ("CUT", 1), ("FW", 3), ("FL", 0, 3),
    ("GA",), ("FT", 0), ("FQ", 3), ("FW", 2), ("CUT", 0), ("FQ", 2), ("M", 0, 1), ("M", 2, 3), ("FQ", 1),
    ("J", 3), ("FQ", 0), ("J", 0), ("GB",), ("M", 1, 1), ("J", 1), ("J", 2), ("S1",), ("S2",), ("S3",),
    ("M", 1, 3), ("MR", 1, 0), ("M", 1, 2), ("S4",), ("E", 3), ("E", 1), ("rP", 1, 3), ("E", 2),
    ("rP", 1, 1), ("M", 2, 1), ("MR", 2, 3), ("rP", 0, 3), ("rP", 0, 1), ("MR", 0, 3), ("E", 0),
    ("rA", 1, 3), ("MR", 2, 0), ("rA", 1, 1), ("MR", 0, 1), ("rA", 0, 3), ("MR", 1, 3), ("rP", 0, 2),
    ("MR", 2, 1), ("rA", 0, 2), ("rA", 0, 1), ("rP", 0, 0), ("rP", 1, 2), ("rA", 1, 2), ("MR", 1, 2),
    ("rP", 1, 0), ("rSC", 0), ("rSQ", 0), ("MR", 0, 0), ("M", 2, 2), ("rSC", 1), ("rSD", 0), ("rSQ", 1),
    ("rX", 0), ("rSD", 1), ("rZ", 0), ("rZ", 1), ("rFR", 0, 1), ("rFL", 0, 1), ("rX", 1), ("MR", 2, 2),
    ("rFR", 1, 1), ("rFL", 1, 1), ("rFR", 0, 2), ("rRQ", 0, 0), ("rFL", 1, 2), ("rFL", 0, 2), ("MR", 1, 1),
    ("rFR", 0, 3), ("M", 0, 2), ("rFR", 1, 2), ("rFL", 1, 3), ("rFR", 1, 3), ("rFL", 0, 3), ("rRQ", 0, 1),
    ("MR", 0, 2), ("rRQ", 1, 1), ("rRQ", 1, 2), ("rRQ", 0, 2), ("rRQ", 1, 0), ("rRQ", 1, 3), ("rRQ", 0, 3),
)


def enter_kernel(na, nb, *refs):
    tok_ref, qkv_w_ref, wout_ref, gu_ref, down_ref, cos_ref, sin_ref = refs[:7]
    gain_refs = refs[7:11]
    x_ref, w_ref, mlp_w_ref, width_gain_ref, head_gain_ref, qkv_ref, stats_ref, att_ref = refs[11:19]
    out, proj_ref, inv_ref, res_ref = refs[19:23]
    own_gains, gains_ref, piece_ref, part_ref, held, stats_a = refs[23:29]
    scratch, (local_sem, send_sem, recv_sem) = refs[29:-3], refs[-3:]
    a, b, p, q = (lax.axis_index(axis) for axis in ("a", "b", "p", "q"))
    rows = wout_ref.shape[0]
    quarter = tok_ref.shape[1]
    units = down_ref.shape[1] // na
    own_gains[...] = jnp.zeros_like(own_gains)
    for i, ref in enumerate(gain_refs):
        own_gains[i : i + 1, : ref.shape[1]] = ref[...].astype(f32)
    gains_ref[a, b] = own_gains[...]
    greet(
        [{"q": 1 - q}, {"p": 1 - p}]
        + [{"a": across(a, k)} for k in range(1, na)]
        + [{"b": across(b, j)} for j in range(1, nb)]
    )
    links = Links(send_sem, recv_sem)
    mine, pair = span(2 * q + p, quarter), span(q, 2 * quarter)
    place = span(a * nb + b, rows)
    copies, ends = {}, []
    locals_ = [pltpu.make_async_copy(tok_ref, x_ref.at[0, :, mine], local_sem.at[0])]

    def weight_sources(k):
        block = span(across(a, k), HD)
        sources = [qkv_w_ref.at[c, :, block] for c in range(3)] + [wout_ref.at[:, block]]
        return [(s, w_ref.at[place, c * HD : (c + 1) * HD]) for c, s in enumerate(sources)]

    for c, (source, target) in enumerate(weight_sources(0)):
        locals_.append(pltpu.make_async_copy(source, target, local_sem.at[1 + c]))
    for copy in locals_:
        copy.start()

    def send_gains():
        copies["g"] = [
            links.send(own_gains, gains_ref.at[a, b], {"a": across(a, k)}) for k in range(1, na)
        ]

    def relay_gains():
        for copy in copies["g"]:
            copy.wait_recv()
        at = gains_ref.at[:, b]
        copies["gb"] = [links.send(at, at, {"b": across(b, j)}) for j in range(1, nb)]

    def send_weights(k):
        copies["w", k] = [
            links.send(source, target, {"a": across(a, k)}) for source, target in weight_sources(k)
        ]

    def relay_weights(k):
        if k:
            for copy in copies["w", k]:
                copy.wait_recv()
        else:
            for copy in locals_[1:]:
                copy.wait()
        at = w_ref.at[span(across(a, k) * nb + b, rows), :]
        copies["wb", k] = [links.send(at, at, {"b": across(b, j)}) for j in range(1, nb)]

    line = Line(links, na, lambda k: x_ref.at[k, :, mine], tok_ref)

    def own_tokens(_):
        locals_[0].wait()
        line.to_pair(0).start()

    def pair_tokens(k):
        line.to_pair(k).wait_recv()
        at = x_ref.at[k, :, pair]
        copies["x", k] = links.send(at, at, {"q": 1 - q})

    def cut_weights(k):
        block = span(across(a, k), units)

        def cut(i, carry):
            at = pl.ds(pl.multiple_of(i * TILE, TILE), TILE)
            cuts = (gu_ref[at, 0, block], gu_ref[at, 1, block], down_ref[at, block])
            for c in range(3):
                if k:
                    piece_ref[k - 1, c, at] = cuts[c]
                else:
                    to = pl.ds(pl.multiple_of((a * nb + b) * rows + i * TILE, TILE), TILE)
                    mlp_w_ref[to, c * units : (c + 1) * units] = cuts[c]
            return carry

        lax.fori_loop(0, rows // TILE, cut, 0)

    def send_piece(c, k):
        target = mlp_w_ref.at[place, c * units : (c + 1) * units]
        copies["m", c, k] = links.send(piece_ref.at[k - 1, c], target, {"a": across(a, k)})

    def relay_piece(c, k):
        if k:
            copies["m", c, k].wait_recv()
        at = mlp_w_ref.at[span(across(a, k) * nb + b, rows), c * units : (c + 1) * units]
        ends.extend(links.send(at, at, {"b": across(b, j)}) for j in range(1, nb))

    arrived, ready = set(), []

    def project(k):
        if not arrived:
            held[0] = jnp.zeros_like(held[0])
            for i in range(na):
                for copy in copies["wb", i]:
                    copy.wait_recv()
        arrived.add(k)
        copies["x", k].wait_recv()
        proj = dot(x_ref[k], w_ref[:, : 3 * HD])
        qkv_ref[k] = proj
        queries, key_rows = proj[:, :HD], proj[:, HD : 2 * HD]
        held[0] += to_row(queries * queries, 2 * k) + to_row(key_rows * key_rows, 2 * k + 1)

    over_heads = OverHeads(links, na, a, p, q, held, stats_a, stats_ref)

    def all_stats():
        over_heads.done()
        for copy in copies["gb"]:
            copy.wait_recv()
        n_d, n_h = gain_refs[0].shape[1], gain_refs[2].shape[1]
        width_gain_ref[...] = jnp.zeros_like(width_gain_ref)
        head_gain_ref[...] = jnp.zeros_like(head_gain_ref)
        for i in range(2):
            width_gain_ref[i : i + 1] = jnp.concatenate(
                [gains_ref[2 * q + p, j, i : i + 1, :n_d] for j in range(nb)], axis=1
            )
            head_gain_ref[i : i + 1] = jnp.concatenate(
                [gains_ref[a, j, i + 2 : i + 3, :n_h] for j in range(nb)], axis=1
            )

    r = Reduce(na, links, part_ref, out, scratch)

    def attend(k):
        values, probs = (
            attention(k, qkv_ref[k], stats_ref[...], head_gain_ref, cos_ref, sin_ref)[i] for i in (2, 7)
        )
        attended = dot(probs.astype(bf16), values).astype(bf16)
        att_ref[k] = attended
        part_ref[k] = dot_t(attended, w_ref[:, 3 * HD :]).astype(bf16)
        for h in range(HALVES):
            r.send_q(h, k)

    first, second = attn_math(r, tok_ref, width_gain_ref, proj_ref, inv_ref, res_ref)
    table = {
        "GA": send_gains,
        "GB": relay_gains,
        "W": send_weights,
        "FW": relay_weights,
        "Z": lambda _: line.start(),
        "FL": lambda _, t: line.pass_on(1, t),
        "FR": lambda _, t: line.pass_on(-1, t),
        "FT": own_tokens,
        "FQ": pair_tokens,
        "CUT": cut_weights,
        "M": send_piece,
        "MR": relay_piece,
        "J": project,
        "S1": over_heads.to_pair,
        "S2": over_heads.to_core,
        "S3": over_heads.to_all,
        "S4": all_stats,
        "E": attend,
    }
    table.update({"r" + key: step for key, step in r.steps(first, second, 1, True).items()})
    for key, *where in ENTER:
        table[key](*where)
    for h in range(HALVES):
        for k in range(na):
            r.arrived(h, k)
    for copy in ends:
        copy.wait_recv()
    links.finish()


def enter_call(na, nb, tok_mine, qkv, w_out, gu, down, cos_table, sine_table, gains):
    rows, quarter = tok_mine.shape
    width = 4 * quarter
    w_rows, units = down.shape[0], down.shape[1] // na
    lanes = max(128, gains[0].shape[1])
    vmem = pl.BlockSpec(memory_space=pltpu.VMEM)
    shape = jax.ShapeDtypeStruct
    full = shape((na, rows, width), bf16)
    outs = [
        full,
        shape((width, 4 * HD), bf16),
        shape((width, 3 * units), bf16),
        shape((8, quarter), f32),
        shape((8, HD), f32),
        shape((na, rows, 3 * HD), f32),
        shape((8, rows), f32),
        shape((na, rows, HD), bf16),
        full,
        shape((rows, quarter), f32),
        shape((rows, 128), f32),
        shape((rows, quarter), f32),
    ]
    copies = 90 + 16 * nb
    return pl.pallas_call(
        functools.partial(enter_kernel, na, nb),
        out_shape=tuple(outs),
        in_specs=[vmem] * 11,
        out_specs=(vmem,) * len(outs),
        scratch_shapes=[
            pltpu.VMEM((8, lanes), f32),
            pltpu.VMEM((na, nb, 8, lanes), f32),
            pltpu.VMEM((na - 1, 3, w_rows, units), bf16),
            pltpu.VMEM((na, rows, width), bf16),
            pltpu.VMEM((5, 8, rows), f32),
            pltpu.VMEM((na - 1, 8, rows), f32),
        ]
        + reduce_scratch(na, rows, width)
        + [
            pltpu.SemaphoreType.DMA((5,)),
            pltpu.SemaphoreType.DMA((copies,)),
            pltpu.SemaphoreType.DMA((copies,)),
        ],
        compiler_params=pltpu.CompilerParams(
            collective_id=5, has_side_effects=True, vmem_limit_bytes=VMEM_LIMIT
        ),
        name="enter",
    )(tok_mine, qkv, w_out, gu, down, cos_table, sine_table, *gains)


def rope_tables(length, width):
    half_width = width // 2
    inv_freq = rope_base ** (-(jnp.arange(half_width, dtype=f32) * 2.0) / width)
    angles = jnp.arange(length, dtype=f32)[:, None] * inv_freq[None, :]
    cos_table = jnp.concatenate([jnp.cos(angles), jnp.cos(angles)], axis=1)
    sine_table = jnp.concatenate([jnp.sin(angles), jnp.sin(angles)], axis=1)
    return cos_table, sine_table


def on_device(
    tokens,
    qkv_weight,
    out_weight,
    gu_weight,
    down_weight,
    attn_gain,
    ffn_gain,
    q_gain,
    k_gain,
    out_grad,
):
    na, nb = lax.axis_size("a"), lax.axis_size("b")
    a, b = lax.axis_index("a"), lax.axis_index("b")
    share = lax.axis_index("q") * 2 + lax.axis_index("p")
    rows, width = tokens.shape
    quarter = width // 4
    w_rows = out_weight.shape[0]
    units = down_weight.shape[1] // na

    def quarter_of(operand):
        return lax.dynamic_slice_in_dim(operand, share * quarter, quarter, 1)

    tok_mine, grad_mine = quarter_of(tokens), quarter_of(out_grad)
    cos_table, sine_table = rope_tables(SEQ_LEN, HD)
    (
        x_all,
        w_attn,
        w_mlp,
        width_gain,
        head_gain,
        qkv,
        stats,
        attended,
        res_all,
        proj_mine,
        inv_mine,
        res_mine,
    ) = enter_call(
        na,
        nb,
        tok_mine,
        qkv_weight.transpose(1, 0, 2),
        out_weight,
        gu_weight,
        down_weight,
        cos_table,
        sine_table,
        [gain[None] for gain in (attn_gain, ffn_gain, q_gain, k_gain)],
    )
    n_d, n_h = attn_gain.shape[0], q_gain.shape[0]
    block_rows, grad_proj, ffn_sums, grad_res, attn_sums, down_sum, gu_grad = middle_call(
        nb, res_all, w_mlp, res_mine, grad_mine, proj_mine, inv_mine, width_gain
    )
    grad_rows, sums, down_grad, gu_grad, qkv_grad, out_grad_w = last_call(
        nb,
        grad_proj,
        x_all,
        qkv,
        stats,
        head_gain,
        cos_table,
        sine_table,
        w_attn,
        attended,
        grad_res,
        attn_sums,
        ffn_sums,
        down_sum,
        gu_grad,
    )
    width_sums = lax.dynamic_slice_in_dim(sums[:2, :quarter], b * n_d, n_d, 1)
    head_sums = lax.dynamic_slice_in_dim(sums[:2, quarter:], b * n_h, n_h, 1)
    return (
        block_rows[0].astype(f32),
        grad_rows[0].astype(f32),
        qkv_grad.transpose(1, 0, 2),
        out_grad_w,
        gu_grad.transpose(1, 0, 2),
        down_grad,
        width_sums[0],
        width_sums[1],
        head_sums[0],
        head_sums[1],
    )


def solution(mesh):
    dp, tp = mesh.shape["dp"], mesh.shape["tensor"]
    na = HEADS // tp
    fine = Mesh(mesh.devices.reshape(na, dp // na, tp // 2, 2), ("a", "b", "p", "q"))
    dp_axes, tp_axes = ("a", "b"), ("p", "q")
    both = tp_axes + dp_axes
    return jax.shard_map(
        on_device,
        mesh=fine,
        in_specs=(
            P(dp_axes, None),
            P(dp_axes, None, tp_axes),
            P(dp_axes, tp_axes),
            P(dp_axes, None, tp_axes),
            P(dp_axes, tp_axes),
            P(dp_axes),
            P(dp_axes),
            P(both),
            P(both),
            P(dp_axes, None),
        ),
        out_specs=(
            P(dp_axes, None),
            P(dp_axes, None),
            P(dp_axes, None, tp_axes),
            P(dp_axes, tp_axes),
            P(dp_axes, None, tp_axes),
            P(dp_axes, tp_axes),
            P(dp_axes),
            P(dp_axes),
            P(both),
            P(both),
        ),
        check_vma=False,
    )
```

```python
import functools

import jax
import jax.numpy as jnp
from jax import lax
from jax.experimental import pallas as pl
from jax.experimental.pallas import tpu as pltpu
from jax.sharding import Mesh, PartitionSpec as P

HEADS = 16
HD = 128
SEQ_LEN = 256
HQ = 2048

epsilon = 1e-06
rope_base = 500000.0

f32 = jnp.float32
bf16 = jnp.bfloat16
MESH = pl.DeviceIdType.MESH
EXACT = lax.Precision.HIGHEST
VMEM_LIMIT = 60 * 1024 * 1024
TILE = 32
HALVES = 2


def flip(index, bit):
    return index + bit - 2 * bit * ((index // bit) % 2)


def across(index, k):
    bit = 1
    while bit <= k:
        if k & bit:
            index = flip(index, bit)
        bit *= 2
    return index


def exclusive_or(left, right, count):
    total, bit = 0, 1
    while bit < count:
        total = total + bit * ((left // bit + right // bit) % 2)
        bit *= 2
    return total


def pick(operand, index, axis):
    return lax.dynamic_index_in_dim(operand, index, axis, keepdims=False)


def span(index, size):
    return pl.ds(pl.multiple_of(index * size, size), size)


class Links:
    def __init__(self, send_sem, recv_sem):
        self.send_sem, self.recv_sem, self.count = send_sem, recv_sem, 0
        self.copies, self.lines = [], []

    def send(self, source, target, device):
        copy = self.copy(self.count, source, target, device)
        copy.start()
        self.count += 1
        self.copies.append(copy)
        return copy

    def reserve(self, number):
        self.count += number
        return self.count - number

    def copy(self, index, source, target, device):
        return pltpu.make_async_remote_copy(
            src_ref=source,
            dst_ref=target,
            send_sem=self.send_sem.at[index],
            recv_sem=self.recv_sem.at[index],
            device_id=device,
            device_id_type=MESH,
        )

    def sent(self, copies):
        done = [id(copy) for copy in copies]
        for copy in self.copies:
            if id(copy) in done:
                copy.wait_send()
        self.copies = [copy for copy in self.copies if id(copy) not in done]

    def finish(self):
        for copy in self.copies:
            copy.wait_send()
        for line in self.lines:
            line.finish()


def greet(peers):
    barrier = pltpu.get_barrier_semaphore()
    for peer in peers:
        pl.semaphore_signal(barrier, inc=1, device_id=peer, device_id_type=MESH)
    pl.semaphore_wait(barrier, len(peers))


def fold(block):
    total = block[:, :128]
    for i in range(1, block.shape[1] // 128):
        total = total + block[:, i * 128 : (i + 1) * 128]
    return total


def wide(column, width):
    return jnp.concatenate([column] * (width // 128), axis=1)


def row_mask(row):
    return (lax.broadcasted_iota(jnp.int32, (8, 128), 0) == row).astype(f32)


def to_row(block, row):
    return lax.dot_general(
        row_mask(row), block, (((1,), (1,)), ((), ())), precision=EXACT, preferred_element_type=f32
    )


def to_column(stats, row):
    return lax.dot_general(
        stats, row_mask(row), (((0,), (0,)), ((), ())), precision=EXACT, preferred_element_type=f32
    )


def dot(left, right):
    return jnp.dot(left, right, preferred_element_type=f32)


def dot_t(left, right):
    return lax.dot_general(left, right, (((1,), (1,)), ((), ())), preferred_element_type=f32)


def t_dot(left, right):
    return lax.dot_general(left, right, (((0,), (0,)), ((), ())), preferred_element_type=f32)


def rotate(operand):
    half = HD // 2
    return jnp.concatenate([-operand[:, half:], operand[:, :half]], axis=1)


def rotate_back(operand):
    half = HD // 2
    return jnp.concatenate([operand[:, half:], -operand[:, :half]], axis=1)


def attention(k, qkv, stats, gain_ref, cos_ref, sin_ref):
    stats = stats / HQ
    q_inv = lax.rsqrt(to_column(stats, 2 * k) + epsilon)
    k_inv = lax.rsqrt(to_column(stats, 2 * k + 1) + epsilon)
    queries, key_rows = qkv[:, :HD], qkv[:, HD : 2 * HD]
    values = qkv[:, 2 * HD :].astype(bf16)
    cos_table, sine_table = cos_ref[...], sin_ref[...]
    q_normed = queries * q_inv * gain_ref[0:1]
    k_normed = key_rows * k_inv * gain_ref[1:2]
    q_rot = (q_normed * cos_table + rotate(q_normed) * sine_table).astype(bf16)
    k_rot = (k_normed * cos_table + rotate(k_normed) * sine_table).astype(bf16)
    scores = dot_t(q_rot, k_rot) * HD ** (-0.5)
    ahead = lax.broadcasted_iota(jnp.int32, scores.shape, 1) > lax.broadcasted_iota(
        jnp.int32, scores.shape, 0
    )
    scores = jnp.where(ahead, -1e30, scores)
    shifted = jnp.exp(scores - jnp.max(scores, axis=1, keepdims=True))
    probs = shifted / jnp.sum(shifted, axis=1, keepdims=True)
    return queries, key_rows, values, q_inv, k_inv, q_rot, k_rot, probs


def weight_grad(left, right, out, block, columns=None):
    na, nb, rows = left.shape[0], out.shape[1], out.shape[2]
    columns = columns or slice(0, right.shape[2])
    size = max(rows, 256)


    def chunk(i, carry):
        at = span(block * (nb * rows // size) + i, size)
        total = t_dot(left[0, :, at], right[0])
        for k in range(1, na):
            total = total + t_dot(left[k, :, at], right[k])
        for j in range(size // rows):
            part = total[j * rows : (j + 1) * rows].astype(bf16)
            out[block, i * (size // rows) + j, :, columns] = part
        return carry

    lax.fori_loop(0, nb * rows // size, chunk, 0)


def exchange_b(links, grad, held, columns):
    b = lax.axis_index("b")
    return [
        links.send(
            grad.at[:, across(b, j), :, columns], held.at[j - 1, :, :, columns], {"b": across(b, j)}
        )
        for j in range(1, held.shape[0] + 1)
    ]


def sum_b(copies, own, held, out, columns):
    for copy in copies:
        copy.wait_recv()

    def add(block, carry):
        total = own(block)[:, columns].astype(f32)
        for j in range(held.shape[0]):
            total = total + held[j, block, :, columns].astype(f32)
        out[block, :, columns] = total.astype(bf16)
        return carry

    lax.fori_loop(0, held.shape[1], add, 0)


class Line:
    def __init__(self, links, na, block, own):
        self.links, self.na, self.block, self.own = links, na, block, own
        self.a, self.p = lax.axis_index("a"), lax.axis_index("p")
        self.hop_base = {1: links.reserve(na - 1), -1: links.reserve(na - 1)}
        self.pass_base = links.reserve(na)
        links.lines.append(self)

    def hop(self, way, t):
        a, na = self.a, self.na
        first = a - way * (t - 1)
        source = self.own if t == 1 else self.block(exclusive_or(first, a, na))
        target = self.block(exclusive_or(first, a + way, na))
        return self.links.copy(self.hop_base[way] + t - 1, source, target, {"a": (a + way) % na})

    def sends(self, way, t):
        first, last = self.a - way * (t - 1), self.a + way
        return (first >= 0) & (first < self.na) & (last >= 0) & (last < self.na)

    def to_pair(self, k, source=None):
        at = self.block(k)
        return self.links.copy(self.pass_base + k, at if source is None else source, at, {"p": 1 - self.p})

    def start(self):
        for way in (1, -1):

            @pl.when(self.sends(way, 1))
            def _(way=way):
                self.hop(way, 1).start()

    def pass_on(self, way, t):
        came = self.a - way * t

        @pl.when((came >= 0) & (came < self.na))
        def _():
            self.hop(way, t).wait_recv()
            self.to_pair(exclusive_or(came, self.a, self.na)).start()

        if t < self.na - 1:

            @pl.when(self.sends(way, t + 1))
            def _():
                self.hop(way, t + 1).start()

    def finish(self):
        for way in (1, -1):
            for t in range(1, self.na):

                @pl.when(self.sends(way, t))
                def _(way=way, t=t):
                    self.hop(way, t).wait_send()

        for k in range(self.na):
            self.to_pair(k).wait_send()


class Reduce:
    def __init__(self, na, links, part, out, scratch):
        self.na, self.links, self.part, self.out = na, links, part, out
        self.from_q, self.half_sum, self.from_p, self.to_a, self.from_a = scratch[:5]
        self.total, self.parts, self.cols, self.stat = scratch[5:9]
        self.a, self.p, self.q = (lax.axis_index(axis) for axis in ("a", "p", "q"))
        self.rows, self.width = out.shape[1:]
        self.quarter, self.half = self.width // 4, self.width // 2
        self.count = self.rows // HALVES
        self.mine, self.pair = span(2 * self.q + self.p, self.quarter), span(self.q, self.half)
        self.lead = list(range(2, na)) + [1, 0]
        self.step_q, self.step_p, self.step_a = {}, {}, {}
        self.spread_a, self.spread_p, self.spread_q, self.stats = {}, {}, {}, {}

    def at(self, h):
        return slice(h * self.count, (h + 1) * self.count)

    def each(self, h, body):
        def step(i, carry):
            body(pl.ds(pl.multiple_of(h * self.count + i * TILE, TILE), TILE))
            return carry

        lax.fori_loop(0, self.count // TILE, step, 0)

    def send_q(self, h, k):
        at, q = self.at(h), self.q
        source = self.part.at[k, at, span(1 - q, self.half)]
        self.step_q[h, k] = self.links.send(source, self.from_q.at[k, at], {"q": 1 - q})

    def send_p(self, h, k):
        self.step_q[h, k].wait_recv()

        def add(at):
            own = self.part[k, at, span(self.q, self.half)].astype(f32)
            self.half_sum[k, at] = (own + self.from_q[k, at].astype(f32)).astype(bf16)

        self.each(h, add)
        at, p = self.at(h), self.p
        source = self.half_sum.at[k, at, span(1 - p, self.quarter)]
        self.step_p[h, k] = self.links.send(source, self.from_p.at[k, at], {"p": 1 - p})

    def send_a(self, h, k):
        if not k:
            return
        self.step_p[h, k].wait_recv()

        def add(at):
            own = self.half_sum[k, at, span(self.p, self.quarter)].astype(f32)
            self.to_a[k - 1, at] = (own + self.from_p[k, at].astype(f32)).astype(bf16)

        self.each(h, add)
        at = self.at(h)
        self.step_a[h, k] = self.links.send(
            self.to_a.at[k - 1, at], self.from_a.at[k - 1, at], {"a": across(self.a, k)}
        )

    def add_all(self, at):
        own = self.half_sum[0, at, span(self.p, self.quarter)].astype(f32)
        own = own + self.from_p[0, at].astype(f32)
        for k in range(1, self.na):
            own = own + self.from_a[k - 1, at].astype(f32)
        return own

    def scattered(self, h, first, number):
        self.step_p[h, 0].wait_recv()
        for k in range(1, self.na):
            self.step_a[h, k].wait_recv()
        self.each(h, first)
        if number:
            at = self.at(h)
            stats = to_row(self.parts[0, at], 0)
            if number == 2:
                stats = stats + to_row(self.parts[1, at], 1)
            stat = self.stat
            stat[h, 0] = stats
            self.stats[h] = self.links.send(stat.at[h, 0], stat.at[h, 1], {"p": 1 - self.p})

    def stats_q(self, h):
        stat = self.stat
        self.stats[h].wait_recv()
        stat[h, 2] = stat[h, 0] + stat[h, 1]
        self.stats[h] = self.links.send(stat.at[h, 2], stat.at[h, 3], {"q": 1 - self.q})

    def stats_done(self, h, number):
        stat = self.stat
        self.stats[h].wait_recv()
        stats = (stat[h, 2] + stat[h, 3]) / self.width
        for i in range(number):
            self.cols[i, self.at(h)] = to_column(stats, i)

    def spread(self, h, blocks):
        here = self.out.at[0, self.at(h), self.mine]
        for k in blocks:
            if k:
                target = self.out.at[k, self.at(h), self.mine]
                self.spread_a[h, k] = self.links.send(here, target, {"a": across(self.a, k)})
        self.spread_p[h, 0] = self.links.send(here, here, {"p": 1 - self.p})

    def relay_p(self, h, k):
        if not k:
            return
        self.spread_a[h, k].wait_recv()
        here = self.out.at[k, self.at(h), self.mine]
        self.spread_p[h, k] = self.links.send(here, here, {"p": 1 - self.p})

    def relay_q(self, h, k):
        self.spread_p[h, k].wait_recv()
        here = self.out.at[k, self.at(h), self.pair]
        self.spread_q[h, k] = self.links.send(here, here, {"q": 1 - self.q})

    def arrived(self, h, k):
        self.spread_q[h, k].wait_recv()

    def steps(self, first, second, number, chain=False):
        def normed(h):
            self.stats_done(h, number)
            self.each(h, second)

        def spread_own(h):
            here = self.out.at[0, self.at(h), self.mine]
            self.spread_p[h, 0] = self.links.send(here, here, {"p": 1 - self.p})

        def spread_far(h, k):
            here = self.out.at[0, self.at(h), self.mine]
            target = self.out.at[k, self.at(h), self.mine]
            self.spread_a[h, k] = self.links.send(here, target, {"a": across(self.a, k)})

        table = {
            "P": self.send_p,
            "A": self.send_a,
            "SC": lambda h: self.scattered(h, first, number),
            "SQ": self.stats_q,
            "SD": normed,
            "X": spread_own,
            "Z": spread_far,
            "RP": self.relay_p,
            "RQ": self.relay_q,
        }
        if chain:
            lines = [
                Line(
                    self.links,
                    self.na,
                    lambda k, h=h: self.out.at[k, self.at(h), self.mine],
                    self.out.at[0, self.at(h), self.mine],
                )
                for h in range(HALVES)
            ]

            def pair_arrived(h, k):
                self.spread_p[h, k] = lines[h].to_pair(k)
                self.relay_q(h, k)

            table.update(
                X=lambda h: lines[h].to_pair(0).start(),
                Z=lambda h: lines[h].start(),
                FL=lambda h, t: lines[h].pass_on(1, t),
                FR=lambda h, t: lines[h].pass_on(-1, t),
                RQ=pair_arrived,
            )
        return table


class OverHeads:
    def __init__(self, links, na, a, p, q, held, from_a, out_ref):
        self.links, self.na, self.a, self.p, self.q = links, na, a, p, q
        self.held, self.from_a, self.out_ref = held, from_a, out_ref

    def to_pair(self):
        self.copy = self.links.send(self.held.at[0], self.held.at[1], {"p": 1 - self.p})

    def to_core(self):
        held = self.held
        self.copy.wait_recv()
        held[2] = held[0] + held[1]
        self.copy = self.links.send(held.at[2], held.at[3], {"q": 1 - self.q})

    def to_all(self):
        held = self.held
        self.copy.wait_recv()
        held[4] = held[2] + held[3]
        self.copies = [
            self.links.send(held.at[4], self.from_a.at[k - 1], {"a": across(self.a, k)})
            for k in range(1, self.na)
        ]

    def done(self):
        for copy in self.copies:
            copy.wait_recv()
        for k in range(self.na):
            for i in range(2):
                at = 2 * k + i
                total = self.held[4, at : at + 1]
                for j in range(1, self.na):
                    other = 2 * (k ^ j) + i
                    total = total + self.from_a[j - 1, other : other + 1]
                self.out_ref[at : at + 1] = total


def reduce_peers(na):
    a, p, q = lax.axis_index("a"), lax.axis_index("p"), lax.axis_index("q")
    return [{"q": 1 - q}, {"p": 1 - p}] + [{"a": across(a, k)} for k in range(1, na)]


def attn_math(r, tok_ref, gain_ref, proj_ref, inv_ref, res_ref):
    def first(at):
        own = r.add_all(at)
        proj_ref[at] = own
        r.parts[0, at] = fold(own * own)

    def second(at):
        own = proj_ref[at]
        inv = lax.rsqrt(r.cols[0, at] + epsilon)
        inv_ref[at] = inv
        residual = tok_ref[at].astype(f32) + own * wide(inv, r.quarter) * gain_ref[0:1]
        res_ref[at] = residual
        r.out[0, at, r.mine] = residual.astype(bf16)

    return first, second


def mlp_math(r, res_ref, grad_ref, gain_ref, block_ref, sum_ref):
    def first(at):
        own = r.add_all(at)
        r.total[at] = own
        r.parts[0, at] = fold(own * own)
        r.parts[1, at] = fold(grad_ref[at] * gain_ref[1:2] * own)

    def second(at):
        own = r.total[at]
        inv = wide(lax.rsqrt(r.cols[0, at] + epsilon), r.quarter)
        upstream = grad_ref[at]
        scaled = upstream * gain_ref[1:2]
        normed = own * inv
        block_ref[0, at, r.mine] = (res_ref[at] + normed * gain_ref[1:2]).astype(bf16)
        gains = upstream * normed
        sum_ref[...] += jnp.sum(gains.reshape(TILE // 8, 8, r.quarter), axis=0)
        grad = inv * scaled - own * inv * inv * inv * wide(r.cols[1, at], r.quarter)
        r.out[0, at, r.mine] = grad.astype(bf16)

    return first, second


def back_math(r, grad_ref, proj_ref, inv_ref, gain_ref, res_ref, sum_ref):
    def first(at):
        grad = grad_ref[at] + r.add_all(at)
        res_ref[at] = grad
        r.parts[0, at] = fold(grad * gain_ref[0:1] * proj_ref[at])

    def second(at):
        own = proj_ref[at]
        inv = wide(inv_ref[at], r.quarter)
        upstream = res_ref[at]
        gains = upstream * own * inv
        sum_ref[...] += jnp.sum(gains.reshape(TILE // 8, 8, r.quarter), axis=0)
        grad = inv * (upstream * gain_ref[0:1])
        grad = grad - own * inv * inv * inv * wide(r.cols[0, at], r.quarter)
        r.out[0, at, r.mine] = grad.astype(bf16)

    return first, second


MIDDLE = (
    ("F", 2), ("rP", 0, 2), ("F", 3), ("rP", 0, 3), ("rA", 0, 2), ("rP", 1, 3), ("rP", 1, 2), ("F", 1),
    ("rA", 0, 3), ("F", 0), ("rP", 0, 1), ("rA", 1, 3), ("rP", 1, 1), ("rP", 0, 0), ("rA", 1, 2),
    ("rP", 1, 0), ("rA", 0, 1), ("rA", 1, 1), ("rSC", 0), ("rSQ", 0), ("rSC", 1), ("rSD", 0), ("rZ", 0, 3),
    ("rX", 0), ("rSQ", 1), ("rSD", 1), ("rZ", 0, 1), ("BP",), ("rZ", 1, 3), ("rZ", 0, 2), ("rZ", 1, 1),
    ("rRP", 0, 3), ("rX", 1), ("rRP", 0, 1), ("rZ", 1, 2), ("rRQ", 0, 3), ("B", 0, 3), ("rRP", 0, 2),
    ("rRP", 1, 3), ("sP", 0, 3), ("rRQ", 0, 1), ("rRP", 1, 2), ("rRQ", 0, 2), ("rRQ", 1, 3), ("rRP", 1, 1),
    ("B", 0, 2), ("B", 0, 1), ("rRQ", 0, 0), ("sP", 0, 2), ("B", 1, 3), ("sP", 0, 1), ("rRQ", 1, 2),
    ("sA", 0, 3), ("B", 0, 0), ("sP", 1, 3), ("rRQ", 1, 1), ("sA", 0, 2), ("rRQ", 1, 0), ("B", 1, 2),
    ("sP", 0, 0), ("sA", 0, 1), ("B", 1, 1), ("sP", 1, 2), ("B", 1, 0), ("sA", 1, 3), ("sP", 1, 1),
    ("sSC", 0), ("sA", 1, 2), ("BQ",), ("sP", 1, 0), ("sSQ", 0), ("sA", 1, 1), ("sSD", 0), ("sZ", 0, 2),
    ("D",), ("sX", 0), ("sZ", 0, 1), ("sSC", 1), ("sSQ", 1), ("sZ", 0, 3), ("sRP", 0, 2), ("sSD", 1),
    ("sZ", 1, 1), ("sRP", 0, 1), ("sX", 1), ("sRQ", 0, 0), ("G", 2), ("sZ", 1, 3), ("G", 3), ("G", 1),
    ("sRP", 0, 3), ("G", 0), ("sZ", 1, 2), ("sRP", 1, 3), ("sRQ", 0, 1), ("sRQ", 1, 0), ("sRP", 1, 1),
    ("sRP", 1, 2), ("sRQ", 0, 2), ("sRQ", 0, 3), ("sRQ", 1, 3), ("sRQ", 1, 1), ("DS",), ("sRQ", 1, 2),
)


def middle_kernel(na, nb, *refs):
    x_ref, w_ref, res_ref, grad_ref, proj_ref, inv_ref, gain_ref = refs[:7]
    block_ref, back_out, ffn_sum_ref, grad_res_ref, attn_sum_ref, down_sum_ref, gu_grad_ref = refs[7:14]
    out, hidden_ref, grad_gu_ref, gu_ref, part_ref, down_grad, down_held = refs[14:21]
    scratch, (send_sem, recv_sem) = refs[21:-2], refs[-2:]
    units = hidden_ref.shape[2]
    width = x_ref.shape[2]
    b = lax.axis_index("b")
    greet(reduce_peers(na) + [{"b": across(b, j)} for j in range(1, nb)])
    links = Links(send_sem, recv_sem)
    r = Reduce(na, links, part_ref, out, scratch[:9])
    s = Reduce(na, links, part_ref, back_out, scratch[9:])
    ffn_sum_ref[...] = jnp.zeros_like(ffn_sum_ref)
    attn_sum_ref[...] = jnp.zeros_like(attn_sum_ref)
    wide_tile = 512

    def forward(k):
        def gated(n, carry):
            at, up_at = span(n, 256), pl.ds(pl.multiple_of(units + n * 256, 256), 256)
            gate = dot(x_ref[k], w_ref[:, at])
            up = dot(x_ref[k], w_ref[:, up_at])
            gu_ref[k, :, at] = gate
            gu_ref[k, :, up_at] = up
            hidden_ref[k, :, at] = (gate * jax.nn.sigmoid(gate) * up).astype(bf16)
            return carry

        lax.fori_loop(0, units // 256, gated, 0)

        def down(n, carry):
            at = span(n, wide_tile)
            part_ref[k, :, at] = dot_t(hidden_ref[k], w_ref[at, 2 * units :]).astype(bf16)
            return carry

        lax.fori_loop(0, width // wide_tile, down, 0)

    def backward(h, k):
        rows = r.at(h)

        def gated(n, carry):
            at, up_at = span(n, 256), pl.ds(pl.multiple_of(units + n * 256, 256), 256)
            down_at = pl.ds(pl.multiple_of(2 * units + n * 256, 256), 256)
            grad_hidden = dot(out[k, rows], w_ref[:, down_at])
            gate, up = gu_ref[k, rows, at], gu_ref[k, rows, up_at]
            sigmoid = jax.nn.sigmoid(gate)
            active = gate * sigmoid
            grad_gu_ref[k, rows, at] = (
                grad_hidden * up * (sigmoid * (1.0 + gate * (1.0 - sigmoid)))
            ).astype(bf16)
            grad_gu_ref[k, rows, up_at] = (grad_hidden * active).astype(bf16)
            return carry

        lax.fori_loop(0, units // 256, gated, 0)

        def back(n, carry):
            at = span(n, wide_tile)
            part_ref[k, rows, at] = dot_t(
                grad_gu_ref[k, rows], w_ref[at, : 2 * units]
            ).astype(bf16)
            return carry

        lax.fori_loop(0, width // wide_tile, back, 0)

    first, second = mlp_math(r, res_ref, grad_ref, gain_ref, block_ref, ffn_sum_ref)
    back_first, back_second = back_math(
        s, grad_ref, proj_ref, inv_ref, gain_ref, grad_res_ref, attn_sum_ref
    )
    copies, reused = {}, []
    columns = slice(0, units)

    def forward_step(k):
        forward(k)
        for h in range(HALVES):
            r.send_q(h, k)

    def backward_step(h, k):
        if not reused:
            links.sent(r.step_q.values())
            reused.append(True)
        r.arrived(h, k)
        backward(h, k)
        s.send_q(h, k)

    def block_p():
        here = block_ref.at[0, :, r.mine]
        copies["p"] = links.send(here, here, {"p": 1 - r.p})

    def block_q():
        copies["p"].wait_recv()
        here = block_ref.at[0, :, r.pair]
        copies["q"] = links.send(here, here, {"q": 1 - r.q})

    def down_grads():
        for block in range(na):
            weight_grad(out, hidden_ref, down_grad, block)
        copies["b"] = exchange_b(links, down_grad, down_held, columns)

    table = {
        "F": forward_step,
        "B": backward_step,
        "BP": block_p,
        "BQ": block_q,
        "D": down_grads,
        "DS": lambda: sum_b(
            copies["b"], lambda block: down_grad.at[block, b], down_held, down_sum_ref, columns
        ),
        "G": lambda block: weight_grad(x_ref, grad_gu_ref, gu_grad_ref, block),
    }
    table.update({"r" + key: step for key, step in r.steps(first, second, 2).items()})
    table.update({"s" + key: step for key, step in s.steps(back_first, back_second, 1).items()})
    for key, *where in MIDDLE:
        table[key](*where)
    for h in range(HALVES):
        for k in range(na):
            s.arrived(h, k)
    copies["q"].wait_recv()
    links.finish()


def middle_call(nb, x_all, w_mlp, res_mine, grad_mine, proj_mine, inv_mine, width_gain):
    na, rows, width = x_all.shape
    quarter, units = width // 4, w_mlp.shape[1] // 3
    w_rows = width // (na * nb)
    vmem = pl.BlockSpec(memory_space=pltpu.VMEM)
    shape = jax.ShapeDtypeStruct
    outs = (
        shape((1, rows, width), bf16),
        shape((na, rows, width), bf16),
        shape((8, quarter), f32),
        shape((rows, quarter), f32),
        shape((8, quarter), f32),
        shape((na, w_rows, units), bf16),
        shape((na, nb, w_rows, 2 * units), bf16),
    )
    copies = 2 * HALVES * (6 * na + 1) + 2 + nb
    return pl.pallas_call(
        functools.partial(middle_kernel, na, nb),
        out_shape=outs,
        in_specs=[vmem] * 7,
        out_specs=(vmem,) * len(outs),
        scratch_shapes=[
            pltpu.VMEM((na, rows, width), bf16),
            pltpu.VMEM((na, rows, units), bf16),
            pltpu.VMEM((na, rows, 2 * units), bf16),
            pltpu.VMEM((na, rows, 2 * units), f32),
            pltpu.VMEM((na, rows, width), bf16),
            pltpu.VMEM((na, nb, w_rows, units), bf16),
            pltpu.VMEM((nb - 1, na, w_rows, units), bf16),
        ]
        + reduce_scratch(na, rows, width)
        + reduce_scratch(na, rows, width)
        + [pltpu.SemaphoreType.DMA((copies,)), pltpu.SemaphoreType.DMA((copies,))],
        compiler_params=pltpu.CompilerParams(
            collective_id=2, has_side_effects=True, vmem_limit_bytes=VMEM_LIMIT
        ),
        name="middle",
    )(x_all, w_mlp, res_mine, grad_mine, proj_mine, inv_mine, width_gain)


def last_kernel(na, nb, *refs):
    proj_ref, x_far, qkv_ref, stats_ref, gain_ref, cos_ref, sin_ref, w_ref, att_ref = refs[:9]
    grad_ref, attn_sum_ref, ffn_sum_ref, down_sum_ref, gu_grad_far = refs[9:14]
    out, sums_ref, down_far, gu_far, qkv_out, wout_out = refs[14:20]
    scaled_ref, grad_qkv_ref, part_ref, head_sums, held, stats_a, inner_ref = refs[20:27]
    own_sums, a_sums, b_sums, gu_held, gu_sum, attn_grad, attn_held, attn_sum = refs[27:35]
    down_in, gu_in, attn_in, x_ref, gu_own, down_out, gu_out = refs[35:42]
    scratch, (local_sem, send_sem, recv_sem) = refs[42:-3], refs[-3:]
    links = Links(send_sem, recv_sem)
    load_gu = pltpu.make_async_copy(
        gu_grad_far.at[:, lax.axis_index("b")], gu_own, local_sem.at[0]
    )
    load_gu.start()
    load_x = pltpu.make_async_copy(x_far, x_ref, local_sem.at[1])
    load_x.start()
    r = Reduce(na, links, part_ref, out, scratch)
    a, b, p, q, mine, pair, quarter = (
        r.a, lax.axis_index("b"), r.p, r.q, r.mine, r.pair, r.quarter,
    )
    units = down_sum_ref.shape[2]
    own_sums[...] = jnp.zeros_like(own_sums)
    own_sums[0:1, mine] = jnp.sum(attn_sum_ref[...], axis=0, keepdims=True)
    own_sums[1:2, mine] = jnp.sum(ffn_sum_ref[...], axis=0, keepdims=True)
    greet(reduce_peers(na) + [{"b": across(b, j)} for j in range(1, nb)])
    far = list(range(2, na)) + [1]

    def to_owners(source, target, columns):
        return [
            (k, links.send(
                source.at[across(a, k), :, columns], target.at[k - 1, :, columns], {"a": across(a, k)}
            ))
            for k in far
        ]

    whole = slice(0, units)
    halves = [slice(0, units), slice(units, 2 * units)]
    down_copies = to_owners(down_sum_ref, down_in, whole)
    gu_b = [exchange_b(links, gu_grad_far, gu_held, columns) for columns in halves]
    here = own_sums.at[:, mine]
    sums_p = links.send(here, here, {"p": 1 - p})

    held[0] = jnp.zeros_like(held[0])
    head_sums[...] = jnp.zeros_like(head_sums)

    def attend_back(k, carry):
        queries, key_rows, values, q_inv, k_inv, q_rot, k_rot, probs = attention(
            k, qkv_ref[k], stats_ref[...], gain_ref, cos_ref, sin_ref
        )
        cos_table, sine_table = cos_ref[...], sin_ref[...]
        grad_att = dot(proj_ref[k], w_ref[:, 3 * HD :]).astype(bf16)
        grad_v = t_dot(probs.astype(bf16), grad_att)
        grad_p = dot_t(grad_att, values)
        delta = jnp.sum(probs * grad_p, axis=1, keepdims=True)
        grad_scores = (probs * (grad_p - delta) * HD ** (-0.5)).astype(bf16)
        grad_q = dot(grad_scores, k_rot)
        grad_k = t_dot(grad_scores, q_rot)
        grad_q = grad_q * cos_table + rotate_back(grad_q * sine_table)
        grad_k = grad_k * cos_table + rotate_back(grad_k * sine_table)
        head_sums[0:1] += jnp.sum(grad_q * queries * q_inv, axis=0, keepdims=True)
        head_sums[1:2] += jnp.sum(grad_k * key_rows * k_inv, axis=0, keepdims=True)
        scaled_q = grad_q * gain_ref[0:1]
        scaled_k = grad_k * gain_ref[1:2]
        scaled_ref[k, :, :HD] = scaled_q
        scaled_ref[k, :, HD:] = scaled_k
        grad_qkv_ref[k, :, 2 * HD :] = grad_v.astype(bf16)
        held[0] += to_row(scaled_q * queries, 2 * k) + to_row(scaled_k * key_rows, 2 * k + 1)
        return carry

    lax.fori_loop(0, na, attend_back, 0)
    sums_p.wait_recv()
    here = own_sums.at[:, pair]
    sums_q = links.send(here, here, {"q": 1 - q})
    gu_copies = []

    def sent():
        for block in range(na):
            weight_grad(proj_ref, att_ref, attn_grad, block, slice(3 * HD, 4 * HD))
        load_gu.wait()
        sum_b(gu_b[0], lambda block: gu_own.at[block], gu_held, gu_sum, halves[0])
        gu_copies.append(to_owners(gu_sum, gu_in, halves[0]))

    over_heads = OverHeads(links, na, a, p, q, held, stats_a, inner_ref)
    over_heads.to_pair()
    over_heads.to_core()
    over_heads.to_all()
    sent()
    over_heads.done()

    def qkv_back(k):
        for i in range(2):
            at = slice(i * HD, (i + 1) * HD)
            inv = lax.rsqrt(to_column(stats_ref[...] / HQ, 2 * k + i) + epsilon)
            mean = to_column(inner_ref[...] / HQ, 2 * k + i)
            grad = inv * scaled_ref[k, :, at] - qkv_ref[k, :, at] * inv * inv * inv * mean
            grad_qkv_ref[k, :, at] = grad.astype(bf16)

        def part(n, carry):
            at = span(n, 512)
            part_ref[k, :, at] = dot_t(grad_qkv_ref[k], w_ref[at, : 3 * HD]).astype(bf16)
            return carry

        lax.fori_loop(0, part_ref.shape[2] // 512, part, 0)

    for k in r.lead:
        qkv_back(k)
        for h in range(HALVES):
            r.send_q(h, k)
    for h in range(HALVES):
        for k in r.lead:
            r.send_p(h, k)
    load_x.wait()
    for block in range(na):
        weight_grad(x_ref, grad_qkv_ref, attn_grad, block, slice(0, 3 * HD))
    attn_columns = slice(0, 4 * HD)
    attn_b = exchange_b(links, attn_grad, attn_held, attn_columns)
    for h in range(HALVES):
        for k in r.lead:
            r.send_a(h, k)
    sums_q.wait_recv()
    sums_a = [
        links.send(own_sums.at[:, span(across(a, k), quarter)], a_sums.at[k - 1], {"a": across(a, k)})
        for k in range(1, na)
    ]
    sum_b(gu_b[1], lambda block: gu_own.at[block], gu_held, gu_sum, halves[1])
    gu_copies.append(to_owners(gu_sum, gu_in, halves[1]))

    def first(at):
        out[0, at, mine] = (grad_ref[at] + r.add_all(at)).astype(bf16)

    for h in range(HALVES):
        r.scattered(h, first, 0)
        r.spread(h, [0])
    for copy in sums_a:
        copy.wait_recv()
    total = own_sums[:, span(a, quarter)]
    for k in range(1, na):
        total = total + a_sums[k - 1]
    b_sums[0, :, :quarter] = total
    b_sums[0, :, quarter:] = head_sums[...]
    sums_b = [links.send(b_sums.at[0], b_sums.at[j], {"b": across(b, j)}) for j in range(1, nb)]
    for h in range(HALVES):
        r.relay_q(h, 0)
    sum_b(attn_b, lambda block: attn_grad.at[block, b], attn_held, attn_sum, attn_columns)
    attn_copies = to_owners(attn_sum, attn_in, attn_columns)

    def store(target, index, size, value):
        target[:, span(index, size)] = value.astype(f32)

    store(down_out, a, units, down_sum_ref[a])
    for c in range(2):
        gu_out[:, c, span(a, units)] = gu_sum[a, :, halves[c]].astype(f32)
    for c in range(3):
        store(qkv_out.at[c], a, HD, attn_sum[a, :, c * HD : (c + 1) * HD])
    store(wout_out, a, HD, attn_sum[a, :, 3 * HD :])
    for k, copy in down_copies:
        copy.wait_recv()
        store(down_out, across(a, k), units, down_in[k - 1])
    save_down = pltpu.make_async_copy(down_out, down_far, local_sem.at[2])
    save_down.start()
    for copy in sums_b:
        copy.wait_recv()
    total = b_sums[0]
    for j in range(1, nb):
        total = total + b_sums[j]
    sums_ref[...] = total
    for c in range(2):
        for k, copy in gu_copies[c]:
            copy.wait_recv()
            gu_out[:, c, span(across(a, k), units)] = gu_in[k - 1, :, halves[c]].astype(f32)
    save_gu = pltpu.make_async_copy(gu_out, gu_far, local_sem.at[3])
    save_gu.start()
    for k, copy in attn_copies:
        copy.wait_recv()
        for c in range(3):
            store(qkv_out.at[c], across(a, k), HD, attn_in[k - 1, :, c * HD : (c + 1) * HD])
        store(wout_out, across(a, k), HD, attn_in[k - 1, :, 3 * HD :])
    for h in range(HALVES):
        r.arrived(h, 0)
    save_down.wait()
    save_gu.wait()
    links.finish()


def last_call(nb, *operands):
    na, rows, width = operands[0].shape
    w_rows, units = operands[12].shape[1:]
    quarter = width // 4
    vmem, far = pl.BlockSpec(memory_space=pltpu.VMEM), pl.BlockSpec(memory_space=pl.ANY)
    shape = jax.ShapeDtypeStruct
    outs = (
        shape((1, rows, width), bf16),
        shape((8, quarter + HD), f32),
        shape((w_rows, na * units), f32),
        shape((w_rows, 2, na * units), f32),
        shape((3, w_rows, na * HD), f32),
        shape((w_rows, na * HD), f32),
    )
    copies = HALVES * (3 * na + 1) + 2 + 6 * na + 4 * nb
    return pl.pallas_call(
        functools.partial(last_kernel, na, nb),
        out_shape=outs,
        in_specs=[far if i in (1, 13) else vmem for i in range(14)],
        out_specs=(vmem, vmem, far, far, vmem, vmem),
        scratch_shapes=[
            pltpu.VMEM((na, rows, 2 * HD), f32),
            pltpu.VMEM((na, rows, 3 * HD), bf16),
            pltpu.VMEM((na, rows, width), bf16),
            pltpu.VMEM((8, HD), f32),
            pltpu.VMEM((5, 8, rows), f32),
            pltpu.VMEM((na - 1, 8, rows), f32),
            pltpu.VMEM((8, rows), f32),
            pltpu.VMEM((8, width), f32),
            pltpu.VMEM((na - 1, 8, quarter), f32),
            pltpu.VMEM((nb, 8, quarter + HD), f32),
            pltpu.VMEM((nb - 1, na, w_rows, 2 * units), bf16),
            pltpu.VMEM((na, w_rows, 2 * units), bf16),
            pltpu.VMEM((na, nb, w_rows, 4 * HD), bf16),
            pltpu.VMEM((nb - 1, na, w_rows, 4 * HD), bf16),
            pltpu.VMEM((na, w_rows, 4 * HD), bf16),
            pltpu.VMEM((na - 1, w_rows, units), bf16),
            pltpu.VMEM((na - 1, w_rows, 2 * units), bf16),
            pltpu.VMEM((na - 1, w_rows, 4 * HD), bf16),
            pltpu.VMEM((na, rows, width), bf16),
            pltpu.VMEM((na, w_rows, 2 * units), bf16),
            pltpu.VMEM((w_rows, na * units), f32),
            pltpu.VMEM((w_rows, 2, na * units), f32),
        ]
        + reduce_scratch(na, rows, width)
        + [
            pltpu.SemaphoreType.DMA((4,)),
            pltpu.SemaphoreType.DMA((copies,)),
            pltpu.SemaphoreType.DMA((copies,)),
        ],
        compiler_params=pltpu.CompilerParams(
            collective_id=4, has_side_effects=True, vmem_limit_bytes=VMEM_LIMIT
        ),
        name="last",
    )(*operands)


def reduce_scratch(na, rows, width):
    quarter = width // 4
    return [
        pltpu.VMEM((na, rows, width // 2), bf16),
        pltpu.VMEM((na, rows, width // 2), bf16),
        pltpu.VMEM((na, rows, quarter), bf16),
        pltpu.VMEM((na - 1, rows, quarter), bf16),
        pltpu.VMEM((na - 1, rows, quarter), bf16),
        pltpu.VMEM((rows, quarter), f32),
        pltpu.VMEM((2, rows, 128), f32),
        pltpu.VMEM((2, rows, 128), f32),
        pltpu.VMEM((HALVES, 4, 8, rows // HALVES), f32),
    ]


ENTER = (
    ("Z", 0), ("W", 3), ("FW", 0), ("FR", 0, 1), ("FL", 0, 1), ("W", 1), ("CUT", 2), ("FW", 1), ("W", 2),
    ("FR", 0, 2), ("FR", 0, 3), ("CUT", 3), ("M", 0, 3), ("FL", 0, 2), ("CUT", 1), ("FW", 3), ("FL", 0, 3),
    ("GA",), ("FT", 0), ("FQ", 3), ("FW", 2), ("CUT", 0), ("FQ", 2), ("M", 0, 1), ("M", 2, 3), ("FQ", 1),
    ("J", 3), ("FQ", 0), ("J", 0), ("GB",), ("M", 1, 1), ("J", 1), ("J", 2), ("S1",), ("S2",), ("S3",),
    ("M", 1, 3), ("MR", 1, 0), ("M", 1, 2), ("S4",), ("E", 3), ("E", 1), ("rP", 1, 3), ("E", 2),
    ("rP", 1, 1), ("M", 2, 1), ("MR", 2, 3), ("rP", 0, 3), ("rP", 0, 1), ("MR", 0, 3), ("E", 0),
    ("rA", 1, 3), ("MR", 2, 0), ("rA", 1, 1), ("MR", 0, 1), ("rA", 0, 3), ("MR", 1, 3), ("rP", 0, 2),
    ("MR", 2, 1), ("rA", 0, 2), ("rA", 0, 1), ("rP", 0, 0), ("rP", 1, 2), ("rA", 1, 2), ("MR", 1, 2),
    ("rP", 1, 0), ("rSC", 0), ("rSQ", 0), ("MR", 0, 0), ("M", 2, 2), ("rSC", 1), ("rSD", 0), ("rSQ", 1),
    ("rX", 0), ("rSD", 1), ("rZ", 0), ("rZ", 1), ("rFR", 0, 1), ("rFL", 0, 1), ("rX", 1), ("MR", 2, 2),
    ("rFR", 1, 1), ("rFL", 1, 1), ("rFR", 0, 2), ("rRQ", 0, 0), ("rFL", 1, 2), ("rFL", 0, 2), ("MR", 1, 1),
    ("rFR", 0, 3), ("M", 0, 2), ("rFR", 1, 2), ("rFL", 1, 3), ("rFR", 1, 3), ("rFL", 0, 3), ("rRQ", 0, 1),
    ("MR", 0, 2), ("rRQ", 1, 1), ("rRQ", 1, 2), ("rRQ", 0, 2), ("rRQ", 1, 0), ("rRQ", 1, 3), ("rRQ", 0, 3),
)


def enter_kernel(na, nb, *refs):
    tok_ref, qkv_w_ref, wout_ref, gu_ref, down_ref, cos_ref, sin_ref = refs[:7]
    gain_refs = refs[7:11]
    x_far, w_far, mlp_w_ref, width_gain_ref, head_gain_ref, qkv_far, stats_ref, att_far = refs[11:19]
    out, proj_ref, inv_ref, res_ref = refs[19:23]
    own_gains, gains_ref, piece_ref, part_ref, held, stats_a = refs[23:29]
    x_ref, w_ref, qkv_ref, att_ref = refs[29:33]
    scratch, (local_sem, send_sem, recv_sem) = refs[33:-3], refs[-3:]
    saves = [
        pltpu.make_async_copy(near, there, local_sem.at[5 + i])
        for i, (near, there) in enumerate(
            ((x_ref, x_far), (w_ref, w_far), (qkv_ref, qkv_far), (att_ref, att_far))
        )
    ]
    a, b, p, q = (lax.axis_index(axis) for axis in ("a", "b", "p", "q"))
    rows = wout_ref.shape[0]
    quarter = tok_ref.shape[1]
    units = down_ref.shape[1] // na
    own_gains[...] = jnp.zeros_like(own_gains)
    for i, ref in enumerate(gain_refs):
        own_gains[i : i + 1, : ref.shape[1]] = ref[...].astype(f32)
    gains_ref[a, b] = own_gains[...]
    greet(
        [{"q": 1 - q}, {"p": 1 - p}]
        + [{"a": across(a, k)} for k in range(1, na)]
        + [{"b": across(b, j)} for j in range(1, nb)]
    )
    links = Links(send_sem, recv_sem)
    mine, pair = span(2 * q + p, quarter), span(q, 2 * quarter)
    place = span(a * nb + b, rows)
    copies, ends = {}, []
    locals_ = [pltpu.make_async_copy(tok_ref, x_ref.at[0, :, mine], local_sem.at[0])]

    def weight_sources(k):
        block = span(across(a, k), HD)
        sources = [qkv_w_ref.at[c, :, block] for c in range(3)] + [wout_ref.at[:, block]]
        return [(s, w_ref.at[place, c * HD : (c + 1) * HD]) for c, s in enumerate(sources)]

    for c, (source, target) in enumerate(weight_sources(0)):
        locals_.append(pltpu.make_async_copy(source, target, local_sem.at[1 + c]))
    for copy in locals_:
        copy.start()

    def send_gains():
        copies["g"] = [
            links.send(own_gains, gains_ref.at[a, b], {"a": across(a, k)}) for k in range(1, na)
        ]

    def relay_gains():
        for copy in copies["g"]:
            copy.wait_recv()
        at = gains_ref.at[:, b]
        copies["gb"] = [links.send(at, at, {"b": across(b, j)}) for j in range(1, nb)]

    def send_weights(k):
        copies["w", k] = [
            links.send(source, target, {"a": across(a, k)}) for source, target in weight_sources(k)
        ]

    def relay_weights(k):
        if k:
            for copy in copies["w", k]:
                copy.wait_recv()
        else:
            for copy in locals_[1:]:
                copy.wait()
        at = w_ref.at[span(across(a, k) * nb + b, rows), :]
        copies["wb", k] = [links.send(at, at, {"b": across(b, j)}) for j in range(1, nb)]

    line = Line(links, na, lambda k: x_ref.at[k, :, mine], tok_ref)

    def own_tokens(_):
        locals_[0].wait()
        line.to_pair(0).start()

    def pair_tokens(k):
        line.to_pair(k).wait_recv()
        at = x_ref.at[k, :, pair]
        copies["x", k] = links.send(at, at, {"q": 1 - q})

    def cut_weights(k):
        block = span(across(a, k), units)

        def cut(i, carry):
            at = pl.ds(pl.multiple_of(i * TILE, TILE), TILE)
            cuts = (gu_ref[at, 0, block], gu_ref[at, 1, block], down_ref[at, block])
            for c in range(3):
                if k:
                    piece_ref[k - 1, c, at] = cuts[c]
                else:
                    to = pl.ds(pl.multiple_of((a * nb + b) * rows + i * TILE, TILE), TILE)
                    mlp_w_ref[to, c * units : (c + 1) * units] = cuts[c]
            return carry

        lax.fori_loop(0, rows // TILE, cut, 0)

    def send_piece(c, k):
        target = mlp_w_ref.at[place, c * units : (c + 1) * units]
        copies["m", c, k] = links.send(piece_ref.at[k - 1, c], target, {"a": across(a, k)})

    def relay_piece(c, k):
        if k:
            copies["m", c, k].wait_recv()
        at = mlp_w_ref.at[span(across(a, k) * nb + b, rows), c * units : (c + 1) * units]
        ends.extend(links.send(at, at, {"b": across(b, j)}) for j in range(1, nb))

    arrived, ready = set(), []

    def project(k):
        if not arrived:
            held[0] = jnp.zeros_like(held[0])
            for i in range(na):
                for copy in copies["wb", i]:
                    copy.wait_recv()
        arrived.add(k)
        copies["x", k].wait_recv()

        def chunk(i, carry):
            at = span(i, 128)
            proj = dot(x_ref[k, at], w_ref[:, : 3 * HD])
            qkv_ref[k, at] = proj
            queries, key_rows = proj[:, :HD], proj[:, HD : 2 * HD]
            held[0, :, at] += to_row(queries * queries, 2 * k) + to_row(key_rows * key_rows, 2 * k + 1)
            return carry

        lax.fori_loop(0, x_ref.shape[1] // 128, chunk, 0)

    over_heads = OverHeads(links, na, a, p, q, held, stats_a, stats_ref)

    def all_stats():
        for save in saves[:3]:
            save.start()
        over_heads.done()
        for copy in copies["gb"]:
            copy.wait_recv()
        n_d, n_h = gain_refs[0].shape[1], gain_refs[2].shape[1]
        width_gain_ref[...] = jnp.zeros_like(width_gain_ref)
        head_gain_ref[...] = jnp.zeros_like(head_gain_ref)
        for i in range(2):
            width_gain_ref[i : i + 1] = jnp.concatenate(
                [gains_ref[2 * q + p, j, i : i + 1, :n_d] for j in range(nb)], axis=1
            )
            head_gain_ref[i : i + 1] = jnp.concatenate(
                [gains_ref[a, j, i + 2 : i + 3, :n_h] for j in range(nb)], axis=1
            )

    r = Reduce(na, links, part_ref, out, scratch)

    def attend(k):
        values, probs = (
            attention(k, qkv_ref[k], stats_ref[...], head_gain_ref, cos_ref, sin_ref)[i] for i in (2, 7)
        )
        attended = dot(probs.astype(bf16), values).astype(bf16)
        att_ref[k] = attended

        def part(n, carry):
            at = span(n, 512)
            part_ref[k, :, at] = dot_t(att_ref[k], w_ref[at, 3 * HD :]).astype(bf16)
            return carry

        lax.fori_loop(0, part_ref.shape[2] // 512, part, 0)
        for h in range(HALVES):
            r.send_q(h, k)

    first, second = attn_math(r, tok_ref, width_gain_ref, proj_ref, inv_ref, res_ref)
    table = {
        "GA": send_gains,
        "GB": relay_gains,
        "W": send_weights,
        "FW": relay_weights,
        "Z": lambda _: line.start(),
        "FL": lambda _, t: line.pass_on(1, t),
        "FR": lambda _, t: line.pass_on(-1, t),
        "FT": own_tokens,
        "FQ": pair_tokens,
        "CUT": cut_weights,
        "M": send_piece,
        "MR": relay_piece,
        "J": project,
        "S1": over_heads.to_pair,
        "S2": over_heads.to_core,
        "S3": over_heads.to_all,
        "S4": all_stats,
        "E": attend,
    }
    table.update({"r" + key: step for key, step in r.steps(first, second, 1, True).items()})
    for key, *where in ENTER:
        table[key](*where)
    saves[3].start()
    for h in range(HALVES):
        for k in range(na):
            r.arrived(h, k)
    for copy in ends:
        copy.wait_recv()
    for save in saves:
        save.wait()
    links.finish()


def enter_call(na, nb, tok_mine, qkv, w_out, gu, down, cos_table, sine_table, gains):
    rows, quarter = tok_mine.shape
    width = 4 * quarter
    w_rows, units = down.shape[0], down.shape[1] // na
    lanes = max(128, gains[0].shape[1])
    vmem, far = pl.BlockSpec(memory_space=pltpu.VMEM), pl.BlockSpec(memory_space=pl.ANY)
    shape = jax.ShapeDtypeStruct
    full = shape((na, rows, width), bf16)
    outs = [
        full,
        shape((width, 4 * HD), bf16),
        shape((width, 3 * units), bf16),
        shape((8, quarter), f32),
        shape((8, HD), f32),
        shape((na, rows, 3 * HD), f32),
        shape((8, rows), f32),
        shape((na, rows, HD), bf16),
        full,
        shape((rows, quarter), f32),
        shape((rows, 128), f32),
        shape((rows, quarter), f32),
    ]
    copies = 90 + 16 * nb
    return pl.pallas_call(
        functools.partial(enter_kernel, na, nb),
        out_shape=tuple(outs),
        in_specs=[vmem] * 11,
        out_specs=tuple(far if i in (0, 1, 5, 7) else vmem for i in range(len(outs))),
        scratch_shapes=[
            pltpu.VMEM((8, lanes), f32),
            pltpu.VMEM((na, nb, 8, lanes), f32),
            pltpu.VMEM((na - 1, 3, w_rows, units), bf16),
            pltpu.VMEM((na, rows, width), bf16),
            pltpu.VMEM((5, 8, rows), f32),
            pltpu.VMEM((na - 1, 8, rows), f32),
            pltpu.VMEM((na, rows, width), bf16),
            pltpu.VMEM((width, 4 * HD), bf16),
            pltpu.VMEM((na, rows, 3 * HD), f32),
            pltpu.VMEM((na, rows, HD), bf16),
        ]
        + reduce_scratch(na, rows, width)
        + [
            pltpu.SemaphoreType.DMA((9,)),
            pltpu.SemaphoreType.DMA((copies,)),
            pltpu.SemaphoreType.DMA((copies,)),
        ],
        compiler_params=pltpu.CompilerParams(
            collective_id=5, has_side_effects=True, vmem_limit_bytes=VMEM_LIMIT
        ),
        name="enter",
    )(tok_mine, qkv, w_out, gu, down, cos_table, sine_table, *gains)


def rope_tables(length, width):
    half_width = width // 2
    inv_freq = rope_base ** (-(jnp.arange(half_width, dtype=f32) * 2.0) / width)
    angles = jnp.arange(length, dtype=f32)[:, None] * inv_freq[None, :]
    cos_table = jnp.concatenate([jnp.cos(angles), jnp.cos(angles)], axis=1)
    sine_table = jnp.concatenate([jnp.sin(angles), jnp.sin(angles)], axis=1)
    return cos_table, sine_table


def on_device(
    tokens,
    qkv_weight,
    out_weight,
    gu_weight,
    down_weight,
    attn_gain,
    ffn_gain,
    q_gain,
    k_gain,
    out_grad,
):
    na, nb = lax.axis_size("a"), lax.axis_size("b")
    a, b = lax.axis_index("a"), lax.axis_index("b")
    share = lax.axis_index("q") * 2 + lax.axis_index("p")
    rows, width = tokens.shape
    quarter = width // 4
    w_rows = out_weight.shape[0]
    units = down_weight.shape[1] // na

    def quarter_of(operand):
        return lax.dynamic_slice_in_dim(operand, share * quarter, quarter, 1)

    tok_mine, grad_mine = quarter_of(tokens), quarter_of(out_grad)
    cos_table, sine_table = rope_tables(SEQ_LEN, HD)
    (
        x_all,
        w_attn,
        w_mlp,
        width_gain,
        head_gain,
        qkv,
        stats,
        attended,
        res_all,
        proj_mine,
        inv_mine,
        res_mine,
    ) = enter_call(
        na,
        nb,
        tok_mine,
        qkv_weight.transpose(1, 0, 2),
        out_weight,
        gu_weight,
        down_weight,
        cos_table,
        sine_table,
        [gain[None] for gain in (attn_gain, ffn_gain, q_gain, k_gain)],
    )
    n_d, n_h = attn_gain.shape[0], q_gain.shape[0]
    block_rows, grad_proj, ffn_sums, grad_res, attn_sums, down_sum, gu_grad = middle_call(
        nb, res_all, w_mlp, res_mine, grad_mine, proj_mine, inv_mine, width_gain
    )
    grad_rows, sums, down_grad, gu_grad, qkv_grad, out_grad_w = last_call(
        nb,
        grad_proj,
        x_all,
        qkv,
        stats,
        head_gain,
        cos_table,
        sine_table,
        w_attn,
        attended,
        grad_res,
        attn_sums,
        ffn_sums,
        down_sum,
        gu_grad,
    )
    width_sums = lax.dynamic_slice_in_dim(sums[:2, :quarter], b * n_d, n_d, 1)
    head_sums = lax.dynamic_slice_in_dim(sums[:2, quarter:], b * n_h, n_h, 1)
    return (
        block_rows[0].astype(f32),
        grad_rows[0].astype(f32),
        qkv_grad.transpose(1, 0, 2),
        out_grad_w,
        gu_grad,
        down_grad,
        width_sums[0],
        width_sums[1],
        head_sums[0],
        head_sums[1],
    )


def solution(mesh):
    dp, tp = mesh.shape["dp"], mesh.shape["tensor"]
    na = HEADS // tp
    fine = Mesh(mesh.devices.reshape(na, dp // na, tp // 2, 2), ("a", "b", "p", "q"))
    dp_axes, tp_axes = ("a", "b"), ("p", "q")
    both = tp_axes + dp_axes
    return jax.shard_map(
        on_device,
        mesh=fine,
        in_specs=(
            P(dp_axes, None),
            P(dp_axes, None, tp_axes),
            P(dp_axes, tp_axes),
            P(dp_axes, None, tp_axes),
            P(dp_axes, tp_axes),
            P(dp_axes),
            P(dp_axes),
            P(both),
            P(both),
            P(dp_axes, None),
        ),
        out_specs=(
            P(dp_axes, None),
            P(dp_axes, None),
            P(dp_axes, None, tp_axes),
            P(dp_axes, tp_axes),
            P(dp_axes, None, tp_axes),
            P(dp_axes, tp_axes),
            P(dp_axes),
            P(dp_axes),
            P(both),
            P(both),
        ),
        check_vma=False,
    )
```

```python
import functools

import jax
import jax.numpy as jnp
from jax import lax
from jax.experimental import pallas as pl
from jax.experimental.pallas import tpu as pltpu
from jax.sharding import Mesh, PartitionSpec as P

HEADS = 16
HD = 128
SEQ_LEN = 256
HQ = 2048

epsilon = 1e-06
rope_base = 500000.0

f32 = jnp.float32
bf16 = jnp.bfloat16
MESH = pl.DeviceIdType.MESH
EXACT = lax.Precision.HIGHEST
VMEM_LIMIT = 60 * 1024 * 1024
TILE = 32
HALVES = 2


def flip(index, bit):
    return index + bit - 2 * bit * ((index // bit) % 2)


def across(index, k):
    bit = 1
    while bit <= k:
        if k & bit:
            index = flip(index, bit)
        bit *= 2
    return index


def exclusive_or(left, right, count):
    total, bit = 0, 1
    while bit < count:
        total = total + bit * ((left // bit + right // bit) % 2)
        bit *= 2
    return total


def pick(operand, index, axis):
    return lax.dynamic_index_in_dim(operand, index, axis, keepdims=False)


def span(index, size):
    return pl.ds(pl.multiple_of(index * size, size), size)


class Links:
    def __init__(self, send_sem, recv_sem):
        self.send_sem, self.recv_sem, self.count = send_sem, recv_sem, 0
        self.copies, self.lines = [], []

    def send(self, source, target, device):
        copy = self.copy(self.count, source, target, device)
        copy.start()
        self.count += 1
        self.copies.append(copy)
        return copy

    def reserve(self, number):
        self.count += number
        return self.count - number

    def copy(self, index, source, target, device):
        return pltpu.make_async_remote_copy(
            src_ref=source,
            dst_ref=target,
            send_sem=self.send_sem.at[index],
            recv_sem=self.recv_sem.at[index],
            device_id=device,
            device_id_type=MESH,
        )

    def sent(self, copies):
        done = [id(copy) for copy in copies]
        for copy in self.copies:
            if id(copy) in done:
                copy.wait_send()
        self.copies = [copy for copy in self.copies if id(copy) not in done]

    def finish(self):
        for copy in self.copies:
            copy.wait_send()
        for line in self.lines:
            line.finish()


def greet(peers):
    barrier = pltpu.get_barrier_semaphore()
    for peer in peers:
        pl.semaphore_signal(barrier, inc=1, device_id=peer, device_id_type=MESH)
    pl.semaphore_wait(barrier, len(peers))


def fold(block):
    total = block[:, :128]
    for i in range(1, block.shape[1] // 128):
        total = total + block[:, i * 128 : (i + 1) * 128]
    return total


def wide(column, width):
    return jnp.concatenate([column] * (width // 128), axis=1)


def row_mask(row):
    return (lax.broadcasted_iota(jnp.int32, (8, 128), 0) == row).astype(f32)


def to_row(block, row):
    return lax.dot_general(
        row_mask(row), block, (((1,), (1,)), ((), ())), precision=EXACT, preferred_element_type=f32
    )


def to_column(stats, row):
    return lax.dot_general(
        stats, row_mask(row), (((0,), (0,)), ((), ())), precision=EXACT, preferred_element_type=f32
    )


def dot(left, right):
    return jnp.dot(left, right, preferred_element_type=f32)


def dot_t(left, right):
    return lax.dot_general(left, right, (((1,), (1,)), ((), ())), preferred_element_type=f32)


def t_dot(left, right):
    return lax.dot_general(left, right, (((0,), (0,)), ((), ())), preferred_element_type=f32)


def rotate(operand):
    half = HD // 2
    return jnp.concatenate([-operand[:, half:], operand[:, :half]], axis=1)


def rotate_back(operand):
    half = HD // 2
    return jnp.concatenate([operand[:, half:], -operand[:, :half]], axis=1)


def attention(k, qkv, stats, gain_ref, cos_ref, sin_ref):
    stats = stats / HQ
    q_inv = lax.rsqrt(to_column(stats, 2 * k) + epsilon)
    k_inv = lax.rsqrt(to_column(stats, 2 * k + 1) + epsilon)
    queries, key_rows = qkv[:, :HD], qkv[:, HD : 2 * HD]
    values = qkv[:, 2 * HD :].astype(bf16)
    cos_table, sine_table = cos_ref[...], sin_ref[...]
    q_normed = queries * q_inv * gain_ref[0:1]
    k_normed = key_rows * k_inv * gain_ref[1:2]
    q_rot = (q_normed * cos_table + rotate(q_normed) * sine_table).astype(bf16)
    k_rot = (k_normed * cos_table + rotate(k_normed) * sine_table).astype(bf16)
    scores = dot_t(q_rot, k_rot) * HD ** (-0.5)
    ahead = lax.broadcasted_iota(jnp.int32, scores.shape, 1) > lax.broadcasted_iota(
        jnp.int32, scores.shape, 0
    )
    scores = jnp.where(ahead, -1e30, scores)
    shifted = jnp.exp(scores - jnp.max(scores, axis=1, keepdims=True))
    probs = shifted / jnp.sum(shifted, axis=1, keepdims=True)
    return queries, key_rows, values, q_inv, k_inv, q_rot, k_rot, probs


def weight_grad(left, right, out, block, columns=None):
    na, nb, rows = left.shape[0], out.shape[1], out.shape[2]
    columns = columns or slice(0, right.shape[2])
    size = max(rows, 256)


    def chunk(i, carry):
        at = span(block * (nb * rows // size) + i, size)
        total = t_dot(left[0, :, at], right[0])
        for k in range(1, na):
            total = total + t_dot(left[k, :, at], right[k])
        for j in range(size // rows):
            part = total[j * rows : (j + 1) * rows].astype(bf16)
            out[block, i * (size // rows) + j, :, columns] = part
        return carry

    lax.fori_loop(0, nb * rows // size, chunk, 0)


def exchange_b(links, grad, held, columns):
    b = lax.axis_index("b")
    return [
        links.send(
            grad.at[:, across(b, j), :, columns], held.at[j - 1, :, :, columns], {"b": across(b, j)}
        )
        for j in range(1, held.shape[0] + 1)
    ]


def sum_b(copies, own, held, out, columns):
    for copy in copies:
        copy.wait_recv()

    def add(block, carry):
        total = own(block)[:, columns].astype(f32)
        for j in range(held.shape[0]):
            total = total + held[j, block, :, columns].astype(f32)
        out[block, :, columns] = total.astype(bf16)
        return carry

    lax.fori_loop(0, held.shape[1], add, 0)


class Line:
    def __init__(self, links, na, block, own):
        self.links, self.na, self.block, self.own = links, na, block, own
        self.a, self.p = lax.axis_index("a"), lax.axis_index("p")
        self.hop_base = {1: links.reserve(na - 1), -1: links.reserve(na - 1)}
        self.pass_base = links.reserve(na)
        links.lines.append(self)

    def hop(self, way, t):
        a, na = self.a, self.na
        first = a - way * (t - 1)
        source = self.own if t == 1 else self.block(exclusive_or(first, a, na))
        target = self.block(exclusive_or(first, a + way, na))
        return self.links.copy(self.hop_base[way] + t - 1, source, target, {"a": (a + way) % na})

    def sends(self, way, t):
        first, last = self.a - way * (t - 1), self.a + way
        return (first >= 0) & (first < self.na) & (last >= 0) & (last < self.na)

    def to_pair(self, k, source=None):
        at = self.block(k)
        return self.links.copy(self.pass_base + k, at if source is None else source, at, {"p": 1 - self.p})

    def start(self):
        for way in (1, -1):

            @pl.when(self.sends(way, 1))
            def _(way=way):
                self.hop(way, 1).start()

    def pass_on(self, way, t):
        came = self.a - way * t

        @pl.when((came >= 0) & (came < self.na))
        def _():
            self.hop(way, t).wait_recv()
            self.to_pair(exclusive_or(came, self.a, self.na)).start()

        if t < self.na - 1:

            @pl.when(self.sends(way, t + 1))
            def _():
                self.hop(way, t + 1).start()

    def finish(self):
        for way in (1, -1):
            for t in range(1, self.na):

                @pl.when(self.sends(way, t))
                def _(way=way, t=t):
                    self.hop(way, t).wait_send()

        for k in range(self.na):
            self.to_pair(k).wait_send()


class Reduce:
    def __init__(self, na, links, part, out, scratch):
        self.na, self.links, self.part, self.out = na, links, part, out
        self.from_q, self.half_sum, self.from_p, self.to_a, self.from_a = scratch[:5]
        self.total, self.parts, self.cols, self.stat = scratch[5:9]
        self.a, self.p, self.q = (lax.axis_index(axis) for axis in ("a", "p", "q"))
        self.rows, self.width = out.shape[1:]
        self.quarter, self.half = self.width // 4, self.width // 2
        self.count = self.rows // HALVES
        self.mine, self.pair = span(2 * self.q + self.p, self.quarter), span(self.q, self.half)
        self.lead = list(range(2, na)) + [1, 0]
        self.step_q, self.step_p, self.step_a = {}, {}, {}
        self.spread_a, self.spread_p, self.spread_q, self.stats = {}, {}, {}, {}

    def at(self, h):
        return slice(h * self.count, (h + 1) * self.count)

    def each(self, h, body):
        def step(i, carry):
            body(pl.ds(pl.multiple_of(h * self.count + i * TILE, TILE), TILE))
            return carry

        lax.fori_loop(0, self.count // TILE, step, 0)

    def send_q(self, h, k):
        at, q = self.at(h), self.q
        source = self.part.at[k, at, span(1 - q, self.half)]
        self.step_q[h, k] = self.links.send(source, self.from_q.at[k, at], {"q": 1 - q})

    def send_p(self, h, k):
        self.step_q[h, k].wait_recv()

        def add(at):
            own = self.part[k, at, span(self.q, self.half)].astype(f32)
            self.half_sum[k, at] = (own + self.from_q[k, at].astype(f32)).astype(bf16)

        self.each(h, add)
        at, p = self.at(h), self.p
        source = self.half_sum.at[k, at, span(1 - p, self.quarter)]
        self.step_p[h, k] = self.links.send(source, self.from_p.at[k, at], {"p": 1 - p})

    def send_a(self, h, k):
        if not k:
            return
        self.step_p[h, k].wait_recv()

        def add(at):
            own = self.half_sum[k, at, span(self.p, self.quarter)].astype(f32)
            self.to_a[k - 1, at] = (own + self.from_p[k, at].astype(f32)).astype(bf16)

        self.each(h, add)
        at = self.at(h)
        self.step_a[h, k] = self.links.send(
            self.to_a.at[k - 1, at], self.from_a.at[k - 1, at], {"a": across(self.a, k)}
        )

    def add_all(self, at):
        own = self.half_sum[0, at, span(self.p, self.quarter)].astype(f32)
        own = own + self.from_p[0, at].astype(f32)
        for k in range(1, self.na):
            own = own + self.from_a[k - 1, at].astype(f32)
        return own

    def scattered(self, h, first, number):
        self.step_p[h, 0].wait_recv()
        for k in range(1, self.na):
            self.step_a[h, k].wait_recv()
        self.each(h, first)
        if number:
            at = self.at(h)
            stats = to_row(self.parts[0, at], 0)
            if number == 2:
                stats = stats + to_row(self.parts[1, at], 1)
            stat = self.stat
            stat[h, 0] = stats
            self.stats[h] = self.links.send(stat.at[h, 0], stat.at[h, 1], {"p": 1 - self.p})

    def stats_q(self, h):
        stat = self.stat
        self.stats[h].wait_recv()
        stat[h, 2] = stat[h, 0] + stat[h, 1]
        self.stats[h] = self.links.send(stat.at[h, 2], stat.at[h, 3], {"q": 1 - self.q})

    def stats_done(self, h, number):
        stat = self.stat
        self.stats[h].wait_recv()
        stats = (stat[h, 2] + stat[h, 3]) / self.width
        for i in range(number):
            self.cols[i, self.at(h)] = to_column(stats, i)

    def spread(self, h, blocks):
        here = self.out.at[0, self.at(h), self.mine]
        for k in blocks:
            if k:
                target = self.out.at[k, self.at(h), self.mine]
                self.spread_a[h, k] = self.links.send(here, target, {"a": across(self.a, k)})
        self.spread_p[h, 0] = self.links.send(here, here, {"p": 1 - self.p})

    def relay_p(self, h, k):
        if not k:
            return
        self.spread_a[h, k].wait_recv()
        here = self.out.at[k, self.at(h), self.mine]
        self.spread_p[h, k] = self.links.send(here, here, {"p": 1 - self.p})

    def relay_q(self, h, k):
        self.spread_p[h, k].wait_recv()
        here = self.out.at[k, self.at(h), self.pair]
        self.spread_q[h, k] = self.links.send(here, here, {"q": 1 - self.q})

    def arrived(self, h, k):
        self.spread_q[h, k].wait_recv()

    def steps(self, first, second, number, chain=False):
        def normed(h):
            self.stats_done(h, number)
            self.each(h, second)

        def spread_own(h):
            here = self.out.at[0, self.at(h), self.mine]
            self.spread_p[h, 0] = self.links.send(here, here, {"p": 1 - self.p})

        def spread_far(h, k):
            here = self.out.at[0, self.at(h), self.mine]
            target = self.out.at[k, self.at(h), self.mine]
            self.spread_a[h, k] = self.links.send(here, target, {"a": across(self.a, k)})

        table = {
            "P": self.send_p,
            "A": self.send_a,
            "SC": lambda h: self.scattered(h, first, number),
            "SQ": self.stats_q,
            "SD": normed,
            "X": spread_own,
            "Z": spread_far,
            "RP": self.relay_p,
            "RQ": self.relay_q,
        }
        if chain:
            lines = [
                Line(
                    self.links,
                    self.na,
                    lambda k, h=h: self.out.at[k, self.at(h), self.mine],
                    self.out.at[0, self.at(h), self.mine],
                )
                for h in range(HALVES)
            ]

            def pair_arrived(h, k):
                self.spread_p[h, k] = lines[h].to_pair(k)
                self.relay_q(h, k)

            table.update(
                X=lambda h: lines[h].to_pair(0).start(),
                Z=lambda h: lines[h].start(),
                FL=lambda h, t: lines[h].pass_on(1, t),
                FR=lambda h, t: lines[h].pass_on(-1, t),
                RQ=pair_arrived,
            )
        return table


class OverHeads:
    def __init__(self, links, na, a, p, q, held, from_a, out_ref):
        self.links, self.na, self.a, self.p, self.q = links, na, a, p, q
        self.held, self.from_a, self.out_ref = held, from_a, out_ref

    def to_pair(self):
        self.copy = self.links.send(self.held.at[0], self.held.at[1], {"p": 1 - self.p})

    def to_core(self):
        held = self.held
        self.copy.wait_recv()
        held[2] = held[0] + held[1]
        self.copy = self.links.send(held.at[2], held.at[3], {"q": 1 - self.q})

    def to_all(self):
        held = self.held
        self.copy.wait_recv()
        held[4] = held[2] + held[3]
        self.copies = [
            self.links.send(held.at[4], self.from_a.at[k - 1], {"a": across(self.a, k)})
            for k in range(1, self.na)
        ]

    def done(self):
        for copy in self.copies:
            copy.wait_recv()
        for k in range(self.na):
            for i in range(2):
                at = 2 * k + i
                total = self.held[4, at : at + 1]
                for j in range(1, self.na):
                    other = 2 * (k ^ j) + i
                    total = total + self.from_a[j - 1, other : other + 1]
                self.out_ref[at : at + 1] = total


def reduce_peers(na):
    a, p, q = lax.axis_index("a"), lax.axis_index("p"), lax.axis_index("q")
    return [{"q": 1 - q}, {"p": 1 - p}] + [{"a": across(a, k)} for k in range(1, na)]


def attn_math(r, tok_ref, gain_ref, proj_ref, inv_ref, res_ref):
    def first(at):
        own = r.add_all(at)
        proj_ref[at] = own
        r.parts[0, at] = fold(own * own)

    def second(at):
        own = proj_ref[at]
        inv = lax.rsqrt(r.cols[0, at] + epsilon)
        inv_ref[at] = inv
        residual = tok_ref[at].astype(f32) + own * wide(inv, r.quarter) * gain_ref[0:1]
        res_ref[at] = residual
        r.out[0, at, r.mine] = residual.astype(bf16)

    return first, second


def mlp_math(r, res_ref, grad_ref, gain_ref, block_ref, sum_ref):
    def first(at):
        own = r.add_all(at)
        r.total[at] = own
        r.parts[0, at] = fold(own * own)
        r.parts[1, at] = fold(grad_ref[at] * gain_ref[1:2] * own)

    def second(at):
        own = r.total[at]
        inv = wide(lax.rsqrt(r.cols[0, at] + epsilon), r.quarter)
        upstream = grad_ref[at]
        scaled = upstream * gain_ref[1:2]
        normed = own * inv
        block_ref[0, at, r.mine] = (res_ref[at] + normed * gain_ref[1:2]).astype(bf16)
        gains = upstream * normed
        sum_ref[...] += jnp.sum(gains.reshape(TILE // 8, 8, r.quarter), axis=0)
        grad = inv * scaled - own * inv * inv * inv * wide(r.cols[1, at], r.quarter)
        r.out[0, at, r.mine] = grad.astype(bf16)

    return first, second


def back_math(r, grad_ref, proj_ref, inv_ref, gain_ref, res_ref, sum_ref):
    def first(at):
        grad = grad_ref[at] + r.add_all(at)
        res_ref[at] = grad
        r.parts[0, at] = fold(grad * gain_ref[0:1] * proj_ref[at])

    def second(at):
        own = proj_ref[at]
        inv = wide(inv_ref[at], r.quarter)
        upstream = res_ref[at]
        gains = upstream * own * inv
        sum_ref[...] += jnp.sum(gains.reshape(TILE // 8, 8, r.quarter), axis=0)
        grad = inv * (upstream * gain_ref[0:1])
        grad = grad - own * inv * inv * inv * wide(r.cols[0, at], r.quarter)
        r.out[0, at, r.mine] = grad.astype(bf16)

    return first, second


MIDDLE = (
    ("F", 2), ("rP", 0, 2), ("F", 3), ("rP", 0, 3), ("rA", 0, 2), ("rP", 1, 3), ("rP", 1, 2), ("F", 1),
    ("rA", 0, 3), ("F", 0), ("rP", 0, 1), ("rA", 1, 3), ("rP", 1, 1), ("rP", 0, 0), ("rA", 1, 2),
    ("rP", 1, 0), ("rA", 0, 1), ("rA", 1, 1), ("rSC", 0), ("rSQ", 0), ("rSC", 1), ("rSD", 0), ("rZ", 0, 3),
    ("rX", 0), ("rSQ", 1), ("rSD", 1), ("rZ", 0, 1), ("BP",), ("rZ", 1, 3), ("rZ", 0, 2), ("rZ", 1, 1),
    ("rRP", 0, 3), ("rX", 1), ("rRP", 0, 1), ("rZ", 1, 2), ("rRQ", 0, 3), ("B", 0, 3), ("rRP", 0, 2),
    ("rRP", 1, 3), ("sP", 0, 3), ("rRQ", 0, 1), ("rRP", 1, 2), ("rRQ", 0, 2), ("rRQ", 1, 3), ("rRP", 1, 1),
    ("B", 0, 2), ("B", 0, 1), ("rRQ", 0, 0), ("sP", 0, 2), ("B", 1, 3), ("sP", 0, 1), ("rRQ", 1, 2),
    ("sA", 0, 3), ("B", 0, 0), ("sP", 1, 3), ("rRQ", 1, 1), ("sA", 0, 2), ("rRQ", 1, 0), ("B", 1, 2),
    ("sP", 0, 0), ("sA", 0, 1), ("B", 1, 1), ("sP", 1, 2), ("B", 1, 0), ("sA", 1, 3), ("sP", 1, 1),
    ("sSC", 0), ("sA", 1, 2), ("BQ",), ("sP", 1, 0), ("sSQ", 0), ("sA", 1, 1), ("sSD", 0), ("sZ", 0, 2),
    ("D",), ("sX", 0), ("sZ", 0, 1), ("sSC", 1), ("sSQ", 1), ("sZ", 0, 3), ("sRP", 0, 2), ("sSD", 1),
    ("sZ", 1, 1), ("sRP", 0, 1), ("sX", 1), ("sRQ", 0, 0), ("G", 2), ("sZ", 1, 3), ("G", 3), ("G", 1),
    ("sRP", 0, 3), ("G", 0), ("sZ", 1, 2), ("sRP", 1, 3), ("sRQ", 0, 1), ("sRQ", 1, 0), ("sRP", 1, 1),
    ("sRP", 1, 2), ("sRQ", 0, 2), ("sRQ", 0, 3), ("sRQ", 1, 3), ("sRQ", 1, 1), ("DS",), ("sRQ", 1, 2),
)


def middle_kernel(na, nb, *refs):
    x_ref, w_ref, res_ref, grad_far, proj_ref, inv_ref, gain_ref = refs[:7]
    block_ref, back_out, ffn_sum_ref, grad_res_ref, attn_sum_ref, down_sum_ref, gu_grad_ref = refs[7:14]
    out, hidden_ref, grad_gu_ref, gu_ref, part_ref, down_grad, down_held, grad_ref = refs[14:22]
    scratch, (local_sem, send_sem, recv_sem) = refs[22:-3], refs[-3:]
    share = 2 * lax.axis_index("q") + lax.axis_index("p")
    load = pltpu.make_async_copy(
        grad_far.at[:, span(share, grad_ref.shape[1])], grad_ref, local_sem.at[0]
    )
    load.start()
    units = hidden_ref.shape[2]
    width = x_ref.shape[2]
    b = lax.axis_index("b")
    greet(reduce_peers(na) + [{"b": across(b, j)} for j in range(1, nb)])
    links = Links(send_sem, recv_sem)
    r = Reduce(na, links, part_ref, out, scratch[:9])
    s = Reduce(na, links, part_ref, back_out, scratch[9:])
    ffn_sum_ref[...] = jnp.zeros_like(ffn_sum_ref)
    attn_sum_ref[...] = jnp.zeros_like(attn_sum_ref)
    wide_tile = 512

    def forward(k):
        def gated(n, carry):
            at, up_at = span(n, 256), pl.ds(pl.multiple_of(units + n * 256, 256), 256)
            gate = dot(x_ref[k], w_ref[:, at])
            up = dot(x_ref[k], w_ref[:, up_at])
            gu_ref[k, :, at] = gate
            gu_ref[k, :, up_at] = up
            hidden_ref[k, :, at] = (gate * jax.nn.sigmoid(gate) * up).astype(bf16)
            return carry

        lax.fori_loop(0, units // 256, gated, 0)

        def down(n, carry):
            at = span(n, wide_tile)
            part_ref[k, :, at] = dot_t(hidden_ref[k], w_ref[at, 2 * units :]).astype(bf16)
            return carry

        lax.fori_loop(0, width // wide_tile, down, 0)

    def backward(h, k):
        rows = r.at(h)

        def gated(n, carry):
            at, up_at = span(n, 256), pl.ds(pl.multiple_of(units + n * 256, 256), 256)
            down_at = pl.ds(pl.multiple_of(2 * units + n * 256, 256), 256)
            grad_hidden = dot(out[k, rows], w_ref[:, down_at])
            gate, up = gu_ref[k, rows, at], gu_ref[k, rows, up_at]
            sigmoid = jax.nn.sigmoid(gate)
            active = gate * sigmoid
            grad_gu_ref[k, rows, at] = (
                grad_hidden * up * (sigmoid * (1.0 + gate * (1.0 - sigmoid)))
            ).astype(bf16)
            grad_gu_ref[k, rows, up_at] = (grad_hidden * active).astype(bf16)
            return carry

        lax.fori_loop(0, units // 256, gated, 0)

        def back(n, carry):
            at = span(n, wide_tile)
            part_ref[k, rows, at] = dot_t(
                grad_gu_ref[k, rows], w_ref[at, : 2 * units]
            ).astype(bf16)
            return carry

        lax.fori_loop(0, width // wide_tile, back, 0)

    first, second = mlp_math(r, res_ref, grad_ref, gain_ref, block_ref, ffn_sum_ref)
    back_first, back_second = back_math(
        s, grad_ref, proj_ref, inv_ref, gain_ref, grad_res_ref, attn_sum_ref
    )
    copies, reused = {}, []
    columns = slice(0, units)

    def forward_step(k):
        forward(k)
        for h in range(HALVES):
            r.send_q(h, k)

    def backward_step(h, k):
        if not reused:
            links.sent(r.step_q.values())
            reused.append(True)
        r.arrived(h, k)
        backward(h, k)
        s.send_q(h, k)

    def block_p():
        here = block_ref.at[0, :, r.mine]
        copies["p"] = links.send(here, here, {"p": 1 - r.p})

    def block_q():
        copies["p"].wait_recv()
        here = block_ref.at[0, :, r.pair]
        copies["q"] = links.send(here, here, {"q": 1 - r.q})

    def down_grads():
        for block in range(na):
            weight_grad(out, hidden_ref, down_grad, block)
        copies["b"] = exchange_b(links, down_grad, down_held, columns)

    table = {
        "F": forward_step,
        "B": backward_step,
        "BP": block_p,
        "BQ": block_q,
        "D": down_grads,
        "DS": lambda: sum_b(
            copies["b"], lambda block: down_grad.at[block, b], down_held, down_sum_ref, columns
        ),
        "G": lambda block: weight_grad(x_ref, grad_gu_ref, gu_grad_ref, block),
    }
    table.update({"r" + key: step for key, step in r.steps(first, second, 2).items()})
    table.update({"s" + key: step for key, step in s.steps(back_first, back_second, 1).items()})
    load.wait()
    for key, *where in MIDDLE:
        table[key](*where)
    for h in range(HALVES):
        for k in range(na):
            s.arrived(h, k)
    copies["q"].wait_recv()
    links.finish()


def middle_call(nb, x_all, w_mlp, res_mine, out_grad, proj_mine, inv_mine, width_gain):
    na, rows, width = x_all.shape
    quarter, units = width // 4, w_mlp.shape[1] // 3
    w_rows = width // (na * nb)
    vmem, far = pl.BlockSpec(memory_space=pltpu.VMEM), pl.BlockSpec(memory_space=pl.ANY)
    shape = jax.ShapeDtypeStruct
    outs = (
        shape((1, rows, width), bf16),
        shape((na, rows, width), bf16),
        shape((8, quarter), f32),
        shape((rows, quarter), f32),
        shape((8, quarter), f32),
        shape((na, w_rows, units), bf16),
        shape((na, nb, w_rows, 2 * units), bf16),
    )
    copies = 2 * HALVES * (6 * na + 1) + 2 + nb
    return pl.pallas_call(
        functools.partial(middle_kernel, na, nb),
        out_shape=outs,
        in_specs=[far if i == 3 else vmem for i in range(7)],
        out_specs=(vmem,) * len(outs),
        scratch_shapes=[
            pltpu.VMEM((na, rows, width), bf16),
            pltpu.VMEM((na, rows, units), bf16),
            pltpu.VMEM((na, rows, 2 * units), bf16),
            pltpu.VMEM((na, rows, 2 * units), f32),
            pltpu.VMEM((na, rows, width), bf16),
            pltpu.VMEM((na, nb, w_rows, units), bf16),
            pltpu.VMEM((nb - 1, na, w_rows, units), bf16),
            pltpu.VMEM((rows, quarter), f32),
        ]
        + reduce_scratch(na, rows, width)
        + reduce_scratch(na, rows, width)
        + [
            pltpu.SemaphoreType.DMA((1,)),
            pltpu.SemaphoreType.DMA((copies,)),
            pltpu.SemaphoreType.DMA((copies,)),
        ],
        compiler_params=pltpu.CompilerParams(
            collective_id=2, has_side_effects=True, vmem_limit_bytes=VMEM_LIMIT
        ),
        name="middle",
    )(x_all, w_mlp, res_mine, out_grad, proj_mine, inv_mine, width_gain)


def last_kernel(na, nb, *refs):
    proj_ref, x_far, qkv_ref, stats_ref, gain_ref, cos_ref, sin_ref, w_ref, att_ref = refs[:9]
    grad_ref, attn_sum_ref, ffn_sum_ref, down_sum_ref, gu_grad_far = refs[9:14]
    out, sums_ref, down_far, gu_far, qkv_out, wout_out = refs[14:20]
    scaled_ref, grad_qkv_ref, part_ref, head_sums, held, stats_a, inner_ref = refs[20:27]
    own_sums, a_sums, b_sums, gu_held, gu_sum, attn_grad, attn_held, attn_sum = refs[27:35]
    down_in, gu_in, attn_in, x_ref, gu_own, down_out, gu_out = refs[35:42]
    scratch, (local_sem, send_sem, recv_sem) = refs[42:-3], refs[-3:]
    links = Links(send_sem, recv_sem)
    load_gu = pltpu.make_async_copy(
        gu_grad_far.at[:, lax.axis_index("b")], gu_own, local_sem.at[0]
    )
    load_gu.start()
    load_x = pltpu.make_async_copy(x_far, x_ref, local_sem.at[1])
    load_x.start()
    r = Reduce(na, links, part_ref, out, scratch)
    a, b, p, q, mine, pair, quarter = (
        r.a, lax.axis_index("b"), r.p, r.q, r.mine, r.pair, r.quarter,
    )
    units = down_sum_ref.shape[2]
    own_sums[...] = jnp.zeros_like(own_sums)
    own_sums[0:1, mine] = jnp.sum(attn_sum_ref[...], axis=0, keepdims=True)
    own_sums[1:2, mine] = jnp.sum(ffn_sum_ref[...], axis=0, keepdims=True)
    greet(reduce_peers(na) + [{"b": across(b, j)} for j in range(1, nb)])
    far = list(range(2, na)) + [1]

    def to_owners(source, target, columns):
        return [
            (k, links.send(
                source.at[across(a, k), :, columns], target.at[k - 1, :, columns], {"a": across(a, k)}
            ))
            for k in far
        ]

    whole = slice(0, units)
    halves = [slice(0, units), slice(units, 2 * units)]
    down_copies = to_owners(down_sum_ref, down_in, whole)
    gu_b = [exchange_b(links, gu_grad_far, gu_held, columns) for columns in halves]
    here = own_sums.at[:, mine]
    sums_p = links.send(here, here, {"p": 1 - p})

    held[0] = jnp.zeros_like(held[0])
    head_sums[...] = jnp.zeros_like(head_sums)

    def attend_back(k, carry):
        queries, key_rows, values, q_inv, k_inv, q_rot, k_rot, probs = attention(
            k, qkv_ref[k], stats_ref[...], gain_ref, cos_ref, sin_ref
        )
        cos_table, sine_table = cos_ref[...], sin_ref[...]
        grad_att = dot(proj_ref[k], w_ref[:, 3 * HD :]).astype(bf16)
        grad_v = t_dot(probs.astype(bf16), grad_att)
        grad_p = dot_t(grad_att, values)
        delta = jnp.sum(probs * grad_p, axis=1, keepdims=True)
        grad_scores = (probs * (grad_p - delta) * HD ** (-0.5)).astype(bf16)
        grad_q = dot(grad_scores, k_rot)
        grad_k = t_dot(grad_scores, q_rot)
        grad_q = grad_q * cos_table + rotate_back(grad_q * sine_table)
        grad_k = grad_k * cos_table + rotate_back(grad_k * sine_table)
        head_sums[0:1] += jnp.sum(grad_q * queries * q_inv, axis=0, keepdims=True)
        head_sums[1:2] += jnp.sum(grad_k * key_rows * k_inv, axis=0, keepdims=True)
        scaled_q = grad_q * gain_ref[0:1]
        scaled_k = grad_k * gain_ref[1:2]
        scaled_ref[k, :, :HD] = scaled_q
        scaled_ref[k, :, HD:] = scaled_k
        grad_qkv_ref[k, :, 2 * HD :] = grad_v.astype(bf16)
        held[0] += to_row(scaled_q * queries, 2 * k) + to_row(scaled_k * key_rows, 2 * k + 1)
        return carry

    lax.fori_loop(0, na, attend_back, 0)
    sums_p.wait_recv()
    here = own_sums.at[:, pair]
    sums_q = links.send(here, here, {"q": 1 - q})
    gu_copies = []

    def sent():
        for block in range(na):
            weight_grad(proj_ref, att_ref, attn_grad, block, slice(3 * HD, 4 * HD))
        load_gu.wait()
        sum_b(gu_b[0], lambda block: gu_own.at[block], gu_held, gu_sum, halves[0])
        gu_copies.append(to_owners(gu_sum, gu_in, halves[0]))

    over_heads = OverHeads(links, na, a, p, q, held, stats_a, inner_ref)
    over_heads.to_pair()
    over_heads.to_core()
    over_heads.to_all()
    sent()
    over_heads.done()

    def qkv_back(k):
        for i in range(2):
            at = slice(i * HD, (i + 1) * HD)
            inv = lax.rsqrt(to_column(stats_ref[...] / HQ, 2 * k + i) + epsilon)
            mean = to_column(inner_ref[...] / HQ, 2 * k + i)
            grad = inv * scaled_ref[k, :, at] - qkv_ref[k, :, at] * inv * inv * inv * mean
            grad_qkv_ref[k, :, at] = grad.astype(bf16)

        def part(n, carry):
            at = span(n, 512)
            part_ref[k, :, at] = dot_t(grad_qkv_ref[k], w_ref[at, : 3 * HD]).astype(bf16)
            return carry

        lax.fori_loop(0, part_ref.shape[2] // 512, part, 0)

    for k in r.lead:
        qkv_back(k)
        for h in range(HALVES):
            r.send_q(h, k)
    for h in range(HALVES):
        for k in r.lead:
            r.send_p(h, k)
    load_x.wait()
    for block in range(na):
        weight_grad(x_ref, grad_qkv_ref, attn_grad, block, slice(0, 3 * HD))
    attn_columns = slice(0, 4 * HD)
    attn_b = exchange_b(links, attn_grad, attn_held, attn_columns)
    for h in range(HALVES):
        for k in r.lead:
            r.send_a(h, k)
    sums_q.wait_recv()
    sums_a = [
        links.send(own_sums.at[:, span(across(a, k), quarter)], a_sums.at[k - 1], {"a": across(a, k)})
        for k in range(1, na)
    ]
    sum_b(gu_b[1], lambda block: gu_own.at[block], gu_held, gu_sum, halves[1])
    gu_copies.append(to_owners(gu_sum, gu_in, halves[1]))

    def first(at):
        out[0, at, mine] = (grad_ref[at] + r.add_all(at)).astype(bf16)

    for h in range(HALVES):
        r.scattered(h, first, 0)
        r.spread(h, [0])
    for copy in sums_a:
        copy.wait_recv()
    total = own_sums[:, span(a, quarter)]
    for k in range(1, na):
        total = total + a_sums[k - 1]
    b_sums[0, :, :quarter] = total
    b_sums[0, :, quarter:] = head_sums[...]
    sums_b = [links.send(b_sums.at[0], b_sums.at[j], {"b": across(b, j)}) for j in range(1, nb)]
    for h in range(HALVES):
        r.relay_q(h, 0)
    sum_b(attn_b, lambda block: attn_grad.at[block, b], attn_held, attn_sum, attn_columns)
    attn_copies = to_owners(attn_sum, attn_in, attn_columns)

    def store(target, index, size, value):
        target[:, span(index, size)] = value.astype(f32)

    store(down_out, a, units, down_sum_ref[a])
    for c in range(2):
        gu_out[:, c, span(a, units)] = gu_sum[a, :, halves[c]].astype(f32)
    for c in range(3):
        store(qkv_out.at[c], a, HD, attn_sum[a, :, c * HD : (c + 1) * HD])
    store(wout_out, a, HD, attn_sum[a, :, 3 * HD :])
    for k, copy in down_copies:
        copy.wait_recv()
        store(down_out, across(a, k), units, down_in[k - 1])
    save_down = pltpu.make_async_copy(down_out, down_far, local_sem.at[2])
    save_down.start()
    for copy in sums_b:
        copy.wait_recv()
    total = b_sums[0]
    for j in range(1, nb):
        total = total + b_sums[j]
    sums_ref[...] = total
    for c in range(2):
        for k, copy in gu_copies[c]:
            copy.wait_recv()
            gu_out[:, c, span(across(a, k), units)] = gu_in[k - 1, :, halves[c]].astype(f32)
    save_gu = pltpu.make_async_copy(gu_out, gu_far, local_sem.at[3])
    save_gu.start()
    for k, copy in attn_copies:
        copy.wait_recv()
        for c in range(3):
            store(qkv_out.at[c], across(a, k), HD, attn_in[k - 1, :, c * HD : (c + 1) * HD])
        store(wout_out, across(a, k), HD, attn_in[k - 1, :, 3 * HD :])
    for h in range(HALVES):
        r.arrived(h, 0)
    save_down.wait()
    save_gu.wait()
    links.finish()


def last_call(nb, *operands):
    na, rows, width = operands[0].shape
    w_rows, units = operands[12].shape[1:]
    quarter = width // 4
    vmem, far = pl.BlockSpec(memory_space=pltpu.VMEM), pl.BlockSpec(memory_space=pl.ANY)
    shape = jax.ShapeDtypeStruct
    outs = (
        shape((1, rows, width), bf16),
        shape((8, quarter + HD), f32),
        shape((w_rows, na * units), f32),
        shape((w_rows, 2, na * units), f32),
        shape((3, w_rows, na * HD), f32),
        shape((w_rows, na * HD), f32),
    )
    copies = HALVES * (3 * na + 1) + 2 + 6 * na + 4 * nb
    return pl.pallas_call(
        functools.partial(last_kernel, na, nb),
        out_shape=outs,
        in_specs=[far if i in (1, 13) else vmem for i in range(14)],
        out_specs=(vmem, vmem, far, far, vmem, vmem),
        scratch_shapes=[
            pltpu.VMEM((na, rows, 2 * HD), f32),
            pltpu.VMEM((na, rows, 3 * HD), bf16),
            pltpu.VMEM((na, rows, width), bf16),
            pltpu.VMEM((8, HD), f32),
            pltpu.VMEM((5, 8, rows), f32),
            pltpu.VMEM((na - 1, 8, rows), f32),
            pltpu.VMEM((8, rows), f32),
            pltpu.VMEM((8, width), f32),
            pltpu.VMEM((na - 1, 8, quarter), f32),
            pltpu.VMEM((nb, 8, quarter + HD), f32),
            pltpu.VMEM((nb - 1, na, w_rows, 2 * units), bf16),
            pltpu.VMEM((na, w_rows, 2 * units), bf16),
            pltpu.VMEM((na, nb, w_rows, 4 * HD), bf16),
            pltpu.VMEM((nb - 1, na, w_rows, 4 * HD), bf16),
            pltpu.VMEM((na, w_rows, 4 * HD), bf16),
            pltpu.VMEM((na - 1, w_rows, units), bf16),
            pltpu.VMEM((na - 1, w_rows, 2 * units), bf16),
            pltpu.VMEM((na - 1, w_rows, 4 * HD), bf16),
            pltpu.VMEM((na, rows, width), bf16),
            pltpu.VMEM((na, w_rows, 2 * units), bf16),
            pltpu.VMEM((w_rows, na * units), f32),
            pltpu.VMEM((w_rows, 2, na * units), f32),
        ]
        + reduce_scratch(na, rows, width)
        + [
            pltpu.SemaphoreType.DMA((4,)),
            pltpu.SemaphoreType.DMA((copies,)),
            pltpu.SemaphoreType.DMA((copies,)),
        ],
        compiler_params=pltpu.CompilerParams(
            collective_id=4, has_side_effects=True, vmem_limit_bytes=VMEM_LIMIT
        ),
        name="last",
    )(*operands)


def reduce_scratch(na, rows, width):
    quarter = width // 4
    return [
        pltpu.VMEM((na, rows, width // 2), bf16),
        pltpu.VMEM((na, rows, width // 2), bf16),
        pltpu.VMEM((na, rows, quarter), bf16),
        pltpu.VMEM((na - 1, rows, quarter), bf16),
        pltpu.VMEM((na - 1, rows, quarter), bf16),
        pltpu.VMEM((rows, quarter), f32),
        pltpu.VMEM((2, rows, 128), f32),
        pltpu.VMEM((2, rows, 128), f32),
        pltpu.VMEM((HALVES, 4, 8, rows // HALVES), f32),
    ]


ENTER = (
    ("Z", 0), ("W", 3), ("FW", 0), ("FR", 0, 1), ("FL", 0, 1), ("W", 1), ("CUT", 2), ("FW", 1), ("W", 2),
    ("FR", 0, 2), ("FR", 0, 3), ("CUT", 3), ("M", 0, 3), ("FL", 0, 2), ("CUT", 1), ("FW", 3), ("FL", 0, 3),
    ("GA",), ("FT", 0), ("FQ", 3), ("FW", 2), ("CUT", 0), ("FQ", 2), ("M", 0, 1), ("M", 2, 3), ("FQ", 1),
    ("J", 3), ("FQ", 0), ("J", 0), ("GB",), ("M", 1, 1), ("J", 1), ("J", 2), ("S1",), ("S2",), ("S3",),
    ("M", 1, 3), ("MR", 1, 0), ("M", 1, 2), ("S4",), ("E", 3), ("E", 1), ("rP", 1, 3), ("E", 2),
    ("rP", 1, 1), ("M", 2, 1), ("MR", 2, 3), ("rP", 0, 3), ("rP", 0, 1), ("MR", 0, 3), ("E", 0),
    ("rA", 1, 3), ("MR", 2, 0), ("rA", 1, 1), ("MR", 0, 1), ("rA", 0, 3), ("MR", 1, 3), ("rP", 0, 2),
    ("MR", 2, 1), ("rA", 0, 2), ("rA", 0, 1), ("rP", 0, 0), ("rP", 1, 2), ("rA", 1, 2), ("MR", 1, 2),
    ("rP", 1, 0), ("rSC", 0), ("rSQ", 0), ("MR", 0, 0), ("M", 2, 2), ("rSC", 1), ("rSD", 0), ("rSQ", 1),
    ("rX", 0), ("rSD", 1), ("rZ", 0), ("rZ", 1), ("rFR", 0, 1), ("rFL", 0, 1), ("rX", 1), ("MR", 2, 2),
    ("rFR", 1, 1), ("rFL", 1, 1), ("rFR", 0, 2), ("rRQ", 0, 0), ("rFL", 1, 2), ("rFL", 0, 2), ("MR", 1, 1),
    ("rFR", 0, 3), ("M", 0, 2), ("rFR", 1, 2), ("rFL", 1, 3), ("rFR", 1, 3), ("rFL", 0, 3), ("rRQ", 0, 1),
    ("MR", 0, 2), ("rRQ", 1, 1), ("rRQ", 1, 2), ("rRQ", 0, 2), ("rRQ", 1, 0), ("rRQ", 1, 3), ("rRQ", 0, 3),
)


def enter_kernel(na, nb, gain_sizes, *refs):
    tok_far, qkv_w_ref, wout_ref, gu_ref, down_ref, cos_ref, sin_ref, all_gains_ref = refs[:8]
    x_far, w_far, mlp_w_ref, width_gain_ref, head_gain_ref, qkv_far, stats_ref, att_far = refs[8:16]
    out, proj_ref, inv_ref, res_ref = refs[16:20]
    own_gains, gains_ref, piece_ref, part_ref, held, stats_a = refs[20:26]
    x_ref, w_ref, qkv_ref, att_ref = refs[26:30]
    tok_ref = refs[30]
    scratch, (local_sem, send_sem, recv_sem) = refs[31:-3], refs[-3:]
    saves = [
        pltpu.make_async_copy(near, there, local_sem.at[5 + i])
        for i, (near, there) in enumerate(
            ((x_ref, x_far), (w_ref, w_far), (qkv_ref, qkv_far), (att_ref, att_far))
        )
    ]
    a, b, p, q = (lax.axis_index(axis) for axis in ("a", "b", "p", "q"))
    rows = wout_ref.shape[0]
    quarter = tok_ref.shape[1]
    load = pltpu.make_async_copy(
        tok_far.at[:, span(2 * q + p, quarter)], tok_ref, local_sem.at[9]
    )
    load.start()
    units = down_ref.shape[1] // na
    own_gains[...] = jnp.zeros_like(own_gains)
    n_d, n_h = gain_sizes
    place = 0
    for i, size in enumerate((n_d, n_d, n_h, n_h)):
        own_gains[i : i + 1, :size] = all_gains_ref[:, place : place + size].astype(f32)
        place += size
    gains_ref[a, b] = own_gains[...]
    greet(
        [{"q": 1 - q}, {"p": 1 - p}]
        + [{"a": across(a, k)} for k in range(1, na)]
        + [{"b": across(b, j)} for j in range(1, nb)]
    )
    load.wait()
    links = Links(send_sem, recv_sem)
    mine, pair = span(2 * q + p, quarter), span(q, 2 * quarter)
    place = span(a * nb + b, rows)
    copies, ends = {}, []
    locals_ = [pltpu.make_async_copy(tok_ref, x_ref.at[0, :, mine], local_sem.at[0])]

    def weight_sources(k):
        block = span(across(a, k), HD)
        sources = [qkv_w_ref.at[c, :, block] for c in range(3)] + [wout_ref.at[:, block]]
        return [(s, w_ref.at[place, c * HD : (c + 1) * HD]) for c, s in enumerate(sources)]

    for c, (source, target) in enumerate(weight_sources(0)):
        locals_.append(pltpu.make_async_copy(source, target, local_sem.at[1 + c]))
    for copy in locals_:
        copy.start()

    def send_gains():
        copies["g"] = [
            links.send(own_gains, gains_ref.at[a, b], {"a": across(a, k)}) for k in range(1, na)
        ]

    def relay_gains():
        for copy in copies["g"]:
            copy.wait_recv()
        at = gains_ref.at[:, b]
        copies["gb"] = [links.send(at, at, {"b": across(b, j)}) for j in range(1, nb)]

    def send_weights(k):
        copies["w", k] = [
            links.send(source, target, {"a": across(a, k)}) for source, target in weight_sources(k)
        ]

    def relay_weights(k):
        if k:
            for copy in copies["w", k]:
                copy.wait_recv()
        else:
            for copy in locals_[1:]:
                copy.wait()
        at = w_ref.at[span(across(a, k) * nb + b, rows), :]
        copies["wb", k] = [links.send(at, at, {"b": across(b, j)}) for j in range(1, nb)]

    line = Line(links, na, lambda k: x_ref.at[k, :, mine], tok_ref)

    def own_tokens(_):
        locals_[0].wait()
        line.to_pair(0).start()

    def pair_tokens(k):
        line.to_pair(k).wait_recv()
        at = x_ref.at[k, :, pair]
        copies["x", k] = links.send(at, at, {"q": 1 - q})

    def cut_weights(k):
        block = span(across(a, k), units)

        def cut(i, carry):
            at = pl.ds(pl.multiple_of(i * TILE, TILE), TILE)
            cuts = (gu_ref[at, 0, block], gu_ref[at, 1, block], down_ref[at, block])
            for c in range(3):
                if k:
                    piece_ref[k - 1, c, at] = cuts[c]
                else:
                    to = pl.ds(pl.multiple_of((a * nb + b) * rows + i * TILE, TILE), TILE)
                    mlp_w_ref[to, c * units : (c + 1) * units] = cuts[c]
            return carry

        lax.fori_loop(0, rows // TILE, cut, 0)

    def send_piece(c, k):
        target = mlp_w_ref.at[place, c * units : (c + 1) * units]
        copies["m", c, k] = links.send(piece_ref.at[k - 1, c], target, {"a": across(a, k)})

    def relay_piece(c, k):
        if k:
            copies["m", c, k].wait_recv()
        at = mlp_w_ref.at[span(across(a, k) * nb + b, rows), c * units : (c + 1) * units]
        ends.extend(links.send(at, at, {"b": across(b, j)}) for j in range(1, nb))

    arrived, ready = set(), []

    def project(k):
        if not arrived:
            held[0] = jnp.zeros_like(held[0])
            for i in range(na):
                for copy in copies["wb", i]:
                    copy.wait_recv()
        arrived.add(k)
        copies["x", k].wait_recv()

        def chunk(i, carry):
            at = span(i, 128)
            proj = dot(x_ref[k, at], w_ref[:, : 3 * HD])
            qkv_ref[k, at] = proj
            queries, key_rows = proj[:, :HD], proj[:, HD : 2 * HD]
            held[0, :, at] += to_row(queries * queries, 2 * k) + to_row(key_rows * key_rows, 2 * k + 1)
            return carry

        lax.fori_loop(0, x_ref.shape[1] // 128, chunk, 0)

    over_heads = OverHeads(links, na, a, p, q, held, stats_a, stats_ref)

    def all_stats():
        for save in saves[:3]:
            save.start()
        over_heads.done()
        for copy in copies["gb"]:
            copy.wait_recv()
        width_gain_ref[...] = jnp.zeros_like(width_gain_ref)
        head_gain_ref[...] = jnp.zeros_like(head_gain_ref)
        for i in range(2):
            width_gain_ref[i : i + 1] = jnp.concatenate(
                [gains_ref[2 * q + p, j, i : i + 1, :n_d] for j in range(nb)], axis=1
            )
            head_gain_ref[i : i + 1] = jnp.concatenate(
                [gains_ref[a, j, i + 2 : i + 3, :n_h] for j in range(nb)], axis=1
            )

    r = Reduce(na, links, part_ref, out, scratch)

    def attend(k):
        values, probs = (
            attention(k, qkv_ref[k], stats_ref[...], head_gain_ref, cos_ref, sin_ref)[i] for i in (2, 7)
        )
        attended = dot(probs.astype(bf16), values).astype(bf16)
        att_ref[k] = attended

        def part(n, carry):
            at = span(n, 512)
            part_ref[k, :, at] = dot_t(att_ref[k], w_ref[at, 3 * HD :]).astype(bf16)
            return carry

        lax.fori_loop(0, part_ref.shape[2] // 512, part, 0)
        for h in range(HALVES):
            r.send_q(h, k)

    first, second = attn_math(r, tok_ref, width_gain_ref, proj_ref, inv_ref, res_ref)
    table = {
        "GA": send_gains,
        "GB": relay_gains,
        "W": send_weights,
        "FW": relay_weights,
        "Z": lambda _: line.start(),
        "FL": lambda _, t: line.pass_on(1, t),
        "FR": lambda _, t: line.pass_on(-1, t),
        "FT": own_tokens,
        "FQ": pair_tokens,
        "CUT": cut_weights,
        "M": send_piece,
        "MR": relay_piece,
        "J": project,
        "S1": over_heads.to_pair,
        "S2": over_heads.to_core,
        "S3": over_heads.to_all,
        "S4": all_stats,
        "E": attend,
    }
    table.update({"r" + key: step for key, step in r.steps(first, second, 1, True).items()})
    for key, *where in ENTER:
        table[key](*where)
    saves[3].start()
    for h in range(HALVES):
        for k in range(na):
            r.arrived(h, k)
    for copy in ends:
        copy.wait_recv()
    for save in saves:
        save.wait()
    links.finish()


def enter_call(na, nb, tokens, qkv, w_out, gu, down, cos_table, sine_table, gains):
    rows, width = tokens.shape
    quarter = width // 4
    sizes = (gains[0].shape[0], gains[2].shape[0])
    w_rows, units = down.shape[0], down.shape[1] // na
    lanes = max(128, sizes[0])
    vmem, far = pl.BlockSpec(memory_space=pltpu.VMEM), pl.BlockSpec(memory_space=pl.ANY)
    shape = jax.ShapeDtypeStruct
    full = shape((na, rows, width), bf16)
    outs = [
        full,
        shape((width, 4 * HD), bf16),
        shape((width, 3 * units), bf16),
        shape((8, quarter), f32),
        shape((8, HD), f32),
        shape((na, rows, 3 * HD), f32),
        shape((8, rows), f32),
        shape((na, rows, HD), bf16),
        full,
        shape((rows, quarter), f32),
        shape((rows, 128), f32),
        shape((rows, quarter), f32),
    ]
    copies = 90 + 16 * nb
    return pl.pallas_call(
        functools.partial(enter_kernel, na, nb, sizes),
        out_shape=tuple(outs),
        in_specs=[far] + [vmem] * 7,
        out_specs=tuple(far if i in (0, 1, 5, 7) else vmem for i in range(len(outs))),
        scratch_shapes=[
            pltpu.VMEM((8, lanes), f32),
            pltpu.VMEM((na, nb, 8, lanes), f32),
            pltpu.VMEM((na - 1, 3, w_rows, units), bf16),
            pltpu.VMEM((na, rows, width), bf16),
            pltpu.VMEM((5, 8, rows), f32),
            pltpu.VMEM((na - 1, 8, rows), f32),
            pltpu.VMEM((na, rows, width), bf16),
            pltpu.VMEM((width, 4 * HD), bf16),
            pltpu.VMEM((na, rows, 3 * HD), f32),
            pltpu.VMEM((na, rows, HD), bf16),
            pltpu.VMEM((rows, quarter), bf16),
        ]
        + reduce_scratch(na, rows, width)
        + [
            pltpu.SemaphoreType.DMA((10,)),
            pltpu.SemaphoreType.DMA((copies,)),
            pltpu.SemaphoreType.DMA((copies,)),
        ],
        compiler_params=pltpu.CompilerParams(
            collective_id=5, has_side_effects=True, vmem_limit_bytes=VMEM_LIMIT
        ),
        name="enter",
    )(tokens, qkv, w_out, gu, down, cos_table, sine_table, jnp.concatenate(gains)[None])


def rope_tables(length, width):
    half_width = width // 2
    inv_freq = rope_base ** (-(jnp.arange(half_width, dtype=f32) * 2.0) / width)
    angles = jnp.arange(length, dtype=f32)[:, None] * inv_freq[None, :]
    cos_table = jnp.concatenate([jnp.cos(angles), jnp.cos(angles)], axis=1)
    sine_table = jnp.concatenate([jnp.sin(angles), jnp.sin(angles)], axis=1)
    return cos_table, sine_table


def on_device(
    tokens,
    qkv_weight,
    out_weight,
    gu_weight,
    down_weight,
    attn_gain,
    ffn_gain,
    q_gain,
    k_gain,
    out_grad,
):
    na, nb = lax.axis_size("a"), lax.axis_size("b")
    a, b = lax.axis_index("a"), lax.axis_index("b")
    share = lax.axis_index("q") * 2 + lax.axis_index("p")
    rows, width = tokens.shape
    quarter = width // 4
    w_rows = out_weight.shape[0]
    units = down_weight.shape[1] // na

    cos_table, sine_table = rope_tables(SEQ_LEN, HD)
    (
        x_all,
        w_attn,
        w_mlp,
        width_gain,
        head_gain,
        qkv,
        stats,
        attended,
        res_all,
        proj_mine,
        inv_mine,
        res_mine,
    ) = enter_call(
        na,
        nb,
        tokens,
        qkv_weight.transpose(1, 0, 2),
        out_weight,
        gu_weight,
        down_weight,
        cos_table,
        sine_table,
        (attn_gain, ffn_gain, q_gain, k_gain),
    )
    n_d, n_h = attn_gain.shape[0], q_gain.shape[0]
    block_rows, grad_proj, ffn_sums, grad_res, attn_sums, down_sum, gu_grad = middle_call(
        nb, res_all, w_mlp, res_mine, out_grad, proj_mine, inv_mine, width_gain
    )
    grad_rows, sums, down_grad, gu_grad, qkv_grad, out_grad_w = last_call(
        nb,
        grad_proj,
        x_all,
        qkv,
        stats,
        head_gain,
        cos_table,
        sine_table,
        w_attn,
        attended,
        grad_res,
        attn_sums,
        ffn_sums,
        down_sum,
        gu_grad,
    )
    width_sums = lax.dynamic_slice_in_dim(sums[:2, :quarter], b * n_d, n_d, 1)
    head_sums = lax.dynamic_slice_in_dim(sums[:2, quarter:], b * n_h, n_h, 1)
    return (
        block_rows[0].astype(f32),
        grad_rows[0].astype(f32),
        qkv_grad.transpose(1, 0, 2),
        out_grad_w,
        gu_grad,
        down_grad,
        width_sums[0],
        width_sums[1],
        head_sums[0],
        head_sums[1],
    )


def solution(mesh):
    dp, tp = mesh.shape["dp"], mesh.shape["tensor"]
    na = HEADS // tp
    fine = Mesh(mesh.devices.reshape(na, dp // na, tp // 2, 2), ("a", "b", "p", "q"))
    dp_axes, tp_axes = ("a", "b"), ("p", "q")
    both = tp_axes + dp_axes
    return jax.shard_map(
        on_device,
        mesh=fine,
        in_specs=(
            P(dp_axes, None),
            P(dp_axes, None, tp_axes),
            P(dp_axes, tp_axes),
            P(dp_axes, None, tp_axes),
            P(dp_axes, tp_axes),
            P(dp_axes),
            P(dp_axes),
            P(both),
            P(both),
            P(dp_axes, None),
        ),
        out_specs=(
            P(dp_axes, None),
            P(dp_axes, None),
            P(dp_axes, None, tp_axes),
            P(dp_axes, tp_axes),
            P(dp_axes, None, tp_axes),
            P(dp_axes, tp_axes),
            P(dp_axes),
            P(dp_axes),
            P(both),
            P(both),
        ),
        check_vma=False,
    )
```

```python
import functools

import jax
import jax.numpy as jnp
from jax import lax
from jax.experimental import pallas as pl
from jax.experimental.pallas import tpu as pltpu
from jax.sharding import Mesh, PartitionSpec as P

HEADS = 16
HD = 128
SEQ_LEN = 256
HQ = 2048

epsilon = 1e-06
rope_base = 500000.0

f32 = jnp.float32
bf16 = jnp.bfloat16
MESH = pl.DeviceIdType.MESH
EXACT = lax.Precision.HIGHEST
VMEM_LIMIT = 63 * 1024 * 1024
TILE = 32
HALVES = 2


def flip(index, bit):
    return index + bit - 2 * bit * ((index // bit) % 2)


def across(index, k):
    bit = 1
    while bit <= k:
        if k & bit:
            index = flip(index, bit)
        bit *= 2
    return index


def exclusive_or(left, right, count):
    total, bit = 0, 1
    while bit < count:
        total = total + bit * ((left // bit + right // bit) % 2)
        bit *= 2
    return total


def pick(operand, index, axis):
    return lax.dynamic_index_in_dim(operand, index, axis, keepdims=False)


def span(index, size):
    return pl.ds(pl.multiple_of(index * size, size), size)


class Links:
    def __init__(self, send_sem, recv_sem):
        self.send_sem, self.recv_sem, self.count = send_sem, recv_sem, 0
        self.copies, self.lines = [], []

    def send(self, source, target, device):
        copy = self.copy(self.count, source, target, device)
        copy.start()
        self.count += 1
        self.copies.append(copy)
        return copy

    def reserve(self, number):
        self.count += number
        return self.count - number

    def copy(self, index, source, target, device):
        return pltpu.make_async_remote_copy(
            src_ref=source,
            dst_ref=target,
            send_sem=self.send_sem.at[index],
            recv_sem=self.recv_sem.at[index],
            device_id=device,
            device_id_type=MESH,
        )

    def sent(self, copies):
        done = [id(copy) for copy in copies]
        for copy in self.copies:
            if id(copy) in done:
                copy.wait_send()
        self.copies = [copy for copy in self.copies if id(copy) not in done]

    def finish(self):
        for copy in self.copies:
            copy.wait_send()
        for line in self.lines:
            line.finish()


def greet(peers):
    barrier = pltpu.get_barrier_semaphore()
    for peer in peers:
        pl.semaphore_signal(barrier, inc=1, device_id=peer, device_id_type=MESH)
    pl.semaphore_wait(barrier, len(peers))


def fold(block):
    total = block[:, :128]
    for i in range(1, block.shape[1] // 128):
        total = total + block[:, i * 128 : (i + 1) * 128]
    return total


def wide(column, width):
    return jnp.concatenate([column] * (width // 128), axis=1)


def row_mask(row):
    return (lax.broadcasted_iota(jnp.int32, (8, 128), 0) == row).astype(f32)


def to_row(block, row):
    return lax.dot_general(
        row_mask(row), block, (((1,), (1,)), ((), ())), precision=EXACT, preferred_element_type=f32
    )


def to_column(stats, row):
    return lax.dot_general(
        stats, row_mask(row), (((0,), (0,)), ((), ())), precision=EXACT, preferred_element_type=f32
    )


def dot(left, right):
    return jnp.dot(left, right, preferred_element_type=f32)


def dot_t(left, right):
    return lax.dot_general(left, right, (((1,), (1,)), ((), ())), preferred_element_type=f32)


def t_dot(left, right):
    return lax.dot_general(left, right, (((0,), (0,)), ((), ())), preferred_element_type=f32)


def rotate(operand):
    half = HD // 2
    return jnp.concatenate([-operand[:, half:], operand[:, :half]], axis=1)


def rotate_back(operand):
    half = HD // 2
    return jnp.concatenate([operand[:, half:], -operand[:, :half]], axis=1)


def attention(k, qkv, stats, gain_ref, cos_ref, sin_ref):
    stats = stats / HQ
    q_inv = lax.rsqrt(to_column(stats, 2 * k) + epsilon)
    k_inv = lax.rsqrt(to_column(stats, 2 * k + 1) + epsilon)
    queries, key_rows = qkv[:, :HD], qkv[:, HD : 2 * HD]
    values = qkv[:, 2 * HD :].astype(bf16)
    cos_table, sine_table = cos_ref[...], sin_ref[...]
    q_normed = queries * q_inv * gain_ref[0:1]
    k_normed = key_rows * k_inv * gain_ref[1:2]
    q_rot = (q_normed * cos_table + rotate(q_normed) * sine_table).astype(bf16)
    k_rot = (k_normed * cos_table + rotate(k_normed) * sine_table).astype(bf16)
    scores = dot_t(q_rot, k_rot) * HD ** (-0.5)
    ahead = lax.broadcasted_iota(jnp.int32, scores.shape, 1) > lax.broadcasted_iota(
        jnp.int32, scores.shape, 0
    )
    scores = jnp.where(ahead, -1e30, scores)
    shifted = jnp.exp(scores - jnp.max(scores, axis=1, keepdims=True))
    probs = shifted / jnp.sum(shifted, axis=1, keepdims=True)
    return queries, key_rows, values, q_inv, k_inv, q_rot, k_rot, probs


def weight_grad(left, right, out, block, columns=None, take=slice(None)):
    na, nb, rows = left.shape[0], out.shape[1], out.shape[2]
    columns = columns or slice(0, right.shape[2])
    size = max(rows, 256)


    def chunk(i, carry):
        at = span(block * (nb * rows // size) + i, size)
        total = t_dot(left[0, :, at], right[0, :, take])
        for k in range(1, na):
            total = total + t_dot(left[k, :, at], right[k, :, take])
        for j in range(size // rows):
            part = total[j * rows : (j + 1) * rows].astype(bf16)
            out[block, i * (size // rows) + j, :, columns] = part
        return carry

    lax.fori_loop(0, nb * rows // size, chunk, 0)


def exchange_b(links, grad, held, columns):
    b = lax.axis_index("b")
    put = columns if held.shape[3] == grad.shape[3] or columns.stop <= held.shape[3] else slice(None)
    return [
        links.send(
            grad.at[:, across(b, j), :, columns], held.at[j - 1, :, :, put], {"b": across(b, j)}
        )
        for j in range(1, held.shape[0] + 1)
    ]


def sum_b(copies, own, held, out, columns):
    for copy in copies:
        copy.wait_recv()

    def add(block, carry):
        total = own(block)[:, columns].astype(f32)
        for j in range(held.shape[0]):
            total = total + held[j, block, :, columns].astype(f32)
        out[block, :, columns] = total.astype(bf16)
        return carry

    lax.fori_loop(0, held.shape[1], add, 0)


class Line:
    def __init__(self, links, na, block, own):
        self.links, self.na, self.block, self.own = links, na, block, own
        self.a, self.p = lax.axis_index("a"), lax.axis_index("p")
        self.hop_base = {1: links.reserve(na - 1), -1: links.reserve(na - 1)}
        self.pass_base = links.reserve(na)
        links.lines.append(self)

    def hop(self, way, t):
        a, na = self.a, self.na
        first = a - way * (t - 1)
        source = self.own if t == 1 else self.block(exclusive_or(first, a, na))
        target = self.block(exclusive_or(first, a + way, na))
        return self.links.copy(self.hop_base[way] + t - 1, source, target, {"a": (a + way) % na})

    def sends(self, way, t):
        first, last = self.a - way * (t - 1), self.a + way
        return (first >= 0) & (first < self.na) & (last >= 0) & (last < self.na)

    def to_pair(self, k, source=None):
        at = self.block(k)
        return self.links.copy(self.pass_base + k, at if source is None else source, at, {"p": 1 - self.p})

    def start(self):
        for way in (1, -1):

            @pl.when(self.sends(way, 1))
            def _(way=way):
                self.hop(way, 1).start()

    def pass_on(self, way, t):
        came = self.a - way * t

        @pl.when((came >= 0) & (came < self.na))
        def _():
            self.hop(way, t).wait_recv()
            self.to_pair(exclusive_or(came, self.a, self.na)).start()

        if t < self.na - 1:

            @pl.when(self.sends(way, t + 1))
            def _():
                self.hop(way, t + 1).start()

    def finish(self):
        for way in (1, -1):
            for t in range(1, self.na):

                @pl.when(self.sends(way, t))
                def _(way=way, t=t):
                    self.hop(way, t).wait_send()

        for k in range(self.na):
            self.to_pair(k).wait_send()


class Reduce:
    def __init__(self, na, links, part, out, scratch):
        self.na, self.links, self.part, self.out = na, links, part, out
        self.from_q, self.half_sum, self.from_p, self.to_a, self.from_a = scratch[:5]
        self.total, self.parts, self.cols, self.stat = scratch[5:9]
        self.a, self.p, self.q = (lax.axis_index(axis) for axis in ("a", "p", "q"))
        self.rows, self.width = out.shape[1:]
        self.quarter, self.half = self.width // 4, self.width // 2
        self.count = self.rows // HALVES
        self.mine, self.pair = span(2 * self.q + self.p, self.quarter), span(self.q, self.half)
        self.lead = list(range(2, na)) + [1, 0]
        self.step_q, self.step_p, self.step_a = {}, {}, {}
        self.spread_a, self.spread_p, self.spread_q, self.stats = {}, {}, {}, {}
        self.here = set()

    def at(self, h):
        return slice(h * self.count, (h + 1) * self.count)

    def each(self, h, body):
        def step(i, carry):
            body(pl.ds(pl.multiple_of(h * self.count + i * TILE, TILE), TILE))
            return carry

        lax.fori_loop(0, self.count // TILE, step, 0)

    def send_q(self, h, k):
        at, q = self.at(h), self.q
        source = self.part.at[k, at, span(1 - q, self.half)]
        self.step_q[h, k] = self.links.send(source, self.from_q.at[k, at], {"q": 1 - q})

    def send_p(self, h, k):
        self.step_q[h, k].wait_recv()

        def add(at):
            own = self.part[k, at, span(self.q, self.half)].astype(f32)
            self.half_sum[k, at] = (own + self.from_q[k, at].astype(f32)).astype(bf16)

        self.each(h, add)
        at, p = self.at(h), self.p
        source = self.half_sum.at[k, at, span(1 - p, self.quarter)]
        self.step_p[h, k] = self.links.send(source, self.from_p.at[k, at], {"p": 1 - p})

    def send_a(self, h, k):
        if not k:
            return
        self.step_p[h, k].wait_recv()

        def add(at):
            own = self.half_sum[k, at, span(self.p, self.quarter)].astype(f32)
            self.to_a[k - 1, at] = (own + self.from_p[k, at].astype(f32)).astype(bf16)

        self.each(h, add)
        at = self.at(h)
        self.step_a[h, k] = self.links.send(
            self.to_a.at[k - 1, at], self.from_a.at[k - 1, at], {"a": across(self.a, k)}
        )

    def add_all(self, at):
        own = self.half_sum[0, at, span(self.p, self.quarter)].astype(f32)
        own = own + self.from_p[0, at].astype(f32)
        for k in range(1, self.na):
            own = own + self.from_a[k - 1, at].astype(f32)
        return own

    def scattered(self, h, first, number):
        self.step_p[h, 0].wait_recv()
        for k in range(1, self.na):
            self.step_a[h, k].wait_recv()
        self.each(h, first)
        if number:
            at = self.at(h)
            stats = to_row(self.parts[0, at], 0)
            if number == 2:
                stats = stats + to_row(self.parts[1, at], 1)
            stat = self.stat
            stat[h, 0] = stats
            self.stats[h] = self.links.send(stat.at[h, 0], stat.at[h, 1], {"p": 1 - self.p})

    def stats_q(self, h):
        stat = self.stat
        self.stats[h].wait_recv()
        stat[h, 2] = stat[h, 0] + stat[h, 1]
        self.stats[h] = self.links.send(stat.at[h, 2], stat.at[h, 3], {"q": 1 - self.q})

    def stats_done(self, h, number):
        stat = self.stat
        self.stats[h].wait_recv()
        stats = (stat[h, 2] + stat[h, 3]) / self.width
        for i in range(number):
            self.cols[i, self.at(h)] = to_column(stats, i)

    def spread(self, h, blocks):
        here = self.out.at[0, self.at(h), self.mine]
        for k in blocks:
            if k:
                target = self.out.at[k, self.at(h), self.mine]
                self.spread_a[h, k] = self.links.send(here, target, {"a": across(self.a, k)})
        self.spread_p[h, 0] = self.links.send(here, here, {"p": 1 - self.p})

    def relay_p(self, h, k):
        if not k:
            return
        self.spread_a[h, k].wait_recv()
        here = self.out.at[k, self.at(h), self.mine]
        self.spread_p[h, k] = self.links.send(here, here, {"p": 1 - self.p})

    def relay_q(self, h, k):
        self.spread_p[h, k].wait_recv()
        here = self.out.at[k, self.at(h), self.pair]
        self.spread_q[h, k] = self.links.send(here, here, {"q": 1 - self.q})

    def arrived(self, h, k):
        if (h, k) not in self.here:
            self.here.add((h, k))
            self.spread_q[h, k].wait_recv()

    def steps(self, first, second, number, chain=False):
        def normed(h):
            self.stats_done(h, number)
            self.each(h, second)

        def spread_own(h):
            here = self.out.at[0, self.at(h), self.mine]
            self.spread_p[h, 0] = self.links.send(here, here, {"p": 1 - self.p})

        def spread_far(h, k):
            here = self.out.at[0, self.at(h), self.mine]
            target = self.out.at[k, self.at(h), self.mine]
            self.spread_a[h, k] = self.links.send(here, target, {"a": across(self.a, k)})

        table = {
            "P": self.send_p,
            "A": self.send_a,
            "SC": lambda h: self.scattered(h, first, number),
            "SQ": self.stats_q,
            "SD": normed,
            "X": spread_own,
            "Z": spread_far,
            "RP": self.relay_p,
            "RQ": self.relay_q,
        }
        if chain:
            lines = [
                Line(
                    self.links,
                    self.na,
                    lambda k, h=h: self.out.at[k, self.at(h), self.mine],
                    self.out.at[0, self.at(h), self.mine],
                )
                for h in range(HALVES)
            ]

            def pair_arrived(h, k):
                self.spread_p[h, k] = lines[h].to_pair(k)
                self.relay_q(h, k)

            table.update(
                X=lambda h: lines[h].to_pair(0).start(),
                Z=lambda h: lines[h].start(),
                FL=lambda h, t: lines[h].pass_on(1, t),
                FR=lambda h, t: lines[h].pass_on(-1, t),
                RQ=pair_arrived,
            )
        return table


class OverHeads:
    def __init__(self, links, na, a, p, q, held, from_a, out_ref):
        self.links, self.na, self.a, self.p, self.q = links, na, a, p, q
        self.held, self.from_a, self.out_ref = held, from_a, out_ref

    def to_pair(self):
        self.copy = self.links.send(self.held.at[0], self.held.at[1], {"p": 1 - self.p})

    def to_core(self):
        held = self.held
        self.copy.wait_recv()
        held[2] = held[0] + held[1]
        self.copy = self.links.send(held.at[2], held.at[3], {"q": 1 - self.q})

    def to_all(self):
        held = self.held
        self.copy.wait_recv()
        held[4] = held[2] + held[3]
        self.copies = [
            self.links.send(held.at[4], self.from_a.at[k - 1], {"a": across(self.a, k)})
            for k in range(1, self.na)
        ]

    def done(self):
        for copy in self.copies:
            copy.wait_recv()
        for k in range(self.na):
            for i in range(2):
                at = 2 * k + i
                total = self.held[4, at : at + 1]
                for j in range(1, self.na):
                    other = 2 * (k ^ j) + i
                    total = total + self.from_a[j - 1, other : other + 1]
                self.out_ref[at : at + 1] = total


def reduce_peers(na):
    a, p, q = lax.axis_index("a"), lax.axis_index("p"), lax.axis_index("q")
    return [{"q": 1 - q}, {"p": 1 - p}] + [{"a": across(a, k)} for k in range(1, na)]


def attn_math(r, tok_ref, gain_ref, proj_ref, inv_ref, res_ref):
    def first(at):
        own = r.add_all(at)
        proj_ref[at] = own
        r.parts[0, at] = fold(own * own)

    def second(at):
        own = proj_ref[at]
        inv = lax.rsqrt(r.cols[0, at] + epsilon)
        inv_ref[at] = inv
        residual = tok_ref[at].astype(f32) + own * wide(inv, r.quarter) * gain_ref[0:1]
        res_ref[at] = residual
        r.out[0, at, r.mine] = residual.astype(bf16)

    return first, second


def mlp_math(r, res_ref, grad_ref, gain_ref, block_ref, sum_ref):
    def first(at):
        own = r.add_all(at)
        r.total[at] = own
        r.parts[0, at] = fold(own * own)
        r.parts[1, at] = fold(grad_ref[at] * gain_ref[1:2] * own)

    def second(at):
        own = r.total[at]
        inv = wide(lax.rsqrt(r.cols[0, at] + epsilon), r.quarter)
        upstream = grad_ref[at]
        scaled = upstream * gain_ref[1:2]
        normed = own * inv
        block_ref[0, at, r.mine] = (res_ref[at] + normed * gain_ref[1:2]).astype(bf16)
        gains = upstream * normed
        sum_ref[...] += jnp.sum(gains.reshape(TILE // 8, 8, r.quarter), axis=0)
        grad = inv * scaled - own * inv * inv * inv * wide(r.cols[1, at], r.quarter)
        r.out[0, at, r.mine] = grad.astype(bf16)

    return first, second


def back_math(r, grad_ref, proj_ref, inv_ref, gain_ref, res_ref, sum_ref):
    def first(at):
        grad = grad_ref[at] + r.add_all(at)
        res_ref[at] = grad
        r.parts[0, at] = fold(grad * gain_ref[0:1] * proj_ref[at])

    def second(at):
        own = proj_ref[at]
        inv = wide(inv_ref[at], r.quarter)
        upstream = res_ref[at]
        gains = upstream * own * inv
        sum_ref[...] += jnp.sum(gains.reshape(TILE // 8, 8, r.quarter), axis=0)
        grad = inv * (upstream * gain_ref[0:1])
        grad = grad - own * inv * inv * inv * wide(r.cols[0, at], r.quarter)
        r.out[0, at, r.mine] = grad.astype(bf16)

    return first, second


MIDDLE = (
    ("F", 2), ("F", 3), ("rP", 0, 2), ("F", 1), ("rP", 0, 3), ("rA", 0, 2), ("rP", 0, 1), ("rP", 1, 3),
    ("F", 0), ("rP", 1, 2), ("rA", 0, 3), ("rP", 1, 1), ("rA", 0, 1), ("rP", 0, 0), ("rA", 1, 3),
    ("rA", 1, 1), ("rA", 1, 2), ("rSC", 0), ("rP", 1, 0), ("rSQ", 0), ("rSD", 0), ("rZ", 0, 1), ("rX", 0),
    ("rZ", 0, 3), ("rSC", 1), ("rRP", 0, 1), ("rRQ", 0, 0), ("rSQ", 1), ("rZ", 0, 2), ("rSD", 1),
    ("rRP", 0, 3), ("rX", 1), ("rZ", 1, 1), ("rZ", 1, 2), ("rRP", 0, 2), ("rRQ", 0, 1), ("rRQ", 0, 3),
    ("rRP", 1, 1), ("B", 0, 3), ("rZ", 1, 3), ("rRP", 1, 2), ("rRQ", 1, 0), ("B", 0, 1), ("rRQ", 0, 2),
    ("sP", 0, 3), ("B", 0, 0), ("B", 0, 2), ("rRP", 1, 3), ("rRQ", 1, 2), ("sA", 0, 3), ("sP", 0, 2),
    ("B", 1, 2), ("sP", 0, 1), ("rRQ", 1, 1), ("rRQ", 1, 3), ("sA", 0, 2), ("sP", 1, 2), ("D", 0),
    ("sA", 0, 1), ("B", 1, 3), ("sA", 1, 2), ("sP", 1, 3), ("B", 1, 0), ("sP", 0, 0), ("D", 1),
    ("sA", 1, 3), ("sP", 1, 0), ("B", 1, 1), ("sSC", 0), ("sP", 1, 1), ("DS", 0), ("ZD", 0, 2), ("sSQ", 0),
    ("G", 0), ("sSD", 0), ("BP",), ("sA", 1, 1), ("G", 2), ("sZ", 0, 3), ("G", 3), ("sZ", 0, 2), ("sSC", 1),
    ("G", 1), ("YG",), ("sSQ", 1), ("sRP", 0, 3), ("sSD", 1), ("sZ", 1, 3), ("DS", 1), ("sZ", 1, 1),
    ("sZ", 0, 1), ("BQ",), ("sX", 0), ("ZD", 1, 3), ("sRP", 1, 1), ("sX", 1), ("sRQ", 1, 1), ("sZ", 1, 2),
    ("sRP", 0, 2), ("sRP", 0, 1), ("ZD", 0, 1), ("ZD", 1, 1), ("sRP", 1, 2), ("sRP", 1, 3), ("ZD", 1, 2),
    ("sRQ", 0, 0), ("sRQ", 0, 3), ("ZD", 0, 3), ("sRQ", 1, 0), ("sRQ", 1, 2), ("sRQ", 0, 2), ("sRQ", 0, 1),
    ("sRQ", 1, 3), ("SG",),
)


def middle_kernel(na, nb, *refs):
    x_ref, w_ref, res_ref, grad_far, proj_ref, inv_ref, gain_ref = refs[:7]
    block_ref, back_out, ffn_sum_ref, grad_res_ref, attn_sum_ref, down_sum_ref, gu_grad_ref = refs[7:14]
    down_in, gate_sum_ref = refs[14:16]
    out, hidden_ref, grad_gu_ref, gu_ref, part_ref, down_grad, down_held, grad_ref, gu_held = refs[16:25]
    scratch, (local_sem, send_sem, recv_sem) = refs[25:-3], refs[-3:]
    share = 2 * lax.axis_index("q") + lax.axis_index("p")
    load = pltpu.make_async_copy(
        grad_far.at[:, span(share, grad_ref.shape[1])], grad_ref, local_sem.at[0]
    )
    load.start()
    units = hidden_ref.shape[2]
    width = x_ref.shape[2]
    b = lax.axis_index("b")
    greet(reduce_peers(na) + [{"b": across(b, j)} for j in range(1, nb)])
    links = Links(send_sem, recv_sem)
    r = Reduce(na, links, part_ref, out, scratch[:9])
    s = Reduce(na, links, part_ref, back_out, scratch[9:])
    ffn_sum_ref[...] = jnp.zeros_like(ffn_sum_ref)
    attn_sum_ref[...] = jnp.zeros_like(attn_sum_ref)
    wide_tile = 512

    def forward(k):
        def gated(n, carry):
            at, up_at = span(n, 256), pl.ds(pl.multiple_of(units + n * 256, 256), 256)
            gate = dot(x_ref[k], w_ref[:, at])
            up = dot(x_ref[k], w_ref[:, up_at])
            gu_ref[k, :, at] = gate
            gu_ref[k, :, up_at] = up
            hidden_ref[k, :, at] = (gate * jax.nn.sigmoid(gate) * up).astype(bf16)
            return carry

        lax.fori_loop(0, units // 256, gated, 0)

        def down(n, carry):
            at = span(n, wide_tile)
            part_ref[k, :, at] = dot_t(hidden_ref[k], w_ref[at, 2 * units :]).astype(bf16)
            return carry

        lax.fori_loop(0, width // wide_tile, down, 0)

    def backward(h, k):
        rows = r.at(h)

        def gated(n, carry):
            at, up_at = span(n, 256), pl.ds(pl.multiple_of(units + n * 256, 256), 256)
            down_at = pl.ds(pl.multiple_of(2 * units + n * 256, 256), 256)
            grad_hidden = dot(out[k, rows], w_ref[:, down_at])
            gate, up = gu_ref[k, rows, at], gu_ref[k, rows, up_at]
            sigmoid = jax.nn.sigmoid(gate)
            active = gate * sigmoid
            grad_gu_ref[k, rows, at] = (
                grad_hidden * up * (sigmoid * (1.0 + gate * (1.0 - sigmoid)))
            ).astype(bf16)
            grad_gu_ref[k, rows, up_at] = (grad_hidden * active).astype(bf16)
            return carry

        lax.fori_loop(0, units // 256, gated, 0)

        def back(n, carry):
            at = span(n, wide_tile)
            part_ref[k, rows, at] = dot_t(
                grad_gu_ref[k, rows], w_ref[at, : 2 * units]
            ).astype(bf16)
            return carry

        lax.fori_loop(0, width // wide_tile, back, 0)

    first, second = mlp_math(r, res_ref, grad_ref, gain_ref, block_ref, ffn_sum_ref)
    back_first, back_second = back_math(
        s, grad_ref, proj_ref, inv_ref, gain_ref, grad_res_ref, attn_sum_ref
    )
    copies, reused = {}, []
    gate = slice(0, units)

    def half(c):
        return slice(c * units // 2, (c + 1) * units // 2)

    def forward_step(k):
        forward(k)
        for h in range(HALVES):
            r.send_q(h, k)

    def backward_step(h, k):
        if not reused:
            links.sent(r.step_q.values())
            reused.append(True)
        r.arrived(h, k)
        backward(h, k)
        s.send_q(h, k)

    def block_p():
        here = block_ref.at[0, :, r.mine]
        copies["p"] = links.send(here, here, {"p": 1 - r.p})

    def block_q():
        copies["p"].wait_recv()
        here = block_ref.at[0, :, r.pair]
        copies["q"] = links.send(here, here, {"q": 1 - r.q})

    def down_grads(c):
        for h in range(HALVES):
            for k in range(na):
                r.arrived(h, k)
        for block in range(na):
            weight_grad(out, hidden_ref, down_grad, block, half(c), half(c))
        copies["d", c] = exchange_b(links, down_grad, down_held, half(c))

    def down_sums(c):
        own = lambda block: down_grad.at[block, b]
        sum_b(copies["d", c], own, down_held, down_sum_ref, half(c))

    def down_owner(c, k):
        copies["z", c, k] = links.send(
            down_sum_ref.at[across(r.a, k), :, half(c)], down_in.at[k - 1, :, half(c)], {"a": across(r.a, k)}
        )

    def gate_rows():
        copies["g"] = exchange_b(links, gu_grad_ref, gu_held, gate)

    table = {
        "F": forward_step,
        "B": backward_step,
        "BP": block_p,
        "BQ": block_q,
        "D": down_grads,
        "DS": down_sums,
        "ZD": down_owner,
        "YG": gate_rows,
        "SG": lambda: sum_b(
            copies["g"], lambda block: gu_grad_ref.at[block, b], gu_held, gate_sum_ref, gate
        ),
        "G": lambda block: weight_grad(x_ref, grad_gu_ref, gu_grad_ref, block),
    }
    table.update({"r" + key: step for key, step in r.steps(first, second, 2).items()})
    table.update({"s" + key: step for key, step in s.steps(back_first, back_second, 1).items()})
    load.wait()
    for key, *where in MIDDLE:
        table[key](*where)
    for h in range(HALVES):
        for k in range(na):
            s.arrived(h, k)
    copies["q"].wait_recv()
    for c in range(2):
        for k in range(1, na):
            copies["z", c, k].wait_recv()
    links.finish()


def middle_call(nb, x_all, w_mlp, res_mine, out_grad, proj_mine, inv_mine, width_gain):
    na, rows, width = x_all.shape
    quarter, units = width // 4, w_mlp.shape[1] // 3
    w_rows = width // (na * nb)
    vmem, far = pl.BlockSpec(memory_space=pltpu.VMEM), pl.BlockSpec(memory_space=pl.ANY)
    shape = jax.ShapeDtypeStruct
    outs = (
        shape((1, rows, width), bf16),
        shape((na, rows, width), bf16),
        shape((8, quarter), f32),
        shape((rows, quarter), f32),
        shape((8, quarter), f32),
        shape((na, w_rows, units), bf16),
        shape((na, nb, w_rows, 2 * units), bf16),
        shape((na - 1, w_rows, units), bf16),
        shape((na, w_rows, units), bf16),
    )
    copies = 2 * HALVES * (6 * na + 1) + 2 + 3 * nb + 2 * na
    return pl.pallas_call(
        functools.partial(middle_kernel, na, nb),
        out_shape=outs,
        in_specs=[far if i == 3 else vmem for i in range(7)],
        out_specs=(vmem,) * len(outs),
        scratch_shapes=[
            pltpu.VMEM((na, rows, width), bf16),
            pltpu.VMEM((na, rows, units), bf16),
            pltpu.VMEM((na, rows, 2 * units), bf16),
            pltpu.VMEM((na, rows, 2 * units), f32),
            pltpu.VMEM((na, rows, width), bf16),
            pltpu.VMEM((na, nb, w_rows, units), bf16),
            pltpu.VMEM((nb - 1, na, w_rows, units), bf16),
            pltpu.VMEM((rows, quarter), f32),
            pltpu.VMEM((nb - 1, na, w_rows, units), bf16),
        ]
        + reduce_scratch(na, rows, width)
        + reduce_scratch(na, rows, width)
        + [
            pltpu.SemaphoreType.DMA((1,)),
            pltpu.SemaphoreType.DMA((copies,)),
            pltpu.SemaphoreType.DMA((copies,)),
        ],
        compiler_params=pltpu.CompilerParams(
            collective_id=2, has_side_effects=True, vmem_limit_bytes=VMEM_LIMIT
        ),
        name="middle",
    )(x_all, w_mlp, res_mine, out_grad, proj_mine, inv_mine, width_gain)


LAST = (
    ("ZG", 0, 2), ("U1",), ("YG", 1), ("AB", 0), ("U2",), ("AB", 1), ("ZG", 0, 1), ("AB", 2),
    ("WO", 3), ("U3",), ("ZG", 0, 3), ("AB", 3), ("OD", 2), ("S1",), ("S2",), ("S3",), ("WO", 0),
    ("SG", 1), ("ZG", 1, 2), ("S4",), ("QB", 1), ("QB", 0), ("QB", 2), ("QB", 3), ("U4",), ("OWNG",),
    ("OG", 0, 3), ("WQ", 1), ("ZG", 1, 3), ("rP", 1, 3), ("WQ", 2), ("rP", 0, 0), ("ZG", 1, 1),
    ("OG", 0, 1), ("rP", 1, 2), ("rP", 0, 1), ("WQ", 0), ("rP", 1, 0), ("WO", 1), ("rA", 1, 3),
    ("WO", 2), ("WQ", 3), ("YA",), ("OG", 0, 2), ("OD", 1), ("rP", 0, 2), ("rA", 1, 2), ("rA", 0, 1),
    ("OG", 1, 1), ("OG", 1, 2), ("rA", 0, 2), ("rP", 1, 1), ("rP", 0, 3), ("rA", 1, 1), ("OD", 3),
    ("rA", 0, 3), ("OG", 1, 3), ("rSC", 1), ("SA",), ("ZA", 2), ("U5",), ("rSC", 0), ("rX", 0), ("ZA", 3),
    ("ZA", 1), ("OWN",), ("rX", 1), ("rRQ", 0, 0), ("OA", 2), ("OA", 1), ("rRQ", 1, 0),
    ("OA", 3),
)


def last_kernel(na, nb, *refs):
    proj_ref, x_far, qkv_ref, stats_ref, gain_ref, cos_ref, sin_ref, w_ref, att_ref = refs[:9]
    grad_ref, attn_sum_ref, ffn_sum_ref, down_sum_ref, gu_grad_far, down_in, gate_ref = refs[9:16]
    out, sums_ref, down_far, gu_far, qkv_out, wout_out = refs[16:22]
    scaled_ref, grad_qkv_ref, part_ref, head_sums, held, stats_a, inner_ref = refs[22:29]
    own_sums, a_sums, b_sums, up_held, up_sum, attn_grad, attn_held, attn_sum = refs[29:37]
    gu_in, attn_in, x_ref, up_own, down_out, gu_out = refs[37:43]
    scratch, (local_sem, send_sem, recv_sem) = refs[43:-3], refs[-3:]
    links = Links(send_sem, recv_sem)
    load_gu = pltpu.make_async_copy(
        gu_grad_far.at[:, lax.axis_index("b"), :, gate_ref.shape[2] :], up_own, local_sem.at[0]
    )
    load_gu.start()
    load_x = pltpu.make_async_copy(x_far, x_ref, local_sem.at[1])
    load_x.start()
    save_down = pltpu.make_async_copy(down_out, down_far, local_sem.at[2])
    save_gu = pltpu.make_async_copy(gu_out, gu_far, local_sem.at[3])
    r = Reduce(na, links, part_ref, out, scratch)
    a, b, p, q, mine, pair, quarter = (
        r.a, lax.axis_index("b"), r.p, r.q, r.mine, r.pair, r.quarter,
    )
    units = down_sum_ref.shape[2]
    own_sums[...] = jnp.zeros_like(own_sums)
    own_sums[0:1, mine] = jnp.sum(attn_sum_ref[...], axis=0, keepdims=True)
    own_sums[1:2, mine] = jnp.sum(ffn_sum_ref[...], axis=0, keepdims=True)
    held[0] = jnp.zeros_like(held[0])
    head_sums[...] = jnp.zeros_like(head_sums)
    greet(reduce_peers(na) + [{"b": across(b, j)} for j in range(1, nb)])
    copies, stored = {}, []
    whole, upper = slice(0, units), slice(units, 2 * units)
    attn_columns = slice(0, 4 * HD)
    over_heads = OverHeads(links, na, a, p, q, held, stats_a, inner_ref)

    def sums_pair():
        here = own_sums.at[:, mine]
        copies["u"] = links.send(here, here, {"p": 1 - p})

    def sums_core():
        copies["u"].wait_recv()
        here = own_sums.at[:, pair]
        copies["u"] = links.send(here, here, {"q": 1 - q})

    def sums_far():
        copies["u"].wait_recv()
        copies["u"] = [
            links.send(
                own_sums.at[:, span(across(a, k), quarter)], a_sums.at[k - 1], {"a": across(a, k)}
            )
            for k in range(1, na)
        ]

    def sums_b():
        for copy in copies["u"]:
            copy.wait_recv()
        total = own_sums[:, span(a, quarter)]
        for k in range(1, na):
            total = total + a_sums[k - 1]
        b_sums[0, :, :quarter] = total
        b_sums[0, :, quarter:] = head_sums[...]
        copies["u"] = [
            links.send(b_sums.at[0], b_sums.at[j], {"b": across(b, j)}) for j in range(1, nb)
        ]

    def sums_done():
        for copy in copies["u"]:
            copy.wait_recv()
        total = b_sums[0]
        for j in range(1, nb):
            total = total + b_sums[j]
        sums_ref[...] = total

    def attend_back(k):
        if k % 2 == 0:
            lax.fori_loop(k, k + 2, attend_back_block, 0)

    def attend_back_block(k, carry):
        queries, key_rows, values, q_inv, k_inv, q_rot, k_rot, probs = attention(
            k, qkv_ref[k], stats_ref[...], gain_ref, cos_ref, sin_ref
        )
        cos_table, sine_table = cos_ref[...], sin_ref[...]
        grad_att = dot(proj_ref[k], w_ref[:, 3 * HD :]).astype(bf16)
        grad_v = t_dot(probs.astype(bf16), grad_att)
        grad_p = dot_t(grad_att, values)
        delta = jnp.sum(probs * grad_p, axis=1, keepdims=True)
        grad_scores = (probs * (grad_p - delta) * HD ** (-0.5)).astype(bf16)
        grad_q = dot(grad_scores, k_rot)
        grad_k = t_dot(grad_scores, q_rot)
        grad_q = grad_q * cos_table + rotate_back(grad_q * sine_table)
        grad_k = grad_k * cos_table + rotate_back(grad_k * sine_table)
        head_sums[0:1] += jnp.sum(grad_q * queries * q_inv, axis=0, keepdims=True)
        head_sums[1:2] += jnp.sum(grad_k * key_rows * k_inv, axis=0, keepdims=True)
        scaled_q = grad_q * gain_ref[0:1]
        scaled_k = grad_k * gain_ref[1:2]
        scaled_ref[k, :, :HD] = scaled_q
        scaled_ref[k, :, HD:] = scaled_k
        grad_qkv_ref[k, :, 2 * HD :] = grad_v.astype(bf16)
        held[0] += to_row(scaled_q * queries, 2 * k) + to_row(scaled_k * key_rows, 2 * k + 1)
        return carry

    def qkv_back(k):
        for i in range(2):
            at = slice(i * HD, (i + 1) * HD)
            inv = lax.rsqrt(to_column(stats_ref[...] / HQ, 2 * k + i) + epsilon)
            mean = to_column(inner_ref[...] / HQ, 2 * k + i)
            grad = inv * scaled_ref[k, :, at] - qkv_ref[k, :, at] * inv * inv * inv * mean
            grad_qkv_ref[k, :, at] = grad.astype(bf16)

        def part(n, carry):
            at = span(n, 512)
            part_ref[k, :, at] = dot_t(grad_qkv_ref[k], w_ref[at, : 3 * HD]).astype(bf16)
            return carry

        lax.fori_loop(0, part_ref.shape[2] // 512, part, 0)
        for h in range(HALVES):
            r.send_q(h, k)

    def qkv_grads(block):
        if "x" not in copies:
            load_x.wait()
            copies["x"] = True
        weight_grad(x_ref, grad_qkv_ref, attn_grad, block, slice(0, 3 * HD))

    def up_rows(_):
        copies["up"] = exchange_b(links, gu_grad_far, up_held, upper)

    def up_sums(_):
        load_gu.wait()
        own = lambda block: up_own.at[block]
        sum_b(copies["up"], own, up_held, up_sum, whole)

    def gu_owner(c, k):
        source = up_sum if c else gate_ref
        copies["g", c, k] = links.send(
            source.at[across(a, k)], gu_in.at[k - 1, c], {"a": across(a, k)}
        )

    def attn_rows():
        copies["at"] = exchange_b(links, attn_grad, attn_held, attn_columns)

    def attn_sums():
        own = lambda block: attn_grad.at[block, b]
        sum_b(copies["at"], own, attn_held, attn_sum, attn_columns)

    def attn_owner(k):
        copies["a", k] = links.send(attn_sum.at[across(a, k)], attn_in.at[k - 1], {"a": across(a, k)})

    def store(target, index, size, value):
        target[:, span(index, size)] = value.astype(f32)

    def store_gu(c, k, value):
        gu_out[:, c, span(across(a, k), units)] = value.astype(f32)
        stored.append((c, k))
        if len(stored) == 2 * na:
            save_gu.start()

    def store_attn(k, values):
        for c in range(3):
            store(qkv_out.at[c], across(a, k), HD, values[:, c * HD : (c + 1) * HD])
        store(wout_out, across(a, k), HD, values[:, 3 * HD :])

    def own_gu():
        store_gu(0, 0, gate_ref[a])
        store_gu(1, 0, up_sum[a])

    def gu_arrived(c, k):
        copies["g", c, k].wait_recv()
        store_gu(c, k, gu_in[k - 1, c])

    def attn_arrived(k):
        copies["a", k].wait_recv()
        store_attn(k, attn_in[k - 1])

    def down_rows(k):
        if "down" not in copies:
            copies["down"] = 0
            store(down_out, a, units, down_sum_ref[a])
        store(down_out, across(a, k), units, down_in[k - 1])
        copies["down"] += 1
        if copies["down"] == na - 1:
            save_down.start()

    def first(at):
        out[0, at, mine] = (grad_ref[at] + r.add_all(at)).astype(bf16)

    table = {
        "U1": sums_pair,
        "U2": sums_core,
        "U3": sums_far,
        "U4": sums_b,
        "U5": sums_done,
        "AB": attend_back,
        "S1": over_heads.to_pair,
        "S2": over_heads.to_core,
        "S3": over_heads.to_all,
        "S4": over_heads.done,
        "WO": lambda block: weight_grad(proj_ref, att_ref, attn_grad, block, slice(3 * HD, 4 * HD)),
        "WQ": qkv_grads,
        "QB": qkv_back,
        "YG": up_rows,
        "SG": up_sums,
        "ZG": gu_owner,
        "YA": attn_rows,
        "SA": attn_sums,
        "ZA": attn_owner,
        "OWNG": own_gu,
        "OWN": lambda: store_attn(0, attn_sum[a]),
        "OD": down_rows,
        "OG": gu_arrived,
        "OA": attn_arrived,
    }
    table.update({"r" + key: step for key, step in r.steps(first, None, 0).items()})
    for key, *where in LAST:
        table[key](*where)
    for h in range(HALVES):
        r.arrived(h, 0)
    save_down.wait()
    save_gu.wait()
    links.finish()


def last_call(nb, *operands):
    na, rows, width = operands[0].shape
    w_rows, units = operands[12].shape[1:]
    quarter = width // 4
    vmem, far = pl.BlockSpec(memory_space=pltpu.VMEM), pl.BlockSpec(memory_space=pl.ANY)
    shape = jax.ShapeDtypeStruct
    outs = (
        shape((1, rows, width), bf16),
        shape((8, quarter + HD), f32),
        shape((w_rows, na * units), f32),
        shape((w_rows, 2, na * units), f32),
        shape((3, w_rows, na * HD), f32),
        shape((w_rows, na * HD), f32),
    )
    copies = HALVES * (3 * na + 1) + 2 + 6 * na + 4 * nb
    return pl.pallas_call(
        functools.partial(last_kernel, na, nb),
        out_shape=outs,
        in_specs=[far if i in (1, 13) else vmem for i in range(16)],
        out_specs=(vmem, vmem, far, far, vmem, vmem),
        scratch_shapes=[
            pltpu.VMEM((na, rows, 2 * HD), f32),
            pltpu.VMEM((na, rows, 3 * HD), bf16),
            pltpu.VMEM((na, rows, width), bf16),
            pltpu.VMEM((8, HD), f32),
            pltpu.VMEM((5, 8, rows), f32),
            pltpu.VMEM((na - 1, 8, rows), f32),
            pltpu.VMEM((8, rows), f32),
            pltpu.VMEM((8, width), f32),
            pltpu.VMEM((na - 1, 8, quarter), f32),
            pltpu.VMEM((nb, 8, quarter + HD), f32),
            pltpu.VMEM((nb - 1, na, w_rows, units), bf16),
            pltpu.VMEM((na, w_rows, units), bf16),
            pltpu.VMEM((na, nb, w_rows, 4 * HD), bf16),
            pltpu.VMEM((nb - 1, na, w_rows, 4 * HD), bf16),
            pltpu.VMEM((na, w_rows, 4 * HD), bf16),
            pltpu.VMEM((na - 1, 2, w_rows, units), bf16),
            pltpu.VMEM((na - 1, w_rows, 4 * HD), bf16),
            pltpu.VMEM((na, rows, width), bf16),
            pltpu.VMEM((na, w_rows, units), bf16),
            pltpu.VMEM((w_rows, na * units), f32),
            pltpu.VMEM((w_rows, 2, na * units), f32),
        ]
        + reduce_scratch(na, rows, width)
        + [
            pltpu.SemaphoreType.DMA((4,)),
            pltpu.SemaphoreType.DMA((copies,)),
            pltpu.SemaphoreType.DMA((copies,)),
        ],
        compiler_params=pltpu.CompilerParams(
            collective_id=4, has_side_effects=True, vmem_limit_bytes=VMEM_LIMIT
        ),
        name="last",
    )(*operands)


def reduce_scratch(na, rows, width):
    quarter = width // 4
    return [
        pltpu.VMEM((na, rows, width // 2), bf16),
        pltpu.VMEM((na, rows, width // 2), bf16),
        pltpu.VMEM((na, rows, quarter), bf16),
        pltpu.VMEM((na - 1, rows, quarter), bf16),
        pltpu.VMEM((na - 1, rows, quarter), bf16),
        pltpu.VMEM((rows, quarter), f32),
        pltpu.VMEM((2, rows, 128), f32),
        pltpu.VMEM((2, rows, 128), f32),
        pltpu.VMEM((HALVES, 4, 8, rows // HALVES), f32),
    ]


ENTER = (
    ("Z", 0), ("W", 3), ("FW", 0), ("FR", 0, 1), ("FL", 0, 1), ("W", 1), ("CUT", 2), ("FW", 1), ("W", 2),
    ("FR", 0, 2), ("FR", 0, 3), ("CUT", 3), ("M", 0, 3), ("FL", 0, 2), ("CUT", 1), ("FW", 3), ("FL", 0, 3),
    ("GA",), ("FT", 0), ("FQ", 3), ("FW", 2), ("CUT", 0), ("FQ", 2), ("M", 0, 1), ("M", 2, 3), ("FQ", 1),
    ("J", 3), ("FQ", 0), ("J", 0), ("GB",), ("M", 1, 1), ("J", 1), ("J", 2), ("S1",), ("S2",), ("S3",),
    ("M", 1, 3), ("MR", 1, 0), ("M", 1, 2), ("S4",), ("E", 3), ("E", 1), ("rP", 1, 3), ("E", 2),
    ("rP", 1, 1), ("M", 2, 1), ("MR", 2, 3), ("rP", 0, 3), ("rP", 0, 1), ("MR", 0, 3), ("E", 0),
    ("rA", 1, 3), ("MR", 2, 0), ("rA", 1, 1), ("MR", 0, 1), ("rA", 0, 3), ("MR", 1, 3), ("rP", 0, 2),
    ("MR", 2, 1), ("rA", 0, 2), ("rA", 0, 1), ("rP", 0, 0), ("rP", 1, 2), ("rA", 1, 2), ("MR", 1, 2),
    ("rP", 1, 0), ("rSC", 0), ("rSQ", 0), ("MR", 0, 0), ("M", 2, 2), ("rSC", 1), ("rSD", 0), ("rSQ", 1),
    ("rX", 0), ("rSD", 1), ("rZ", 0), ("rZ", 1), ("rFR", 0, 1), ("rFL", 0, 1), ("rX", 1), ("MR", 2, 2),
    ("rFR", 1, 1), ("rFL", 1, 1), ("rFR", 0, 2), ("rRQ", 0, 0), ("rFL", 1, 2), ("rFL", 0, 2), ("MR", 1, 1),
    ("rFR", 0, 3), ("M", 0, 2), ("rFR", 1, 2), ("rFL", 1, 3), ("rFR", 1, 3), ("rFL", 0, 3), ("rRQ", 0, 1),
    ("MR", 0, 2), ("rRQ", 1, 1), ("rRQ", 1, 2), ("rRQ", 0, 2), ("rRQ", 1, 0), ("rRQ", 1, 3), ("rRQ", 0, 3),
)


def enter_kernel(na, nb, gain_sizes, *refs):
    tok_far, qkv_w_ref, wout_ref, gu_ref, down_ref, cos_ref, sin_ref, all_gains_ref = refs[:8]
    x_far, w_far, mlp_w_ref, width_gain_ref, head_gain_ref, qkv_far, stats_ref, att_far = refs[8:16]
    out, proj_ref, inv_ref, res_ref = refs[16:20]
    own_gains, gains_ref, piece_ref, part_ref, held, stats_a = refs[20:26]
    x_ref, w_ref, qkv_ref, att_ref = refs[26:30]
    tok_ref = refs[30]
    scratch, (local_sem, send_sem, recv_sem) = refs[31:-3], refs[-3:]
    saves = [
        pltpu.make_async_copy(near, there, local_sem.at[5 + i])
        for i, (near, there) in enumerate(
            ((x_ref, x_far), (w_ref, w_far), (qkv_ref, qkv_far), (att_ref, att_far))
        )
    ]
    a, b, p, q = (lax.axis_index(axis) for axis in ("a", "b", "p", "q"))
    rows = wout_ref.shape[0]
    quarter = tok_ref.shape[1]
    load = pltpu.make_async_copy(
        tok_far.at[:, span(2 * q + p, quarter)], tok_ref, local_sem.at[9]
    )
    load.start()
    units = down_ref.shape[1] // na
    own_gains[...] = jnp.zeros_like(own_gains)
    n_d, n_h = gain_sizes
    place = 0
    for i, size in enumerate((n_d, n_d, n_h, n_h)):
        own_gains[i : i + 1, :size] = all_gains_ref[:, place : place + size].astype(f32)
        place += size
    gains_ref[a, b] = own_gains[...]
    greet(
        [{"q": 1 - q}, {"p": 1 - p}]
        + [{"a": across(a, k)} for k in range(1, na)]
        + [{"b": across(b, j)} for j in range(1, nb)]
    )
    load.wait()
    links = Links(send_sem, recv_sem)
    mine, pair = span(2 * q + p, quarter), span(q, 2 * quarter)
    place = span(a * nb + b, rows)
    copies, ends = {}, []
    locals_ = [pltpu.make_async_copy(tok_ref, x_ref.at[0, :, mine], local_sem.at[0])]

    def weight_sources(k):
        block = span(across(a, k), HD)
        sources = [qkv_w_ref.at[c, :, block] for c in range(3)] + [wout_ref.at[:, block]]
        return [(s, w_ref.at[place, c * HD : (c + 1) * HD]) for c, s in enumerate(sources)]

    for c, (source, target) in enumerate(weight_sources(0)):
        locals_.append(pltpu.make_async_copy(source, target, local_sem.at[1 + c]))
    for copy in locals_:
        copy.start()

    def send_gains():
        copies["g"] = [
            links.send(own_gains, gains_ref.at[a, b], {"a": across(a, k)}) for k in range(1, na)
        ]

    def relay_gains():
        for copy in copies["g"]:
            copy.wait_recv()
        at = gains_ref.at[:, b]
        copies["gb"] = [links.send(at, at, {"b": across(b, j)}) for j in range(1, nb)]

    def send_weights(k):
        copies["w", k] = [
            links.send(source, target, {"a": across(a, k)}) for source, target in weight_sources(k)
        ]

    def relay_weights(k):
        if k:
            for copy in copies["w", k]:
                copy.wait_recv()
        else:
            for copy in locals_[1:]:
                copy.wait()
        at = w_ref.at[span(across(a, k) * nb + b, rows), :]
        copies["wb", k] = [links.send(at, at, {"b": across(b, j)}) for j in range(1, nb)]

    line = Line(links, na, lambda k: x_ref.at[k, :, mine], tok_ref)

    def own_tokens(_):
        locals_[0].wait()
        line.to_pair(0).start()

    def pair_tokens(k):
        line.to_pair(k).wait_recv()
        at = x_ref.at[k, :, pair]
        copies["x", k] = links.send(at, at, {"q": 1 - q})

    def cut_weights(k):
        block = span(across(a, k), units)

        def cut(i, carry):
            at = pl.ds(pl.multiple_of(i * TILE, TILE), TILE)
            cuts = (gu_ref[at, 0, block], gu_ref[at, 1, block], down_ref[at, block])
            for c in range(3):
                if k:
                    piece_ref[k - 1, c, at] = cuts[c]
                else:
                    to = pl.ds(pl.multiple_of((a * nb + b) * rows + i * TILE, TILE), TILE)
                    mlp_w_ref[to, c * units : (c + 1) * units] = cuts[c]
            return carry

        lax.fori_loop(0, rows // TILE, cut, 0)

    def send_piece(c, k):
        target = mlp_w_ref.at[place, c * units : (c + 1) * units]
        copies["m", c, k] = links.send(piece_ref.at[k - 1, c], target, {"a": across(a, k)})

    def relay_piece(c, k):
        if k:
            copies["m", c, k].wait_recv()
        at = mlp_w_ref.at[span(across(a, k) * nb + b, rows), c * units : (c + 1) * units]
        ends.extend(links.send(at, at, {"b": across(b, j)}) for j in range(1, nb))

    arrived, ready = set(), []

    def project(k):
        if not arrived:
            held[0] = jnp.zeros_like(held[0])
            for i in range(na):
                for copy in copies["wb", i]:
                    copy.wait_recv()
        arrived.add(k)
        copies["x", k].wait_recv()

        def chunk(i, carry):
            at = span(i, 128)
            proj = dot(x_ref[k, at], w_ref[:, : 3 * HD])
            qkv_ref[k, at] = proj
            queries, key_rows = proj[:, :HD], proj[:, HD : 2 * HD]
            held[0, :, at] += to_row(queries * queries, 2 * k) + to_row(key_rows * key_rows, 2 * k + 1)
            return carry

        lax.fori_loop(0, x_ref.shape[1] // 128, chunk, 0)

    over_heads = OverHeads(links, na, a, p, q, held, stats_a, stats_ref)

    def all_stats():
        for save in saves[:3]:
            save.start()
        over_heads.done()
        for copy in copies["gb"]:
            copy.wait_recv()
        width_gain_ref[...] = jnp.zeros_like(width_gain_ref)
        head_gain_ref[...] = jnp.zeros_like(head_gain_ref)
        for i in range(2):
            width_gain_ref[i : i + 1] = jnp.concatenate(
                [gains_ref[2 * q + p, j, i : i + 1, :n_d] for j in range(nb)], axis=1
            )
            head_gain_ref[i : i + 1] = jnp.concatenate(
                [gains_ref[a, j, i + 2 : i + 3, :n_h] for j in range(nb)], axis=1
            )

    r = Reduce(na, links, part_ref, out, scratch)

    def attend(k):
        values, probs = (
            attention(k, qkv_ref[k], stats_ref[...], head_gain_ref, cos_ref, sin_ref)[i] for i in (2, 7)
        )
        attended = dot(probs.astype(bf16), values).astype(bf16)
        att_ref[k] = attended

        def part(n, carry):
            at = span(n, 512)
            part_ref[k, :, at] = dot_t(att_ref[k], w_ref[at, 3 * HD :]).astype(bf16)
            return carry

        lax.fori_loop(0, part_ref.shape[2] // 512, part, 0)
        for h in range(HALVES):
            r.send_q(h, k)

    first, second = attn_math(r, tok_ref, width_gain_ref, proj_ref, inv_ref, res_ref)
    table = {
        "GA": send_gains,
        "GB": relay_gains,
        "W": send_weights,
        "FW": relay_weights,
        "Z": lambda _: line.start(),
        "FL": lambda _, t: line.pass_on(1, t),
        "FR": lambda _, t: line.pass_on(-1, t),
        "FT": own_tokens,
        "FQ": pair_tokens,
        "CUT": cut_weights,
        "M": send_piece,
        "MR": relay_piece,
        "J": project,
        "S1": over_heads.to_pair,
        "S2": over_heads.to_core,
        "S3": over_heads.to_all,
        "S4": all_stats,
        "E": attend,
    }
    table.update({"r" + key: step for key, step in r.steps(first, second, 1, True).items()})
    for key, *where in ENTER:
        table[key](*where)
    saves[3].start()
    for h in range(HALVES):
        for k in range(na):
            r.arrived(h, k)
    for copy in ends:
        copy.wait_recv()
    for save in saves:
        save.wait()
    links.finish()


def enter_call(na, nb, tokens, qkv, w_out, gu, down, cos_table, sine_table, gains):
    rows, width = tokens.shape
    quarter = width // 4
    sizes = (gains[0].shape[0], gains[2].shape[0])
    w_rows, units = down.shape[0], down.shape[1] // na
    lanes = max(128, sizes[0])
    vmem, far = pl.BlockSpec(memory_space=pltpu.VMEM), pl.BlockSpec(memory_space=pl.ANY)
    shape = jax.ShapeDtypeStruct
    full = shape((na, rows, width), bf16)
    outs = [
        full,
        shape((width, 4 * HD), bf16),
        shape((width, 3 * units), bf16),
        shape((8, quarter), f32),
        shape((8, HD), f32),
        shape((na, rows, 3 * HD), f32),
        shape((8, rows), f32),
        shape((na, rows, HD), bf16),
        full,
        shape((rows, quarter), f32),
        shape((rows, 128), f32),
        shape((rows, quarter), f32),
    ]
    copies = 90 + 16 * nb
    return pl.pallas_call(
        functools.partial(enter_kernel, na, nb, sizes),
        out_shape=tuple(outs),
        in_specs=[far] + [vmem] * 7,
        out_specs=tuple(far if i in (0, 1, 5, 7) else vmem for i in range(len(outs))),
        scratch_shapes=[
            pltpu.VMEM((8, lanes), f32),
            pltpu.VMEM((na, nb, 8, lanes), f32),
            pltpu.VMEM((na - 1, 3, w_rows, units), bf16),
            pltpu.VMEM((na, rows, width), bf16),
            pltpu.VMEM((5, 8, rows), f32),
            pltpu.VMEM((na - 1, 8, rows), f32),
            pltpu.VMEM((na, rows, width), bf16),
            pltpu.VMEM((width, 4 * HD), bf16),
            pltpu.VMEM((na, rows, 3 * HD), f32),
            pltpu.VMEM((na, rows, HD), bf16),
            pltpu.VMEM((rows, quarter), bf16),
        ]
        + reduce_scratch(na, rows, width)
        + [
            pltpu.SemaphoreType.DMA((10,)),
            pltpu.SemaphoreType.DMA((copies,)),
            pltpu.SemaphoreType.DMA((copies,)),
        ],
        compiler_params=pltpu.CompilerParams(
            collective_id=5, has_side_effects=True, vmem_limit_bytes=VMEM_LIMIT
        ),
        name="enter",
    )(tokens, qkv, w_out, gu, down, cos_table, sine_table, jnp.concatenate(gains)[None])


def rope_tables(length, width):
    half_width = width // 2
    inv_freq = rope_base ** (-(jnp.arange(half_width, dtype=f32) * 2.0) / width)
    angles = jnp.arange(length, dtype=f32)[:, None] * inv_freq[None, :]
    cos_table = jnp.concatenate([jnp.cos(angles), jnp.cos(angles)], axis=1)
    sine_table = jnp.concatenate([jnp.sin(angles), jnp.sin(angles)], axis=1)
    return cos_table, sine_table


def on_device(
    tokens,
    qkv_weight,
    out_weight,
    gu_weight,
    down_weight,
    attn_gain,
    ffn_gain,
    q_gain,
    k_gain,
    out_grad,
):
    na, nb = lax.axis_size("a"), lax.axis_size("b")
    a, b = lax.axis_index("a"), lax.axis_index("b")
    share = lax.axis_index("q") * 2 + lax.axis_index("p")
    rows, width = tokens.shape
    quarter = width // 4
    w_rows = out_weight.shape[0]
    units = down_weight.shape[1] // na

    cos_table, sine_table = rope_tables(SEQ_LEN, HD)
    (
        x_all,
        w_attn,
        w_mlp,
        width_gain,
        head_gain,
        qkv,
        stats,
        attended,
        res_all,
        proj_mine,
        inv_mine,
        res_mine,
    ) = enter_call(
        na,
        nb,
        tokens,
        qkv_weight.transpose(1, 0, 2),
        out_weight,
        gu_weight,
        down_weight,
        cos_table,
        sine_table,
        (attn_gain, ffn_gain, q_gain, k_gain),
    )
    n_d, n_h = attn_gain.shape[0], q_gain.shape[0]
    block_rows, grad_proj, ffn_sums, grad_res, attn_sums, down_sum, gu_grad, down_in, gate_sum = middle_call(
        nb, res_all, w_mlp, res_mine, out_grad, proj_mine, inv_mine, width_gain
    )
    grad_rows, sums, down_grad, gu_grad, qkv_grad, out_grad_w = last_call(
        nb,
        grad_proj,
        x_all,
        qkv,
        stats,
        head_gain,
        cos_table,
        sine_table,
        w_attn,
        attended,
        grad_res,
        attn_sums,
        ffn_sums,
        down_sum,
        gu_grad,
        down_in,
        gate_sum,
    )
    width_sums = lax.dynamic_slice_in_dim(sums[:2, :quarter], b * n_d, n_d, 1)
    head_sums = lax.dynamic_slice_in_dim(sums[:2, quarter:], b * n_h, n_h, 1)
    return (
        block_rows[0].astype(f32),
        grad_rows[0].astype(f32),
        qkv_grad.transpose(1, 0, 2),
        out_grad_w,
        gu_grad,
        down_grad,
        width_sums[0],
        width_sums[1],
        head_sums[0],
        head_sums[1],
    )


def solution(mesh):
    dp, tp = mesh.shape["dp"], mesh.shape["tensor"]
    na = HEADS // tp
    fine = Mesh(mesh.devices.reshape(na, dp // na, tp // 2, 2), ("a", "b", "p", "q"))
    dp_axes, tp_axes = ("a", "b"), ("p", "q")
    both = tp_axes + dp_axes
    return jax.shard_map(
        on_device,
        mesh=fine,
        in_specs=(
            P(dp_axes, None),
            P(dp_axes, None, tp_axes),
            P(dp_axes, tp_axes),
            P(dp_axes, None, tp_axes),
            P(dp_axes, tp_axes),
            P(dp_axes),
            P(dp_axes),
            P(both),
            P(both),
            P(dp_axes, None),
        ),
        out_specs=(
            P(dp_axes, None),
            P(dp_axes, None),
            P(dp_axes, None, tp_axes),
            P(dp_axes, tp_axes),
            P(dp_axes, None, tp_axes),
            P(dp_axes, tp_axes),
            P(dp_axes),
            P(dp_axes),
            P(both),
            P(both),
        ),
        check_vma=False,
    )
```

```python
import functools

import jax
import jax.numpy as jnp
from jax import lax
from jax.experimental import pallas as pl
from jax.experimental.pallas import tpu as pltpu
from jax.sharding import Mesh, PartitionSpec as P

HEADS = 16
HD = 128
SEQ_LEN = 256
HQ = 2048

epsilon = 1e-06
rope_base = 500000.0

f32 = jnp.float32
bf16 = jnp.bfloat16
MESH = pl.DeviceIdType.MESH
EXACT = lax.Precision.HIGHEST
VMEM_LIMIT = 63 * 1024 * 1024
TILE = 32
HALVES = 2


def flip(index, bit):
    return index + bit - 2 * bit * ((index // bit) % 2)


def across(index, k):
    bit = 1
    while bit <= k:
        if k & bit:
            index = flip(index, bit)
        bit *= 2
    return index


def exclusive_or(left, right, count):
    total, bit = 0, 1
    while bit < count:
        total = total + bit * ((left // bit + right // bit) % 2)
        bit *= 2
    return total


def pick(operand, index, axis):
    return lax.dynamic_index_in_dim(operand, index, axis, keepdims=False)


def span(index, size):
    return pl.ds(pl.multiple_of(index * size, size), size)


class Links:
    def __init__(self, send_sem, recv_sem):
        self.send_sem, self.recv_sem, self.count = send_sem, recv_sem, 0
        self.copies, self.lines = [], []

    def send(self, source, target, device):
        copy = self.copy(self.count, source, target, device)
        copy.start()
        self.count += 1
        self.copies.append(copy)
        return copy

    def reserve(self, number):
        self.count += number
        return self.count - number

    def copy(self, index, source, target, device):
        return pltpu.make_async_remote_copy(
            src_ref=source,
            dst_ref=target,
            send_sem=self.send_sem.at[index],
            recv_sem=self.recv_sem.at[index],
            device_id=device,
            device_id_type=MESH,
        )

    def sent(self, copies):
        done = [id(copy) for copy in copies]
        for copy in self.copies:
            if id(copy) in done:
                copy.wait_send()
        self.copies = [copy for copy in self.copies if id(copy) not in done]

    def finish(self):
        for copy in self.copies:
            copy.wait_send()
        for line in self.lines:
            line.finish()


def greet(peers):
    barrier = pltpu.get_barrier_semaphore()
    for peer in peers:
        pl.semaphore_signal(barrier, inc=1, device_id=peer, device_id_type=MESH)
    pl.semaphore_wait(barrier, len(peers))


def fold(block):
    total = block[:, :128]
    for i in range(1, block.shape[1] // 128):
        total = total + block[:, i * 128 : (i + 1) * 128]
    return total


def wide(column, width):
    return jnp.concatenate([column] * (width // 128), axis=1)


def row_mask(row):
    return (lax.broadcasted_iota(jnp.int32, (8, 128), 0) == row).astype(f32)


def to_row(block, row):
    return lax.dot_general(
        row_mask(row), block, (((1,), (1,)), ((), ())), precision=EXACT, preferred_element_type=f32
    )


def to_column(stats, row):
    return lax.dot_general(
        stats, row_mask(row), (((0,), (0,)), ((), ())), precision=EXACT, preferred_element_type=f32
    )


def dot(left, right):
    return jnp.dot(left, right, preferred_element_type=f32)


def dot_t(left, right):
    return lax.dot_general(left, right, (((1,), (1,)), ((), ())), preferred_element_type=f32)


def t_dot(left, right):
    return lax.dot_general(left, right, (((0,), (0,)), ((), ())), preferred_element_type=f32)


def rotate(operand):
    half = HD // 2
    return jnp.concatenate([-operand[:, half:], operand[:, :half]], axis=1)


def rotate_back(operand):
    half = HD // 2
    return jnp.concatenate([operand[:, half:], -operand[:, :half]], axis=1)


def attention(k, qkv, stats, gain_ref, cos_ref, sin_ref):
    stats = stats / HQ
    q_inv = lax.rsqrt(to_column(stats, 2 * k) + epsilon)
    k_inv = lax.rsqrt(to_column(stats, 2 * k + 1) + epsilon)
    queries, key_rows = qkv[:, :HD], qkv[:, HD : 2 * HD]
    values = qkv[:, 2 * HD :].astype(bf16)
    cos_table, sine_table = cos_ref[...], sin_ref[...]
    q_normed = queries * q_inv * gain_ref[0:1]
    k_normed = key_rows * k_inv * gain_ref[1:2]
    q_rot = (q_normed * cos_table + rotate(q_normed) * sine_table).astype(bf16)
    k_rot = (k_normed * cos_table + rotate(k_normed) * sine_table).astype(bf16)
    scores = dot_t(q_rot, k_rot) * HD ** (-0.5)
    ahead = lax.broadcasted_iota(jnp.int32, scores.shape, 1) > lax.broadcasted_iota(
        jnp.int32, scores.shape, 0
    )
    scores = jnp.where(ahead, -1e30, scores)
    shifted = jnp.exp(scores - jnp.max(scores, axis=1, keepdims=True))
    probs = shifted / jnp.sum(shifted, axis=1, keepdims=True)
    return queries, key_rows, values, q_inv, k_inv, q_rot, k_rot, probs


def weight_grad(left, right, out, block, columns=None, take=slice(None)):
    na, nb, rows = left.shape[0], out.shape[1], out.shape[2]
    columns = columns or slice(0, right.shape[2])
    size = max(rows, 256)


    def chunk(i, carry):
        at = span(block * (nb * rows // size) + i, size)
        total = t_dot(left[0, :, at], right[0, :, take])
        for k in range(1, na):
            total = total + t_dot(left[k, :, at], right[k, :, take])
        for j in range(size // rows):
            part = total[j * rows : (j + 1) * rows].astype(bf16)
            out[block, i * (size // rows) + j, :, columns] = part
        return carry

    lax.fori_loop(0, nb * rows // size, chunk, 0)


def exchange_b(links, grad, held, columns):
    b = lax.axis_index("b")
    put = columns if held.shape[3] == grad.shape[3] or columns.stop <= held.shape[3] else slice(None)
    return [
        links.send(
            grad.at[:, across(b, j), :, columns], held.at[j - 1, :, :, put], {"b": across(b, j)}
        )
        for j in range(1, held.shape[0] + 1)
    ]


def sum_b(copies, own, held, out, columns):
    for copy in copies:
        copy.wait_recv()

    def add(block, carry):
        total = own(block)[:, columns].astype(f32)
        for j in range(held.shape[0]):
            total = total + held[j, block, :, columns].astype(f32)
        out[block, :, columns] = total.astype(bf16)
        return carry

    lax.fori_loop(0, held.shape[1], add, 0)


class Line:
    def __init__(self, links, na, block, own):
        self.links, self.na, self.block, self.own = links, na, block, own
        self.a, self.p = lax.axis_index("a"), lax.axis_index("p")
        self.hop_base = {1: links.reserve(na - 1), -1: links.reserve(na - 1)}
        self.pass_base = links.reserve(na)
        links.lines.append(self)

    def hop(self, way, t):
        a, na = self.a, self.na
        first = a - way * (t - 1)
        source = self.own if t == 1 else self.block(exclusive_or(first, a, na))
        target = self.block(exclusive_or(first, a + way, na))
        return self.links.copy(self.hop_base[way] + t - 1, source, target, {"a": (a + way) % na})

    def sends(self, way, t):
        first, last = self.a - way * (t - 1), self.a + way
        return (first >= 0) & (first < self.na) & (last >= 0) & (last < self.na)

    def to_pair(self, k, source=None):
        at = self.block(k)
        return self.links.copy(self.pass_base + k, at if source is None else source, at, {"p": 1 - self.p})

    def start(self):
        for way in (1, -1):

            @pl.when(self.sends(way, 1))
            def _(way=way):
                self.hop(way, 1).start()

    def pass_on(self, way, t):
        came = self.a - way * t

        @pl.when((came >= 0) & (came < self.na))
        def _():
            self.hop(way, t).wait_recv()
            self.to_pair(exclusive_or(came, self.a, self.na)).start()

        if t < self.na - 1:

            @pl.when(self.sends(way, t + 1))
            def _():
                self.hop(way, t + 1).start()

    def finish(self):
        for way in (1, -1):
            for t in range(1, self.na):

                @pl.when(self.sends(way, t))
                def _(way=way, t=t):
                    self.hop(way, t).wait_send()

        for k in range(self.na):
            self.to_pair(k).wait_send()


class Reduce:
    def __init__(self, na, links, part, out, scratch):
        self.na, self.links, self.part, self.out = na, links, part, out
        self.from_q, self.half_sum, self.from_p, self.to_a, self.from_a = scratch[:5]
        self.total, self.parts, self.cols, self.stat = scratch[5:9]
        self.a, self.p, self.q = (lax.axis_index(axis) for axis in ("a", "p", "q"))
        self.rows, self.width = out.shape[1:]
        self.quarter, self.half = self.width // 4, self.width // 2
        self.count = self.rows // HALVES
        self.mine, self.pair = span(2 * self.q + self.p, self.quarter), span(self.q, self.half)
        self.lead = list(range(2, na)) + [1, 0]
        self.step_q, self.step_p, self.step_a = {}, {}, {}
        self.spread_a, self.spread_p, self.spread_q, self.stats = {}, {}, {}, {}
        self.here = set()

    def at(self, h):
        return slice(h * self.count, (h + 1) * self.count)

    def each(self, h, body):
        def step(i, carry):
            body(pl.ds(pl.multiple_of(h * self.count + i * TILE, TILE), TILE))
            return carry

        lax.fori_loop(0, self.count // TILE, step, 0)

    def send_q(self, h, k):
        at, q = self.at(h), self.q
        source = self.part.at[k, at, span(1 - q, self.half)]
        self.step_q[h, k] = self.links.send(source, self.from_q.at[k, at], {"q": 1 - q})

    def send_p(self, h, k):
        self.step_q[h, k].wait_recv()

        def add(at):
            own = self.part[k, at, span(self.q, self.half)].astype(f32)
            self.half_sum[k, at] = (own + self.from_q[k, at].astype(f32)).astype(bf16)

        self.each(h, add)
        at, p = self.at(h), self.p
        source = self.half_sum.at[k, at, span(1 - p, self.quarter)]
        self.step_p[h, k] = self.links.send(source, self.from_p.at[k, at], {"p": 1 - p})

    def send_a(self, h, k):
        if not k:
            return
        self.step_p[h, k].wait_recv()

        def add(at):
            own = self.half_sum[k, at, span(self.p, self.quarter)].astype(f32)
            self.to_a[k - 1, at] = (own + self.from_p[k, at].astype(f32)).astype(bf16)

        self.each(h, add)
        at = self.at(h)
        self.step_a[h, k] = self.links.send(
            self.to_a.at[k - 1, at], self.from_a.at[k - 1, at], {"a": across(self.a, k)}
        )

    def add_all(self, at):
        own = self.half_sum[0, at, span(self.p, self.quarter)].astype(f32)
        own = own + self.from_p[0, at].astype(f32)
        for k in range(1, self.na):
            own = own + self.from_a[k - 1, at].astype(f32)
        return own

    def scattered(self, h, first, number):
        self.step_p[h, 0].wait_recv()
        for k in range(1, self.na):
            self.step_a[h, k].wait_recv()
        self.each(h, first)
        if number:
            at = self.at(h)
            stats = to_row(self.parts[0, at], 0)
            if number == 2:
                stats = stats + to_row(self.parts[1, at], 1)
            stat = self.stat
            stat[h, 0] = stats
            self.stats[h] = self.links.send(stat.at[h, 0], stat.at[h, 1], {"p": 1 - self.p})

    def stats_q(self, h):
        stat = self.stat
        self.stats[h].wait_recv()
        stat[h, 2] = stat[h, 0] + stat[h, 1]
        self.stats[h] = self.links.send(stat.at[h, 2], stat.at[h, 3], {"q": 1 - self.q})

    def stats_done(self, h, number):
        stat = self.stat
        self.stats[h].wait_recv()
        stats = (stat[h, 2] + stat[h, 3]) / self.width
        for i in range(number):
            self.cols[i, self.at(h)] = to_column(stats, i)

    def spread(self, h, blocks):
        here = self.out.at[0, self.at(h), self.mine]
        for k in blocks:
            if k:
                target = self.out.at[k, self.at(h), self.mine]
                self.spread_a[h, k] = self.links.send(here, target, {"a": across(self.a, k)})
        self.spread_p[h, 0] = self.links.send(here, here, {"p": 1 - self.p})

    def relay_p(self, h, k):
        if not k:
            return
        self.spread_a[h, k].wait_recv()
        here = self.out.at[k, self.at(h), self.mine]
        self.spread_p[h, k] = self.links.send(here, here, {"p": 1 - self.p})

    def relay_q(self, h, k):
        self.spread_p[h, k].wait_recv()
        here = self.out.at[k, self.at(h), self.pair]
        self.spread_q[h, k] = self.links.send(here, here, {"q": 1 - self.q})

    def arrived(self, h, k):
        if (h, k) not in self.here:
            self.here.add((h, k))
            self.spread_q[h, k].wait_recv()

    def steps(self, first, second, number, chain=False):
        def normed(h):
            self.stats_done(h, number)
            self.each(h, second)

        def spread_own(h):
            here = self.out.at[0, self.at(h), self.mine]
            self.spread_p[h, 0] = self.links.send(here, here, {"p": 1 - self.p})

        def spread_far(h, k):
            here = self.out.at[0, self.at(h), self.mine]
            target = self.out.at[k, self.at(h), self.mine]
            self.spread_a[h, k] = self.links.send(here, target, {"a": across(self.a, k)})

        table = {
            "P": self.send_p,
            "A": self.send_a,
            "SC": lambda h: self.scattered(h, first, number),
            "SQ": self.stats_q,
            "SD": normed,
            "X": spread_own,
            "Z": spread_far,
            "RP": self.relay_p,
            "RQ": self.relay_q,
        }
        if chain:
            lines = [
                Line(
                    self.links,
                    self.na,
                    lambda k, h=h: self.out.at[k, self.at(h), self.mine],
                    self.out.at[0, self.at(h), self.mine],
                )
                for h in range(HALVES)
            ]

            def pair_arrived(h, k):
                self.spread_p[h, k] = lines[h].to_pair(k)
                self.relay_q(h, k)

            table.update(
                X=lambda h: lines[h].to_pair(0).start(),
                Z=lambda h: lines[h].start(),
                FL=lambda h, t: lines[h].pass_on(1, t),
                FR=lambda h, t: lines[h].pass_on(-1, t),
                RQ=pair_arrived,
            )
        return table


class OverHeads:
    def __init__(self, links, na, a, p, q, held, from_a, out_ref):
        self.links, self.na, self.a, self.p, self.q = links, na, a, p, q
        self.held, self.from_a, self.out_ref = held, from_a, out_ref

    def to_pair(self):
        self.copy = self.links.send(self.held.at[0], self.held.at[1], {"p": 1 - self.p})

    def to_core(self):
        held = self.held
        self.copy.wait_recv()
        held[2] = held[0] + held[1]
        self.copy = self.links.send(held.at[2], held.at[3], {"q": 1 - self.q})

    def to_all(self):
        held = self.held
        self.copy.wait_recv()
        held[4] = held[2] + held[3]
        self.copies = [
            self.links.send(held.at[4], self.from_a.at[k - 1], {"a": across(self.a, k)})
            for k in range(1, self.na)
        ]

    def done(self):
        for copy in self.copies:
            copy.wait_recv()
        for k in range(self.na):
            for i in range(2):
                at = 2 * k + i
                total = self.held[4, at : at + 1]
                for j in range(1, self.na):
                    other = 2 * (k ^ j) + i
                    total = total + self.from_a[j - 1, other : other + 1]
                self.out_ref[at : at + 1] = total


def reduce_peers(na):
    a, p, q = lax.axis_index("a"), lax.axis_index("p"), lax.axis_index("q")
    return [{"q": 1 - q}, {"p": 1 - p}] + [{"a": across(a, k)} for k in range(1, na)]


def attn_math(r, tok_ref, gain_ref, proj_ref, inv_ref, res_ref):
    def first(at):
        own = r.add_all(at)
        proj_ref[at] = own
        r.parts[0, at] = fold(own * own)

    def second(at):
        own = proj_ref[at]
        inv = lax.rsqrt(r.cols[0, at] + epsilon)
        inv_ref[at] = inv
        residual = tok_ref[at].astype(f32) + own * wide(inv, r.quarter) * gain_ref[0:1]
        res_ref[at] = residual
        r.out[0, at, r.mine] = residual.astype(bf16)

    return first, second


def mlp_math(r, res_ref, grad_ref, gain_ref, block_ref, sum_ref):
    def first(at):
        own = r.add_all(at)
        r.total[at] = own
        r.parts[0, at] = fold(own * own)
        r.parts[1, at] = fold(grad_ref[at] * gain_ref[1:2] * own)

    def second(at):
        own = r.total[at]
        inv = wide(lax.rsqrt(r.cols[0, at] + epsilon), r.quarter)
        upstream = grad_ref[at]
        scaled = upstream * gain_ref[1:2]
        normed = own * inv
        block_ref[0, at, r.mine] = (res_ref[at] + normed * gain_ref[1:2]).astype(bf16)
        gains = upstream * normed
        sum_ref[...] += jnp.sum(gains.reshape(TILE // 8, 8, r.quarter), axis=0)
        grad = inv * scaled - own * inv * inv * inv * wide(r.cols[1, at], r.quarter)
        r.out[0, at, r.mine] = grad.astype(bf16)

    return first, second


def back_math(r, grad_ref, proj_ref, inv_ref, gain_ref, res_ref, sum_ref):
    def first(at):
        grad = grad_ref[at] + r.add_all(at)
        res_ref[at] = grad
        r.parts[0, at] = fold(grad * gain_ref[0:1] * proj_ref[at])

    def second(at):
        own = proj_ref[at]
        inv = wide(inv_ref[at], r.quarter)
        upstream = res_ref[at]
        gains = upstream * own * inv
        sum_ref[...] += jnp.sum(gains.reshape(TILE // 8, 8, r.quarter), axis=0)
        grad = inv * (upstream * gain_ref[0:1])
        grad = grad - own * inv * inv * inv * wide(r.cols[0, at], r.quarter)
        r.out[0, at, r.mine] = grad.astype(bf16)

    return first, second


MIDDLE = (
    ("F", 2), ("F", 3), ("rP", 0, 2), ("F", 1), ("rP", 0, 3), ("rA", 0, 2), ("rP", 0, 1), ("rP", 1, 3),
    ("F", 0), ("rP", 1, 2), ("rA", 0, 3), ("rP", 1, 1), ("rA", 0, 1), ("rP", 0, 0), ("rA", 1, 3),
    ("rA", 1, 1), ("rA", 1, 2), ("rSC", 0), ("rP", 1, 0), ("rSQ", 0), ("rSD", 0), ("rZ", 0, 1), ("rX", 0),
    ("rZ", 0, 3), ("rSC", 1), ("rRP", 0, 1), ("rRQ", 0, 0), ("rSQ", 1), ("rZ", 0, 2), ("rSD", 1),
    ("rRP", 0, 3), ("rX", 1), ("rZ", 1, 1), ("rZ", 1, 2), ("rRP", 0, 2), ("rRQ", 0, 1), ("rRQ", 0, 3),
    ("rRP", 1, 1), ("B", 0, 3), ("rZ", 1, 3), ("rRP", 1, 2), ("rRQ", 1, 0), ("B", 0, 1), ("rRQ", 0, 2),
    ("sP", 0, 3), ("B", 0, 0), ("B", 0, 2), ("rRP", 1, 3), ("rRQ", 1, 2), ("sA", 0, 3), ("sP", 0, 2),
    ("B", 1, 2), ("sP", 0, 1), ("rRQ", 1, 1), ("rRQ", 1, 3), ("sA", 0, 2), ("sP", 1, 2), ("D", 0),
    ("sA", 0, 1), ("B", 1, 3), ("sA", 1, 2), ("sP", 1, 3), ("B", 1, 0), ("sP", 0, 0), ("D", 1),
    ("sA", 1, 3), ("sP", 1, 0), ("B", 1, 1), ("sSC", 0), ("sP", 1, 1), ("DS", 0), ("ZD", 0, 2), ("sSQ", 0),
    ("G", 0), ("sSD", 0), ("BP",), ("sA", 1, 1), ("G", 2), ("sZ", 0, 3), ("G", 3), ("sZ", 0, 2), ("sSC", 1),
    ("G", 1), ("YG",), ("sSQ", 1), ("sRP", 0, 3), ("sSD", 1), ("sZ", 1, 3), ("DS", 1), ("sZ", 1, 1),
    ("sZ", 0, 1), ("BQ",), ("sX", 0), ("ZD", 1, 3), ("sRP", 1, 1), ("sX", 1), ("sRQ", 1, 1), ("sZ", 1, 2),
    ("sRP", 0, 2), ("sRP", 0, 1), ("ZD", 0, 1), ("ZD", 1, 1), ("sRP", 1, 2), ("sRP", 1, 3), ("ZD", 1, 2),
    ("sRQ", 0, 0), ("sRQ", 0, 3), ("ZD", 0, 3), ("sRQ", 1, 0), ("sRQ", 1, 2), ("sRQ", 0, 2), ("sRQ", 0, 1),
    ("sRQ", 1, 3), ("SG",),
)


def middle_kernel(na, nb, *refs):
    x_far, w_far, res_ref, grad_far, proj_ref, inv_ref, gain_ref = refs[:7]
    block_ref, back_out, ffn_sum_ref, grad_res_ref, attn_sum_ref, down_sum_ref, up_grad_far = refs[7:14]
    down_in, gate_sum_ref = refs[14:16]
    out, hidden_ref, grad_gu_ref, gu_ref, part_ref, down_grad, down_held, grad_ref, gu_held = refs[16:25]
    x_ref, w_ref, gu_grad_ref = refs[25:28]
    scratch, (local_sem, send_sem, recv_sem) = refs[28:-3], refs[-3:]
    share = 2 * lax.axis_index("q") + lax.axis_index("p")
    load = pltpu.make_async_copy(
        grad_far.at[:, span(share, grad_ref.shape[1])], grad_ref, local_sem.at[0]
    )
    load.start()
    load_w = pltpu.make_async_copy(w_far, w_ref, local_sem.at[1])
    load_w.start()
    load_x = {
        k: pltpu.make_async_copy(x_far.at[k], x_ref.at[k], local_sem.at[2 + k])
        for k in list(range(2, na)) + [1, 0]
    }
    for copy in load_x.values():
        copy.start()
    units = hidden_ref.shape[2]
    width = x_ref.shape[2]
    save_up = pltpu.make_async_copy(
        gu_grad_ref.at[:, :, :, units:], up_grad_far, local_sem.at[2 + na]
    )
    b = lax.axis_index("b")
    greet(reduce_peers(na) + [{"b": across(b, j)} for j in range(1, nb)])
    links = Links(send_sem, recv_sem)
    r = Reduce(na, links, part_ref, out, scratch[:9])
    s = Reduce(na, links, part_ref, back_out, scratch[9:])
    ffn_sum_ref[...] = jnp.zeros_like(ffn_sum_ref)
    attn_sum_ref[...] = jnp.zeros_like(attn_sum_ref)
    wide_tile = 512

    def forward(k):
        def gated(n, carry):
            at, up_at = span(n, 256), pl.ds(pl.multiple_of(units + n * 256, 256), 256)
            gate = dot(x_ref[k], w_ref[:, at])
            up = dot(x_ref[k], w_ref[:, up_at])
            gu_ref[k, :, at] = gate
            gu_ref[k, :, up_at] = up
            hidden_ref[k, :, at] = (gate * jax.nn.sigmoid(gate) * up).astype(bf16)
            return carry

        lax.fori_loop(0, units // 256, gated, 0)

        def down(n, carry):
            at = span(n, wide_tile)
            part_ref[k, :, at] = dot_t(hidden_ref[k], w_ref[at, 2 * units :]).astype(bf16)
            return carry

        lax.fori_loop(0, width // wide_tile, down, 0)

    def backward(h, k):
        rows = r.at(h)

        def gated(n, carry):
            at, up_at = span(n, 256), pl.ds(pl.multiple_of(units + n * 256, 256), 256)
            down_at = pl.ds(pl.multiple_of(2 * units + n * 256, 256), 256)
            grad_hidden = dot(out[k, rows], w_ref[:, down_at])
            gate, up = gu_ref[k, rows, at], gu_ref[k, rows, up_at]
            sigmoid = jax.nn.sigmoid(gate)
            active = gate * sigmoid
            grad_gu_ref[k, rows, at] = (
                grad_hidden * up * (sigmoid * (1.0 + gate * (1.0 - sigmoid)))
            ).astype(bf16)
            grad_gu_ref[k, rows, up_at] = (grad_hidden * active).astype(bf16)
            return carry

        lax.fori_loop(0, units // 256, gated, 0)

        def back(n, carry):
            at = span(n, wide_tile)
            part_ref[k, rows, at] = dot_t(
                grad_gu_ref[k, rows], w_ref[at, : 2 * units]
            ).astype(bf16)
            return carry

        lax.fori_loop(0, width // wide_tile, back, 0)

    first, second = mlp_math(r, res_ref, grad_ref, gain_ref, block_ref, ffn_sum_ref)
    back_first, back_second = back_math(
        s, grad_ref, proj_ref, inv_ref, gain_ref, grad_res_ref, attn_sum_ref
    )
    copies, reused, loaded, blocks = {}, [], [], []
    gate = slice(0, units)

    def half(c):
        return slice(c * units // 2, (c + 1) * units // 2)

    def forward_step(k):
        if not loaded:
            load_w.wait()
        loaded.append(k)
        load_x[k].wait()
        forward(k)
        for h in range(HALVES):
            r.send_q(h, k)

    def backward_step(h, k):
        if not reused:
            links.sent(r.step_q.values())
            reused.append(True)
        r.arrived(h, k)
        backward(h, k)
        s.send_q(h, k)

    def block_p():
        here = block_ref.at[0, :, r.mine]
        copies["p"] = links.send(here, here, {"p": 1 - r.p})

    def block_q():
        copies["p"].wait_recv()
        here = block_ref.at[0, :, r.pair]
        copies["q"] = links.send(here, here, {"q": 1 - r.q})

    def down_grads(c):
        for h in range(HALVES):
            for k in range(na):
                r.arrived(h, k)
        for block in range(na):
            weight_grad(out, hidden_ref, down_grad, block, half(c), half(c))
        copies["d", c] = exchange_b(links, down_grad, down_held, half(c))

    def down_sums(c):
        own = lambda block: down_grad.at[block, b]
        sum_b(copies["d", c], own, down_held, down_sum_ref, half(c))

    def down_owner(c, k):
        copies["z", c, k] = links.send(
            down_sum_ref.at[across(r.a, k), :, half(c)], down_in.at[k - 1, :, half(c)], {"a": across(r.a, k)}
        )

    def gu_grads(block):
        weight_grad(x_ref, grad_gu_ref, gu_grad_ref, block)
        blocks.append(block)
        if len(blocks) == na:
            save_up.start()

    def gate_rows():
        copies["g"] = exchange_b(links, gu_grad_ref, gu_held, gate)

    table = {
        "F": forward_step,
        "B": backward_step,
        "BP": block_p,
        "BQ": block_q,
        "D": down_grads,
        "DS": down_sums,
        "ZD": down_owner,
        "YG": gate_rows,
        "SG": lambda: sum_b(
            copies["g"], lambda block: gu_grad_ref.at[block, b], gu_held, gate_sum_ref, gate
        ),
        "G": gu_grads,
    }
    table.update({"r" + key: step for key, step in r.steps(first, second, 2).items()})
    table.update({"s" + key: step for key, step in s.steps(back_first, back_second, 1).items()})
    load.wait()
    for key, *where in MIDDLE:
        table[key](*where)
    for h in range(HALVES):
        for k in range(na):
            s.arrived(h, k)
    copies["q"].wait_recv()
    for c in range(2):
        for k in range(1, na):
            copies["z", c, k].wait_recv()
    save_up.wait()
    links.finish()


def middle_call(nb, x_all, w_mlp, res_mine, out_grad, proj_mine, inv_mine, width_gain):
    na, rows, width = x_all.shape
    quarter, units = width // 4, w_mlp.shape[1] // 3
    w_rows = width // (na * nb)
    vmem, far = pl.BlockSpec(memory_space=pltpu.VMEM), pl.BlockSpec(memory_space=pl.ANY)
    shape = jax.ShapeDtypeStruct
    outs = (
        shape((1, rows, width), bf16),
        shape((na, rows, width), bf16),
        shape((8, quarter), f32),
        shape((rows, quarter), f32),
        shape((8, quarter), f32),
        shape((na, w_rows, units), bf16),
        shape((na, nb, w_rows, units), bf16),
        shape((na - 1, w_rows, units), bf16),
        shape((na, w_rows, units), bf16),
    )
    copies = 2 * HALVES * (6 * na + 1) + 2 + 3 * nb + 2 * na
    return pl.pallas_call(
        functools.partial(middle_kernel, na, nb),
        out_shape=outs,
        in_specs=[far if i in (0, 1, 3) else vmem for i in range(7)],
        out_specs=tuple(far if i == 6 else vmem for i in range(len(outs))),
        scratch_shapes=[
            pltpu.VMEM((na, rows, width), bf16),
            pltpu.VMEM((na, rows, units), bf16),
            pltpu.VMEM((na, rows, 2 * units), bf16),
            pltpu.VMEM((na, rows, 2 * units), f32),
            pltpu.VMEM((na, rows, width), bf16),
            pltpu.VMEM((na, nb, w_rows, units), bf16),
            pltpu.VMEM((nb - 1, na, w_rows, units), bf16),
            pltpu.VMEM((rows, quarter), f32),
            pltpu.VMEM((nb - 1, na, w_rows, units), bf16),
            pltpu.VMEM((na, rows, width), bf16),
            pltpu.VMEM((width, 3 * units), bf16),
            pltpu.VMEM((na, nb, w_rows, 2 * units), bf16),
        ]
        + reduce_scratch(na, rows, width)
        + reduce_scratch(na, rows, width)
        + [
            pltpu.SemaphoreType.DMA((3 + na,)),
            pltpu.SemaphoreType.DMA((copies,)),
            pltpu.SemaphoreType.DMA((copies,)),
        ],
        compiler_params=pltpu.CompilerParams(
            collective_id=2, has_side_effects=True, vmem_limit_bytes=VMEM_LIMIT
        ),
        name="middle",
    )(x_all, w_mlp, res_mine, out_grad, proj_mine, inv_mine, width_gain)


LAST = (
    ("ZG", 0, 2), ("U1",), ("YG", 1), ("AB", 0), ("U2",), ("AB", 1), ("ZG", 0, 1), ("AB", 2),
    ("WO", 3), ("U3",), ("ZG", 0, 3), ("AB", 3), ("OD", 2), ("S1",), ("S2",), ("S3",), ("WO", 0),
    ("SG", 1), ("ZG", 1, 2), ("S4",), ("QB", 1), ("QB", 0), ("QB", 2), ("QB", 3), ("U4",), ("OWNG",),
    ("OG", 0, 3), ("WQ", 1), ("ZG", 1, 3), ("rP", 1, 3), ("WQ", 2), ("rP", 0, 0), ("ZG", 1, 1),
    ("OG", 0, 1), ("rP", 1, 2), ("rP", 0, 1), ("WQ", 0), ("rP", 1, 0), ("WO", 1), ("rA", 1, 3),
    ("WO", 2), ("WQ", 3), ("YA",), ("OG", 0, 2), ("OD", 1), ("rP", 0, 2), ("rA", 1, 2), ("rA", 0, 1),
    ("OG", 1, 1), ("OG", 1, 2), ("rA", 0, 2), ("rP", 1, 1), ("rP", 0, 3), ("rA", 1, 1), ("OD", 3),
    ("rA", 0, 3), ("OG", 1, 3), ("rSC", 1), ("SA",), ("ZA", 2), ("U5",), ("rSC", 0), ("rX", 0), ("ZA", 3),
    ("ZA", 1), ("OWN",), ("rX", 1), ("rRQ", 0, 0), ("OA", 2), ("OA", 1), ("rRQ", 1, 0),
    ("OA", 3),
)


def last_kernel(na, nb, *refs):
    proj_far, x_far, qkv_ref, stats_ref, gain_ref, cos_ref, sin_ref, w_ref, att_ref = refs[:9]
    grad_ref, attn_sum_ref, ffn_sum_ref, down_sum_far, up_grad_far, down_in_far, gate_ref = refs[9:16]
    out, sums_ref, down_far, gu_far, qkv_out, wout_out = refs[16:22]
    scaled_ref, grad_qkv_ref, part_ref, head_sums, held, stats_a, inner_ref = refs[22:29]
    own_sums, a_sums, b_sums, up_held, up_sum, attn_grad, attn_held, attn_sum = refs[29:37]
    gu_in, attn_in, x_ref, up_own, down_out, gu_out = refs[37:43]
    proj_ref, down_sum_ref, down_in = refs[43:46]
    scratch, (local_sem, send_sem, recv_sem) = refs[46:-3], refs[-3:]
    load_proj = [
        pltpu.make_async_copy(proj_far.at[k], proj_ref.at[k], local_sem.at[4 + k]) for k in range(na)
    ]
    for copy in load_proj:
        copy.start()
    links = Links(send_sem, recv_sem)
    load_gu = pltpu.make_async_copy(
        up_grad_far.at[:, lax.axis_index("b")], up_own, local_sem.at[0]
    )
    load_gu.start()
    load_x = pltpu.make_async_copy(x_far, x_ref, local_sem.at[1])
    load_x.start()
    load_down = [
        pltpu.make_async_copy(down_sum_far, down_sum_ref, local_sem.at[4 + na]),
        pltpu.make_async_copy(down_in_far, down_in, local_sem.at[5 + na]),
    ]
    for copy in load_down:
        copy.start()
    save_down = pltpu.make_async_copy(down_out, down_far, local_sem.at[2])
    save_gu = pltpu.make_async_copy(gu_out, gu_far, local_sem.at[3])
    r = Reduce(na, links, part_ref, out, scratch)
    a, b, p, q, mine, pair, quarter = (
        r.a, lax.axis_index("b"), r.p, r.q, r.mine, r.pair, r.quarter,
    )
    units = down_sum_ref.shape[2]
    own_sums[...] = jnp.zeros_like(own_sums)
    own_sums[0:1, mine] = jnp.sum(attn_sum_ref[...], axis=0, keepdims=True)
    own_sums[1:2, mine] = jnp.sum(ffn_sum_ref[...], axis=0, keepdims=True)
    held[0] = jnp.zeros_like(held[0])
    head_sums[...] = jnp.zeros_like(head_sums)
    greet(reduce_peers(na) + [{"b": across(b, j)} for j in range(1, nb)])
    copies, stored = {}, []
    whole = slice(0, units)
    attn_columns = slice(0, 4 * HD)
    over_heads = OverHeads(links, na, a, p, q, held, stats_a, inner_ref)

    def sums_pair():
        here = own_sums.at[:, mine]
        copies["u"] = links.send(here, here, {"p": 1 - p})

    def sums_core():
        copies["u"].wait_recv()
        here = own_sums.at[:, pair]
        copies["u"] = links.send(here, here, {"q": 1 - q})

    def sums_far():
        copies["u"].wait_recv()
        copies["u"] = [
            links.send(
                own_sums.at[:, span(across(a, k), quarter)], a_sums.at[k - 1], {"a": across(a, k)}
            )
            for k in range(1, na)
        ]

    def sums_b():
        for copy in copies["u"]:
            copy.wait_recv()
        total = own_sums[:, span(a, quarter)]
        for k in range(1, na):
            total = total + a_sums[k - 1]
        b_sums[0, :, :quarter] = total
        b_sums[0, :, quarter:] = head_sums[...]
        copies["u"] = [
            links.send(b_sums.at[0], b_sums.at[j], {"b": across(b, j)}) for j in range(1, nb)
        ]

    def sums_done():
        for copy in copies["u"]:
            copy.wait_recv()
        total = b_sums[0]
        for j in range(1, nb):
            total = total + b_sums[j]
        sums_ref[...] = total

    def proj_here(k):
        if ("proj", k) not in copies:
            copies["proj", k] = True
            load_proj[k].wait()

    def out_grads(block):
        for k in range(na):
            proj_here(k)
        weight_grad(proj_ref, att_ref, attn_grad, block, slice(3 * HD, 4 * HD))

    def attend_back(k):
        proj_here(k)
        if k % 2:
            lax.fori_loop(k - 1, k + 1, attend_back_block, 0)

    def attend_back_block(k, carry):
        queries, key_rows, values, q_inv, k_inv, q_rot, k_rot, probs = attention(
            k, qkv_ref[k], stats_ref[...], gain_ref, cos_ref, sin_ref
        )
        cos_table, sine_table = cos_ref[...], sin_ref[...]
        grad_att = dot(proj_ref[k], w_ref[:, 3 * HD :]).astype(bf16)
        grad_v = t_dot(probs.astype(bf16), grad_att)
        grad_p = dot_t(grad_att, values)
        delta = jnp.sum(probs * grad_p, axis=1, keepdims=True)
        grad_scores = (probs * (grad_p - delta) * HD ** (-0.5)).astype(bf16)
        grad_q = dot(grad_scores, k_rot)
        grad_k = t_dot(grad_scores, q_rot)
        grad_q = grad_q * cos_table + rotate_back(grad_q * sine_table)
        grad_k = grad_k * cos_table + rotate_back(grad_k * sine_table)
        head_sums[0:1] += jnp.sum(grad_q * queries * q_inv, axis=0, keepdims=True)
        head_sums[1:2] += jnp.sum(grad_k * key_rows * k_inv, axis=0, keepdims=True)
        scaled_q = grad_q * gain_ref[0:1]
        scaled_k = grad_k * gain_ref[1:2]
        scaled_ref[k, :, :HD] = scaled_q
        scaled_ref[k, :, HD:] = scaled_k
        grad_qkv_ref[k, :, 2 * HD :] = grad_v.astype(bf16)
        held[0] += to_row(scaled_q * queries, 2 * k) + to_row(scaled_k * key_rows, 2 * k + 1)
        return carry

    def qkv_back(k):
        for i in range(2):
            at = slice(i * HD, (i + 1) * HD)
            inv = lax.rsqrt(to_column(stats_ref[...] / HQ, 2 * k + i) + epsilon)
            mean = to_column(inner_ref[...] / HQ, 2 * k + i)
            grad = inv * scaled_ref[k, :, at] - qkv_ref[k, :, at] * inv * inv * inv * mean
            grad_qkv_ref[k, :, at] = grad.astype(bf16)

        def part(n, carry):
            at = span(n, 512)
            part_ref[k, :, at] = dot_t(grad_qkv_ref[k], w_ref[at, : 3 * HD]).astype(bf16)
            return carry

        lax.fori_loop(0, part_ref.shape[2] // 512, part, 0)
        for h in range(HALVES):
            r.send_q(h, k)

    def qkv_grads(block):
        if "x" not in copies:
            load_x.wait()
            copies["x"] = True
        weight_grad(x_ref, grad_qkv_ref, attn_grad, block, slice(0, 3 * HD))

    def up_rows(_):
        copies["up"] = exchange_b(links, up_grad_far, up_held, whole)

    def up_sums(_):
        load_gu.wait()
        own = lambda block: up_own.at[block]
        sum_b(copies["up"], own, up_held, up_sum, whole)

    def gu_owner(c, k):
        source = up_sum if c else gate_ref
        copies["g", c, k] = links.send(
            source.at[across(a, k)], gu_in.at[k - 1, c], {"a": across(a, k)}
        )

    def attn_rows():
        copies["at"] = exchange_b(links, attn_grad, attn_held, attn_columns)

    def attn_sums():
        own = lambda block: attn_grad.at[block, b]
        sum_b(copies["at"], own, attn_held, attn_sum, attn_columns)

    def attn_owner(k):
        copies["a", k] = links.send(attn_sum.at[across(a, k)], attn_in.at[k - 1], {"a": across(a, k)})

    def store(target, index, size, value):
        target[:, span(index, size)] = value.astype(f32)

    def store_gu(c, k, value):
        gu_out[:, c, span(across(a, k), units)] = value.astype(f32)
        stored.append((c, k))
        if len(stored) == 2 * na:
            save_gu.start()

    def store_attn(k, values):
        for c in range(3):
            store(qkv_out.at[c], across(a, k), HD, values[:, c * HD : (c + 1) * HD])
        store(wout_out, across(a, k), HD, values[:, 3 * HD :])

    def own_gu():
        store_gu(0, 0, gate_ref[a])
        store_gu(1, 0, up_sum[a])

    def gu_arrived(c, k):
        copies["g", c, k].wait_recv()
        store_gu(c, k, gu_in[k - 1, c])

    def attn_arrived(k):
        copies["a", k].wait_recv()
        store_attn(k, attn_in[k - 1])

    def down_rows(k):
        if "down" not in copies:
            copies["down"] = 0
            for copy in load_down:
                copy.wait()
            store(down_out, a, units, down_sum_ref[a])
        store(down_out, across(a, k), units, down_in[k - 1])
        copies["down"] += 1
        if copies["down"] == na - 1:
            save_down.start()

    def first(at):
        out[0, at, mine] = (grad_ref[at] + r.add_all(at)).astype(bf16)

    table = {
        "U1": sums_pair,
        "U2": sums_core,
        "U3": sums_far,
        "U4": sums_b,
        "U5": sums_done,
        "AB": attend_back,
        "S1": over_heads.to_pair,
        "S2": over_heads.to_core,
        "S3": over_heads.to_all,
        "S4": over_heads.done,
        "WO": out_grads,
        "WQ": qkv_grads,
        "QB": qkv_back,
        "YG": up_rows,
        "SG": up_sums,
        "ZG": gu_owner,
        "YA": attn_rows,
        "SA": attn_sums,
        "ZA": attn_owner,
        "OWNG": own_gu,
        "OWN": lambda: store_attn(0, attn_sum[a]),
        "OD": down_rows,
        "OG": gu_arrived,
        "OA": attn_arrived,
    }
    table.update({"r" + key: step for key, step in r.steps(first, None, 0).items()})
    for key, *where in LAST:
        table[key](*where)
    for h in range(HALVES):
        r.arrived(h, 0)
    save_down.wait()
    save_gu.wait()
    links.finish()


def last_call(nb, *operands):
    na, rows, width = operands[0].shape
    w_rows, units = operands[12].shape[1:]
    quarter = width // 4
    vmem, far = pl.BlockSpec(memory_space=pltpu.VMEM), pl.BlockSpec(memory_space=pl.ANY)
    shape = jax.ShapeDtypeStruct
    outs = (
        shape((1, rows, width), bf16),
        shape((8, quarter + HD), f32),
        shape((w_rows, na * units), f32),
        shape((w_rows, 2, na * units), f32),
        shape((3, w_rows, na * HD), f32),
        shape((w_rows, na * HD), f32),
    )
    copies = HALVES * (3 * na + 1) + 2 + 6 * na + 4 * nb
    return pl.pallas_call(
        functools.partial(last_kernel, na, nb),
        out_shape=outs,
        in_specs=[far if i in (0, 1, 12, 13, 14) else vmem for i in range(16)],
        out_specs=(vmem, vmem, far, far, vmem, vmem),
        scratch_shapes=[
            pltpu.VMEM((na, rows, 2 * HD), f32),
            pltpu.VMEM((na, rows, 3 * HD), bf16),
            pltpu.VMEM((na, rows, width), bf16),
            pltpu.VMEM((8, HD), f32),
            pltpu.VMEM((5, 8, rows), f32),
            pltpu.VMEM((na - 1, 8, rows), f32),
            pltpu.VMEM((8, rows), f32),
            pltpu.VMEM((8, width), f32),
            pltpu.VMEM((na - 1, 8, quarter), f32),
            pltpu.VMEM((nb, 8, quarter + HD), f32),
            pltpu.VMEM((nb - 1, na, w_rows, units), bf16),
            pltpu.VMEM((na, w_rows, units), bf16),
            pltpu.VMEM((na, nb, w_rows, 4 * HD), bf16),
            pltpu.VMEM((nb - 1, na, w_rows, 4 * HD), bf16),
            pltpu.VMEM((na, w_rows, 4 * HD), bf16),
            pltpu.VMEM((na - 1, 2, w_rows, units), bf16),
            pltpu.VMEM((na - 1, w_rows, 4 * HD), bf16),
            pltpu.VMEM((na, rows, width), bf16),
            pltpu.VMEM((na, w_rows, units), bf16),
            pltpu.VMEM((w_rows, na * units), f32),
            pltpu.VMEM((w_rows, 2, na * units), f32),
            pltpu.VMEM((na, rows, width), bf16),
            pltpu.VMEM((na, w_rows, units), bf16),
            pltpu.VMEM((na - 1, w_rows, units), bf16),
        ]
        + reduce_scratch(na, rows, width)
        + [
            pltpu.SemaphoreType.DMA((6 + na,)),
            pltpu.SemaphoreType.DMA((copies,)),
            pltpu.SemaphoreType.DMA((copies,)),
        ],
        compiler_params=pltpu.CompilerParams(
            collective_id=4, has_side_effects=True, vmem_limit_bytes=VMEM_LIMIT
        ),
        name="last",
    )(*operands)


def reduce_scratch(na, rows, width):
    quarter = width // 4
    return [
        pltpu.VMEM((na, rows, width // 2), bf16),
        pltpu.VMEM((na, rows, width // 2), bf16),
        pltpu.VMEM((na, rows, quarter), bf16),
        pltpu.VMEM((na - 1, rows, quarter), bf16),
        pltpu.VMEM((na - 1, rows, quarter), bf16),
        pltpu.VMEM((rows, quarter), f32),
        pltpu.VMEM((2, rows, 128), f32),
        pltpu.VMEM((2, rows, 128), f32),
        pltpu.VMEM((HALVES, 4, 8, rows // HALVES), f32),
    ]


ENTER = (
    ("Z", 0), ("W", 3), ("FW", 0), ("FR", 0, 1), ("FL", 0, 1), ("W", 1), ("CUT", 2), ("FW", 1), ("W", 2),
    ("FR", 0, 2), ("FR", 0, 3), ("CUT", 3), ("M", 0, 3), ("FL", 0, 2), ("CUT", 1), ("FW", 3), ("FL", 0, 3),
    ("GA",), ("FT", 0), ("FQ", 3), ("FW", 2), ("CUT", 0), ("FQ", 2), ("M", 0, 1), ("M", 2, 3), ("FQ", 1),
    ("J", 3), ("FQ", 0), ("J", 0), ("GB",), ("M", 1, 1), ("J", 1), ("J", 2), ("S1",), ("S2",), ("S3",),
    ("M", 1, 3), ("MR", 1, 0), ("M", 1, 2), ("S4",), ("E", 3), ("E", 1), ("rP", 1, 3), ("E", 2),
    ("rP", 1, 1), ("M", 2, 1), ("MR", 2, 3), ("rP", 0, 3), ("rP", 0, 1), ("MR", 0, 3), ("E", 0),
    ("rA", 1, 3), ("MR", 2, 0), ("rA", 1, 1), ("MR", 0, 1), ("rA", 0, 3), ("MR", 1, 3), ("rP", 0, 2),
    ("MR", 2, 1), ("rA", 0, 2), ("rA", 0, 1), ("rP", 0, 0), ("rP", 1, 2), ("rA", 1, 2), ("MR", 1, 2),
    ("rP", 1, 0), ("rSC", 0), ("rSQ", 0), ("MR", 0, 0), ("M", 2, 2), ("rSC", 1), ("rSD", 0), ("rSQ", 1),
    ("rX", 0), ("rSD", 1), ("rZ", 0), ("rZ", 1), ("rFR", 0, 1), ("rFL", 0, 1), ("rX", 1), ("MR", 2, 2),
    ("rFR", 1, 1), ("rFL", 1, 1), ("rFR", 0, 2), ("rRQ", 0, 0), ("rFL", 1, 2), ("rFL", 0, 2), ("MR", 1, 1),
    ("rFR", 0, 3), ("M", 0, 2), ("rFR", 1, 2), ("rFL", 1, 3), ("rFR", 1, 3), ("rFL", 0, 3), ("rRQ", 0, 1),
    ("MR", 0, 2), ("rRQ", 1, 1), ("rRQ", 1, 2), ("rRQ", 0, 2), ("rRQ", 1, 0), ("rRQ", 1, 3), ("rRQ", 0, 3),
)


def enter_kernel(na, nb, gain_sizes, *refs):
    tok_far, qkv_w_ref, wout_ref, gu_far, down_far, cos_ref, sin_ref, all_gains_ref = refs[:8]
    x_far, w_far, mlp_w_ref, width_gain_ref, head_gain_ref, qkv_far, stats_ref, att_far = refs[8:16]
    out, proj_ref, inv_ref, res_ref = refs[16:20]
    own_gains, gains_ref, piece_ref, part_ref, held, stats_a = refs[20:26]
    x_ref, w_ref, qkv_ref, att_ref = refs[26:30]
    tok_ref, gu_ref, down_ref = refs[30:33]
    scratch, (local_sem, send_sem, recv_sem) = refs[33:-3], refs[-3:]
    load_mlp = [
        pltpu.make_async_copy(gu_far, gu_ref, local_sem.at[10]),
        pltpu.make_async_copy(down_far, down_ref, local_sem.at[11]),
    ]
    for copy in load_mlp:
        copy.start()
    saves = [
        pltpu.make_async_copy(near, there, local_sem.at[5 + i])
        for i, (near, there) in enumerate(
            ((x_ref, x_far), (w_ref, w_far), (qkv_ref, qkv_far), (att_ref, att_far))
        )
    ]
    a, b, p, q = (lax.axis_index(axis) for axis in ("a", "b", "p", "q"))
    rows = wout_ref.shape[0]
    quarter = tok_ref.shape[1]
    load = pltpu.make_async_copy(
        tok_far.at[:, span(2 * q + p, quarter)], tok_ref, local_sem.at[9]
    )
    load.start()
    units = down_ref.shape[1] // na
    own_gains[...] = jnp.zeros_like(own_gains)
    n_d, n_h = gain_sizes
    place = 0
    for i, size in enumerate((n_d, n_d, n_h, n_h)):
        own_gains[i : i + 1, :size] = all_gains_ref[:, place : place + size].astype(f32)
        place += size
    gains_ref[a, b] = own_gains[...]
    greet(
        [{"q": 1 - q}, {"p": 1 - p}]
        + [{"a": across(a, k)} for k in range(1, na)]
        + [{"b": across(b, j)} for j in range(1, nb)]
    )
    load.wait()
    links = Links(send_sem, recv_sem)
    mine, pair = span(2 * q + p, quarter), span(q, 2 * quarter)
    place = span(a * nb + b, rows)
    copies, ends = {}, []
    locals_ = [pltpu.make_async_copy(tok_ref, x_ref.at[0, :, mine], local_sem.at[0])]

    def weight_sources(k):
        block = span(across(a, k), HD)
        sources = [qkv_w_ref.at[c, :, block] for c in range(3)] + [wout_ref.at[:, block]]
        return [(s, w_ref.at[place, c * HD : (c + 1) * HD]) for c, s in enumerate(sources)]

    for c, (source, target) in enumerate(weight_sources(0)):
        locals_.append(pltpu.make_async_copy(source, target, local_sem.at[1 + c]))
    for copy in locals_:
        copy.start()

    def send_gains():
        copies["g"] = [
            links.send(own_gains, gains_ref.at[a, b], {"a": across(a, k)}) for k in range(1, na)
        ]

    def relay_gains():
        for copy in copies["g"]:
            copy.wait_recv()
        at = gains_ref.at[:, b]
        copies["gb"] = [links.send(at, at, {"b": across(b, j)}) for j in range(1, nb)]

    def send_weights(k):
        copies["w", k] = [
            links.send(source, target, {"a": across(a, k)}) for source, target in weight_sources(k)
        ]

    def relay_weights(k):
        if k:
            for copy in copies["w", k]:
                copy.wait_recv()
        else:
            for copy in locals_[1:]:
                copy.wait()
        at = w_ref.at[span(across(a, k) * nb + b, rows), :]
        copies["wb", k] = [links.send(at, at, {"b": across(b, j)}) for j in range(1, nb)]

    line = Line(links, na, lambda k: x_ref.at[k, :, mine], tok_ref)

    def own_tokens(_):
        locals_[0].wait()
        line.to_pair(0).start()

    def pair_tokens(k):
        line.to_pair(k).wait_recv()
        at = x_ref.at[k, :, pair]
        copies["x", k] = links.send(at, at, {"q": 1 - q})

    def cut_weights(k):
        if "cut" not in copies:
            copies["cut"] = True
            for copy in load_mlp:
                copy.wait()
        block = span(across(a, k), units)

        def cut(i, carry):
            at = pl.ds(pl.multiple_of(i * TILE, TILE), TILE)
            cuts = (gu_ref[at, 0, block], gu_ref[at, 1, block], down_ref[at, block])
            for c in range(3):
                if k:
                    piece_ref[k - 1, c, at] = cuts[c]
                else:
                    to = pl.ds(pl.multiple_of((a * nb + b) * rows + i * TILE, TILE), TILE)
                    mlp_w_ref[to, c * units : (c + 1) * units] = cuts[c]
            return carry

        lax.fori_loop(0, rows // TILE, cut, 0)

    def send_piece(c, k):
        target = mlp_w_ref.at[place, c * units : (c + 1) * units]
        copies["m", c, k] = links.send(piece_ref.at[k - 1, c], target, {"a": across(a, k)})

    def relay_piece(c, k):
        if k:
            copies["m", c, k].wait_recv()
        at = mlp_w_ref.at[span(across(a, k) * nb + b, rows), c * units : (c + 1) * units]
        ends.extend(links.send(at, at, {"b": across(b, j)}) for j in range(1, nb))

    arrived, ready = set(), []

    def project(k):
        if not arrived:
            held[0] = jnp.zeros_like(held[0])
            for i in range(na):
                for copy in copies["wb", i]:
                    copy.wait_recv()
        arrived.add(k)
        copies["x", k].wait_recv()

        def chunk(i, carry):
            at = span(i, 128)
            proj = dot(x_ref[k, at], w_ref[:, : 3 * HD])
            qkv_ref[k, at] = proj
            queries, key_rows = proj[:, :HD], proj[:, HD : 2 * HD]
            held[0, :, at] += to_row(queries * queries, 2 * k) + to_row(key_rows * key_rows, 2 * k + 1)
            return carry

        lax.fori_loop(0, x_ref.shape[1] // 128, chunk, 0)

    over_heads = OverHeads(links, na, a, p, q, held, stats_a, stats_ref)

    def all_stats():
        for save in saves[:3]:
            save.start()
        over_heads.done()
        for copy in copies["gb"]:
            copy.wait_recv()
        width_gain_ref[...] = jnp.zeros_like(width_gain_ref)
        head_gain_ref[...] = jnp.zeros_like(head_gain_ref)
        for i in range(2):
            width_gain_ref[i : i + 1] = jnp.concatenate(
                [gains_ref[2 * q + p, j, i : i + 1, :n_d] for j in range(nb)], axis=1
            )
            head_gain_ref[i : i + 1] = jnp.concatenate(
                [gains_ref[a, j, i + 2 : i + 3, :n_h] for j in range(nb)], axis=1
            )

    r = Reduce(na, links, part_ref, out, scratch)

    def attend(k):
        values, probs = (
            attention(k, qkv_ref[k], stats_ref[...], head_gain_ref, cos_ref, sin_ref)[i] for i in (2, 7)
        )
        attended = dot(probs.astype(bf16), values).astype(bf16)
        att_ref[k] = attended

        def part(n, carry):
            at = span(n, 512)
            part_ref[k, :, at] = dot_t(att_ref[k], w_ref[at, 3 * HD :]).astype(bf16)
            return carry

        lax.fori_loop(0, part_ref.shape[2] // 512, part, 0)
        for h in range(HALVES):
            r.send_q(h, k)

    first, second = attn_math(r, tok_ref, width_gain_ref, proj_ref, inv_ref, res_ref)
    table = {
        "GA": send_gains,
        "GB": relay_gains,
        "W": send_weights,
        "FW": relay_weights,
        "Z": lambda _: line.start(),
        "FL": lambda _, t: line.pass_on(1, t),
        "FR": lambda _, t: line.pass_on(-1, t),
        "FT": own_tokens,
        "FQ": pair_tokens,
        "CUT": cut_weights,
        "M": send_piece,
        "MR": relay_piece,
        "J": project,
        "S1": over_heads.to_pair,
        "S2": over_heads.to_core,
        "S3": over_heads.to_all,
        "S4": all_stats,
        "E": attend,
    }
    table.update({"r" + key: step for key, step in r.steps(first, second, 1, True).items()})
    for key, *where in ENTER:
        table[key](*where)
    saves[3].start()
    for h in range(HALVES):
        for k in range(na):
            r.arrived(h, k)
    for copy in ends:
        copy.wait_recv()
    for save in saves:
        save.wait()
    links.finish()


def enter_call(na, nb, tokens, qkv, w_out, gu, down, cos_table, sine_table, gains):
    rows, width = tokens.shape
    quarter = width // 4
    sizes = (gains[0].shape[0], gains[2].shape[0])
    w_rows, units = down.shape[0], down.shape[1] // na
    lanes = max(128, sizes[0])
    vmem, far = pl.BlockSpec(memory_space=pltpu.VMEM), pl.BlockSpec(memory_space=pl.ANY)
    shape = jax.ShapeDtypeStruct
    full = shape((na, rows, width), bf16)
    outs = [
        full,
        shape((width, 4 * HD), bf16),
        shape((width, 3 * units), bf16),
        shape((8, quarter), f32),
        shape((8, HD), f32),
        shape((na, rows, 3 * HD), f32),
        shape((8, rows), f32),
        shape((na, rows, HD), bf16),
        full,
        shape((rows, quarter), f32),
        shape((rows, 128), f32),
        shape((rows, quarter), f32),
    ]
    copies = 90 + 16 * nb
    return pl.pallas_call(
        functools.partial(enter_kernel, na, nb, sizes),
        out_shape=tuple(outs),
        in_specs=[far if i in (0, 3, 4) else vmem for i in range(8)],
        out_specs=tuple(far if i in (0, 1, 5, 7) else vmem for i in range(len(outs))),
        scratch_shapes=[
            pltpu.VMEM((8, lanes), f32),
            pltpu.VMEM((na, nb, 8, lanes), f32),
            pltpu.VMEM((na - 1, 3, w_rows, units), bf16),
            pltpu.VMEM((na, rows, width), bf16),
            pltpu.VMEM((5, 8, rows), f32),
            pltpu.VMEM((na - 1, 8, rows), f32),
            pltpu.VMEM((na, rows, width), bf16),
            pltpu.VMEM((width, 4 * HD), bf16),
            pltpu.VMEM((na, rows, 3 * HD), f32),
            pltpu.VMEM((na, rows, HD), bf16),
            pltpu.VMEM((rows, quarter), bf16),
            pltpu.VMEM(gu.shape, bf16),
            pltpu.VMEM(down.shape, bf16),
        ]
        + reduce_scratch(na, rows, width)
        + [
            pltpu.SemaphoreType.DMA((12,)),
            pltpu.SemaphoreType.DMA((copies,)),
            pltpu.SemaphoreType.DMA((copies,)),
        ],
        compiler_params=pltpu.CompilerParams(
            collective_id=5, has_side_effects=True, vmem_limit_bytes=VMEM_LIMIT
        ),
        name="enter",
    )(tokens, qkv, w_out, gu, down, cos_table, sine_table, jnp.concatenate(gains)[None])


def rope_tables(length, width):
    half_width = width // 2
    inv_freq = rope_base ** (-(jnp.arange(half_width, dtype=f32) * 2.0) / width)
    angles = jnp.arange(length, dtype=f32)[:, None] * inv_freq[None, :]
    cos_table = jnp.concatenate([jnp.cos(angles), jnp.cos(angles)], axis=1)
    sine_table = jnp.concatenate([jnp.sin(angles), jnp.sin(angles)], axis=1)
    return cos_table, sine_table


def on_device(
    tokens,
    qkv_weight,
    out_weight,
    gu_weight,
    down_weight,
    attn_gain,
    ffn_gain,
    q_gain,
    k_gain,
    out_grad,
):
    na, nb = lax.axis_size("a"), lax.axis_size("b")
    a, b = lax.axis_index("a"), lax.axis_index("b")
    share = lax.axis_index("q") * 2 + lax.axis_index("p")
    rows, width = tokens.shape
    quarter = width // 4
    w_rows = out_weight.shape[0]
    units = down_weight.shape[1] // na

    cos_table, sine_table = rope_tables(SEQ_LEN, HD)
    (
        x_all,
        w_attn,
        w_mlp,
        width_gain,
        head_gain,
        qkv,
        stats,
        attended,
        res_all,
        proj_mine,
        inv_mine,
        res_mine,
    ) = enter_call(
        na,
        nb,
        tokens,
        qkv_weight.transpose(1, 0, 2),
        out_weight,
        gu_weight,
        down_weight,
        cos_table,
        sine_table,
        (attn_gain, ffn_gain, q_gain, k_gain),
    )
    n_d, n_h = attn_gain.shape[0], q_gain.shape[0]
    block_rows, grad_proj, ffn_sums, grad_res, attn_sums, down_sum, gu_grad, down_in, gate_sum = middle_call(
        nb, res_all, w_mlp, res_mine, out_grad, proj_mine, inv_mine, width_gain
    )
    grad_rows, sums, down_grad, gu_grad, qkv_grad, out_grad_w = last_call(
        nb,
        grad_proj,
        x_all,
        qkv,
        stats,
        head_gain,
        cos_table,
        sine_table,
        w_attn,
        attended,
        grad_res,
        attn_sums,
        ffn_sums,
        down_sum,
        gu_grad,
        down_in,
        gate_sum,
    )
    width_sums = lax.dynamic_slice_in_dim(sums[:2, :quarter], b * n_d, n_d, 1)
    head_sums = lax.dynamic_slice_in_dim(sums[:2, quarter:], b * n_h, n_h, 1)
    return (
        block_rows[0].astype(f32),
        grad_rows[0].astype(f32),
        qkv_grad.transpose(1, 0, 2),
        out_grad_w,
        gu_grad,
        down_grad,
        width_sums[0],
        width_sums[1],
        head_sums[0],
        head_sums[1],
    )


def solution(mesh):
    dp, tp = mesh.shape["dp"], mesh.shape["tensor"]
    na = HEADS // tp
    fine = Mesh(mesh.devices.reshape(na, dp // na, tp // 2, 2), ("a", "b", "p", "q"))
    dp_axes, tp_axes = ("a", "b"), ("p", "q")
    both = tp_axes + dp_axes
    return jax.shard_map(
        on_device,
        mesh=fine,
        in_specs=(
            P(dp_axes, None),
            P(dp_axes, None, tp_axes),
            P(dp_axes, tp_axes),
            P(dp_axes, None, tp_axes),
            P(dp_axes, tp_axes),
            P(dp_axes),
            P(dp_axes),
            P(both),
            P(both),
            P(dp_axes, None),
        ),
        out_specs=(
            P(dp_axes, None),
            P(dp_axes, None),
            P(dp_axes, None, tp_axes),
            P(dp_axes, tp_axes),
            P(dp_axes, None, tp_axes),
            P(dp_axes, tp_axes),
            P(dp_axes),
            P(dp_axes),
            P(both),
            P(both),
        ),
        check_vma=False,
    )
```

```python
import functools

import jax
import jax.numpy as jnp
from jax import lax
from jax.experimental import pallas as pl
from jax.experimental.pallas import tpu as pltpu
from jax.sharding import Mesh, PartitionSpec as P

HEADS = 16
HD = 128
SEQ_LEN = 256
HQ = 2048

epsilon = 1e-06
rope_base = 500000.0

f32 = jnp.float32
bf16 = jnp.bfloat16
MESH = pl.DeviceIdType.MESH
EXACT = lax.Precision.HIGHEST
VMEM_LIMIT = 63 * 1024 * 1024
TILE = 32
HALVES = 2


def flip(index, bit):
    return index + bit - 2 * bit * ((index // bit) % 2)


def across(index, k):
    bit = 1
    while bit <= k:
        if k & bit:
            index = flip(index, bit)
        bit *= 2
    return index


def exclusive_or(left, right, count):
    total, bit = 0, 1
    while bit < count:
        total = total + bit * ((left // bit + right // bit) % 2)
        bit *= 2
    return total


def pick(operand, index, axis):
    return lax.dynamic_index_in_dim(operand, index, axis, keepdims=False)


def span(index, size):
    return pl.ds(pl.multiple_of(index * size, size), size)


class Links:
    def __init__(self, send_sem, recv_sem):
        self.send_sem, self.recv_sem, self.count = send_sem, recv_sem, 0
        self.copies, self.lines = [], []

    def send(self, source, target, device):
        copy = self.copy(self.count, source, target, device)
        copy.start()
        self.count += 1
        self.copies.append(copy)
        return copy

    def reserve(self, number):
        self.count += number
        return self.count - number

    def copy(self, index, source, target, device):
        return pltpu.make_async_remote_copy(
            src_ref=source,
            dst_ref=target,
            send_sem=self.send_sem.at[index],
            recv_sem=self.recv_sem.at[index],
            device_id=device,
            device_id_type=MESH,
        )

    def sent(self, copies):
        done = [id(copy) for copy in copies]
        for copy in self.copies:
            if id(copy) in done:
                copy.wait_send()
        self.copies = [copy for copy in self.copies if id(copy) not in done]

    def finish(self):
        for copy in self.copies:
            copy.wait_send()
        for line in self.lines:
            line.finish()


def greet(peers):
    barrier = pltpu.get_barrier_semaphore()
    for peer in peers:
        pl.semaphore_signal(barrier, inc=1, device_id=peer, device_id_type=MESH)
    pl.semaphore_wait(barrier, len(peers))


def fold(block):
    total = block[:, :128]
    for i in range(1, block.shape[1] // 128):
        total = total + block[:, i * 128 : (i + 1) * 128]
    return total


def wide(column, width):
    return jnp.concatenate([column] * (width // 128), axis=1)


def row_mask(row):
    return (lax.broadcasted_iota(jnp.int32, (8, 128), 0) == row).astype(f32)


def to_row(block, row):
    return lax.dot_general(
        row_mask(row), block, (((1,), (1,)), ((), ())), precision=EXACT, preferred_element_type=f32
    )


def to_column(stats, row):
    return lax.dot_general(
        stats, row_mask(row), (((0,), (0,)), ((), ())), precision=EXACT, preferred_element_type=f32
    )


def dot(left, right):
    return jnp.dot(left, right, preferred_element_type=f32)


def dot_t(left, right):
    return lax.dot_general(left, right, (((1,), (1,)), ((), ())), preferred_element_type=f32)


def t_dot(left, right):
    return lax.dot_general(left, right, (((0,), (0,)), ((), ())), preferred_element_type=f32)


def rotate(operand):
    half = HD // 2
    return jnp.concatenate([-operand[:, half:], operand[:, :half]], axis=1)


def rotate_back(operand):
    half = HD // 2
    return jnp.concatenate([operand[:, half:], -operand[:, :half]], axis=1)


def attention(k, qkv, stats, gain_ref, cos_ref, sin_ref):
    stats = stats / HQ
    q_inv = lax.rsqrt(to_column(stats, 2 * k) + epsilon)
    k_inv = lax.rsqrt(to_column(stats, 2 * k + 1) + epsilon)
    queries, key_rows = qkv[:, :HD], qkv[:, HD : 2 * HD]
    values = qkv[:, 2 * HD :].astype(bf16)
    cos_table, sine_table = cos_ref[...], sin_ref[...]
    q_normed = queries * q_inv * gain_ref[0:1]
    k_normed = key_rows * k_inv * gain_ref[1:2]
    q_rot = (q_normed * cos_table + rotate(q_normed) * sine_table).astype(bf16)
    k_rot = (k_normed * cos_table + rotate(k_normed) * sine_table).astype(bf16)
    scores = dot_t(q_rot, k_rot) * HD ** (-0.5)
    ahead = lax.broadcasted_iota(jnp.int32, scores.shape, 1) > lax.broadcasted_iota(
        jnp.int32, scores.shape, 0
    )
    scores = jnp.where(ahead, -1e30, scores)
    shifted = jnp.exp(scores - jnp.max(scores, axis=1, keepdims=True))
    probs = shifted / jnp.sum(shifted, axis=1, keepdims=True)
    return queries, key_rows, values, q_inv, k_inv, q_rot, k_rot, probs


def weight_grad(left, right, out, block, columns=None, take=slice(None)):
    na, nb, rows = left.shape[0], out.shape[1], out.shape[2]
    columns = columns or slice(0, right.shape[2])
    size = max(rows, 256)


    def chunk(i, carry):
        at = span(block * (nb * rows // size) + i, size)
        total = t_dot(left[0, :, at], right[0, :, take])
        for k in range(1, na):
            total = total + t_dot(left[k, :, at], right[k, :, take])
        for j in range(size // rows):
            part = total[j * rows : (j + 1) * rows].astype(bf16)
            out[block, i * (size // rows) + j, :, columns] = part
        return carry

    lax.fori_loop(0, nb * rows // size, chunk, 0)


def exchange_b(links, grad, held, columns):
    b = lax.axis_index("b")
    put = columns if held.shape[3] == grad.shape[3] or columns.stop <= held.shape[3] else slice(None)
    return [
        links.send(
            grad.at[:, across(b, j), :, columns], held.at[j - 1, :, :, put], {"b": across(b, j)}
        )
        for j in range(1, held.shape[0] + 1)
    ]


def sum_b(copies, own, held, out, columns):
    for copy in copies:
        copy.wait_recv()

    def add(block, carry):
        total = own(block)[:, columns].astype(f32)
        for j in range(held.shape[0]):
            total = total + held[j, block, :, columns].astype(f32)
        out[block, :, columns] = total.astype(bf16)
        return carry

    lax.fori_loop(0, held.shape[1], add, 0)


class Line:
    def __init__(self, links, na, block, own):
        self.links, self.na, self.block, self.own = links, na, block, own
        self.a, self.p = lax.axis_index("a"), lax.axis_index("p")
        self.hop_base = {1: links.reserve(na - 1), -1: links.reserve(na - 1)}
        self.pass_base = links.reserve(na)
        links.lines.append(self)

    def hop(self, way, t):
        a, na = self.a, self.na
        first = a - way * (t - 1)
        source = self.own if t == 1 else self.block(exclusive_or(first, a, na))
        target = self.block(exclusive_or(first, a + way, na))
        return self.links.copy(self.hop_base[way] + t - 1, source, target, {"a": (a + way) % na})

    def sends(self, way, t):
        first, last = self.a - way * (t - 1), self.a + way
        return (first >= 0) & (first < self.na) & (last >= 0) & (last < self.na)

    def to_pair(self, k, source=None):
        at = self.block(k)
        return self.links.copy(self.pass_base + k, at if source is None else source, at, {"p": 1 - self.p})

    def start(self):
        for way in (1, -1):

            @pl.when(self.sends(way, 1))
            def _(way=way):
                self.hop(way, 1).start()

    def pass_on(self, way, t):
        came = self.a - way * t

        @pl.when((came >= 0) & (came < self.na))
        def _():
            self.hop(way, t).wait_recv()
            self.to_pair(exclusive_or(came, self.a, self.na)).start()

        if t < self.na - 1:

            @pl.when(self.sends(way, t + 1))
            def _():
                self.hop(way, t + 1).start()

    def finish(self):
        for way in (1, -1):
            for t in range(1, self.na):

                @pl.when(self.sends(way, t))
                def _(way=way, t=t):
                    self.hop(way, t).wait_send()

        for k in range(self.na):
            self.to_pair(k).wait_send()


class Reduce:
    def __init__(self, na, links, part, out, scratch):
        self.na, self.links, self.part, self.out = na, links, part, out
        self.from_q, self.half_sum, self.from_p, self.to_a, self.from_a = scratch[:5]
        self.total, self.parts, self.cols, self.stat = scratch[5:9]
        self.a, self.p, self.q = (lax.axis_index(axis) for axis in ("a", "p", "q"))
        self.rows, self.width = out.shape[1:]
        self.quarter, self.half = self.width // 4, self.width // 2
        self.count = self.rows // HALVES
        self.mine, self.pair = span(2 * self.q + self.p, self.quarter), span(self.q, self.half)
        self.lead = list(range(2, na)) + [1, 0]
        self.step_q, self.step_p, self.step_a = {}, {}, {}
        self.spread_a, self.spread_p, self.spread_q, self.stats = {}, {}, {}, {}
        self.here, self.slots = set(), None

    def at(self, h):
        return slice(h * self.count, (h + 1) * self.count)

    def each(self, h, body):
        def step(i, carry):
            body(pl.ds(pl.multiple_of(h * self.count + i * TILE, TILE), TILE))
            return carry

        lax.fori_loop(0, self.count // TILE, step, 0)

    def send_q(self, h, k):
        at, q = self.at(h), self.q
        source = self.part.at[k, at, span(1 - q, self.half)]
        self.step_q[h, k] = self.links.send(source, self.from_q.at[k, at], {"q": 1 - q})

    def send_p(self, h, k):
        self.step_q[h, k].wait_recv()

        def add(at):
            own = self.part[k, at, span(self.q, self.half)].astype(f32)
            self.half_sum[k, at] = (own + self.from_q[k, at].astype(f32)).astype(bf16)

        self.each(h, add)
        at, p = self.at(h), self.p
        source = self.half_sum.at[k, at, span(1 - p, self.quarter)]
        self.step_p[h, k] = self.links.send(source, self.from_p.at[k, at], {"p": 1 - p})

    def send_a(self, h, k):
        if not k:
            return
        self.step_p[h, k].wait_recv()

        def add(at):
            own = self.half_sum[k, at, span(self.p, self.quarter)].astype(f32)
            self.to_a[k - 1, at] = (own + self.from_p[k, at].astype(f32)).astype(bf16)

        self.each(h, add)
        at = self.at(h)
        self.step_a[h, k] = self.links.send(
            self.to_a.at[k - 1, at], self.from_a.at[k - 1, at], {"a": across(self.a, k)}
        )

    def add_all(self, at):
        if self.slots is not None:
            return self.total[at]
        own = self.half_sum[0, at, span(self.p, self.quarter)].astype(f32)
        own = own + self.from_p[0, at].astype(f32)
        for k in range(1, self.na):
            own = own + self.from_a[k - 1, at].astype(f32)
        return own

    def scattered(self, h, first, number):
        if self.slots is not None:
            self.gather_sums(h)
        else:
            self.step_p[h, 0].wait_recv()
            for k in range(1, self.na):
                self.step_a[h, k].wait_recv()
        self.each(h, first)
        if number:
            at = self.at(h)
            stats = to_row(self.parts[0, at], 0)
            if number == 2:
                stats = stats + to_row(self.parts[1, at], 1)
            stat = self.stat
            stat[h, 0] = stats
            self.stats[h] = self.links.send(stat.at[h, 0], stat.at[h, 1], {"p": 1 - self.p})

    def stats_q(self, h):
        stat = self.stat
        self.stats[h].wait_recv()
        stat[h, 2] = stat[h, 0] + stat[h, 1]
        self.stats[h] = self.links.send(stat.at[h, 2], stat.at[h, 3], {"q": 1 - self.q})

    def stats_done(self, h, number):
        stat = self.stat
        self.stats[h].wait_recv()
        stats = (stat[h, 2] + stat[h, 3]) / self.width
        for i in range(number):
            self.cols[i, self.at(h)] = to_column(stats, i)

    def spread(self, h, blocks):
        here = self.out.at[0, self.at(h), self.mine]
        for k in blocks:
            if k:
                target = self.out.at[k, self.at(h), self.mine]
                self.spread_a[h, k] = self.links.send(here, target, {"a": across(self.a, k)})
        self.spread_p[h, 0] = self.links.send(here, here, {"p": 1 - self.p})

    def relay_p(self, h, k):
        if not k:
            return
        self.spread_a[h, k].wait_recv()
        here = self.out.at[k, self.at(h), self.mine]
        self.spread_p[h, k] = self.links.send(here, here, {"p": 1 - self.p})

    def relay_q(self, h, k):
        self.spread_p[h, k].wait_recv()
        here = self.out.at[k, self.at(h), self.pair]
        self.spread_q[h, k] = self.links.send(here, here, {"q": 1 - self.q})

    def arrived(self, h, k):
        if (h, k) not in self.here:
            self.here.add((h, k))
            self.spread_q[h, k].wait_recv()

    def chained(self, slots):
        self.slots = slots
        na = self.na
        self.base_p = [self.links.reserve(na) for _ in range(HALVES)]
        self.base_c = [{w: self.links.reserve(na - 1) for w in (1, -1)} for _ in range(HALVES)]
        self.links.lines.append(self)

    def copy_p(self, h, k):
        at = self.at(h)
        source = self.half_sum.at[k, at, span(1 - self.p, self.quarter)]
        return self.links.copy(self.base_p[h] + k, source, self.from_p.at[k, at], {"p": 1 - self.p})

    def copy_c(self, h, way, t):
        at, side = self.at(h), 0 if way == 1 else 1
        return self.links.copy(
            self.base_c[h][way] + t - 1,
            self.slots.at[0, side, t - 1, at],
            self.slots.at[1, side, t - 1, at],
            {"a": (self.a + way) % self.na},
        )

    def inside(self, index):
        return (index >= 0) & (index < self.na)

    def send_p_chained(self, h, k):
        self.step_q[h, k].wait_recv()

        def add(at):
            own = self.part[k, at, span(self.q, self.half)].astype(f32)
            self.half_sum[k, at] = (own + self.from_q[k, at].astype(f32)).astype(bf16)

        self.each(h, add)
        self.copy_p(h, k).start()

    def pass_sums(self, h, way, t):
        side = 0 if way == 1 else 1

        @pl.when(self.inside(self.a + way * t))
        def _():
            k = exclusive_or(self.a, self.a + way * t, self.na)
            self.copy_p(h, k).wait_recv()

            def add(at):
                own = self.half_sum[k, at, span(self.p, self.quarter)].astype(f32)
                self.slots[0, side, t - 1, at] = (own + self.from_p[k, at].astype(f32)).astype(bf16)

            self.each(h, add)
            if t < self.na - 1:

                @pl.when(self.inside(self.a - way))
                def _():
                    self.copy_c(h, way, t + 1).wait_recv()

                    def more(at):
                        own = self.slots[0, side, t - 1, at].astype(f32)
                        came = self.slots[1, side, t, at].astype(f32)
                        self.slots[0, side, t - 1, at] = (own + came).astype(bf16)

                    self.each(h, more)

            self.copy_c(h, way, t).start()

    def gather_sums(self, h):
        self.copy_p(h, 0).wait_recv()

        def own(at):
            here = self.half_sum[0, at, span(self.p, self.quarter)].astype(f32)
            self.total[at] = here + self.from_p[0, at].astype(f32)

        self.each(h, own)
        for side, way in enumerate((1, -1)):

            @pl.when(self.inside(self.a - way))
            def _(side=side, way=way):
                self.copy_c(h, way, 1).wait_recv()

                def more(at):
                    self.total[at] += self.slots[1, side, 0, at].astype(f32)

                self.each(h, more)

    def finish(self):
        for h in range(HALVES):
            for k in range(self.na):
                self.copy_p(h, k).wait_send()
            for way in (1, -1):
                for t in range(1, self.na):

                    @pl.when(self.inside(self.a + way * t))
                    def _(h=h, way=way, t=t):
                        self.copy_c(h, way, t).wait_send()

    def steps(self, first, second, number, chain=False):
        def normed(h):
            self.stats_done(h, number)
            self.each(h, second)

        def spread_own(h):
            here = self.out.at[0, self.at(h), self.mine]
            self.spread_p[h, 0] = self.links.send(here, here, {"p": 1 - self.p})

        def spread_far(h, k):
            here = self.out.at[0, self.at(h), self.mine]
            target = self.out.at[k, self.at(h), self.mine]
            self.spread_a[h, k] = self.links.send(here, target, {"a": across(self.a, k)})

        table = {
            "P": self.send_p,
            "A": self.send_a,
            "SC": lambda h: self.scattered(h, first, number),
            "SQ": self.stats_q,
            "SD": normed,
            "X": spread_own,
            "Z": spread_far,
            "RP": self.relay_p,
            "RQ": self.relay_q,
        }
        if self.slots is not None:
            table.update(
                P=self.send_p_chained,
                CR=lambda h, t: self.pass_sums(h, 1, t),
                CL=lambda h, t: self.pass_sums(h, -1, t),
            )
        if chain:
            lines = [
                Line(
                    self.links,
                    self.na,
                    lambda k, h=h: self.out.at[k, self.at(h), self.mine],
                    self.out.at[0, self.at(h), self.mine],
                )
                for h in range(HALVES)
            ]

            def pair_arrived(h, k):
                self.spread_p[h, k] = lines[h].to_pair(k)
                self.relay_q(h, k)

            table.update(
                X=lambda h: lines[h].to_pair(0).start(),
                Z=lambda h: lines[h].start(),
                FL=lambda h, t: lines[h].pass_on(1, t),
                FR=lambda h, t: lines[h].pass_on(-1, t),
                RQ=pair_arrived,
            )
        return table


class OverHeads:
    def __init__(self, links, na, a, p, q, held, from_a, out_ref):
        self.links, self.na, self.a, self.p, self.q = links, na, a, p, q
        self.held, self.from_a, self.out_ref = held, from_a, out_ref

    def to_pair(self):
        self.copy = self.links.send(self.held.at[0], self.held.at[1], {"p": 1 - self.p})

    def to_core(self):
        held = self.held
        self.copy.wait_recv()
        held[2] = held[0] + held[1]
        self.copy = self.links.send(held.at[2], held.at[3], {"q": 1 - self.q})

    def to_all(self):
        held = self.held
        self.copy.wait_recv()
        held[4] = held[2] + held[3]
        self.copies = [
            self.links.send(held.at[4], self.from_a.at[k - 1], {"a": across(self.a, k)})
            for k in range(1, self.na)
        ]

    def done(self):
        for copy in self.copies:
            copy.wait_recv()
        for k in range(self.na):
            for i in range(2):
                at = 2 * k + i
                total = self.held[4, at : at + 1]
                for j in range(1, self.na):
                    other = 2 * (k ^ j) + i
                    total = total + self.from_a[j - 1, other : other + 1]
                self.out_ref[at : at + 1] = total


def reduce_peers(na):
    a, p, q = lax.axis_index("a"), lax.axis_index("p"), lax.axis_index("q")
    return [{"q": 1 - q}, {"p": 1 - p}] + [{"a": across(a, k)} for k in range(1, na)]


def attn_math(r, tok_ref, gain_ref, proj_ref, inv_ref, res_ref):
    def first(at):
        own = r.add_all(at)
        proj_ref[at] = own
        r.parts[0, at] = fold(own * own)

    def second(at):
        own = proj_ref[at]
        inv = lax.rsqrt(r.cols[0, at] + epsilon)
        inv_ref[at] = inv
        residual = tok_ref[at].astype(f32) + own * wide(inv, r.quarter) * gain_ref[0:1]
        res_ref[at] = residual
        r.out[0, at, r.mine] = residual.astype(bf16)

    return first, second


def mlp_math(r, res_ref, grad_ref, gain_ref, block_ref, sum_ref):
    def first(at):
        own = r.add_all(at)
        r.total[at] = own
        r.parts[0, at] = fold(own * own)
        r.parts[1, at] = fold(grad_ref[at] * gain_ref[1:2] * own)

    def second(at):
        own = r.total[at]
        inv = wide(lax.rsqrt(r.cols[0, at] + epsilon), r.quarter)
        upstream = grad_ref[at]
        scaled = upstream * gain_ref[1:2]
        normed = own * inv
        block_ref[0, at, r.mine] = (res_ref[at] + normed * gain_ref[1:2]).astype(bf16)
        gains = upstream * normed
        sum_ref[...] += jnp.sum(gains.reshape(TILE // 8, 8, r.quarter), axis=0)
        grad = inv * scaled - own * inv * inv * inv * wide(r.cols[1, at], r.quarter)
        r.out[0, at, r.mine] = grad.astype(bf16)

    return first, second


def back_math(r, grad_ref, proj_ref, inv_ref, gain_ref, res_ref, sum_ref):
    def first(at):
        grad = grad_ref[at] + r.add_all(at)
        res_ref[at] = grad
        r.parts[0, at] = fold(grad * gain_ref[0:1] * proj_ref[at])

    def second(at):
        own = proj_ref[at]
        inv = wide(inv_ref[at], r.quarter)
        upstream = res_ref[at]
        gains = upstream * own * inv
        sum_ref[...] += jnp.sum(gains.reshape(TILE // 8, 8, r.quarter), axis=0)
        grad = inv * (upstream * gain_ref[0:1])
        grad = grad - own * inv * inv * inv * wide(r.cols[0, at], r.quarter)
        r.out[0, at, r.mine] = grad.astype(bf16)

    return first, second


MIDDLE = (
    ("F", 2), ("F", 3), ("rP", 0, 2), ("F", 1), ("rP", 0, 3), ("rA", 0, 2), ("rP", 0, 1), ("rP", 1, 3),
    ("F", 0), ("rP", 1, 2), ("rA", 0, 3), ("rP", 1, 1), ("rA", 0, 1), ("rP", 0, 0), ("rA", 1, 3),
    ("rA", 1, 1), ("rA", 1, 2), ("rSC", 0), ("rP", 1, 0), ("rSQ", 0), ("rSD", 0), ("rZ", 0, 1), ("rX", 0),
    ("rZ", 0, 3), ("rSC", 1), ("rRP", 0, 1), ("rRQ", 0, 0), ("rSQ", 1), ("rZ", 0, 2), ("rSD", 1),
    ("rRP", 0, 3), ("rX", 1), ("rZ", 1, 1), ("rZ", 1, 2), ("rRP", 0, 2), ("rRQ", 0, 1), ("rRQ", 0, 3),
    ("rRP", 1, 1), ("B", 0, 3), ("rZ", 1, 3), ("rRP", 1, 2), ("rRQ", 1, 0), ("B", 0, 1), ("rRQ", 0, 2),
    ("sP", 0, 3), ("B", 0, 0), ("B", 0, 2), ("rRP", 1, 3), ("rRQ", 1, 2), ("sA", 0, 3), ("sP", 0, 2),
    ("B", 1, 2), ("sP", 0, 1), ("rRQ", 1, 1), ("rRQ", 1, 3), ("sA", 0, 2), ("sP", 1, 2), ("D", 0),
    ("sA", 0, 1), ("B", 1, 3), ("sA", 1, 2), ("sP", 1, 3), ("B", 1, 0), ("sP", 0, 0), ("D", 1),
    ("sA", 1, 3), ("sP", 1, 0), ("B", 1, 1), ("sSC", 0), ("sP", 1, 1), ("DS", 0), ("ZD", 0, 2), ("sSQ", 0),
    ("G", 0), ("sSD", 0), ("BP",), ("sA", 1, 1), ("G", 2), ("sZ", 0, 3), ("G", 3), ("sZ", 0, 2), ("sSC", 1),
    ("G", 1), ("YG",), ("sSQ", 1), ("sRP", 0, 3), ("sSD", 1), ("sZ", 1, 3), ("DS", 1), ("sZ", 1, 1),
    ("sZ", 0, 1), ("BQ",), ("sX", 0), ("ZD", 1, 3), ("sRP", 1, 1), ("sX", 1), ("sRQ", 1, 1), ("sZ", 1, 2),
    ("sRP", 0, 2), ("sRP", 0, 1), ("ZD", 0, 1), ("ZD", 1, 1), ("sRP", 1, 2), ("sRP", 1, 3), ("ZD", 1, 2),
    ("sRQ", 0, 0), ("sRQ", 0, 3), ("ZD", 0, 3), ("sRQ", 1, 0), ("sRQ", 1, 2), ("sRQ", 0, 2), ("sRQ", 0, 1),
    ("sRQ", 1, 3), ("SG",),
)


def middle_kernel(na, nb, *refs):
    x_far, w_far, res_ref, grad_far, proj_ref, inv_ref, gain_ref = refs[:7]
    block_ref, back_out, ffn_sum_ref, grad_res_ref, attn_sum_ref, down_sum_ref, up_grad_far = refs[7:14]
    down_in, gate_sum_ref = refs[14:16]
    out, hidden_ref, grad_gu_ref, gu_ref, part_ref, down_grad, down_held, grad_ref, gu_held = refs[16:25]
    x_ref, w_ref, gu_grad_ref = refs[25:28]
    scratch, (local_sem, send_sem, recv_sem) = refs[28:-3], refs[-3:]
    share = 2 * lax.axis_index("q") + lax.axis_index("p")
    load = pltpu.make_async_copy(
        grad_far.at[:, span(share, grad_ref.shape[1])], grad_ref, local_sem.at[0]
    )
    load.start()
    load_w = pltpu.make_async_copy(w_far, w_ref, local_sem.at[1])
    load_w.start()
    load_x = {
        k: pltpu.make_async_copy(x_far.at[k], x_ref.at[k], local_sem.at[2 + k])
        for k in list(range(2, na)) + [1, 0]
    }
    for copy in load_x.values():
        copy.start()
    units = hidden_ref.shape[2]
    width = x_ref.shape[2]
    save_up = pltpu.make_async_copy(
        gu_grad_ref.at[:, :, :, units:], up_grad_far, local_sem.at[2 + na]
    )
    b = lax.axis_index("b")
    greet(reduce_peers(na) + [{"b": across(b, j)} for j in range(1, nb)])
    links = Links(send_sem, recv_sem)
    r = Reduce(na, links, part_ref, out, scratch[:9])
    s = Reduce(na, links, part_ref, back_out, scratch[9:])
    ffn_sum_ref[...] = jnp.zeros_like(ffn_sum_ref)
    attn_sum_ref[...] = jnp.zeros_like(attn_sum_ref)
    wide_tile = 512

    def forward(k):
        def gated(n, carry):
            at, up_at = span(n, 256), pl.ds(pl.multiple_of(units + n * 256, 256), 256)
            gate = dot(x_ref[k], w_ref[:, at])
            up = dot(x_ref[k], w_ref[:, up_at])
            gu_ref[k, :, at] = gate
            gu_ref[k, :, up_at] = up
            hidden_ref[k, :, at] = (gate * jax.nn.sigmoid(gate) * up).astype(bf16)
            return carry

        lax.fori_loop(0, units // 256, gated, 0)

        def down(n, carry):
            at = span(n, wide_tile)
            part_ref[k, :, at] = dot_t(hidden_ref[k], w_ref[at, 2 * units :]).astype(bf16)
            return carry

        lax.fori_loop(0, width // wide_tile, down, 0)

    def backward(h, k):
        rows = r.at(h)

        def gated(n, carry):
            at, up_at = span(n, 256), pl.ds(pl.multiple_of(units + n * 256, 256), 256)
            down_at = pl.ds(pl.multiple_of(2 * units + n * 256, 256), 256)
            grad_hidden = dot(out[k, rows], w_ref[:, down_at])
            gate, up = gu_ref[k, rows, at], gu_ref[k, rows, up_at]
            sigmoid = jax.nn.sigmoid(gate)
            active = gate * sigmoid
            grad_gu_ref[k, rows, at] = (
                grad_hidden * up * (sigmoid * (1.0 + gate * (1.0 - sigmoid)))
            ).astype(bf16)
            grad_gu_ref[k, rows, up_at] = (grad_hidden * active).astype(bf16)
            return carry

        lax.fori_loop(0, units // 256, gated, 0)

        def back(n, carry):
            at = span(n, wide_tile)
            part_ref[k, rows, at] = dot_t(
                grad_gu_ref[k, rows], w_ref[at, : 2 * units]
            ).astype(bf16)
            return carry

        lax.fori_loop(0, width // wide_tile, back, 0)

    first, second = mlp_math(r, res_ref, grad_ref, gain_ref, block_ref, ffn_sum_ref)
    back_first, back_second = back_math(
        s, grad_ref, proj_ref, inv_ref, gain_ref, grad_res_ref, attn_sum_ref
    )
    copies, reused, loaded, blocks = {}, [], [], []
    gate = slice(0, units)

    def half(c):
        return slice(c * units // 2, (c + 1) * units // 2)

    def forward_step(k):
        if not loaded:
            load_w.wait()
        loaded.append(k)
        load_x[k].wait()
        forward(k)
        for h in range(HALVES):
            r.send_q(h, k)

    def backward_step(h, k):
        if not reused:
            links.sent(r.step_q.values())
            reused.append(True)
        r.arrived(h, k)
        backward(h, k)
        s.send_q(h, k)

    def block_p():
        here = block_ref.at[0, :, r.mine]
        copies["p"] = links.send(here, here, {"p": 1 - r.p})

    def block_q():
        copies["p"].wait_recv()
        here = block_ref.at[0, :, r.pair]
        copies["q"] = links.send(here, here, {"q": 1 - r.q})

    def down_grads(c):
        for h in range(HALVES):
            for k in range(na):
                r.arrived(h, k)
        for block in range(na):
            weight_grad(out, hidden_ref, down_grad, block, half(c), half(c))
        copies["d", c] = exchange_b(links, down_grad, down_held, half(c))

    def down_sums(c):
        own = lambda block: down_grad.at[block, b]
        sum_b(copies["d", c], own, down_held, down_sum_ref, half(c))

    def down_owner(c, k):
        copies["z", c, k] = links.send(
            down_sum_ref.at[across(r.a, k), :, half(c)], down_in.at[k - 1, :, half(c)], {"a": across(r.a, k)}
        )

    def gu_grads(block):
        weight_grad(x_ref, grad_gu_ref, gu_grad_ref, block)
        blocks.append(block)
        if len(blocks) == na:
            save_up.start()

    def gate_rows():
        copies["g"] = exchange_b(links, gu_grad_ref, gu_held, gate)

    table = {
        "F": forward_step,
        "B": backward_step,
        "BP": block_p,
        "BQ": block_q,
        "D": down_grads,
        "DS": down_sums,
        "ZD": down_owner,
        "YG": gate_rows,
        "SG": lambda: sum_b(
            copies["g"], lambda block: gu_grad_ref.at[block, b], gu_held, gate_sum_ref, gate
        ),
        "G": gu_grads,
    }
    table.update({"r" + key: step for key, step in r.steps(first, second, 2).items()})
    table.update({"s" + key: step for key, step in s.steps(back_first, back_second, 1).items()})
    load.wait()
    for key, *where in MIDDLE:
        table[key](*where)
    for h in range(HALVES):
        for k in range(na):
            s.arrived(h, k)
    copies["q"].wait_recv()
    for c in range(2):
        for k in range(1, na):
            copies["z", c, k].wait_recv()
    save_up.wait()
    links.finish()


def middle_call(nb, x_all, w_mlp, res_mine, out_grad, proj_mine, inv_mine, width_gain):
    na, rows, width = x_all.shape
    quarter, units = width // 4, w_mlp.shape[1] // 3
    w_rows = width // (na * nb)
    vmem, far = pl.BlockSpec(memory_space=pltpu.VMEM), pl.BlockSpec(memory_space=pl.ANY)
    shape = jax.ShapeDtypeStruct
    outs = (
        shape((1, rows, width), bf16),
        shape((na, rows, width), bf16),
        shape((8, quarter), f32),
        shape((rows, quarter), f32),
        shape((8, quarter), f32),
        shape((na, w_rows, units), bf16),
        shape((na, nb, w_rows, units), bf16),
        shape((na - 1, w_rows, units), bf16),
        shape((na, w_rows, units), bf16),
    )
    copies = 2 * HALVES * (6 * na + 1) + 2 + 3 * nb + 2 * na
    return pl.pallas_call(
        functools.partial(middle_kernel, na, nb),
        out_shape=outs,
        in_specs=[far if i in (0, 1, 3) else vmem for i in range(7)],
        out_specs=tuple(far if i == 6 else vmem for i in range(len(outs))),
        scratch_shapes=[
            pltpu.VMEM((na, rows, width), bf16),
            pltpu.VMEM((na, rows, units), bf16),
            pltpu.VMEM((na, rows, 2 * units), bf16),
            pltpu.VMEM((na, rows, 2 * units), f32),
            pltpu.VMEM((na, rows, width), bf16),
            pltpu.VMEM((na, nb, w_rows, units), bf16),
            pltpu.VMEM((nb - 1, na, w_rows, units), bf16),
            pltpu.VMEM((rows, quarter), f32),
            pltpu.VMEM((nb - 1, na, w_rows, units), bf16),
            pltpu.VMEM((na, rows, width), bf16),
            pltpu.VMEM((width, 3 * units), bf16),
            pltpu.VMEM((na, nb, w_rows, 2 * units), bf16),
        ]
        + reduce_scratch(na, rows, width)
        + reduce_scratch(na, rows, width)
        + [
            pltpu.SemaphoreType.DMA((3 + na,)),
            pltpu.SemaphoreType.DMA((copies,)),
            pltpu.SemaphoreType.DMA((copies,)),
        ],
        compiler_params=pltpu.CompilerParams(
            collective_id=2, has_side_effects=True, vmem_limit_bytes=VMEM_LIMIT
        ),
        name="middle",
    )(x_all, w_mlp, res_mine, out_grad, proj_mine, inv_mine, width_gain)


LAST = (
    ("U1",), ("ZG", 0, 3), ("YG", 1), ("AB", 0), ("AB", 1), ("U2",), ("AB", 2), ("AB", 3),
    ("S1",), ("WO", 1), ("U3",), ("S2",), ("WO", 2), ("S3",), ("ZG", 0, 1), ("ZG", 0, 2), ("WO", 3),
    ("WO", 0), ("OG", 0, 3), ("S4",), ("QB", 3), ("OD", 2), ("QB", 2), ("QB", 0), ("SG", 1), ("rP", 1, 3),
    ("ZG", 1, 2), ("QB", 1), ("ZG", 1, 3), ("rP", 1, 0), ("rP", 0, 0), ("WQ", 1), ("rP", 1, 2),
    ("WQ", 2), ("WQ", 0), ("rP", 0, 2), ("OD", 1), ("rP", 0, 3), ("WQ", 3), ("ZG", 1, 1),
    ("YA",), ("rP", 1, 1), ("rP", 0, 1), ("OG", 0, 1), ("rCL", 1, 3), ("rCR", 0, 3),
    ("rCR", 1, 3), ("OG", 0, 2), ("OD", 3), ("rCL", 0, 3), ("rCR", 0, 2), ("rCR", 1, 2), ("rCL", 1, 2),
    ("rCL", 0, 2), ("OG", 1, 1), ("OG", 1, 2), ("rCR", 0, 1), ("rCL", 1, 1), ("rCR", 1, 1), ("rCL", 0, 1),
    ("SA",), ("ZA", 2), ("OG", 1, 3), ("ZA", 1), ("rSC", 0), ("ZA", 3), ("rSC", 1), ("rX", 0), ("U4",), ("OWNG",),
    ("OA", 2), ("rX", 1), ("U5",), ("OWN",), ("rRQ", 0, 0), ("rRQ", 1, 0), ("OA", 1), ("OA", 3),
)


def last_kernel(na, nb, *refs):
    proj_far, x_far, qkv_ref, stats_ref, gain_ref, cos_ref, sin_ref, w_ref, att_ref = refs[:9]
    grad_ref, attn_sum_ref, ffn_sum_ref, down_sum_far, up_grad_far, down_in_far, gate_ref = refs[9:16]
    out, sums_ref, down_far, gu_far, qkv_out, wout_out = refs[16:22]
    scaled_ref, grad_qkv_ref, part_ref, head_sums, held, stats_a, inner_ref = refs[22:29]
    own_sums, a_sums, b_sums, up_held, up_sum, attn_grad, attn_held, attn_sum = refs[29:37]
    gu_in, attn_in, x_ref, up_own, down_out, gu_out = refs[37:43]
    proj_ref, down_sum_ref, down_in = refs[43:46]
    scratch, (local_sem, send_sem, recv_sem) = refs[46:-3], refs[-3:]
    load_proj = [
        pltpu.make_async_copy(proj_far.at[k], proj_ref.at[k], local_sem.at[4 + k]) for k in range(na)
    ]
    for copy in load_proj:
        copy.start()
    links = Links(send_sem, recv_sem)
    load_gu = pltpu.make_async_copy(
        up_grad_far.at[:, lax.axis_index("b")], up_own, local_sem.at[0]
    )
    load_gu.start()
    load_x = pltpu.make_async_copy(x_far, x_ref, local_sem.at[1])
    load_x.start()
    load_down = [
        pltpu.make_async_copy(down_sum_far, down_sum_ref, local_sem.at[4 + na]),
        pltpu.make_async_copy(down_in_far, down_in, local_sem.at[5 + na]),
    ]
    for copy in load_down:
        copy.start()
    save_down = pltpu.make_async_copy(down_out, down_far, local_sem.at[2])
    save_gu = pltpu.make_async_copy(gu_out, gu_far, local_sem.at[3])
    r = Reduce(na, links, part_ref, out, scratch)
    r.chained(scratch[9])
    a, b, p, q, mine, pair, quarter = (
        r.a, lax.axis_index("b"), r.p, r.q, r.mine, r.pair, r.quarter,
    )
    units = down_sum_ref.shape[2]
    own_sums[...] = jnp.zeros_like(own_sums)
    own_sums[0:1, mine] = jnp.sum(attn_sum_ref[...], axis=0, keepdims=True)
    own_sums[1:2, mine] = jnp.sum(ffn_sum_ref[...], axis=0, keepdims=True)
    held[0] = jnp.zeros_like(held[0])
    head_sums[...] = jnp.zeros_like(head_sums)
    greet(reduce_peers(na) + [{"b": across(b, j)} for j in range(1, nb)])
    copies, stored = {}, []
    whole = slice(0, units)
    attn_columns = slice(0, 4 * HD)
    over_heads = OverHeads(links, na, a, p, q, held, stats_a, inner_ref)

    def sums_pair():
        here = own_sums.at[:, mine]
        copies["u"] = links.send(here, here, {"p": 1 - p})

    def sums_core():
        copies["u"].wait_recv()
        here = own_sums.at[:, pair]
        copies["u"] = links.send(here, here, {"q": 1 - q})

    def sums_far():
        copies["u"].wait_recv()
        copies["u"] = [
            links.send(
                own_sums.at[:, span(across(a, k), quarter)], a_sums.at[k - 1], {"a": across(a, k)}
            )
            for k in range(1, na)
        ]

    def sums_b():
        for copy in copies["u"]:
            copy.wait_recv()
        total = own_sums[:, span(a, quarter)]
        for k in range(1, na):
            total = total + a_sums[k - 1]
        b_sums[0, :, :quarter] = total
        b_sums[0, :, quarter:] = head_sums[...]
        copies["u"] = [
            links.send(b_sums.at[0], b_sums.at[j], {"b": across(b, j)}) for j in range(1, nb)
        ]

    def sums_done():
        for copy in copies["u"]:
            copy.wait_recv()
        total = b_sums[0]
        for j in range(1, nb):
            total = total + b_sums[j]
        sums_ref[...] = total

    def proj_here(k):
        if ("proj", k) not in copies:
            copies["proj", k] = True
            load_proj[k].wait()

    def out_grads(block):
        for k in range(na):
            proj_here(k)
        weight_grad(proj_ref, att_ref, attn_grad, block, slice(3 * HD, 4 * HD))

    def attend_back(k):
        proj_here(k)
        if k % 2:
            lax.fori_loop(k - 1, k + 1, attend_back_block, 0)

    def attend_back_block(k, carry):
        queries, key_rows, values, q_inv, k_inv, q_rot, k_rot, probs = attention(
            k, qkv_ref[k], stats_ref[...], gain_ref, cos_ref, sin_ref
        )
        cos_table, sine_table = cos_ref[...], sin_ref[...]
        grad_att = dot(proj_ref[k], w_ref[:, 3 * HD :]).astype(bf16)
        grad_v = t_dot(probs.astype(bf16), grad_att)
        grad_p = dot_t(grad_att, values)
        delta = jnp.sum(probs * grad_p, axis=1, keepdims=True)
        grad_scores = (probs * (grad_p - delta) * HD ** (-0.5)).astype(bf16)
        grad_q = dot(grad_scores, k_rot)
        grad_k = t_dot(grad_scores, q_rot)
        grad_q = grad_q * cos_table + rotate_back(grad_q * sine_table)
        grad_k = grad_k * cos_table + rotate_back(grad_k * sine_table)
        head_sums[0:1] += jnp.sum(grad_q * queries * q_inv, axis=0, keepdims=True)
        head_sums[1:2] += jnp.sum(grad_k * key_rows * k_inv, axis=0, keepdims=True)
        scaled_q = grad_q * gain_ref[0:1]
        scaled_k = grad_k * gain_ref[1:2]
        scaled_ref[k, :, :HD] = scaled_q
        scaled_ref[k, :, HD:] = scaled_k
        grad_qkv_ref[k, :, 2 * HD :] = grad_v.astype(bf16)
        held[0] += to_row(scaled_q * queries, 2 * k) + to_row(scaled_k * key_rows, 2 * k + 1)
        return carry

    def qkv_back(k):
        for i in range(2):
            at = slice(i * HD, (i + 1) * HD)
            inv = lax.rsqrt(to_column(stats_ref[...] / HQ, 2 * k + i) + epsilon)
            mean = to_column(inner_ref[...] / HQ, 2 * k + i)
            grad = inv * scaled_ref[k, :, at] - qkv_ref[k, :, at] * inv * inv * inv * mean
            grad_qkv_ref[k, :, at] = grad.astype(bf16)

        def part(n, carry):
            at = span(n, 512)
            part_ref[k, :, at] = dot_t(grad_qkv_ref[k], w_ref[at, : 3 * HD]).astype(bf16)
            return carry

        lax.fori_loop(0, part_ref.shape[2] // 512, part, 0)
        for h in range(HALVES):
            r.send_q(h, k)

    def qkv_grads(block):
        if "x" not in copies:
            load_x.wait()
            copies["x"] = True
        weight_grad(x_ref, grad_qkv_ref, attn_grad, block, slice(0, 3 * HD))

    def up_rows(_):
        copies["up"] = exchange_b(links, up_grad_far, up_held, whole)

    def up_sums(_):
        load_gu.wait()
        own = lambda block: up_own.at[block]
        sum_b(copies["up"], own, up_held, up_sum, whole)

    def gu_owner(c, k):
        source = up_sum if c else gate_ref
        copies["g", c, k] = links.send(
            source.at[across(a, k)], gu_in.at[k - 1, c], {"a": across(a, k)}
        )

    def attn_rows():
        copies["at"] = exchange_b(links, attn_grad, attn_held, attn_columns)

    def attn_sums():
        own = lambda block: attn_grad.at[block, b]
        sum_b(copies["at"], own, attn_held, attn_sum, attn_columns)

    def attn_owner(k):
        copies["a", k] = links.send(attn_sum.at[across(a, k)], attn_in.at[k - 1], {"a": across(a, k)})

    def store(target, index, size, value):
        target[:, span(index, size)] = value.astype(f32)

    def store_gu(c, k, value):
        gu_out[:, c, span(across(a, k), units)] = value.astype(f32)
        stored.append((c, k))
        if len(stored) == 2 * na:
            save_gu.start()

    def store_attn(k, values):
        for c in range(3):
            store(qkv_out.at[c], across(a, k), HD, values[:, c * HD : (c + 1) * HD])
        store(wout_out, across(a, k), HD, values[:, 3 * HD :])

    def own_gu():
        store_gu(0, 0, gate_ref[a])
        store_gu(1, 0, up_sum[a])

    def gu_arrived(c, k):
        copies["g", c, k].wait_recv()
        store_gu(c, k, gu_in[k - 1, c])

    def attn_arrived(k):
        copies["a", k].wait_recv()
        store_attn(k, attn_in[k - 1])

    def down_rows(k):
        if "down" not in copies:
            copies["down"] = 0
            for copy in load_down:
                copy.wait()
            store(down_out, a, units, down_sum_ref[a])
        store(down_out, across(a, k), units, down_in[k - 1])
        copies["down"] += 1
        if copies["down"] == na - 1:
            save_down.start()

    def first(at):
        out[0, at, mine] = (grad_ref[at] + r.add_all(at)).astype(bf16)

    table = {
        "U1": sums_pair,
        "U2": sums_core,
        "U3": sums_far,
        "U4": sums_b,
        "U5": sums_done,
        "AB": attend_back,
        "S1": over_heads.to_pair,
        "S2": over_heads.to_core,
        "S3": over_heads.to_all,
        "S4": over_heads.done,
        "WO": out_grads,
        "WQ": qkv_grads,
        "QB": qkv_back,
        "YG": up_rows,
        "SG": up_sums,
        "ZG": gu_owner,
        "YA": attn_rows,
        "SA": attn_sums,
        "ZA": attn_owner,
        "OWNG": own_gu,
        "OWN": lambda: store_attn(0, attn_sum[a]),
        "OD": down_rows,
        "OG": gu_arrived,
        "OA": attn_arrived,
    }
    table.update({"r" + key: step for key, step in r.steps(first, None, 0).items()})
    for key, *where in LAST:
        table[key](*where)
    for h in range(HALVES):
        r.arrived(h, 0)
    save_down.wait()
    save_gu.wait()
    links.finish()


def last_call(nb, *operands):
    na, rows, width = operands[0].shape
    w_rows, units = operands[12].shape[1:]
    quarter = width // 4
    vmem, far = pl.BlockSpec(memory_space=pltpu.VMEM), pl.BlockSpec(memory_space=pl.ANY)
    shape = jax.ShapeDtypeStruct
    outs = (
        shape((1, rows, width), bf16),
        shape((8, quarter + HD), f32),
        shape((w_rows, na * units), f32),
        shape((w_rows, 2, na * units), f32),
        shape((3, w_rows, na * HD), f32),
        shape((w_rows, na * HD), f32),
    )
    copies = HALVES * (6 * na + 1) + 2 + 6 * na + 4 * nb
    return pl.pallas_call(
        functools.partial(last_kernel, na, nb),
        out_shape=outs,
        in_specs=[far if i in (0, 1, 12, 13, 14) else vmem for i in range(16)],
        out_specs=(vmem, vmem, far, far, vmem, vmem),
        scratch_shapes=[
            pltpu.VMEM((na, rows, 2 * HD), f32),
            pltpu.VMEM((na, rows, 3 * HD), bf16),
            pltpu.VMEM((na, rows, width), bf16),
            pltpu.VMEM((8, HD), f32),
            pltpu.VMEM((5, 8, rows), f32),
            pltpu.VMEM((na - 1, 8, rows), f32),
            pltpu.VMEM((8, rows), f32),
            pltpu.VMEM((8, width), f32),
            pltpu.VMEM((na - 1, 8, quarter), f32),
            pltpu.VMEM((nb, 8, quarter + HD), f32),
            pltpu.VMEM((nb - 1, na, w_rows, units), bf16),
            pltpu.VMEM((na, w_rows, units), bf16),
            pltpu.VMEM((na, nb, w_rows, 4 * HD), bf16),
            pltpu.VMEM((nb - 1, na, w_rows, 4 * HD), bf16),
            pltpu.VMEM((na, w_rows, 4 * HD), bf16),
            pltpu.VMEM((na - 1, 2, w_rows, units), bf16),
            pltpu.VMEM((na - 1, w_rows, 4 * HD), bf16),
            pltpu.VMEM((na, rows, width), bf16),
            pltpu.VMEM((na, w_rows, units), bf16),
            pltpu.VMEM((w_rows, na * units), f32),
            pltpu.VMEM((w_rows, 2, na * units), f32),
            pltpu.VMEM((na, rows, width), bf16),
            pltpu.VMEM((na, w_rows, units), bf16),
            pltpu.VMEM((na - 1, w_rows, units), bf16),
        ]
        + reduce_scratch(na, rows, width, True)
        + [
            pltpu.SemaphoreType.DMA((6 + na,)),
            pltpu.SemaphoreType.DMA((copies,)),
            pltpu.SemaphoreType.DMA((copies,)),
        ],
        compiler_params=pltpu.CompilerParams(
            collective_id=4, has_side_effects=True, vmem_limit_bytes=VMEM_LIMIT
        ),
        name="last",
    )(*operands)


def reduce_scratch(na, rows, width, chained=False):
    quarter = width // 4
    slots = [pltpu.VMEM((2, 2, na - 1, rows, quarter), bf16)] if chained else []
    return [
        pltpu.VMEM((na, rows, width // 2), bf16),
        pltpu.VMEM((na, rows, width // 2), bf16),
        pltpu.VMEM((na, rows, quarter), bf16),
        pltpu.VMEM((na - 1, rows, quarter), bf16),
        pltpu.VMEM((na - 1, rows, quarter), bf16),
        pltpu.VMEM((rows, quarter), f32),
        pltpu.VMEM((2, rows, 128), f32),
        pltpu.VMEM((2, rows, 128), f32),
        pltpu.VMEM((HALVES, 4, 8, rows // HALVES), f32),
    ] + slots


ENTER = (
    ("Z", 0), ("W", 3), ("FL", 0, 1), ("FR", 0, 1), ("W", 1), ("GA",), ("CUT", 0), ("FW", 0), ("FT", 0),
    ("CUT", 3), ("FW", 1), ("W", 2), ("CUT", 1), ("M", 0, 1), ("FL", 0, 2), ("FW", 3), ("CUT", 2),
    ("FW", 2), ("FL", 0, 3), ("FR", 0, 2), ("FQ", 0), ("FR", 0, 3), ("M", 0, 3), ("FQ", 2), ("M", 1, 2),
    ("M", 2, 1), ("J", 2), ("FQ", 1), ("FQ", 3), ("J", 0), ("J", 1), ("J", 3), ("GB",), ("S1",),
    ("MR", 1, 0), ("MR", 0, 0), ("S2",), ("S3",), ("M", 2, 3), ("M", 0, 2), ("M", 1, 1), ("S4",), ("E", 1),
    ("E", 2), ("MR", 2, 1), ("MR", 2, 0), ("rP", 1, 1), ("M", 2, 2), ("MR", 1, 2), ("rP", 0, 1), ("E", 3),
    ("E", 0), ("rP", 1, 0), ("rP", 0, 3), ("rP", 1, 3), ("rP", 1, 2), ("rP", 0, 0), ("rCL", 1, 3),
    ("rCL", 1, 2), ("rP", 0, 2), ("rCR", 1, 3), ("rCR", 1, 2), ("rCR", 0, 3), ("rCL", 1, 1), ("rCR", 1, 1),
    ("rCL", 0, 3), ("MR", 0, 1), ("rCR", 0, 2), ("MR", 0, 2), ("MR", 0, 3), ("rCL", 0, 2), ("rSC", 1),
    ("rCL", 0, 1), ("rCR", 0, 1), ("rSQ", 1), ("rSD", 1), ("rZ", 1), ("MR", 1, 1), ("rSC", 0), ("MR", 2, 2),
    ("rFL", 1, 1), ("rFR", 1, 1), ("rSQ", 0), ("rSD", 0), ("rX", 0), ("rX", 1), ("rZ", 0), ("rFR", 1, 2),
    ("rFL", 1, 2), ("rFR", 0, 1), ("rFL", 0, 1), ("M", 1, 3), ("rRQ", 0, 0), ("rFL", 1, 3), ("rFR", 1, 3),
    ("rRQ", 1, 1), ("MR", 2, 3), ("rRQ", 1, 0), ("rRQ", 1, 2), ("rFR", 0, 2), ("rFR", 0, 3), ("rFL", 0, 2),
    ("MR", 1, 3), ("rFL", 0, 3), ("rRQ", 0, 3), ("rRQ", 1, 3), ("rRQ", 0, 1), ("rRQ", 0, 2),
)


def enter_kernel(na, nb, gain_sizes, *refs):
    tok_far, qkv_w_ref, wout_ref, gu_far, down_far, cos_ref, sin_ref, all_gains_ref = refs[:8]
    x_far, w_far, mlp_w_ref, width_gain_ref, head_gain_ref, qkv_far, stats_ref, att_far = refs[8:16]
    out, proj_ref, inv_ref, res_ref = refs[16:20]
    own_gains, gains_ref, piece_ref, part_ref, held, stats_a = refs[20:26]
    x_ref, w_ref, qkv_ref, att_ref = refs[26:30]
    tok_ref, gu_ref, down_ref = refs[30:33]
    scratch, (local_sem, send_sem, recv_sem) = refs[33:-3], refs[-3:]
    load_mlp = [
        pltpu.make_async_copy(gu_far, gu_ref, local_sem.at[10]),
        pltpu.make_async_copy(down_far, down_ref, local_sem.at[11]),
    ]
    for copy in load_mlp:
        copy.start()
    saves = [
        pltpu.make_async_copy(near, there, local_sem.at[5 + i])
        for i, (near, there) in enumerate(
            ((x_ref, x_far), (w_ref, w_far), (qkv_ref, qkv_far), (att_ref, att_far))
        )
    ]
    a, b, p, q = (lax.axis_index(axis) for axis in ("a", "b", "p", "q"))
    rows = wout_ref.shape[0]
    quarter = tok_ref.shape[1]
    load = pltpu.make_async_copy(
        tok_far.at[:, span(2 * q + p, quarter)], tok_ref, local_sem.at[9]
    )
    load.start()
    units = down_ref.shape[1] // na
    own_gains[...] = jnp.zeros_like(own_gains)
    n_d, n_h = gain_sizes
    place = 0
    for i, size in enumerate((n_d, n_d, n_h, n_h)):
        own_gains[i : i + 1, :size] = all_gains_ref[:, place : place + size].astype(f32)
        place += size
    gains_ref[a, b] = own_gains[...]
    greet(
        [{"q": 1 - q}, {"p": 1 - p}]
        + [{"a": across(a, k)} for k in range(1, na)]
        + [{"b": across(b, j)} for j in range(1, nb)]
    )
    load.wait()
    links = Links(send_sem, recv_sem)
    mine, pair = span(2 * q + p, quarter), span(q, 2 * quarter)
    place = span(a * nb + b, rows)
    copies, ends = {}, []
    locals_ = [pltpu.make_async_copy(tok_ref, x_ref.at[0, :, mine], local_sem.at[0])]

    def weight_sources(k):
        block = span(across(a, k), HD)
        sources = [qkv_w_ref.at[c, :, block] for c in range(3)] + [wout_ref.at[:, block]]
        return [(s, w_ref.at[place, c * HD : (c + 1) * HD]) for c, s in enumerate(sources)]

    for c, (source, target) in enumerate(weight_sources(0)):
        locals_.append(pltpu.make_async_copy(source, target, local_sem.at[1 + c]))
    for copy in locals_:
        copy.start()

    def send_gains():
        copies["g"] = [
            links.send(own_gains, gains_ref.at[a, b], {"a": across(a, k)}) for k in range(1, na)
        ]

    def relay_gains():
        for copy in copies["g"]:
            copy.wait_recv()
        at = gains_ref.at[:, b]
        copies["gb"] = [links.send(at, at, {"b": across(b, j)}) for j in range(1, nb)]

    def send_weights(k):
        copies["w", k] = [
            links.send(source, target, {"a": across(a, k)}) for source, target in weight_sources(k)
        ]

    def relay_weights(k):
        if k:
            for copy in copies["w", k]:
                copy.wait_recv()
        else:
            for copy in locals_[1:]:
                copy.wait()
        at = w_ref.at[span(across(a, k) * nb + b, rows), :]
        copies["wb", k] = [links.send(at, at, {"b": across(b, j)}) for j in range(1, nb)]

    line = Line(links, na, lambda k: x_ref.at[k, :, mine], tok_ref)

    def own_tokens(_):
        locals_[0].wait()
        line.to_pair(0).start()

    def pair_tokens(k):
        line.to_pair(k).wait_recv()
        at = x_ref.at[k, :, pair]
        copies["x", k] = links.send(at, at, {"q": 1 - q})

    def cut_weights(k):
        if "cut" not in copies:
            copies["cut"] = True
            for copy in load_mlp:
                copy.wait()
        block = span(across(a, k), units)

        def cut(i, carry):
            at = pl.ds(pl.multiple_of(i * TILE, TILE), TILE)
            cuts = (gu_ref[at, 0, block], gu_ref[at, 1, block], down_ref[at, block])
            for c in range(3):
                if k:
                    piece_ref[k - 1, c, at] = cuts[c]
                else:
                    to = pl.ds(pl.multiple_of((a * nb + b) * rows + i * TILE, TILE), TILE)
                    mlp_w_ref[to, c * units : (c + 1) * units] = cuts[c]
            return carry

        lax.fori_loop(0, rows // TILE, cut, 0)

    def send_piece(c, k):
        target = mlp_w_ref.at[place, c * units : (c + 1) * units]
        copies["m", c, k] = links.send(piece_ref.at[k - 1, c], target, {"a": across(a, k)})

    def relay_piece(c, k):
        if k:
            copies["m", c, k].wait_recv()
        at = mlp_w_ref.at[span(across(a, k) * nb + b, rows), c * units : (c + 1) * units]
        ends.extend(links.send(at, at, {"b": across(b, j)}) for j in range(1, nb))

    arrived, ready = set(), []

    def project(k):
        if not arrived:
            held[0] = jnp.zeros_like(held[0])
            for i in range(na):
                for copy in copies["wb", i]:
                    copy.wait_recv()
        arrived.add(k)
        copies["x", k].wait_recv()

        def chunk(i, carry):
            at = span(i, 128)
            proj = dot(x_ref[k, at], w_ref[:, : 3 * HD])
            qkv_ref[k, at] = proj
            queries, key_rows = proj[:, :HD], proj[:, HD : 2 * HD]
            held[0, :, at] += to_row(queries * queries, 2 * k) + to_row(key_rows * key_rows, 2 * k + 1)
            return carry

        lax.fori_loop(0, x_ref.shape[1] // 128, chunk, 0)

    over_heads = OverHeads(links, na, a, p, q, held, stats_a, stats_ref)

    def all_stats():
        for save in saves[:3]:
            save.start()
        over_heads.done()
        for copy in copies["gb"]:
            copy.wait_recv()
        width_gain_ref[...] = jnp.zeros_like(width_gain_ref)
        head_gain_ref[...] = jnp.zeros_like(head_gain_ref)
        for i in range(2):
            width_gain_ref[i : i + 1] = jnp.concatenate(
                [gains_ref[2 * q + p, j, i : i + 1, :n_d] for j in range(nb)], axis=1
            )
            head_gain_ref[i : i + 1] = jnp.concatenate(
                [gains_ref[a, j, i + 2 : i + 3, :n_h] for j in range(nb)], axis=1
            )

    r = Reduce(na, links, part_ref, out, scratch)
    r.chained(scratch[9])

    def attend(k):
        values, probs = (
            attention(k, qkv_ref[k], stats_ref[...], head_gain_ref, cos_ref, sin_ref)[i] for i in (2, 7)
        )
        attended = dot(probs.astype(bf16), values).astype(bf16)
        att_ref[k] = attended

        def part(n, carry):
            at = span(n, 512)
            part_ref[k, :, at] = dot_t(att_ref[k], w_ref[at, 3 * HD :]).astype(bf16)
            return carry

        lax.fori_loop(0, part_ref.shape[2] // 512, part, 0)
        for h in range(HALVES):
            r.send_q(h, k)

    first, second = attn_math(r, tok_ref, width_gain_ref, proj_ref, inv_ref, res_ref)
    table = {
        "GA": send_gains,
        "GB": relay_gains,
        "W": send_weights,
        "FW": relay_weights,
        "Z": lambda _: line.start(),
        "FL": lambda _, t: line.pass_on(1, t),
        "FR": lambda _, t: line.pass_on(-1, t),
        "FT": own_tokens,
        "FQ": pair_tokens,
        "CUT": cut_weights,
        "M": send_piece,
        "MR": relay_piece,
        "J": project,
        "S1": over_heads.to_pair,
        "S2": over_heads.to_core,
        "S3": over_heads.to_all,
        "S4": all_stats,
        "E": attend,
    }
    table.update({"r" + key: step for key, step in r.steps(first, second, 1, True).items()})
    for key, *where in ENTER:
        table[key](*where)
    saves[3].start()
    for h in range(HALVES):
        for k in range(na):
            r.arrived(h, k)
    for copy in ends:
        copy.wait_recv()
    for save in saves:
        save.wait()
    links.finish()


def enter_call(na, nb, tokens, qkv, w_out, gu, down, cos_table, sine_table, gains):
    rows, width = tokens.shape
    quarter = width // 4
    sizes = (gains[0].shape[0], gains[2].shape[0])
    w_rows, units = down.shape[0], down.shape[1] // na
    lanes = max(128, sizes[0])
    vmem, far = pl.BlockSpec(memory_space=pltpu.VMEM), pl.BlockSpec(memory_space=pl.ANY)
    shape = jax.ShapeDtypeStruct
    full = shape((na, rows, width), bf16)
    outs = [
        full,
        shape((width, 4 * HD), bf16),
        shape((width, 3 * units), bf16),
        shape((8, quarter), f32),
        shape((8, HD), f32),
        shape((na, rows, 3 * HD), f32),
        shape((8, rows), f32),
        shape((na, rows, HD), bf16),
        full,
        shape((rows, quarter), f32),
        shape((rows, 128), f32),
        shape((rows, quarter), f32),
    ]
    copies = 120 + 16 * nb
    return pl.pallas_call(
        functools.partial(enter_kernel, na, nb, sizes),
        out_shape=tuple(outs),
        in_specs=[far if i in (0, 3, 4) else vmem for i in range(8)],
        out_specs=tuple(far if i in (0, 1, 5, 7) else vmem for i in range(len(outs))),
        scratch_shapes=[
            pltpu.VMEM((8, lanes), f32),
            pltpu.VMEM((na, nb, 8, lanes), f32),
            pltpu.VMEM((na - 1, 3, w_rows, units), bf16),
            pltpu.VMEM((na, rows, width), bf16),
            pltpu.VMEM((5, 8, rows), f32),
            pltpu.VMEM((na - 1, 8, rows), f32),
            pltpu.VMEM((na, rows, width), bf16),
            pltpu.VMEM((width, 4 * HD), bf16),
            pltpu.VMEM((na, rows, 3 * HD), f32),
            pltpu.VMEM((na, rows, HD), bf16),
            pltpu.VMEM((rows, quarter), bf16),
            pltpu.VMEM(gu.shape, bf16),
            pltpu.VMEM(down.shape, bf16),
        ]
        + reduce_scratch(na, rows, width, True)
        + [
            pltpu.SemaphoreType.DMA((12,)),
            pltpu.SemaphoreType.DMA((copies,)),
            pltpu.SemaphoreType.DMA((copies,)),
        ],
        compiler_params=pltpu.CompilerParams(
            collective_id=5, has_side_effects=True, vmem_limit_bytes=VMEM_LIMIT
        ),
        name="enter",
    )(tokens, qkv, w_out, gu, down, cos_table, sine_table, jnp.concatenate(gains)[None])


def rope_tables(length, width):
    half_width = width // 2
    inv_freq = rope_base ** (-(jnp.arange(half_width, dtype=f32) * 2.0) / width)
    angles = jnp.arange(length, dtype=f32)[:, None] * inv_freq[None, :]
    cos_table = jnp.concatenate([jnp.cos(angles), jnp.cos(angles)], axis=1)
    sine_table = jnp.concatenate([jnp.sin(angles), jnp.sin(angles)], axis=1)
    return cos_table, sine_table


def on_device(
    tokens,
    qkv_weight,
    out_weight,
    gu_weight,
    down_weight,
    attn_gain,
    ffn_gain,
    q_gain,
    k_gain,
    out_grad,
):
    na, nb = lax.axis_size("a"), lax.axis_size("b")
    a, b = lax.axis_index("a"), lax.axis_index("b")
    share = lax.axis_index("q") * 2 + lax.axis_index("p")
    rows, width = tokens.shape
    quarter = width // 4
    w_rows = out_weight.shape[0]
    units = down_weight.shape[1] // na

    cos_table, sine_table = rope_tables(SEQ_LEN, HD)
    (
        x_all,
        w_attn,
        w_mlp,
        width_gain,
        head_gain,
        qkv,
        stats,
        attended,
        res_all,
        proj_mine,
        inv_mine,
        res_mine,
    ) = enter_call(
        na,
        nb,
        tokens,
        qkv_weight.transpose(1, 0, 2),
        out_weight,
        gu_weight,
        down_weight,
        cos_table,
        sine_table,
        (attn_gain, ffn_gain, q_gain, k_gain),
    )
    n_d, n_h = attn_gain.shape[0], q_gain.shape[0]
    block_rows, grad_proj, ffn_sums, grad_res, attn_sums, down_sum, gu_grad, down_in, gate_sum = middle_call(
        nb, res_all, w_mlp, res_mine, out_grad, proj_mine, inv_mine, width_gain
    )
    grad_rows, sums, down_grad, gu_grad, qkv_grad, out_grad_w = last_call(
        nb,
        grad_proj,
        x_all,
        qkv,
        stats,
        head_gain,
        cos_table,
        sine_table,
        w_attn,
        attended,
        grad_res,
        attn_sums,
        ffn_sums,
        down_sum,
        gu_grad,
        down_in,
        gate_sum,
    )
    width_sums = lax.dynamic_slice_in_dim(sums[:2, :quarter], b * n_d, n_d, 1)
    head_sums = lax.dynamic_slice_in_dim(sums[:2, quarter:], b * n_h, n_h, 1)
    return (
        block_rows[0].astype(f32),
        grad_rows[0].astype(f32),
        qkv_grad.transpose(1, 0, 2),
        out_grad_w,
        gu_grad,
        down_grad,
        width_sums[0],
        width_sums[1],
        head_sums[0],
        head_sums[1],
    )


def solution(mesh):
    dp, tp = mesh.shape["dp"], mesh.shape["tensor"]
    na = HEADS // tp
    fine = Mesh(mesh.devices.reshape(na, dp // na, tp // 2, 2), ("a", "b", "p", "q"))
    dp_axes, tp_axes = ("a", "b"), ("p", "q")
    both = tp_axes + dp_axes
    return jax.shard_map(
        on_device,
        mesh=fine,
        in_specs=(
            P(dp_axes, None),
            P(dp_axes, None, tp_axes),
            P(dp_axes, tp_axes),
            P(dp_axes, None, tp_axes),
            P(dp_axes, tp_axes),
            P(dp_axes),
            P(dp_axes),
            P(both),
            P(both),
            P(dp_axes, None),
        ),
        out_specs=(
            P(dp_axes, None),
            P(dp_axes, None),
            P(dp_axes, None, tp_axes),
            P(dp_axes, tp_axes),
            P(dp_axes, None, tp_axes),
            P(dp_axes, tp_axes),
            P(dp_axes),
            P(dp_axes),
            P(both),
            P(both),
        ),
        check_vma=False,
    )
```

```python
import functools

import jax
import jax.numpy as jnp
from jax import lax
from jax.experimental import pallas as pl
from jax.experimental.pallas import tpu as pltpu
from jax.sharding import Mesh, PartitionSpec as P

HEADS = 16
HD = 128
SEQ_LEN = 256
HQ = 2048

epsilon = 1e-06
rope_base = 500000.0

f32 = jnp.float32
bf16 = jnp.bfloat16
MESH = pl.DeviceIdType.MESH
EXACT = lax.Precision.HIGHEST
VMEM_LIMIT = 63 * 1024 * 1024
TILE = 32
HALVES = 2


def flip(index, bit):
    return index + bit - 2 * bit * ((index // bit) % 2)


def across(index, k):
    bit = 1
    while bit <= k:
        if k & bit:
            index = flip(index, bit)
        bit *= 2
    return index


def exclusive_or(left, right, count):
    total, bit = 0, 1
    while bit < count:
        total = total + bit * ((left // bit + right // bit) % 2)
        bit *= 2
    return total


def pick(operand, index, axis):
    return lax.dynamic_index_in_dim(operand, index, axis, keepdims=False)


def span(index, size):
    return pl.ds(pl.multiple_of(index * size, size), size)


class Links:
    def __init__(self, send_sem, recv_sem):
        self.send_sem, self.recv_sem, self.count = send_sem, recv_sem, 0
        self.copies, self.lines = [], []

    def send(self, source, target, device):
        copy = self.copy(self.count, source, target, device)
        copy.start()
        self.count += 1
        self.copies.append(copy)
        return copy

    def reserve(self, number):
        self.count += number
        return self.count - number

    def copy(self, index, source, target, device):
        return pltpu.make_async_remote_copy(
            src_ref=source,
            dst_ref=target,
            send_sem=self.send_sem.at[index],
            recv_sem=self.recv_sem.at[index],
            device_id=device,
            device_id_type=MESH,
        )

    def sent(self, copies):
        done = [id(copy) for copy in copies]
        for copy in self.copies:
            if id(copy) in done:
                copy.wait_send()
        self.copies = [copy for copy in self.copies if id(copy) not in done]

    def finish(self):
        for copy in self.copies:
            copy.wait_send()
        for line in self.lines:
            line.finish()


def greet(peers):
    barrier = pltpu.get_barrier_semaphore()
    for peer in peers:
        pl.semaphore_signal(barrier, inc=1, device_id=peer, device_id_type=MESH)
    pl.semaphore_wait(barrier, len(peers))


def fold(block):
    total = block[:, :128]
    for i in range(1, block.shape[1] // 128):
        total = total + block[:, i * 128 : (i + 1) * 128]
    return total


def wide(column, width):
    return jnp.concatenate([column] * (width // 128), axis=1)


def row_mask(row):
    return (lax.broadcasted_iota(jnp.int32, (8, 128), 0) == row).astype(f32)


def to_row(block, row):
    return lax.dot_general(
        row_mask(row), block, (((1,), (1,)), ((), ())), precision=EXACT, preferred_element_type=f32
    )


def to_column(stats, row):
    return lax.dot_general(
        stats, row_mask(row), (((0,), (0,)), ((), ())), precision=EXACT, preferred_element_type=f32
    )


def dot(left, right):
    return jnp.dot(left, right, preferred_element_type=f32)


def dot_t(left, right):
    return lax.dot_general(left, right, (((1,), (1,)), ((), ())), preferred_element_type=f32)


def t_dot(left, right):
    return lax.dot_general(left, right, (((0,), (0,)), ((), ())), preferred_element_type=f32)


def rotate(operand):
    half = HD // 2
    return jnp.concatenate([-operand[:, half:], operand[:, :half]], axis=1)


def rotate_back(operand):
    half = HD // 2
    return jnp.concatenate([operand[:, half:], -operand[:, :half]], axis=1)


def attention(k, qkv, stats, gain_ref, cos_ref, sin_ref):
    stats = stats / HQ
    q_inv = lax.rsqrt(to_column(stats, 2 * k) + epsilon)
    k_inv = lax.rsqrt(to_column(stats, 2 * k + 1) + epsilon)
    queries, key_rows = qkv[:, :HD], qkv[:, HD : 2 * HD]
    values = qkv[:, 2 * HD :].astype(bf16)
    cos_table, sine_table = cos_ref[...], sin_ref[...]
    q_normed = queries * q_inv * gain_ref[0:1]
    k_normed = key_rows * k_inv * gain_ref[1:2]
    q_rot = (q_normed * cos_table + rotate(q_normed) * sine_table).astype(bf16)
    k_rot = (k_normed * cos_table + rotate(k_normed) * sine_table).astype(bf16)
    scores = dot_t(q_rot, k_rot) * HD ** (-0.5)
    ahead = lax.broadcasted_iota(jnp.int32, scores.shape, 1) > lax.broadcasted_iota(
        jnp.int32, scores.shape, 0
    )
    scores = jnp.where(ahead, -1e30, scores)
    shifted = jnp.exp(scores - jnp.max(scores, axis=1, keepdims=True))
    probs = shifted / jnp.sum(shifted, axis=1, keepdims=True)
    return queries, key_rows, values, q_inv, k_inv, q_rot, k_rot, probs


def weight_grad(left, right, out, block, columns=None, take=slice(None)):
    na, nb, rows = left.shape[0], out.shape[1], out.shape[2]
    columns = columns or slice(0, right.shape[2])
    size = max(rows, 256)


    def chunk(i, carry):
        at = span(block * (nb * rows // size) + i, size)
        total = t_dot(left[0, :, at], right[0, :, take])
        for k in range(1, na):
            total = total + t_dot(left[k, :, at], right[k, :, take])
        for j in range(size // rows):
            part = total[j * rows : (j + 1) * rows].astype(bf16)
            out[block, i * (size // rows) + j, :, columns] = part
        return carry

    lax.fori_loop(0, nb * rows // size, chunk, 0)


def exchange_b(links, grad, held, columns):
    b = lax.axis_index("b")
    put = columns if held.shape[3] == grad.shape[3] or columns.stop <= held.shape[3] else slice(None)
    return [
        links.send(
            grad.at[:, across(b, j), :, columns], held.at[j - 1, :, :, put], {"b": across(b, j)}
        )
        for j in range(1, held.shape[0] + 1)
    ]


def sum_b(copies, own, held, out, columns):
    for copy in copies:
        copy.wait_recv()

    def add(block, carry):
        total = own(block)[:, columns].astype(f32)
        for j in range(held.shape[0]):
            total = total + held[j, block, :, columns].astype(f32)
        out[block, :, columns] = total.astype(bf16)
        return carry

    lax.fori_loop(0, held.shape[1], add, 0)


class Line:
    def __init__(self, links, na, block, own):
        self.links, self.na, self.block, self.own = links, na, block, own
        self.a, self.p = lax.axis_index("a"), lax.axis_index("p")
        self.hop_base = {1: links.reserve(na - 1), -1: links.reserve(na - 1)}
        self.pass_base = links.reserve(na)
        links.lines.append(self)

    def hop(self, way, t):
        a, na = self.a, self.na
        first = a - way * (t - 1)
        source = self.own if t == 1 else self.block(exclusive_or(first, a, na))
        target = self.block(exclusive_or(first, a + way, na))
        return self.links.copy(self.hop_base[way] + t - 1, source, target, {"a": (a + way) % na})

    def sends(self, way, t):
        first, last = self.a - way * (t - 1), self.a + way
        return (first >= 0) & (first < self.na) & (last >= 0) & (last < self.na)

    def to_pair(self, k, source=None):
        at = self.block(k)
        return self.links.copy(self.pass_base + k, at if source is None else source, at, {"p": 1 - self.p})

    def start(self):
        for way in (1, -1):

            @pl.when(self.sends(way, 1))
            def _(way=way):
                self.hop(way, 1).start()

    def pass_on(self, way, t):
        came = self.a - way * t

        @pl.when((came >= 0) & (came < self.na))
        def _():
            self.hop(way, t).wait_recv()
            self.to_pair(exclusive_or(came, self.a, self.na)).start()

        if t < self.na - 1:

            @pl.when(self.sends(way, t + 1))
            def _():
                self.hop(way, t + 1).start()

    def finish(self):
        for way in (1, -1):
            for t in range(1, self.na):

                @pl.when(self.sends(way, t))
                def _(way=way, t=t):
                    self.hop(way, t).wait_send()

        for k in range(self.na):
            self.to_pair(k).wait_send()


class Reduce:
    def __init__(self, na, links, part, out, scratch):
        self.na, self.links, self.part, self.out = na, links, part, out
        self.from_q, self.half_sum, self.from_p, self.to_a, self.from_a = scratch[:5]
        self.total, self.parts, self.cols, self.stat = scratch[5:9]
        self.a, self.p, self.q = (lax.axis_index(axis) for axis in ("a", "p", "q"))
        self.rows, self.width = out.shape[1:]
        self.quarter, self.half = self.width // 4, self.width // 2
        self.count = self.rows // HALVES
        self.mine, self.pair = span(2 * self.q + self.p, self.quarter), span(self.q, self.half)
        self.lead = list(range(2, na)) + [1, 0]
        self.step_q, self.step_p, self.step_a = {}, {}, {}
        self.spread_a, self.spread_p, self.spread_q, self.stats = {}, {}, {}, {}
        self.here, self.slots = set(), None

    def at(self, h):
        return slice(h * self.count, (h + 1) * self.count)

    def each(self, h, body):
        def step(i, carry):
            body(pl.ds(pl.multiple_of(h * self.count + i * TILE, TILE), TILE))
            return carry

        lax.fori_loop(0, self.count // TILE, step, 0)

    def send_q(self, h, k):
        at, q = self.at(h), self.q
        source = self.part.at[k, at, span(1 - q, self.half)]
        self.step_q[h, k] = self.links.send(source, self.from_q.at[k, at], {"q": 1 - q})

    def send_p(self, h, k):
        self.step_q[h, k].wait_recv()

        def add(at):
            own = self.part[k, at, span(self.q, self.half)].astype(f32)
            self.half_sum[k, at] = (own + self.from_q[k, at].astype(f32)).astype(bf16)

        self.each(h, add)
        at, p = self.at(h), self.p
        source = self.half_sum.at[k, at, span(1 - p, self.quarter)]
        self.step_p[h, k] = self.links.send(source, self.from_p.at[k, at], {"p": 1 - p})

    def send_a(self, h, k):
        if not k:
            return
        self.step_p[h, k].wait_recv()

        def add(at):
            own = self.half_sum[k, at, span(self.p, self.quarter)].astype(f32)
            self.to_a[k - 1, at] = (own + self.from_p[k, at].astype(f32)).astype(bf16)

        self.each(h, add)
        at = self.at(h)
        self.step_a[h, k] = self.links.send(
            self.to_a.at[k - 1, at], self.from_a.at[k - 1, at], {"a": across(self.a, k)}
        )

    def add_all(self, at):
        if self.slots is not None:
            return self.total[at]
        own = self.half_sum[0, at, span(self.p, self.quarter)].astype(f32)
        own = own + self.from_p[0, at].astype(f32)
        for k in range(1, self.na):
            own = own + self.from_a[k - 1, at].astype(f32)
        return own

    def scattered(self, h, first, number):
        if self.slots is not None:
            self.gather_sums(h)
        else:
            self.step_p[h, 0].wait_recv()
            for k in range(1, self.na):
                self.step_a[h, k].wait_recv()
        self.each(h, first)
        if number:
            at = self.at(h)
            stats = to_row(self.parts[0, at], 0)
            if number == 2:
                stats = stats + to_row(self.parts[1, at], 1)
            stat = self.stat
            stat[h, 0] = stats
            self.stats[h] = self.links.send(stat.at[h, 0], stat.at[h, 1], {"p": 1 - self.p})

    def stats_q(self, h):
        stat = self.stat
        self.stats[h].wait_recv()
        stat[h, 2] = stat[h, 0] + stat[h, 1]
        self.stats[h] = self.links.send(stat.at[h, 2], stat.at[h, 3], {"q": 1 - self.q})

    def stats_done(self, h, number):
        stat = self.stat
        self.stats[h].wait_recv()
        stats = (stat[h, 2] + stat[h, 3]) / self.width
        for i in range(number):
            self.cols[i, self.at(h)] = to_column(stats, i)

    def spread(self, h, blocks):
        here = self.out.at[0, self.at(h), self.mine]
        for k in blocks:
            if k:
                target = self.out.at[k, self.at(h), self.mine]
                self.spread_a[h, k] = self.links.send(here, target, {"a": across(self.a, k)})
        self.spread_p[h, 0] = self.links.send(here, here, {"p": 1 - self.p})

    def relay_p(self, h, k):
        if not k:
            return
        self.spread_a[h, k].wait_recv()
        here = self.out.at[k, self.at(h), self.mine]
        self.spread_p[h, k] = self.links.send(here, here, {"p": 1 - self.p})

    def relay_q(self, h, k):
        self.spread_p[h, k].wait_recv()
        here = self.out.at[k, self.at(h), self.pair]
        self.spread_q[h, k] = self.links.send(here, here, {"q": 1 - self.q})

    def arrived(self, h, k):
        if (h, k) not in self.here:
            self.here.add((h, k))
            self.spread_q[h, k].wait_recv()

    def chained(self, slots):
        self.slots = slots
        na = self.na
        self.base_p = [self.links.reserve(na) for _ in range(HALVES)]
        self.base_c = [{w: self.links.reserve(na - 1) for w in (1, -1)} for _ in range(HALVES)]
        self.links.lines.append(self)

    def copy_p(self, h, k):
        at = self.at(h)
        source = self.half_sum.at[k, at, span(1 - self.p, self.quarter)]
        return self.links.copy(self.base_p[h] + k, source, self.from_p.at[k, at], {"p": 1 - self.p})

    def copy_c(self, h, way, t):
        at, side = self.at(h), 0 if way == 1 else 1
        return self.links.copy(
            self.base_c[h][way] + t - 1,
            self.slots.at[0, side, t - 1, at],
            self.slots.at[1, side, t - 1, at],
            {"a": (self.a + way) % self.na},
        )

    def inside(self, index):
        return (index >= 0) & (index < self.na)

    def send_p_chained(self, h, k):
        self.step_q[h, k].wait_recv()

        def add(at):
            own = self.part[k, at, span(self.q, self.half)].astype(f32)
            self.half_sum[k, at] = (own + self.from_q[k, at].astype(f32)).astype(bf16)

        self.each(h, add)
        self.copy_p(h, k).start()

    def pass_sums(self, h, way, t):
        side = 0 if way == 1 else 1

        @pl.when(self.inside(self.a + way * t))
        def _():
            k = exclusive_or(self.a, self.a + way * t, self.na)
            self.copy_p(h, k).wait_recv()

            def add(at):
                own = self.half_sum[k, at, span(self.p, self.quarter)].astype(f32)
                self.slots[0, side, t - 1, at] = (own + self.from_p[k, at].astype(f32)).astype(bf16)

            self.each(h, add)
            if t < self.na - 1:

                @pl.when(self.inside(self.a - way))
                def _():
                    self.copy_c(h, way, t + 1).wait_recv()

                    def more(at):
                        own = self.slots[0, side, t - 1, at].astype(f32)
                        came = self.slots[1, side, t, at].astype(f32)
                        self.slots[0, side, t - 1, at] = (own + came).astype(bf16)

                    self.each(h, more)

            self.copy_c(h, way, t).start()

    def gather_sums(self, h):
        self.copy_p(h, 0).wait_recv()

        def own(at):
            here = self.half_sum[0, at, span(self.p, self.quarter)].astype(f32)
            self.total[at] = here + self.from_p[0, at].astype(f32)

        self.each(h, own)
        for side, way in enumerate((1, -1)):

            @pl.when(self.inside(self.a - way))
            def _(side=side, way=way):
                self.copy_c(h, way, 1).wait_recv()

                def more(at):
                    self.total[at] += self.slots[1, side, 0, at].astype(f32)

                self.each(h, more)

    def finish(self):
        for h in range(HALVES):
            for k in range(self.na):
                self.copy_p(h, k).wait_send()
            for way in (1, -1):
                for t in range(1, self.na):

                    @pl.when(self.inside(self.a + way * t))
                    def _(h=h, way=way, t=t):
                        self.copy_c(h, way, t).wait_send()

    def steps(self, first, second, number, chain=False):
        def normed(h):
            self.stats_done(h, number)
            self.each(h, second)

        def spread_own(h):
            here = self.out.at[0, self.at(h), self.mine]
            self.spread_p[h, 0] = self.links.send(here, here, {"p": 1 - self.p})

        def spread_far(h, k):
            here = self.out.at[0, self.at(h), self.mine]
            target = self.out.at[k, self.at(h), self.mine]
            self.spread_a[h, k] = self.links.send(here, target, {"a": across(self.a, k)})

        table = {
            "P": self.send_p,
            "A": self.send_a,
            "SC": lambda h: self.scattered(h, first, number),
            "SQ": self.stats_q,
            "SD": normed,
            "X": spread_own,
            "Z": spread_far,
            "RP": self.relay_p,
            "RQ": self.relay_q,
        }
        if self.slots is not None:
            table.update(
                P=self.send_p_chained,
                CR=lambda h, t: self.pass_sums(h, 1, t),
                CL=lambda h, t: self.pass_sums(h, -1, t),
            )
        if chain:
            lines = [
                Line(
                    self.links,
                    self.na,
                    lambda k, h=h: self.out.at[k, self.at(h), self.mine],
                    self.out.at[0, self.at(h), self.mine],
                )
                for h in range(HALVES)
            ]

            def pair_arrived(h, k):
                self.spread_p[h, k] = lines[h].to_pair(k)
                self.relay_q(h, k)

            table.update(
                X=lambda h: lines[h].to_pair(0).start(),
                Z=lambda h: lines[h].start(),
                FL=lambda h, t: lines[h].pass_on(1, t),
                FR=lambda h, t: lines[h].pass_on(-1, t),
                RQ=pair_arrived,
            )
        return table


class OverHeads:
    def __init__(self, links, na, a, p, q, held, from_a, out_ref):
        self.links, self.na, self.a, self.p, self.q = links, na, a, p, q
        self.held, self.from_a, self.out_ref = held, from_a, out_ref

    def to_pair(self):
        self.copy = self.links.send(self.held.at[0], self.held.at[1], {"p": 1 - self.p})

    def to_core(self):
        held = self.held
        self.copy.wait_recv()
        held[2] = held[0] + held[1]
        self.copy = self.links.send(held.at[2], held.at[3], {"q": 1 - self.q})

    def to_all(self):
        held = self.held
        self.copy.wait_recv()
        held[4] = held[2] + held[3]
        self.copies = [
            self.links.send(held.at[4], self.from_a.at[k - 1], {"a": across(self.a, k)})
            for k in range(1, self.na)
        ]

    def done(self):
        for copy in self.copies:
            copy.wait_recv()
        for k in range(self.na):
            for i in range(2):
                at = 2 * k + i
                total = self.held[4, at : at + 1]
                for j in range(1, self.na):
                    other = 2 * (k ^ j) + i
                    total = total + self.from_a[j - 1, other : other + 1]
                self.out_ref[at : at + 1] = total


def reduce_peers(na):
    a, p, q = lax.axis_index("a"), lax.axis_index("p"), lax.axis_index("q")
    return [{"q": 1 - q}, {"p": 1 - p}] + [{"a": across(a, k)} for k in range(1, na)]


def attn_math(r, tok_ref, gain_ref, proj_ref, inv_ref, res_ref):
    def first(at):
        own = r.add_all(at)
        proj_ref[at] = own
        r.parts[0, at] = fold(own * own)

    def second(at):
        own = proj_ref[at]
        inv = lax.rsqrt(r.cols[0, at] + epsilon)
        inv_ref[at] = inv
        residual = tok_ref[at].astype(f32) + own * wide(inv, r.quarter) * gain_ref[0:1]
        res_ref[at] = residual
        r.out[0, at, r.mine] = residual.astype(bf16)

    return first, second


def mlp_math(r, res_ref, grad_ref, gain_ref, block_ref, sum_ref):
    def first(at):
        own = r.add_all(at)
        r.total[at] = own
        r.parts[0, at] = fold(own * own)
        r.parts[1, at] = fold(grad_ref[at] * gain_ref[1:2] * own)

    def second(at):
        own = r.total[at]
        inv = wide(lax.rsqrt(r.cols[0, at] + epsilon), r.quarter)
        upstream = grad_ref[at]
        scaled = upstream * gain_ref[1:2]
        normed = own * inv
        block_ref[0, at, r.mine] = (res_ref[at] + normed * gain_ref[1:2]).astype(bf16)
        gains = upstream * normed
        sum_ref[...] += jnp.sum(gains.reshape(TILE // 8, 8, r.quarter), axis=0)
        grad = inv * scaled - own * inv * inv * inv * wide(r.cols[1, at], r.quarter)
        r.out[0, at, r.mine] = grad.astype(bf16)

    return first, second


def back_math(r, grad_ref, proj_ref, inv_ref, gain_ref, res_ref, sum_ref):
    def first(at):
        grad = grad_ref[at] + r.add_all(at)
        res_ref[at] = grad
        r.parts[0, at] = fold(grad * gain_ref[0:1] * proj_ref[at])

    def second(at):
        own = proj_ref[at]
        inv = wide(inv_ref[at], r.quarter)
        upstream = res_ref[at]
        gains = upstream * own * inv
        sum_ref[...] += jnp.sum(gains.reshape(TILE // 8, 8, r.quarter), axis=0)
        grad = inv * (upstream * gain_ref[0:1])
        grad = grad - own * inv * inv * inv * wide(r.cols[0, at], r.quarter)
        r.out[0, at, r.mine] = grad.astype(bf16)

    return first, second


MIDDLE = (
    ("F", 2), ("F", 3), ("rP", 0, 2), ("F", 1), ("rP", 0, 3), ("rA", 0, 2), ("rP", 0, 1), ("rP", 1, 3),
    ("F", 0), ("rP", 1, 2), ("rA", 0, 3), ("rP", 1, 1), ("rA", 0, 1), ("rP", 0, 0), ("rA", 1, 3),
    ("rA", 1, 1), ("rA", 1, 2), ("rSC", 0), ("rP", 1, 0), ("rSQ", 0), ("rSD", 0), ("rZ", 0, 1), ("rX", 0),
    ("rZ", 0, 3), ("rSC", 1), ("rRP", 0, 1), ("rRQ", 0, 0), ("rSQ", 1), ("rZ", 0, 2), ("rSD", 1),
    ("rRP", 0, 3), ("rX", 1), ("rZ", 1, 1), ("rZ", 1, 2), ("rRP", 0, 2), ("rRQ", 0, 1), ("rRQ", 0, 3),
    ("rRP", 1, 1), ("B", 0, 3), ("rZ", 1, 3), ("rRP", 1, 2), ("rRQ", 1, 0), ("B", 0, 1), ("rRQ", 0, 2),
    ("sP", 0, 3), ("B", 0, 0), ("B", 0, 2), ("rRP", 1, 3), ("rRQ", 1, 2), ("sA", 0, 3), ("sP", 0, 2),
    ("B", 1, 2), ("sP", 0, 1), ("rRQ", 1, 1), ("rRQ", 1, 3), ("sA", 0, 2), ("sP", 1, 2), ("D", 0),
    ("sA", 0, 1), ("B", 1, 3), ("sA", 1, 2), ("sP", 1, 3), ("B", 1, 0), ("sP", 0, 0), ("D", 1),
    ("sA", 1, 3), ("sP", 1, 0), ("B", 1, 1), ("sSC", 0), ("sP", 1, 1), ("DS", 0), ("ZD", 0, 2), ("sSQ", 0),
    ("G", 0), ("sSD", 0), ("BP",), ("sA", 1, 1), ("G", 2), ("sZ", 0, 3), ("G", 3), ("sZ", 0, 2), ("sSC", 1),
    ("G", 1), ("YG",), ("sSQ", 1), ("sRP", 0, 3), ("sSD", 1), ("sZ", 1, 3), ("DS", 1), ("sZ", 1, 1),
    ("sZ", 0, 1), ("BQ",), ("sX", 0), ("ZD", 1, 3), ("sRP", 1, 1), ("sX", 1), ("sRQ", 1, 1), ("sZ", 1, 2),
    ("sRP", 0, 2), ("sRP", 0, 1), ("ZD", 0, 1), ("ZD", 1, 1), ("sRP", 1, 2), ("sRP", 1, 3), ("ZD", 1, 2),
    ("sRQ", 0, 0), ("sRQ", 0, 3), ("ZD", 0, 3), ("sRQ", 1, 0), ("sRQ", 1, 2), ("sRQ", 0, 2), ("sRQ", 0, 1),
    ("sRQ", 1, 3), ("SG",),
)


def middle_kernel(na, nb, *refs):
    x_far, w_far, res_ref, grad_far, proj_ref, inv_ref, gain_ref = refs[:7]
    block_ref, back_out, ffn_sum_ref, grad_res_ref, attn_sum_ref, down_sum_ref, up_grad_far = refs[7:14]
    down_in, gate_sum_ref = refs[14:16]
    out, hidden_ref, grad_gu_ref, gu_ref, part_ref, down_grad, down_held, grad_ref, gu_held = refs[16:25]
    x_ref, w_ref, gu_grad_ref = refs[25:28]
    scratch, (local_sem, send_sem, recv_sem) = refs[28:-3], refs[-3:]
    share = 2 * lax.axis_index("q") + lax.axis_index("p")
    load = pltpu.make_async_copy(
        grad_far.at[:, span(share, grad_ref.shape[1])], grad_ref, local_sem.at[0]
    )
    load.start()
    load_w = pltpu.make_async_copy(w_far, w_ref, local_sem.at[1])
    load_w.start()
    load_x = {
        k: pltpu.make_async_copy(x_far.at[k], x_ref.at[k], local_sem.at[2 + k])
        for k in list(range(2, na)) + [1, 0]
    }
    for copy in load_x.values():
        copy.start()
    units = hidden_ref.shape[2]
    width = x_ref.shape[2]
    save_up = pltpu.make_async_copy(
        gu_grad_ref.at[:, :, :, units:], up_grad_far, local_sem.at[2 + na]
    )
    b = lax.axis_index("b")
    greet(reduce_peers(na) + [{"b": across(b, j)} for j in range(1, nb)])
    links = Links(send_sem, recv_sem)
    r = Reduce(na, links, part_ref, out, scratch[:9])
    s = Reduce(na, links, part_ref, back_out, scratch[9:])
    ffn_sum_ref[...] = jnp.zeros_like(ffn_sum_ref)
    attn_sum_ref[...] = jnp.zeros_like(attn_sum_ref)
    wide_tile = 512

    def forward(k):
        def gated(n, carry):
            at, up_at = span(n, 256), pl.ds(pl.multiple_of(units + n * 256, 256), 256)
            gate = dot(x_ref[k], w_ref[:, at])
            up = dot(x_ref[k], w_ref[:, up_at])
            gu_ref[k, :, at] = gate
            gu_ref[k, :, up_at] = up
            hidden_ref[k, :, at] = (gate * jax.nn.sigmoid(gate) * up).astype(bf16)
            return carry

        lax.fori_loop(0, units // 256, gated, 0)

        def down(n, carry):
            at = span(n, wide_tile)
            part_ref[k, :, at] = dot_t(hidden_ref[k], w_ref[at, 2 * units :]).astype(bf16)
            return carry

        lax.fori_loop(0, width // wide_tile, down, 0)

    def backward(h, k):
        rows = r.at(h)

        def gated(n, carry):
            at, up_at = span(n, 256), pl.ds(pl.multiple_of(units + n * 256, 256), 256)
            down_at = pl.ds(pl.multiple_of(2 * units + n * 256, 256), 256)
            grad_hidden = dot(out[k, rows], w_ref[:, down_at])
            gate, up = gu_ref[k, rows, at], gu_ref[k, rows, up_at]
            sigmoid = jax.nn.sigmoid(gate)
            active = gate * sigmoid
            grad_gu_ref[k, rows, at] = (
                grad_hidden * up * (sigmoid * (1.0 + gate * (1.0 - sigmoid)))
            ).astype(bf16)
            grad_gu_ref[k, rows, up_at] = (grad_hidden * active).astype(bf16)
            return carry

        lax.fori_loop(0, units // 256, gated, 0)

        def back(n, carry):
            at = span(n, wide_tile)
            part_ref[k, rows, at] = dot_t(
                grad_gu_ref[k, rows], w_ref[at, : 2 * units]
            ).astype(bf16)
            return carry

        lax.fori_loop(0, width // wide_tile, back, 0)

    first, second = mlp_math(r, res_ref, grad_ref, gain_ref, block_ref, ffn_sum_ref)
    back_first, back_second = back_math(
        s, grad_ref, proj_ref, inv_ref, gain_ref, grad_res_ref, attn_sum_ref
    )
    copies, reused, loaded, blocks = {}, [], [], []
    gate = slice(0, units)

    def half(c):
        return slice(c * units // 2, (c + 1) * units // 2)

    def forward_step(k):
        if not loaded:
            load_w.wait()
        loaded.append(k)
        load_x[k].wait()
        forward(k)
        for h in range(HALVES):
            r.send_q(h, k)

    def backward_step(h, k):
        if not reused:
            links.sent(r.step_q.values())
            reused.append(True)
        r.arrived(h, k)
        backward(h, k)
        s.send_q(h, k)

    def block_p():
        here = block_ref.at[0, :, r.mine]
        copies["p"] = links.send(here, here, {"p": 1 - r.p})

    def block_q():
        copies["p"].wait_recv()
        here = block_ref.at[0, :, r.pair]
        copies["q"] = links.send(here, here, {"q": 1 - r.q})

    def down_grads(c):
        for h in range(HALVES):
            for k in range(na):
                r.arrived(h, k)
        for block in range(na):
            weight_grad(out, hidden_ref, down_grad, block, half(c), half(c))
        copies["d", c] = exchange_b(links, down_grad, down_held, half(c))

    def down_sums(c):
        own = lambda block: down_grad.at[block, b]
        sum_b(copies["d", c], own, down_held, down_sum_ref, half(c))

    def down_owner(c, k):
        copies["z", c, k] = links.send(
            down_sum_ref.at[across(r.a, k), :, half(c)], down_in.at[k - 1, :, half(c)], {"a": across(r.a, k)}
        )

    def gu_grads(block):
        weight_grad(x_ref, grad_gu_ref, gu_grad_ref, block)
        blocks.append(block)
        if len(blocks) == na:
            save_up.start()

    def gate_rows():
        copies["g"] = exchange_b(links, gu_grad_ref, gu_held, gate)

    table = {
        "F": forward_step,
        "B": backward_step,
        "BP": block_p,
        "BQ": block_q,
        "D": down_grads,
        "DS": down_sums,
        "ZD": down_owner,
        "YG": gate_rows,
        "SG": lambda: sum_b(
            copies["g"], lambda block: gu_grad_ref.at[block, b], gu_held, gate_sum_ref, gate
        ),
        "G": gu_grads,
    }
    table.update({"r" + key: step for key, step in r.steps(first, second, 2).items()})
    table.update({"s" + key: step for key, step in s.steps(back_first, back_second, 1).items()})
    load.wait()
    for key, *where in MIDDLE:
        table[key](*where)
    for h in range(HALVES):
        for k in range(na):
            s.arrived(h, k)
    copies["q"].wait_recv()
    for c in range(2):
        for k in range(1, na):
            copies["z", c, k].wait_recv()
    save_up.wait()
    links.finish()


def middle_call(nb, x_all, w_mlp, res_mine, out_grad, proj_mine, inv_mine, width_gain):
    na, rows, width = x_all.shape
    quarter, units = width // 4, w_mlp.shape[1] // 3
    w_rows = width // (na * nb)
    vmem, far = pl.BlockSpec(memory_space=pltpu.VMEM), pl.BlockSpec(memory_space=pl.ANY)
    shape = jax.ShapeDtypeStruct
    outs = (
        shape((1, rows, width), bf16),
        shape((na, rows, width), bf16),
        shape((8, quarter), f32),
        shape((rows, quarter), f32),
        shape((8, quarter), f32),
        shape((na, w_rows, units), bf16),
        shape((na, nb, w_rows, units), bf16),
        shape((na - 1, w_rows, units), bf16),
        shape((na, w_rows, units), bf16),
    )
    copies = 2 * HALVES * (6 * na + 1) + 2 + 3 * nb + 2 * na
    return pl.pallas_call(
        functools.partial(middle_kernel, na, nb),
        out_shape=outs,
        in_specs=[far if i in (0, 1, 3) else vmem for i in range(7)],
        out_specs=tuple(far if i == 6 else vmem for i in range(len(outs))),
        scratch_shapes=[
            pltpu.VMEM((na, rows, width), bf16),
            pltpu.VMEM((na, rows, units), bf16),
            pltpu.VMEM((na, rows, 2 * units), bf16),
            pltpu.VMEM((na, rows, 2 * units), f32),
            pltpu.VMEM((na, rows, width), bf16),
            pltpu.VMEM((na, nb, w_rows, units), bf16),
            pltpu.VMEM((nb - 1, na, w_rows, units), bf16),
            pltpu.VMEM((rows, quarter), f32),
            pltpu.VMEM((nb - 1, na, w_rows, units), bf16),
            pltpu.VMEM((na, rows, width), bf16),
            pltpu.VMEM((width, 3 * units), bf16),
            pltpu.VMEM((na, nb, w_rows, 2 * units), bf16),
        ]
        + reduce_scratch(na, rows, width)
        + reduce_scratch(na, rows, width)
        + [
            pltpu.SemaphoreType.DMA((3 + na,)),
            pltpu.SemaphoreType.DMA((copies,)),
            pltpu.SemaphoreType.DMA((copies,)),
        ],
        compiler_params=pltpu.CompilerParams(
            collective_id=2, has_side_effects=True, vmem_limit_bytes=VMEM_LIMIT
        ),
        name="middle",
    )(x_all, w_mlp, res_mine, out_grad, proj_mine, inv_mine, width_gain)


LAST = (
    ("U1",), ("ZG", 0, 3), ("YG", 1), ("AB", 0), ("AB", 1), ("U2",), ("AB", 2), ("AB", 3), ("S1",),
    ("WO", 1), ("U3",), ("S2",), ("WO", 2), ("S3",), ("ZG", 0, 1), ("ZG", 0, 2), ("WO", 3), ("WO", 0),
    ("OG", 0, 3), ("S4",), ("QB", 3), ("OD", 2), ("QB", 2), ("QB", 0), ("SG", 1), ("rP", 1, 3),
    ("ZG", 1, 2), ("QB", 1), ("ZG", 1, 3), ("rP", 1, 0), ("rP", 0, 0), ("WQ", 1), ("rP", 1, 2), ("WQ", 2),
    ("WQ", 0), ("rP", 0, 2), ("OD", 1), ("rP", 0, 3), ("WQ", 3), ("ZG", 1, 1), ("YA",), ("OWNG",),
    ("rP", 1, 1), ("rP", 0, 1), ("OG", 0, 1), ("rCL", 1, 3), ("rCR", 0, 3), ("rCR", 1, 3), ("OG", 0, 2),
    ("OD", 3), ("rCL", 0, 3), ("rCR", 0, 2), ("rCR", 1, 2), ("rCL", 1, 2), ("rCL", 0, 2), ("OG", 1, 1),
    ("OG", 1, 2), ("rCR", 0, 1), ("rCL", 1, 1), ("rCR", 1, 1), ("rCL", 0, 1), ("SA",), ("ZA", 2),
    ("OG", 1, 3), ("ZA", 1), ("rSC", 0), ("ZA", 3), ("rSC", 1), ("rX", 0), ("U4",), ("OA", 2), ("rX", 1),
    ("U5",), ("OWN",), ("rRQ", 0, 0), ("rRQ", 1, 0), ("OA", 1), ("OA", 3),
)


def last_kernel(na, nb, *refs):
    proj_far, x_far, qkv_ref, stats_ref, gain_ref, cos_ref, sin_ref, w_ref, att_ref = refs[:9]
    grad_ref, attn_sum_ref, ffn_sum_ref, down_sum_far, up_grad_far, down_in_far, gate_ref = refs[9:16]
    out, sums_ref, down_far, gu_far, qkv_out, wout_out = refs[16:22]
    scaled_ref, grad_qkv_ref, part_ref, head_sums, held, stats_a, inner_ref = refs[22:29]
    own_sums, a_sums, b_sums, up_held, up_sum, attn_grad, attn_held, attn_sum = refs[29:37]
    gu_in, attn_in, x_ref, up_own, down_out, gu_out = refs[37:43]
    proj_ref, down_sum_ref, down_in = refs[43:46]
    scratch, (local_sem, send_sem, recv_sem) = refs[46:-3], refs[-3:]
    load_proj = [
        pltpu.make_async_copy(proj_far.at[k], proj_ref.at[k], local_sem.at[4 + k]) for k in range(na)
    ]
    for copy in load_proj:
        copy.start()
    links = Links(send_sem, recv_sem)
    load_gu = pltpu.make_async_copy(
        up_grad_far.at[:, lax.axis_index("b")], up_own, local_sem.at[0]
    )
    load_gu.start()
    load_x = pltpu.make_async_copy(x_far, x_ref, local_sem.at[1])
    load_x.start()
    load_down = [
        pltpu.make_async_copy(down_sum_far, down_sum_ref, local_sem.at[4 + na]),
        pltpu.make_async_copy(down_in_far, down_in, local_sem.at[5 + na]),
    ]
    for copy in load_down:
        copy.start()
    save_down = pltpu.make_async_copy(down_out, down_far, local_sem.at[2])
    save_gu = pltpu.make_async_copy(gu_out, gu_far, local_sem.at[3])
    r = Reduce(na, links, part_ref, out, scratch)
    r.chained(scratch[9])
    a, b, p, q, mine, pair, quarter = (
        r.a, lax.axis_index("b"), r.p, r.q, r.mine, r.pair, r.quarter,
    )
    units = down_sum_ref.shape[2]
    own_sums[...] = jnp.zeros_like(own_sums)
    own_sums[0:1, mine] = jnp.sum(attn_sum_ref[...], axis=0, keepdims=True)
    own_sums[1:2, mine] = jnp.sum(ffn_sum_ref[...], axis=0, keepdims=True)
    held[0] = jnp.zeros_like(held[0])
    head_sums[...] = jnp.zeros_like(head_sums)
    greet(reduce_peers(na) + [{"b": across(b, j)} for j in range(1, nb)])
    copies, stored = {}, []
    whole = slice(0, units)
    attn_columns = slice(0, 4 * HD)
    over_heads = OverHeads(links, na, a, p, q, held, stats_a, inner_ref)

    def sums_pair():
        here = own_sums.at[:, mine]
        copies["u"] = links.send(here, here, {"p": 1 - p})

    def sums_core():
        copies["u"].wait_recv()
        here = own_sums.at[:, pair]
        copies["u"] = links.send(here, here, {"q": 1 - q})

    def sums_far():
        copies["u"].wait_recv()
        copies["u"] = [
            links.send(
                own_sums.at[:, span(across(a, k), quarter)], a_sums.at[k - 1], {"a": across(a, k)}
            )
            for k in range(1, na)
        ]

    def sums_b():
        for copy in copies["u"]:
            copy.wait_recv()
        total = own_sums[:, span(a, quarter)]
        for k in range(1, na):
            total = total + a_sums[k - 1]
        b_sums[0, :, :quarter] = total
        b_sums[0, :, quarter:] = head_sums[...]
        copies["u"] = [
            links.send(b_sums.at[0], b_sums.at[j], {"b": across(b, j)}) for j in range(1, nb)
        ]

    def sums_done():
        for copy in copies["u"]:
            copy.wait_recv()
        total = b_sums[0]
        for j in range(1, nb):
            total = total + b_sums[j]
        sums_ref[...] = total

    def proj_here(k):
        if ("proj", k) not in copies:
            copies["proj", k] = True
            load_proj[k].wait()

    def out_grads(block):
        for k in range(na):
            proj_here(k)
        weight_grad(proj_ref, att_ref, attn_grad, block, slice(3 * HD, 4 * HD))

    def attend_back(k):
        proj_here(k)
        if k % 2:
            lax.fori_loop(k - 1, k + 1, attend_back_block, 0)

    def attend_back_block(k, carry):
        queries, key_rows, values, q_inv, k_inv, q_rot, k_rot, probs = attention(
            k, qkv_ref[k], stats_ref[...], gain_ref, cos_ref, sin_ref
        )
        cos_table, sine_table = cos_ref[...], sin_ref[...]
        grad_att = dot(proj_ref[k], w_ref[:, 3 * HD :]).astype(bf16)
        grad_v = t_dot(probs.astype(bf16), grad_att)
        grad_p = dot_t(grad_att, values)
        delta = jnp.sum(probs * grad_p, axis=1, keepdims=True)
        grad_scores = (probs * (grad_p - delta) * HD ** (-0.5)).astype(bf16)
        grad_q = dot(grad_scores, k_rot)
        grad_k = t_dot(grad_scores, q_rot)
        grad_q = grad_q * cos_table + rotate_back(grad_q * sine_table)
        grad_k = grad_k * cos_table + rotate_back(grad_k * sine_table)
        head_sums[0:1] += jnp.sum(grad_q * queries * q_inv, axis=0, keepdims=True)
        head_sums[1:2] += jnp.sum(grad_k * key_rows * k_inv, axis=0, keepdims=True)
        scaled_q = grad_q * gain_ref[0:1]
        scaled_k = grad_k * gain_ref[1:2]
        scaled_ref[k, :, :HD] = scaled_q
        scaled_ref[k, :, HD:] = scaled_k
        grad_qkv_ref[k, :, 2 * HD :] = grad_v.astype(bf16)
        held[0] += to_row(scaled_q * queries, 2 * k) + to_row(scaled_k * key_rows, 2 * k + 1)
        return carry

    def qkv_back(k):
        for i in range(2):
            at = slice(i * HD, (i + 1) * HD)
            inv = lax.rsqrt(to_column(stats_ref[...] / HQ, 2 * k + i) + epsilon)
            mean = to_column(inner_ref[...] / HQ, 2 * k + i)
            grad = inv * scaled_ref[k, :, at] - qkv_ref[k, :, at] * inv * inv * inv * mean
            grad_qkv_ref[k, :, at] = grad.astype(bf16)

        def part(n, carry):
            at = span(n, 512)
            part_ref[k, :, at] = dot_t(grad_qkv_ref[k], w_ref[at, : 3 * HD]).astype(bf16)
            return carry

        lax.fori_loop(0, part_ref.shape[2] // 512, part, 0)
        for h in range(HALVES):
            r.send_q(h, k)

    def qkv_grads(block):
        if "x" not in copies:
            load_x.wait()
            copies["x"] = True
        weight_grad(x_ref, grad_qkv_ref, attn_grad, block, slice(0, 3 * HD))

    def up_rows(_):
        copies["up"] = exchange_b(links, up_grad_far, up_held, whole)

    def up_sums(_):
        load_gu.wait()
        own = lambda block: up_own.at[block]
        sum_b(copies["up"], own, up_held, up_sum, whole)

    def gu_owner(c, k):
        source = up_sum if c else gate_ref
        copies["g", c, k] = links.send(
            source.at[across(a, k)], gu_in.at[k - 1, c], {"a": across(a, k)}
        )

    def attn_rows():
        copies["at"] = exchange_b(links, attn_grad, attn_held, attn_columns)

    def attn_sums():
        own = lambda block: attn_grad.at[block, b]
        sum_b(copies["at"], own, attn_held, attn_sum, attn_columns)

    def attn_owner(k):
        copies["a", k] = links.send(attn_sum.at[across(a, k)], attn_in.at[k - 1], {"a": across(a, k)})

    def store(target, index, size, value):
        target[:, span(index, size)] = value.astype(f32)

    def store_gu(c, k, value):
        gu_out[:, c, span(across(a, k), units)] = value.astype(f32)
        stored.append((c, k))
        if len(stored) == 2 * na:
            save_gu.start()

    def store_attn(k, values):
        for c in range(3):
            store(qkv_out.at[c], across(a, k), HD, values[:, c * HD : (c + 1) * HD])
        store(wout_out, across(a, k), HD, values[:, 3 * HD :])

    def own_gu():
        store_gu(0, 0, gate_ref[a])
        store_gu(1, 0, up_sum[a])

    def gu_arrived(c, k):
        copies["g", c, k].wait_recv()
        store_gu(c, k, gu_in[k - 1, c])

    def attn_arrived(k):
        copies["a", k].wait_recv()
        store_attn(k, attn_in[k - 1])

    def down_rows(k):
        if "down" not in copies:
            copies["down"] = 0
            for copy in load_down:
                copy.wait()
            store(down_out, a, units, down_sum_ref[a])
        store(down_out, across(a, k), units, down_in[k - 1])
        copies["down"] += 1
        if copies["down"] == na - 1:
            save_down.start()

    def first(at):
        out[0, at, mine] = (grad_ref[at] + r.add_all(at)).astype(bf16)

    table = {
        "U1": sums_pair,
        "U2": sums_core,
        "U3": sums_far,
        "U4": sums_b,
        "U5": sums_done,
        "AB": attend_back,
        "S1": over_heads.to_pair,
        "S2": over_heads.to_core,
        "S3": over_heads.to_all,
        "S4": over_heads.done,
        "WO": out_grads,
        "WQ": qkv_grads,
        "QB": qkv_back,
        "YG": up_rows,
        "SG": up_sums,
        "ZG": gu_owner,
        "YA": attn_rows,
        "SA": attn_sums,
        "ZA": attn_owner,
        "OWNG": own_gu,
        "OWN": lambda: store_attn(0, attn_sum[a]),
        "OD": down_rows,
        "OG": gu_arrived,
        "OA": attn_arrived,
    }
    table.update({"r" + key: step for key, step in r.steps(first, None, 0).items()})
    for key, *where in LAST:
        table[key](*where)
    for h in range(HALVES):
        r.arrived(h, 0)
    save_down.wait()
    save_gu.wait()
    links.finish()


def last_call(nb, *operands):
    na, rows, width = operands[0].shape
    w_rows, units = operands[12].shape[1:]
    quarter = width // 4
    vmem, far = pl.BlockSpec(memory_space=pltpu.VMEM), pl.BlockSpec(memory_space=pl.ANY)
    shape = jax.ShapeDtypeStruct
    outs = (
        shape((1, rows, width), bf16),
        shape((8, quarter + HD), f32),
        shape((w_rows, na * units), f32),
        shape((w_rows, 2, na * units), f32),
        shape((3, w_rows, na * HD), f32),
        shape((w_rows, na * HD), f32),
    )
    copies = HALVES * (6 * na + 1) + 2 + 6 * na + 4 * nb
    return pl.pallas_call(
        functools.partial(last_kernel, na, nb),
        out_shape=outs,
        in_specs=[far if i in (0, 1, 12, 13, 14) else vmem for i in range(16)],
        out_specs=(vmem, vmem, far, far, vmem, vmem),
        scratch_shapes=[
            pltpu.VMEM((na, rows, 2 * HD), f32),
            pltpu.VMEM((na, rows, 3 * HD), bf16),
            pltpu.VMEM((na, rows, width), bf16),
            pltpu.VMEM((8, HD), f32),
            pltpu.VMEM((5, 8, rows), f32),
            pltpu.VMEM((na - 1, 8, rows), f32),
            pltpu.VMEM((8, rows), f32),
            pltpu.VMEM((8, width), f32),
            pltpu.VMEM((na - 1, 8, quarter), f32),
            pltpu.VMEM((nb, 8, quarter + HD), f32),
            pltpu.VMEM((nb - 1, na, w_rows, units), bf16),
            pltpu.VMEM((na, w_rows, units), bf16),
            pltpu.VMEM((na, nb, w_rows, 4 * HD), bf16),
            pltpu.VMEM((nb - 1, na, w_rows, 4 * HD), bf16),
            pltpu.VMEM((na, w_rows, 4 * HD), bf16),
            pltpu.VMEM((na - 1, 2, w_rows, units), bf16),
            pltpu.VMEM((na - 1, w_rows, 4 * HD), bf16),
            pltpu.VMEM((na, rows, width), bf16),
            pltpu.VMEM((na, w_rows, units), bf16),
            pltpu.VMEM((w_rows, na * units), f32),
            pltpu.VMEM((w_rows, 2, na * units), f32),
            pltpu.VMEM((na, rows, width), bf16),
            pltpu.VMEM((na, w_rows, units), bf16),
            pltpu.VMEM((na - 1, w_rows, units), bf16),
        ]
        + reduce_scratch(na, rows, width, True)
        + [
            pltpu.SemaphoreType.DMA((6 + na,)),
            pltpu.SemaphoreType.DMA((copies,)),
            pltpu.SemaphoreType.DMA((copies,)),
        ],
        compiler_params=pltpu.CompilerParams(
            collective_id=4, has_side_effects=True, vmem_limit_bytes=VMEM_LIMIT
        ),
        name="last",
    )(*operands)


def reduce_scratch(na, rows, width, chained=False):
    quarter = width // 4
    slots = [pltpu.VMEM((2, 2, na - 1, rows, quarter), bf16)] if chained else []
    return [
        pltpu.VMEM((na, rows, width // 2), bf16),
        pltpu.VMEM((na, rows, width // 2), bf16),
        pltpu.VMEM((na, rows, quarter), bf16),
        pltpu.VMEM((na - 1, rows, quarter), bf16),
        pltpu.VMEM((na - 1, rows, quarter), bf16),
        pltpu.VMEM((rows, quarter), f32),
        pltpu.VMEM((2, rows, 128), f32),
        pltpu.VMEM((2, rows, 128), f32),
        pltpu.VMEM((HALVES, 4, 8, rows // HALVES), f32),
    ] + slots


ENTER = (
    ("Z", 0), ("W", 3), ("FL", 0, 1), ("FR", 0, 1), ("W", 1), ("GA",), ("CUT", 0), ("FW", 0), ("FT", 0),
    ("CUT", 3), ("FW", 1), ("W", 2), ("CUT", 1), ("M", 0, 1), ("FL", 0, 2), ("FW", 3), ("CUT", 2),
    ("FW", 2), ("FL", 0, 3), ("FR", 0, 2), ("FQ", 0), ("FR", 0, 3), ("M", 0, 3), ("FQ", 2), ("M", 1, 2),
    ("M", 2, 1), ("J", 2), ("FQ", 1), ("FQ", 3), ("J", 0), ("J", 1), ("J", 3), ("GB",), ("S1",),
    ("MR", 1, 0), ("MR", 0, 0), ("S2",), ("S3",), ("M", 2, 3), ("M", 0, 2), ("M", 1, 1), ("S4",), ("E", 1),
    ("E", 2), ("MR", 2, 1), ("MR", 2, 0), ("rP", 1, 1), ("M", 2, 2), ("MR", 1, 2), ("rP", 0, 1), ("E", 3),
    ("E", 0), ("rP", 1, 0), ("rP", 0, 3), ("rP", 1, 3), ("rP", 1, 2), ("rP", 0, 0), ("rCL", 1, 3),
    ("rCL", 1, 2), ("rP", 0, 2), ("rCR", 1, 3), ("rCR", 1, 2), ("rCR", 0, 3), ("rCL", 1, 1), ("rCR", 1, 1),
    ("rCL", 0, 3), ("MR", 0, 1), ("rCR", 0, 2), ("MR", 0, 2), ("MR", 0, 3), ("rCL", 0, 2), ("rSC", 1),
    ("rCL", 0, 1), ("rCR", 0, 1), ("rSQ", 1), ("rSD", 1), ("rZ", 1), ("MR", 1, 1), ("rSC", 0), ("MR", 2, 2),
    ("rFL", 1, 1), ("rFR", 1, 1), ("rSQ", 0), ("rSD", 0), ("rX", 0), ("rX", 1), ("rZ", 0), ("rFR", 1, 2),
    ("rFL", 1, 2), ("rFR", 0, 1), ("rFL", 0, 1), ("M", 1, 3), ("rRQ", 0, 0), ("rFL", 1, 3), ("rFR", 1, 3),
    ("rRQ", 1, 1), ("MR", 2, 3), ("rRQ", 1, 0), ("rRQ", 1, 2), ("rFR", 0, 2), ("rFR", 0, 3), ("rFL", 0, 2),
    ("MR", 1, 3), ("rFL", 0, 3), ("rRQ", 0, 3), ("rRQ", 1, 3), ("rRQ", 0, 1), ("rRQ", 0, 2),
)


def enter_kernel(na, nb, gain_sizes, *refs):
    tok_far, qkv_w_ref, wout_ref, gu_far, down_far, cos_ref, sin_ref, all_gains_ref = refs[:8]
    x_far, w_far, mlp_w_ref, width_gain_ref, head_gain_ref, qkv_far, stats_ref, att_far = refs[8:16]
    out, proj_ref, inv_ref, res_ref = refs[16:20]
    own_gains, gains_ref, piece_ref, part_ref, held, stats_a = refs[20:26]
    x_ref, w_ref, qkv_ref, att_ref = refs[26:30]
    tok_ref, gu_ref, down_ref = refs[30:33]
    scratch, (local_sem, send_sem, recv_sem) = refs[33:-3], refs[-3:]
    load_mlp = [
        pltpu.make_async_copy(gu_far, gu_ref, local_sem.at[10]),
        pltpu.make_async_copy(down_far, down_ref, local_sem.at[11]),
    ]
    for copy in load_mlp:
        copy.start()
    saves = [
        pltpu.make_async_copy(near, there, local_sem.at[5 + i])
        for i, (near, there) in enumerate(
            ((x_ref, x_far), (w_ref, w_far), (qkv_ref, qkv_far), (att_ref, att_far))
        )
    ]
    a, b, p, q = (lax.axis_index(axis) for axis in ("a", "b", "p", "q"))
    rows = wout_ref.shape[0]
    quarter = tok_ref.shape[1]
    load = pltpu.make_async_copy(
        tok_far.at[:, span(2 * q + p, quarter)], tok_ref, local_sem.at[9]
    )
    load.start()
    units = down_ref.shape[1] // na
    own_gains[...] = jnp.zeros_like(own_gains)
    n_d, n_h = gain_sizes
    place = 0
    for i, size in enumerate((n_d, n_d, n_h, n_h)):
        own_gains[i : i + 1, :size] = all_gains_ref[:, place : place + size].astype(f32)
        place += size
    gains_ref[a, b] = own_gains[...]
    greet(
        [{"q": 1 - q}, {"p": 1 - p}]
        + [{"a": across(a, k)} for k in range(1, na)]
        + [{"b": across(b, j)} for j in range(1, nb)]
    )
    load.wait()
    links = Links(send_sem, recv_sem)
    mine, pair = span(2 * q + p, quarter), span(q, 2 * quarter)
    place = span(a * nb + b, rows)
    copies, ends = {}, []
    locals_ = [pltpu.make_async_copy(tok_ref, x_ref.at[0, :, mine], local_sem.at[0])]

    def weight_sources(k):
        block = span(across(a, k), HD)
        sources = [qkv_w_ref.at[c, :, block] for c in range(3)] + [wout_ref.at[:, block]]
        return [(s, w_ref.at[place, c * HD : (c + 1) * HD]) for c, s in enumerate(sources)]

    for c, (source, target) in enumerate(weight_sources(0)):
        locals_.append(pltpu.make_async_copy(source, target, local_sem.at[1 + c]))
    for copy in locals_:
        copy.start()

    def send_gains():
        copies["g"] = [
            links.send(own_gains, gains_ref.at[a, b], {"a": across(a, k)}) for k in range(1, na)
        ]

    def relay_gains():
        for copy in copies["g"]:
            copy.wait_recv()
        at = gains_ref.at[:, b]
        copies["gb"] = [links.send(at, at, {"b": across(b, j)}) for j in range(1, nb)]

    def send_weights(k):
        copies["w", k] = [
            links.send(source, target, {"a": across(a, k)}) for source, target in weight_sources(k)
        ]

    def relay_weights(k):
        if k:
            for copy in copies["w", k]:
                copy.wait_recv()
        else:
            for copy in locals_[1:]:
                copy.wait()
        at = w_ref.at[span(across(a, k) * nb + b, rows), :]
        copies["wb", k] = [links.send(at, at, {"b": across(b, j)}) for j in range(1, nb)]

    line = Line(links, na, lambda k: x_ref.at[k, :, mine], tok_ref)

    def own_tokens(_):
        locals_[0].wait()
        line.to_pair(0).start()

    def pair_tokens(k):
        line.to_pair(k).wait_recv()
        at = x_ref.at[k, :, pair]
        copies["x", k] = links.send(at, at, {"q": 1 - q})

    def cut_weights(k):
        if "cut" not in copies:
            copies["cut"] = True
            for copy in load_mlp:
                copy.wait()
        block = span(across(a, k), units)

        def cut(i, carry):
            at = pl.ds(pl.multiple_of(i * TILE, TILE), TILE)
            cuts = (gu_ref[at, 0, block], gu_ref[at, 1, block], down_ref[at, block])
            for c in range(3):
                if k:
                    piece_ref[k - 1, c, at] = cuts[c]
                else:
                    to = pl.ds(pl.multiple_of((a * nb + b) * rows + i * TILE, TILE), TILE)
                    mlp_w_ref[to, c * units : (c + 1) * units] = cuts[c]
            return carry

        lax.fori_loop(0, rows // TILE, cut, 0)

    def send_piece(c, k):
        target = mlp_w_ref.at[place, c * units : (c + 1) * units]
        copies["m", c, k] = links.send(piece_ref.at[k - 1, c], target, {"a": across(a, k)})

    def relay_piece(c, k):
        if k:
            copies["m", c, k].wait_recv()
        at = mlp_w_ref.at[span(across(a, k) * nb + b, rows), c * units : (c + 1) * units]
        ends.extend(links.send(at, at, {"b": across(b, j)}) for j in range(1, nb))

    arrived, ready = set(), []

    def project(k):
        if not arrived:
            held[0] = jnp.zeros_like(held[0])
            for i in range(na):
                for copy in copies["wb", i]:
                    copy.wait_recv()
        arrived.add(k)
        copies["x", k].wait_recv()

        def chunk(i, carry):
            at = span(i, 128)
            proj = dot(x_ref[k, at], w_ref[:, : 3 * HD])
            qkv_ref[k, at] = proj
            queries, key_rows = proj[:, :HD], proj[:, HD : 2 * HD]
            held[0, :, at] += to_row(queries * queries, 2 * k) + to_row(key_rows * key_rows, 2 * k + 1)
            return carry

        lax.fori_loop(0, x_ref.shape[1] // 128, chunk, 0)

    over_heads = OverHeads(links, na, a, p, q, held, stats_a, stats_ref)

    def all_stats():
        for save in saves[:3]:
            save.start()
        over_heads.done()
        for copy in copies["gb"]:
            copy.wait_recv()
        width_gain_ref[...] = jnp.zeros_like(width_gain_ref)
        head_gain_ref[...] = jnp.zeros_like(head_gain_ref)
        for i in range(2):
            width_gain_ref[i : i + 1] = jnp.concatenate(
                [gains_ref[2 * q + p, j, i : i + 1, :n_d] for j in range(nb)], axis=1
            )
            head_gain_ref[i : i + 1] = jnp.concatenate(
                [gains_ref[a, j, i + 2 : i + 3, :n_h] for j in range(nb)], axis=1
            )

    r = Reduce(na, links, part_ref, out, scratch)
    r.chained(scratch[9])

    def attend(k):
        values, probs = (
            attention(k, qkv_ref[k], stats_ref[...], head_gain_ref, cos_ref, sin_ref)[i] for i in (2, 7)
        )
        attended = dot(probs.astype(bf16), values).astype(bf16)
        att_ref[k] = attended

        def part(n, carry):
            at = span(n, 512)
            part_ref[k, :, at] = dot_t(att_ref[k], w_ref[at, 3 * HD :]).astype(bf16)
            return carry

        lax.fori_loop(0, part_ref.shape[2] // 512, part, 0)
        for h in range(HALVES):
            r.send_q(h, k)

    first, second = attn_math(r, tok_ref, width_gain_ref, proj_ref, inv_ref, res_ref)
    table = {
        "GA": send_gains,
        "GB": relay_gains,
        "W": send_weights,
        "FW": relay_weights,
        "Z": lambda _: line.start(),
        "FL": lambda _, t: line.pass_on(1, t),
        "FR": lambda _, t: line.pass_on(-1, t),
        "FT": own_tokens,
        "FQ": pair_tokens,
        "CUT": cut_weights,
        "M": send_piece,
        "MR": relay_piece,
        "J": project,
        "S1": over_heads.to_pair,
        "S2": over_heads.to_core,
        "S3": over_heads.to_all,
        "S4": all_stats,
        "E": attend,
    }
    table.update({"r" + key: step for key, step in r.steps(first, second, 1, True).items()})
    for key, *where in ENTER:
        table[key](*where)
    saves[3].start()
    for h in range(HALVES):
        for k in range(na):
            r.arrived(h, k)
    for copy in ends:
        copy.wait_recv()
    for save in saves:
        save.wait()
    links.finish()


def enter_call(na, nb, tokens, qkv, w_out, gu, down, cos_table, sine_table, gains):
    rows, width = tokens.shape
    quarter = width // 4
    sizes = (gains[0].shape[0], gains[2].shape[0])
    w_rows, units = down.shape[0], down.shape[1] // na
    lanes = max(128, sizes[0])
    vmem, far = pl.BlockSpec(memory_space=pltpu.VMEM), pl.BlockSpec(memory_space=pl.ANY)
    shape = jax.ShapeDtypeStruct
    full = shape((na, rows, width), bf16)
    outs = [
        full,
        shape((width, 4 * HD), bf16),
        shape((width, 3 * units), bf16),
        shape((8, quarter), f32),
        shape((8, HD), f32),
        shape((na, rows, 3 * HD), f32),
        shape((8, rows), f32),
        shape((na, rows, HD), bf16),
        full,
        shape((rows, quarter), f32),
        shape((rows, 128), f32),
        shape((rows, quarter), f32),
    ]
    copies = 120 + 16 * nb
    return pl.pallas_call(
        functools.partial(enter_kernel, na, nb, sizes),
        out_shape=tuple(outs),
        in_specs=[far if i in (0, 3, 4) else vmem for i in range(8)],
        out_specs=tuple(far if i in (0, 1, 5, 7) else vmem for i in range(len(outs))),
        scratch_shapes=[
            pltpu.VMEM((8, lanes), f32),
            pltpu.VMEM((na, nb, 8, lanes), f32),
            pltpu.VMEM((na - 1, 3, w_rows, units), bf16),
            pltpu.VMEM((na, rows, width), bf16),
            pltpu.VMEM((5, 8, rows), f32),
            pltpu.VMEM((na - 1, 8, rows), f32),
            pltpu.VMEM((na, rows, width), bf16),
            pltpu.VMEM((width, 4 * HD), bf16),
            pltpu.VMEM((na, rows, 3 * HD), f32),
            pltpu.VMEM((na, rows, HD), bf16),
            pltpu.VMEM((rows, quarter), bf16),
            pltpu.VMEM(gu.shape, bf16),
            pltpu.VMEM(down.shape, bf16),
        ]
        + reduce_scratch(na, rows, width, True)
        + [
            pltpu.SemaphoreType.DMA((12,)),
            pltpu.SemaphoreType.DMA((copies,)),
            pltpu.SemaphoreType.DMA((copies,)),
        ],
        compiler_params=pltpu.CompilerParams(
            collective_id=5, has_side_effects=True, vmem_limit_bytes=VMEM_LIMIT
        ),
        name="enter",
    )(tokens, qkv, w_out, gu, down, cos_table, sine_table, jnp.concatenate(gains)[None])


def rope_tables(length, width):
    half_width = width // 2
    inv_freq = rope_base ** (-(jnp.arange(half_width, dtype=f32) * 2.0) / width)
    angles = jnp.arange(length, dtype=f32)[:, None] * inv_freq[None, :]
    cos_table = jnp.concatenate([jnp.cos(angles), jnp.cos(angles)], axis=1)
    sine_table = jnp.concatenate([jnp.sin(angles), jnp.sin(angles)], axis=1)
    return cos_table, sine_table


def on_device(
    tokens,
    qkv_weight,
    out_weight,
    gu_weight,
    down_weight,
    attn_gain,
    ffn_gain,
    q_gain,
    k_gain,
    out_grad,
):
    na, nb = lax.axis_size("a"), lax.axis_size("b")
    a, b = lax.axis_index("a"), lax.axis_index("b")
    share = lax.axis_index("q") * 2 + lax.axis_index("p")
    rows, width = tokens.shape
    quarter = width // 4
    w_rows = out_weight.shape[0]
    units = down_weight.shape[1] // na

    cos_table, sine_table = rope_tables(SEQ_LEN, HD)
    (
        x_all,
        w_attn,
        w_mlp,
        width_gain,
        head_gain,
        qkv,
        stats,
        attended,
        res_all,
        proj_mine,
        inv_mine,
        res_mine,
    ) = enter_call(
        na,
        nb,
        tokens,
        qkv_weight.transpose(1, 0, 2),
        out_weight,
        gu_weight,
        down_weight,
        cos_table,
        sine_table,
        (attn_gain, ffn_gain, q_gain, k_gain),
    )
    n_d, n_h = attn_gain.shape[0], q_gain.shape[0]
    block_rows, grad_proj, ffn_sums, grad_res, attn_sums, down_sum, gu_grad, down_in, gate_sum = middle_call(
        nb, res_all, w_mlp, res_mine, out_grad, proj_mine, inv_mine, width_gain
    )
    grad_rows, sums, down_grad, gu_grad, qkv_grad, out_grad_w = last_call(
        nb,
        grad_proj,
        x_all,
        qkv,
        stats,
        head_gain,
        cos_table,
        sine_table,
        w_attn,
        attended,
        grad_res,
        attn_sums,
        ffn_sums,
        down_sum,
        gu_grad,
        down_in,
        gate_sum,
    )
    width_sums = lax.dynamic_slice_in_dim(sums[:2, :quarter], b * n_d, n_d, 1)
    head_sums = lax.dynamic_slice_in_dim(sums[:2, quarter:], b * n_h, n_h, 1)
    return (
        block_rows[0].astype(f32),
        grad_rows[0].astype(f32),
        qkv_grad.transpose(1, 0, 2),
        out_grad_w,
        gu_grad,
        down_grad,
        width_sums[0],
        width_sums[1],
        head_sums[0],
        head_sums[1],
    )


def solution(mesh):
    dp, tp = mesh.shape["dp"], mesh.shape["tensor"]
    na = HEADS // tp
    fine = Mesh(mesh.devices.reshape(na, dp // na, tp // 2, 2), ("a", "b", "p", "q"))
    dp_axes, tp_axes = ("a", "b"), ("p", "q")
    both = tp_axes + dp_axes
    return jax.shard_map(
        on_device,
        mesh=fine,
        in_specs=(
            P(dp_axes, None),
            P(dp_axes, None, tp_axes),
            P(dp_axes, tp_axes),
            P(dp_axes, None, tp_axes),
            P(dp_axes, tp_axes),
            P(dp_axes),
            P(dp_axes),
            P(both),
            P(both),
            P(dp_axes, None),
        ),
        out_specs=(
            P(dp_axes, None),
            P(dp_axes, None),
            P(dp_axes, None, tp_axes),
            P(dp_axes, tp_axes),
            P(dp_axes, None, tp_axes),
            P(dp_axes, tp_axes),
            P(dp_axes),
            P(dp_axes),
            P(both),
            P(both),
        ),
        check_vma=False,
    )
```
